32 devices in a mesh: rep: 8 (over y, x, core), shard: 4 (over z).
Axes of the slice: x: 2, y: 2, z: 4, core: 2. Of those that a mesh axis runs over, the one named last changes fastest.
Arguments:
- hidden_in: bfloat16 [8, 512, 2048], P('rep', 'shard'), may hold values from -6 to 6
- segment_ids: int32 [8, 512], P('rep', 'shard'), may hold values from 0 to 7, never falling along the last dimension, each value on 1 to 320 neighbouring positions
- out_grad: bfloat16 [8, 512, 2048], P('rep', 'shard'), may hold values from -6 to 6
- qkv_weight_state: float32 [3, 2048, 6144], P(None, ('rep', 'shard')), as said below
- qkv_bias_state: float32 [3, 6144], P(None, ('rep', 'shard')), as said below
- dense_weight_state: float32 [3, 2048, 2048], P(None, ('rep', 'shard')), as said below
- up_weight_state: float32 [3, 2048, 8192], P(None, ('rep', 'shard')), as said below
- up_bias_state: float32 [3, 8192], P(None, ('rep', 'shard')), as said below
- down_weight_state: float32 [3, 8192, 2048], P(None, ('rep', 'shard')), as said below
- vector_state: float32 [3, 2048, 4], P(None, ('rep', 'shard')), as said below
Outputs:
- output: bfloat16 [8, 512, 2048], P('rep', 'shard')
- input_grad: float32 [8, 512, 2048], P('rep', 'shard')
- qkv_weight_grad: float32 [2048, 6144], P(('rep', 'shard'))
- qkv_bias_grad: float32 [6144], P(('rep', 'shard'))
- dense_weight_grad: float32 [2048, 2048], P(('rep', 'shard'))
- up_weight_grad: float32 [2048, 8192], P(('rep', 'shard'))
- up_bias_grad: float32 [8192], P(('rep', 'shard'))
- down_weight_grad: float32 [8192, 2048], P(('rep', 'shard'))
- vector_grad: float32 [2048, 4], P(('rep', 'shard'))
- weights_new: float32 [8, 4, 1573568], P('rep', 'shard')
- first_moments_new: float32 [8, 4, 1573568], P('rep', 'shard')
- second_moments_new: float32 [8, 4, 1573568], P('rep', 'shard')
The draws below stay inside these ranges and needn't reach their ends.
Inputs may be any that keep to these rules, and one draw needn't show every extreme that they name: `qkv_weight_state`: entry 0 along dimension 0 is the weight, entries 1 and 2 its first and second moment estimates; second moments are positive. `qkv_bias_state`: entry 0 is the bias, entries 1 and 2 its moment estimates; second moments are positive. `dense_weight_state`: entry 0 is the weight, entries 1 and 2 its moment estimates; second moments are positive. `up_weight_state`: entry 0 is the weight, entries 1 and 2 its moment estimates; second moments are positive. `up_bias_state`: entry 0 is the bias, entries 1 and 2 its moment estimates; second moments are positive. `down_weight_state`: entry 0 is the weight, entries 1 and 2 its moment estimates; second moments are positive. `vector_state`: entry 0 holds the vectors, entries 1 and 2 their moment estimates; the gains are positive, second moments are positive.
All inputs are finite; a program needn't handle non-finite values.
Results may differ from the reference program's by a relative error of at most 0.012.
Values may be sent and summed in bfloat16 or wider, within the bound.
A program may use at most 320 MiB of HBM per device.

```python
import math
from functools import partial
import jax
import jax.numpy as jnp
import numpy as np
from jax import lax

D = 2048
HEADS = 32
HD = 64
ROT = 32
FF = 8192
DOCS = 8
STEP = 5
SEQ = 512
SEQS = 8
SHARDS = 4
MOST = 320


def moment_stack(key, weight, grad_size):
    key_one = jax.random.fold_in(key, 101)
    key_two = jax.random.fold_in(key, 202)
    moment_one = 0.25 * grad_size * jax.random.normal(key_one, weight.shape, jnp.float32)
    moment_two = grad_size * grad_size * jnp.exp(jax.random.uniform(key_two, weight.shape, jnp.float32, math.log(0.02), math.log(0.2)))
    return jnp.stack([weight, moment_one, moment_two])


def token_root():
    return math.sqrt(SEQS * SEQ)


def draw_qkv_weight_state(key, part):
    base = jax.random.normal(jax.random.fold_in(key, 1), (D, 3 * D), jnp.float32) / math.sqrt(D)
    return moment_stack(key, base, 1.5 * token_root())


def draw_qkv_bias_state(key, part):
    base = 0.3 * jax.random.normal(jax.random.fold_in(key, 1), (3 * D,), jnp.float32)
    return moment_stack(key, base, 3.0 * token_root())


def draw_dense_weight_state(key, part):
    base = jax.random.normal(jax.random.fold_in(key, 1), (D, D), jnp.float32) * (8.0 / math.sqrt(D))
    return moment_stack(key, base, 0.4 * token_root())


def draw_up_weight_state(key, part):
    base = jax.random.normal(jax.random.fold_in(key, 1), (D, FF), jnp.float32) / math.sqrt(D)
    return moment_stack(key, base, 0.3 * token_root())


def draw_up_bias_state(key, part):
    base = 0.3 * jax.random.normal(jax.random.fold_in(key, 1), (FF,), jnp.float32)
    return moment_stack(key, base, 0.3 * token_root())


def draw_down_weight_state(key, part):
    base = jax.random.normal(jax.random.fold_in(key, 1), (FF, D), jnp.float32) / math.sqrt(FF)
    return moment_stack(key, base, 0.33 * token_root())


def draw_vector_state(key, part):
    gain_column = 1.0 + 0.2 * jax.random.uniform(jax.random.fold_in(key, 1), (D, 1), jnp.float32, -1.0, 1.0)
    others = 0.3 * jax.random.normal(jax.random.fold_in(key, 2), (D, 3), jnp.float32)
    column_size = jnp.array([3.0, 3.0, 1.0, 1.0], jnp.float32) * token_root()
    return moment_stack(key, jnp.concatenate([gain_column, others], axis=1), column_size[None, :])


def steps_of(stream_key, dims, split, smallest, high):
    def one(dim, shards_of):
        steps = jax.random.uniform(jax.random.fold_in(jax.random.fold_in(stream_key, 6), dim), (shards_of,), jnp.float32, smallest / len(split), high / len(split))
        return jnp.repeat(jnp.exp(steps), dims[dim] // shards_of).reshape((-1,) + (1,) * (len(dims) - dim - 1))

    factor_of = one(*split[0])
    for cut in split[1:]:
        factor_of = factor_of * one(*cut)
    return factor_of


def split_up(number_of, total, limit, lean):
    portions = [(1 << 20) // math.isqrt(grade ** lean) + 1 for grade in range(2, number_of + 1)]
    rest, given = total - limit - (number_of - 1), [1] * (number_of - 1)
    while rest > 0:
        free = [i for i in range(number_of - 1) if given[i] < limit]
        pool, budget = sum([portions[i] for i in free]), rest
        for i in free:
            extra = min(limit - given[i], max(1, budget * portions[i] // pool), rest)
            given[i] = given[i] + extra
            rest = rest - extra
    return np.array([limit] + given)


def ragged(key, count, total, limit, skew):
    if count == 2:
        one = jax.random.randint(key, (), max(1, total - limit), min(limit, total - 1) + 1)
        return jnp.stack([one, total - one])
    tallies = jnp.asarray(split_up(count, total, limit, skew), jnp.int32)
    pairs = (count - 1) // 2
    source_of, receiver = tallies[1:1 + 2 * pairs:2], tallies[2:2 + 2 * pairs:2]
    margin = jnp.minimum(source_of - 1, limit - receiver)
    passed = jax.random.randint(jax.random.fold_in(key, 1), (pairs,), 0, 1 << 20) % (margin + 1)
    tallies = tallies.at[1:1 + 2 * pairs:2].set(source_of - passed).at[2:2 + 2 * pairs:2].set(receiver + passed)
    return tallies[jax.random.permutation(jax.random.fold_in(key, 2), count)]


def bell_draw(own_key, shape, width, bound, cuts=(), kind=jnp.bfloat16):
    result = width * jax.random.normal(own_key, shape, jnp.float32)
    if cuts:
        result = result * steps_of(own_key, shape, cuts, -0.22, 0.18)
    return jnp.clip(result, -bound, bound).astype(kind)


def setup_inputs(seed: int = 0) -> dict:
    seeds = jax.random.split(jax.random.key(seed), 11)
    hidden_in = bell_draw(seeds[0], (SEQS, SEQ, D), 1.0, 6.0, ((0, 8), (1, 4)))
    segment_ids = jax.vmap(lambda own: jnp.searchsorted(jnp.cumsum(ragged(own, DOCS, SEQ, MOST, 2)), jnp.arange(SEQ), side="right"))(jax.random.split(seeds[1], SEQS)).reshape((SEQS, SEQ)).astype(jnp.int32)
    out_grad = bell_draw(seeds[2], (SEQS, SEQ, D), 1.0, 6.0, ((0, 8), (1, 4)))
    qkv_weight_state = draw_qkv_weight_state(jax.random.fold_in(seeds[10], 71), 0)
    qkv_bias_state = draw_qkv_bias_state(jax.random.fold_in(seeds[10], 71), 0)
    dense_weight_state = draw_dense_weight_state(jax.random.fold_in(seeds[10], 71), 0)
    up_weight_state = draw_up_weight_state(jax.random.fold_in(seeds[10], 71), 0)
    up_bias_state = draw_up_bias_state(jax.random.fold_in(seeds[10], 71), 0)
    down_weight_state = draw_down_weight_state(jax.random.fold_in(seeds[10], 71), 0)
    vector_state = draw_vector_state(jax.random.fold_in(seeds[10], 71), 0)
    return dict(hidden_in=hidden_in, segment_ids=segment_ids, out_grad=out_grad, qkv_weight_state=qkv_weight_state, qkv_bias_state=qkv_bias_state, dense_weight_state=dense_weight_state, up_weight_state=up_weight_state, up_bias_state=up_bias_state, down_weight_state=down_weight_state, vector_state=vector_state)


learn_rate = 0.02
beta_one = 0.9
beta_two = 0.95
adam_eps = 1e-08
weight_decay = 0.1
norm_eps = 1e-05
big_negative = -1e+30

def layer_norm(x, norm_gain, norm_shift):
    center = x - lax.optimization_barrier(jnp.mean(x, axis=-1, keepdims=True))
    variance = lax.optimization_barrier(jnp.mean(center * center, axis=-1, keepdims=True))
    return center * lax.rsqrt(variance + norm_eps) * norm_gain + norm_shift

def gelu_tanh(v):
    return 0.5 * v * (1.0 + jnp.tanh(0.7978845608028654 * (v + 0.044715 * v * v * v)))

def rotary(x, positions):
    half_rot = ROT // 2
    frequency = jnp.exp(jnp.arange(half_rot, dtype=jnp.float32) * (-2.0 * math.log(10000.0) / ROT))
    angles = positions.astype(jnp.float32)[:, None] * frequency[None, :]
    cosine = jnp.cos(angles)[:, None, :]
    sine_val = jnp.sin(angles)[:, None, :]
    lower_part = x[..., :half_rot]
    upper_part = x[..., half_rot:ROT]
    return jnp.concatenate([lower_part * cosine - upper_part * sine_val, upper_part * cosine + lower_part * sine_val, x[..., ROT:]], axis=-1)

def adam_update(state, grad):
    moment_one = beta_one * state[1] + (1.0 - beta_one) * grad
    moment_two = beta_two * state[2] + (1.0 - beta_two) * grad * grad
    corrected = moment_one / (1.0 - beta_one ** STEP)
    divisor = jnp.sqrt(moment_two / (1.0 - beta_two ** STEP)) + adam_eps
    weight = state[0] - learn_rate * (corrected / divisor + weight_decay * state[0])
    return jnp.stack([weight, moment_one, moment_two])

def owner_layout(new_states, entry):
    return jnp.concatenate([state_new[entry].reshape(SEQS, SHARDS, -1) for state_new in new_states], axis=2)

def block_mask(q_pos, q_seg, k_pos, k_seg):
    return (k_pos[None, :] <= q_pos[:, None]) & (k_seg[None, :] == q_seg[:, None])

def attention_forward(queries, key_rows, value_rows, segments):
    score_scale = 1.0 / math.sqrt(HD)
    block_rows = math.gcd(SEQ, 512)
    block_count = SEQ // block_rows
    key_pos = jnp.arange(SEQ, dtype=jnp.int32)
    key_all = key_rows.astype(jnp.float32)
    value_all = value_rows.astype(jnp.float32)

    def forward_block(block_index):
        row_start = block_index * block_rows
        q_rows = lax.dynamic_slice_in_dim(queries, row_start, block_rows, 0).astype(jnp.float32)
        q_pos = row_start + jnp.arange(block_rows, dtype=jnp.int32)
        q_seg = lax.dynamic_slice_in_dim(segments, row_start, block_rows, 0)
        allowed = block_mask(q_pos, q_seg, key_pos, segments)
        scores = jnp.einsum('qhd,khd->hqk', q_rows, key_all) * score_scale
        scores = jnp.where(allowed[None], scores, big_negative)
        row_max = lax.optimization_barrier(jnp.max(scores, axis=-1))
        probabilities = jnp.where(allowed[None], jnp.exp(scores - row_max[..., None]), 0.0)
        totals = lax.optimization_barrier(jnp.sum(probabilities, axis=-1))
        mixed = jnp.einsum('hqk,khd->hqd', probabilities.astype(jnp.bfloat16).astype(jnp.float32), value_all)
        return ((mixed / totals[..., None]).transpose(1, 0, 2), row_max + jnp.log(totals))
    outputs, lse_blocks = lax.map(forward_block, jnp.arange(block_count, dtype=jnp.int32))
    lse_all = lse_blocks.transpose(1, 0, 2).reshape(HEADS, SEQ)
    return (outputs.reshape(SEQ, HEADS, HD), lse_all)

def attention_backward(queries, key_rows, value_rows, segments, out_heads, grad_heads, lse_all):
    score_scale = 1.0 / math.sqrt(HD)
    block_rows = math.gcd(SEQ, 512)
    block_count = SEQ // block_rows
    key_pos = jnp.arange(SEQ, dtype=jnp.int32)
    key_all = key_rows.astype(jnp.float32)
    value_all = value_rows.astype(jnp.float32)
    delta_all = lax.optimization_barrier(jnp.sum(grad_heads.astype(jnp.float32) * out_heads.astype(jnp.float32), axis=-1)).T

    def backward_block(carry, block_index):
        key_grad, value_grad = carry
        row_start = block_index * block_rows
        q_rows = lax.dynamic_slice_in_dim(queries, row_start, block_rows, 0).astype(jnp.float32)
        g_rows = lax.dynamic_slice_in_dim(grad_heads, row_start, block_rows, 0).astype(jnp.float32)
        q_pos = row_start + jnp.arange(block_rows, dtype=jnp.int32)
        q_seg = lax.dynamic_slice_in_dim(segments, row_start, block_rows, 0)
        lse_rows = lax.dynamic_slice_in_dim(lse_all, row_start, block_rows, 1)
        delta_rows = lax.dynamic_slice_in_dim(delta_all, row_start, block_rows, 1)
        allowed = block_mask(q_pos, q_seg, key_pos, segments)
        scores = jnp.einsum('qhd,khd->hqk', q_rows, key_all) * score_scale
        scores = jnp.where(allowed[None], scores, big_negative)
        probabilities = jnp.where(allowed[None], jnp.exp(scores - lse_rows[..., None]), 0.0)
        prob_bf = probabilities.astype(jnp.bfloat16).astype(jnp.float32)
        value_grad = value_grad + jnp.einsum('hqk,qhd->khd', prob_bf, g_rows)
        prob_grad = jnp.einsum('qhd,khd->hqk', g_rows, value_all)
        score_grad = (probabilities * (prob_grad - delta_rows[..., None]) * score_scale).astype(jnp.bfloat16).astype(jnp.float32)
        query_grad = jnp.einsum('hqk,khd->qhd', score_grad, key_all)
        key_grad = key_grad + jnp.einsum('hqk,qhd->khd', score_grad, q_rows)
        return ((key_grad, value_grad), query_grad)
    zeros_heads = jnp.zeros((SEQ, HEADS, HD), jnp.float32)
    (key_grad, value_grad), query_blocks = lax.scan(backward_block, (zeros_heads, zeros_heads), jnp.arange(block_count, dtype=jnp.int32))
    return (query_blocks.reshape(SEQ, HEADS, HD), key_grad, value_grad)

def reference(hidden_in, segment_ids, out_grad, qkv_weight_state, qkv_bias_state, dense_weight_state, up_weight_state, up_bias_state, down_weight_state, vector_state):
    qkv_w = qkv_weight_state[0].astype(jnp.bfloat16)
    qkv_b = lax.optimization_barrier(qkv_bias_state[0].astype(jnp.bfloat16)).astype(jnp.float32)
    dense_w = dense_weight_state[0].astype(jnp.bfloat16)
    up_w = up_weight_state[0].astype(jnp.bfloat16)
    up_b = lax.optimization_barrier(up_bias_state[0].astype(jnp.bfloat16)).astype(jnp.float32)
    down_w = down_weight_state[0].astype(jnp.bfloat16)
    vec_all = lax.optimization_barrier(vector_state[0].astype(jnp.bfloat16)).astype(jnp.float32)
    norm_gain = vec_all[:, 0]
    norm_shift = vec_all[:, 1]
    dense_bias = vec_all[:, 2]
    down_bias = vec_all[:, 3]
    positions = jnp.arange(SEQ, dtype=jnp.int32)

    def one_sequence(totals, items):
        tokens, segments, cotangent = items
        x_full = tokens.astype(jnp.float32)
        normed = layer_norm(x_full, norm_gain, norm_shift)
        norm_bf = normed.astype(jnp.bfloat16)
        joined = jnp.dot(norm_bf, qkv_w, preferred_element_type=jnp.float32) + qkv_b
        q_pre = joined[:, :D].reshape(SEQ, HEADS, HD)
        k_pre = joined[:, D:2 * D].reshape(SEQ, HEADS, HD)
        queries = rotary(q_pre, positions).astype(jnp.bfloat16)
        key_rows = rotary(k_pre, positions).astype(jnp.bfloat16)
        value_rows = joined[:, 2 * D:].reshape(SEQ, HEADS, HD).astype(jnp.bfloat16)
        out_heads, lse_all = attention_forward(queries, key_rows, value_rows, segments)
        out_heads = out_heads.astype(jnp.bfloat16)
        attn_bf = out_heads.reshape(SEQ, D)
        attn_out = jnp.dot(attn_bf, dense_w, preferred_element_type=jnp.float32) + dense_bias
        pre_act = jnp.dot(norm_bf, up_w, preferred_element_type=jnp.float32) + up_b
        hidden = gelu_tanh(pre_act).astype(jnp.bfloat16)
        mlp_out = jnp.dot(hidden, down_w, preferred_element_type=jnp.float32) + down_bias
        output = (x_full + attn_out + mlp_out).astype(jnp.bfloat16)
        grad_down = jnp.dot(hidden.T, cotangent, preferred_element_type=jnp.float32)
        grad_dense = jnp.dot(attn_bf.T, cotangent, preferred_element_type=jnp.float32)
        out_bias_grad = lax.optimization_barrier(jnp.sum(cotangent.astype(jnp.float32), axis=0))
        grad_hidden = jnp.dot(cotangent, down_w.T, preferred_element_type=jnp.float32)
        grad_pre = jax.vjp(gelu_tanh, pre_act)[1](grad_hidden)[0]
        grad_pre_bf = grad_pre.astype(jnp.bfloat16)
        grad_up = jnp.dot(norm_bf.T, grad_pre_bf, preferred_element_type=jnp.float32)
        grad_up_bias = lax.optimization_barrier(jnp.sum(grad_pre, axis=0))
        grad_norm = jnp.dot(grad_pre_bf, up_w.T, preferred_element_type=jnp.float32)
        grad_heads = jnp.dot(cotangent, dense_w.T, preferred_element_type=jnp.float32).astype(jnp.bfloat16).reshape(SEQ, HEADS, HD)
        query_grad, key_grad, value_grad = attention_backward(queries, key_rows, value_rows, segments, out_heads, grad_heads, lse_all)
        rotate_back = partial(rotary, positions=positions)
        query_pre = jax.vjp(rotate_back, q_pre)[1](query_grad)[0]
        key_pre = jax.vjp(rotate_back, k_pre)[1](key_grad)[0]
        grad_joined = jnp.concatenate([query_pre.reshape(SEQ, D), key_pre.reshape(SEQ, D), value_grad.reshape(SEQ, D)], axis=1)
        grad_joined_bf = grad_joined.astype(jnp.bfloat16)
        grad_qkv = jnp.dot(norm_bf.T, grad_joined_bf, preferred_element_type=jnp.float32)
        grad_qkv_bias = lax.optimization_barrier(jnp.sum(grad_joined, axis=0))
        grad_norm = grad_norm + jnp.dot(grad_joined_bf, qkv_w.T, preferred_element_type=jnp.float32)
        grad_x, grad_gain, grad_shift = jax.vjp(layer_norm, x_full, norm_gain, norm_shift)[1](grad_norm)
        grad_vec = jnp.stack([grad_gain, grad_shift, out_bias_grad, out_bias_grad], axis=1)
        input_grad = cotangent.astype(jnp.float32) + grad_x
        new_totals = (totals[0] + grad_qkv, totals[1] + grad_qkv_bias, totals[2] + grad_dense, totals[3] + grad_up, totals[4] + grad_up_bias, totals[5] + grad_down, totals[6] + grad_vec)
        return (new_totals, (output, input_grad))
    init = (jnp.zeros((D, 3 * D), jnp.float32), jnp.zeros((3 * D,), jnp.float32), jnp.zeros((D, D), jnp.float32), jnp.zeros((D, FF), jnp.float32), jnp.zeros((FF,), jnp.float32), jnp.zeros((FF, D), jnp.float32), jnp.zeros((D, 4), jnp.float32))
    grads, (output, input_grad) = lax.scan(one_sequence, init, (hidden_in, segment_ids, out_grad))
    qkv_wg, qkv_bg, dense_g, up_wg, up_bg, down_g, vec_g = grads
    new_states = (adam_update(qkv_weight_state, qkv_wg), adam_update(qkv_bias_state, qkv_bg), adam_update(dense_weight_state, dense_g), adam_update(up_weight_state, up_wg), adam_update(up_bias_state, up_bg), adam_update(down_weight_state, down_g), adam_update(vector_state, vec_g))
    return (output, input_grad, qkv_wg, qkv_bg, dense_g, up_wg, up_bg, down_g, vec_g, owner_layout(new_states, 0), owner_layout(new_states, 1), owner_layout(new_states, 2))
```

```python
from functools import partial
import math

import jax
import jax.numpy as jnp
from jax import lax
from jax.experimental import pallas as pl
from jax.experimental.pallas import tpu as pltpu
from jax.sharding import Mesh
from jax.sharding import PartitionSpec as P

D = 2048
HD = 64
ROT = 32
FF = 8192
STEP = 5


learn_rate = 0.02
beta_one = 0.9
beta_two = 0.95
adam_eps = 1e-08
weight_decay = 0.1
norm_eps = 1e-05
big_negative = -1e30


def layer_norm(x, norm_gain, norm_shift):
    center = x - jnp.mean(x, axis=-1, keepdims=True)
    variance = jnp.mean(center * center, axis=-1, keepdims=True)
    return center * lax.rsqrt(variance + norm_eps) * norm_gain + norm_shift


def gelu_tanh(v):
    return 0.5 * v * (1.0 + jnp.tanh(0.7978845608028654 * (v + 0.044715 * v * v * v)))


def rotary(x, positions):
    half_rot = ROT // 2
    frequency = jnp.exp(jnp.arange(half_rot, dtype=jnp.float32) * (-2.0 * math.log(10000.0) / ROT))
    angles = positions.astype(jnp.float32)[:, None] * frequency[None, :]
    cosine = jnp.cos(angles)[:, None, :]
    sine_val = jnp.sin(angles)[:, None, :]
    lower_part = x[..., :half_rot]
    upper_part = x[..., half_rot:ROT]
    return jnp.concatenate(
        [
            lower_part * cosine - upper_part * sine_val,
            upper_part * cosine + lower_part * sine_val,
            x[..., ROT:],
        ],
        axis=-1,
    )


def adam_update(state, grad):
    moment_one = beta_one * state[1] + (1.0 - beta_one) * grad
    moment_two = beta_two * state[2] + (1.0 - beta_two) * grad * grad
    corrected = moment_one / (1.0 - beta_one**STEP)
    divisor = jnp.sqrt(moment_two / (1.0 - beta_two**STEP)) + adam_eps
    weight = state[0] - learn_rate * (corrected / divisor + weight_decay * state[0])
    return jnp.stack([weight, moment_one, moment_two])


def owner_entries(new_states, entry):
    return jnp.concatenate(
        [state_new[entry].reshape(-1) for state_new in new_states], axis=0
    ).reshape(1, 1, -1)


def block_mask(q_pos, q_seg, k_pos, k_seg):
    return (k_pos[None, :] <= q_pos[:, None]) & (k_seg[None, :] == q_seg[:, None])


def attend_keys(kv_all, seg_all, queries, q_pos, q_seg):
    key_count = kv_all.shape[0]
    width = kv_all.shape[1] // 2
    heads_here = queries.shape[1]
    query_rows = queries.shape[0]
    block_rows = math.gcd(key_count, 512)
    block_count = key_count // block_rows
    kv_blocks = kv_all.reshape(block_count, block_rows, 2 * width)
    seg_blocks = seg_all.reshape(block_count, block_rows)
    score_scale = 1.0 / math.sqrt(HD)

    def attend_step_block(carry, block_items):
        kv_rows, seg_rows, block_index = block_items
        row_max, totals, accumulated = carry
        key_rows = kv_rows[:, :width].reshape(block_rows, heads_here, HD)
        value_rows = kv_rows[:, width:].reshape(block_rows, heads_here, HD)
        k_pos = block_index * block_rows + jnp.arange(block_rows, dtype=jnp.int32)
        allowed = block_mask(q_pos, q_seg, k_pos, seg_rows)
        scores = (
            jnp.einsum("qhd,khd->hqk", queries, key_rows, preferred_element_type=jnp.float32)
            * score_scale
        )
        scores = jnp.where(allowed[None], scores, big_negative)
        new_max = jnp.maximum(row_max, jnp.max(scores, axis=-1))
        probabilities = jnp.where(allowed[None], jnp.exp(scores - new_max[..., None]), 0.0)
        factor = jnp.exp(row_max - new_max)
        totals = totals * factor + jnp.sum(probabilities, axis=-1)
        accumulated = accumulated * factor[..., None] + jnp.einsum(
            "hqk,khd->hqd",
            probabilities.astype(jnp.bfloat16),
            value_rows,
            preferred_element_type=jnp.float32,
        )
        return ((new_max, totals, accumulated), None)

    start_state = (
        jnp.full((heads_here, query_rows), big_negative, jnp.float32),
        jnp.zeros((heads_here, query_rows), jnp.float32),
        jnp.zeros((heads_here, query_rows, HD), jnp.float32),
    )
    running, unused = lax.scan(
        attend_step_block,
        start_state,
        (kv_blocks, seg_blocks, jnp.arange(block_count, dtype=jnp.int32)),
    )
    return running


def attention_grads(queries, kv_all, seg_all, q_pos, q_seg, grad_heads, delta_all, lse_all):
    key_count = kv_all.shape[0]
    width = kv_all.shape[1] // 2
    heads_here = queries.shape[1]
    query_rows = queries.shape[0]
    block_rows = math.gcd(key_count, 512)
    block_count = key_count // block_rows
    kv_blocks = kv_all.reshape(block_count, block_rows, 2 * width)
    seg_blocks = seg_all.reshape(block_count, block_rows)
    score_scale = 1.0 / math.sqrt(HD)

    def attention_step_block(query_grad, block_items):
        kv_rows, seg_rows, block_index = block_items
        key_rows = kv_rows[:, :width].reshape(block_rows, heads_here, HD)
        value_rows = kv_rows[:, width:].reshape(block_rows, heads_here, HD)
        k_pos = block_index * block_rows + jnp.arange(block_rows, dtype=jnp.int32)
        allowed = block_mask(q_pos, q_seg, k_pos, seg_rows)
        scores = (
            jnp.einsum("qhd,khd->hqk", queries, key_rows, preferred_element_type=jnp.float32)
            * score_scale
        )
        scores = jnp.where(allowed[None], scores, big_negative)
        probabilities = jnp.where(allowed[None], jnp.exp(scores - lse_all[..., None]), 0.0)
        value_grad = jnp.einsum(
            "hqk,qhd->khd",
            probabilities.astype(jnp.bfloat16),
            grad_heads,
            preferred_element_type=jnp.float32,
        )
        prob_grad = jnp.einsum(
            "qhd,khd->hqk", grad_heads, value_rows, preferred_element_type=jnp.float32
        )
        score_grad = (probabilities * (prob_grad - delta_all[..., None]) * score_scale).astype(
            jnp.bfloat16
        )
        query_grad = query_grad + jnp.einsum(
            "hqk,khd->hqd", score_grad, key_rows, preferred_element_type=jnp.float32
        )
        key_grad = jnp.einsum(
            "hqk,qhd->khd", score_grad, queries, preferred_element_type=jnp.float32
        )
        return (
            query_grad,
            jnp.concatenate(
                [key_grad.reshape(block_rows, width), value_grad.reshape(block_rows, width)], axis=1
            ),
        )

    query_grad, kv_grad_blocks = lax.scan(
        attention_step_block,
        jnp.zeros((heads_here, query_rows, HD), jnp.float32),
        (kv_blocks, seg_blocks, jnp.arange(block_count, dtype=jnp.int32)),
    )
    return (query_grad, kv_grad_blocks.reshape(key_count, 2 * width))


def gather_vectors(own_qkvb, own_upb, own_vec):
    return (
        lax.all_gather(own_qkvb, ("rep", "shard"), axis=0, tiled=True),
        lax.all_gather(own_upb, ("rep", "shard"), axis=0, tiled=True),
        lax.all_gather(own_vec, ("rep", "shard"), axis=0, tiled=True),
    )


def sum_vectors(qkvb_grad, upb_grad, vec_grad):
    return (
        lax.psum_scatter(qkvb_grad, ("rep", "shard"), scatter_dimension=0, tiled=True),
        lax.psum_scatter(upb_grad, ("rep", "shard"), scatter_dimension=0, tiled=True),
        lax.psum_scatter(vec_grad, ("rep", "shard"), scatter_dimension=0, tiled=True),
    )


def sum_positions(partial_rows):
    return lax.psum_scatter(partial_rows, "shard", scatter_dimension=0, tiled=True)


def attention_pass(norm_rows, qkv_w, qkv_b, positions, key_width):
    row_count = norm_rows.shape[0]
    heads_here = key_width // HD
    joined = jnp.dot(norm_rows, qkv_w, preferred_element_type=jnp.float32) + qkv_b
    q_pre = joined[:, :key_width].reshape(row_count, heads_here, HD)
    k_pre = joined[:, key_width : 2 * key_width].reshape(row_count, heads_here, HD)
    queries = rotary(q_pre, positions).astype(jnp.bfloat16)
    key_local = rotary(k_pre, positions).astype(jnp.bfloat16).reshape(row_count, key_width)
    value_local = joined[:, 2 * key_width :].astype(jnp.bfloat16)
    kv_local = jnp.concatenate([key_local, value_local], axis=1)
    return (q_pre, k_pre, queries, kv_local)


def finish_qkv_grad(q_pre, k_pre, positions, query_grad, kv_grad, key_width):
    row_count = q_pre.shape[0]
    heads_here = key_width // HD
    rotate_back = partial(rotary, positions=positions)
    query_pre = jax.vjp(rotate_back, q_pre)[1](query_grad.transpose(1, 0, 2))[0]
    key_pre = jax.vjp(rotate_back, k_pre)[1](
        kv_grad[:, :key_width].reshape(row_count, heads_here, HD)
    )[0]
    return jnp.concatenate(
        [
            query_pre.reshape(row_count, key_width),
            key_pre.reshape(row_count, key_width),
            kv_grad[:, key_width:],
        ],
        axis=1,
    )


def sliced_pass(norm_bf, q_seg, cotangent, own_mats, qkv_bb, up_bb):
    own_qkv, own_dense, own_up, own_down = own_mats
    inner_count = lax.axis_size("shard")
    outer_count = lax.axis_size("rep")
    stride = outer_count // inner_count
    place = lax.axis_index("shard")
    head_width = D // inner_count
    unit_width = FF // inner_count
    qkv_rows = own_qkv.shape[0]
    dense_rows = own_dense.shape[0]
    down_rows = own_down.shape[0]
    qkv_split = own_qkv.reshape(qkv_rows, 3, inner_count, head_width)
    up_split = own_up.reshape(qkv_rows, 1, inner_count, unit_width)
    qkv_cols, up_cols = (
        lax.all_to_all(qkv_split, "shard", split_axis=2, concat_axis=0, tiled=True),
        lax.all_to_all(up_split, "shard", split_axis=2, concat_axis=0, tiled=True),
    )
    qkv_rep, up_rep, dense_rep, down_rep = (
        lax.all_gather(qkv_cols, "rep", axis=0, tiled=True),
        lax.all_gather(up_cols, "rep", axis=0, tiled=True),
        lax.all_gather(own_dense[None], "rep", axis=0, tiled=True),
        lax.all_gather(own_down[None], "rep", axis=0, tiled=True),
    )
    dense_grid = dense_rep.reshape(inner_count, stride, 1, dense_rows, D)
    down_grid = down_rep.reshape(inner_count, stride, 1, down_rows, D)
    dense_moved, down_moved = (
        lax.all_to_all(dense_grid, "shard", split_axis=0, concat_axis=2, tiled=True),
        lax.all_to_all(down_grid, "shard", split_axis=0, concat_axis=2, tiled=True),
    )
    qkv_w = qkv_rep.reshape(D, 3 * head_width)
    up_w = up_rep.reshape(D, unit_width)
    dense_w = dense_moved.reshape(head_width, D)
    down_w = down_moved.reshape(unit_width, D)
    qkv_b = lax.dynamic_index_in_dim(
        qkv_bb.astype(jnp.float32).reshape(3, inner_count, head_width), place, 1, False
    ).reshape(3 * head_width)
    up_b = lax.dynamic_slice_in_dim(up_bb.astype(jnp.float32), place * unit_width, unit_width, 0)
    norm_seq, grad_seq, seg_seq = (
        lax.all_gather(norm_bf, "shard", axis=0, tiled=True),
        lax.all_gather(cotangent, "shard", axis=0, tiled=True),
        lax.all_gather(q_seg, "shard", axis=0, tiled=True),
    )
    seq_rows = norm_seq.shape[0]
    heads_here = head_width // HD
    positions = jnp.arange(seq_rows, dtype=jnp.int32)
    q_pre, k_pre, queries, kv_seq = attention_pass(norm_seq, qkv_w, qkv_b, positions, head_width)
    row_max, totals, accumulated = attend_keys(kv_seq, seg_seq, queries, positions, seg_seq)
    lse_all = row_max + jnp.log(totals)
    out_heads = (accumulated / totals[..., None]).transpose(1, 0, 2).astype(jnp.bfloat16)
    attn_bf = out_heads.reshape(seq_rows, head_width)
    pre_act = jnp.dot(norm_seq, up_w, preferred_element_type=jnp.float32) + up_b
    hidden = gelu_tanh(pre_act).astype(jnp.bfloat16)
    partial_out = jnp.dot(attn_bf, dense_w, preferred_element_type=jnp.float32) + jnp.dot(
        hidden, down_w, preferred_element_type=jnp.float32
    )
    mixed = sum_positions(partial_out)
    grad_down = jnp.dot(hidden.T, grad_seq, preferred_element_type=jnp.float32)
    grad_dense = jnp.dot(attn_bf.T, grad_seq, preferred_element_type=jnp.float32)
    grad_hidden = jnp.dot(grad_seq, down_w.T, preferred_element_type=jnp.float32)
    grad_pre = jax.vjp(gelu_tanh, pre_act)[1](grad_hidden)[0]
    grad_pre_bf = grad_pre.astype(jnp.bfloat16)
    grad_up = jnp.dot(norm_seq.T, grad_pre_bf, preferred_element_type=jnp.float32)
    upb_part = jnp.sum(grad_pre, axis=0)
    norm_part = jnp.dot(grad_pre_bf, up_w.T, preferred_element_type=jnp.float32)
    grad_heads = (
        jnp.dot(grad_seq, dense_w.T, preferred_element_type=jnp.float32)
        .astype(jnp.bfloat16)
        .reshape(seq_rows, heads_here, HD)
    )
    delta_all = jnp.sum(grad_heads.astype(jnp.float32) * out_heads.astype(jnp.float32), axis=-1).T
    query_grad, kv_grad = attention_grads(
        queries, kv_seq, seg_seq, positions, seg_seq, grad_heads, delta_all, lse_all
    )
    grad_joined = finish_qkv_grad(q_pre, k_pre, positions, query_grad, kv_grad, head_width)
    grad_joined_bf = grad_joined.astype(jnp.bfloat16)
    grad_qkv = jnp.dot(norm_seq.T, grad_joined_bf, preferred_element_type=jnp.float32)
    qkvb_part = jnp.sum(grad_joined, axis=0)
    norm_part = norm_part + jnp.dot(grad_joined_bf, qkv_w.T, preferred_element_type=jnp.float32)
    grad_norm = sum_positions(norm_part)
    dense_grid_grad = grad_dense.reshape(1, stride, inner_count, dense_rows, D)
    down_grid_grad = grad_down.reshape(1, stride, inner_count, down_rows, D)
    dense_back, down_back = (
        lax.all_to_all(dense_grid_grad, "shard", split_axis=2, concat_axis=0, tiled=True),
        lax.all_to_all(down_grid_grad, "shard", split_axis=2, concat_axis=0, tiled=True),
    )
    qkv_sum, up_sum, dense_sum, down_sum = (
        lax.psum_scatter(
            grad_qkv.reshape(D, 3, 1, head_width), "rep", scatter_dimension=0, tiled=True
        ),
        lax.psum_scatter(
            grad_up.reshape(D, 1, 1, unit_width), "rep", scatter_dimension=0, tiled=True
        ),
        lax.psum_scatter(
            dense_back.reshape(outer_count, dense_rows, D), "rep", scatter_dimension=0, tiled=True
        ),
        lax.psum_scatter(
            down_back.reshape(outer_count, down_rows, D), "rep", scatter_dimension=0, tiled=True
        ),
    )
    qkv_home, up_home = (
        lax.all_to_all(qkv_sum, "shard", split_axis=0, concat_axis=2, tiled=True),
        lax.all_to_all(up_sum, "shard", split_axis=0, concat_axis=2, tiled=True),
    )
    qkv_own = qkv_home.reshape(qkv_rows, 3 * D)
    up_own = up_home.reshape(qkv_rows, FF)
    dense_own = dense_sum.reshape(dense_rows, D)
    down_own = down_sum.reshape(down_rows, D)
    selector = (jnp.arange(inner_count, dtype=jnp.int32) == place).astype(jnp.float32)
    qkvb_grad = (selector[None, :, None] * qkvb_part.reshape(3, 1, head_width)).reshape(3 * D)
    upb_grad = (selector[:, None] * upb_part[None, :]).reshape(FF)
    return (mixed, grad_norm, (qkv_own, dense_own, up_own, down_own), qkvb_grad, upb_grad)


def body(
    hidden_in,
    segment_ids,
    out_grad,
    qkv_weight_state,
    qkv_bias_state,
    dense_weight_state,
    up_weight_state,
    up_bias_state,
    down_weight_state,
    vector_state,
):
    own_mats = (
        qkv_weight_state[0].astype(jnp.bfloat16),
        dense_weight_state[0].astype(jnp.bfloat16),
        up_weight_state[0].astype(jnp.bfloat16),
        down_weight_state[0].astype(jnp.bfloat16),
    )
    qkv_bb, up_bb, vec_bf = gather_vectors(
        qkv_bias_state[0].astype(jnp.bfloat16),
        up_bias_state[0].astype(jnp.bfloat16),
        vector_state[0].astype(jnp.bfloat16),
    )
    vec_all = vec_bf.astype(jnp.float32)
    norm_gain = vec_all[:, 0]
    norm_shift = vec_all[:, 1]
    dense_bias = vec_all[:, 2]
    down_bias = vec_all[:, 3]
    tokens = hidden_in[0]
    q_seg = segment_ids[0]
    cotangent = out_grad[0]
    x_full = tokens.astype(jnp.float32)
    normed = layer_norm(x_full, norm_gain, norm_shift)
    norm_bf = normed.astype(jnp.bfloat16)
    mixed, grad_norm, owned, qkvb_grad, upb_grad = sliced_pass(
        norm_bf, q_seg, cotangent, own_mats, qkv_bb, up_bb
    )
    qkv_own, dense_own, up_own, down_own = owned
    output = (x_full + (mixed + dense_bias + down_bias)).astype(jnp.bfloat16)
    grad_x, grad_gain, grad_shift = jax.vjp(layer_norm, x_full, norm_gain, norm_shift)[1](grad_norm)
    out_bias_grad = jnp.sum(cotangent.astype(jnp.float32), axis=0)
    grad_vec = jnp.stack([grad_gain, grad_shift, out_bias_grad, out_bias_grad], axis=1)
    input_grad = cotangent.astype(jnp.float32) + grad_x
    qkvb_own, upb_own, vec_own = sum_vectors(qkvb_grad, upb_grad, grad_vec)
    new_states = (
        adam_update(qkv_weight_state, qkv_own),
        adam_update(qkv_bias_state, qkvb_own),
        adam_update(dense_weight_state, dense_own),
        adam_update(up_weight_state, up_own),
        adam_update(up_bias_state, upb_own),
        adam_update(down_weight_state, down_own),
        adam_update(vector_state, vec_own),
    )
    return (
        output[None],
        input_grad[None],
        qkv_own,
        qkvb_own,
        dense_own,
        up_own,
        upb_own,
        down_own,
        vec_own,
        owner_entries(new_states, 0),
        owner_entries(new_states, 1),
        owner_entries(new_states, 2),
    )


def whole_heads(mesh):
    owners = mesh.shape["rep"] * mesh.shape["shard"]
    return D % owners == 0 and D // owners == HD and mesh.shape["rep"] % 2 == 0


def rotation_tables(seq_rows):
    half_rot = ROT // 2
    lane = jnp.arange(2 * HD, dtype=jnp.int32) % HD
    frequency = jnp.exp((lane % half_rot).astype(jnp.float32) * (-2.0 * math.log(10000.0) / ROT))
    angles = jnp.arange(seq_rows, dtype=jnp.int32).astype(jnp.float32)[:, None] * frequency[None, :]
    sine = jnp.sin(angles)
    cosine = jnp.where(lane[None, :] < ROT, jnp.cos(angles), 1.0)
    low = jnp.where(lane[None, :] < half_rot, -sine, 0.0)
    high = jnp.where((lane[None, :] >= half_rot) & (lane[None, :] < ROT), sine, 0.0)
    return cosine, low, high


def attention_kernel(
    fu_ref, do_ref, du_ref, seg_col_ref, seg_row_ref, cos_ref, low_ref, high_ref, o_ref, dcat_ref, sums_ref
):
    rows, width = do_ref.shape
    scale = 1.0 / math.sqrt(HD)
    row_id = lax.broadcasted_iota(jnp.int32, (rows, rows), 0)
    col_id = lax.broadcasted_iota(jnp.int32, (rows, rows), 1)
    allowed = (col_id <= row_id) & (seg_col_ref[...] == seg_row_ref[0])
    cosine, low, high = cos_ref[...], low_ref[...], high_ref[...]
    half = ROT // 2
    lane = lax.broadcasted_iota(jnp.int32, (rows, 2 * HD), 1)

    def rotate(u):
        return (
            u * cosine
            + pltpu.roll(u, 2 * HD - half, 1) * low
            + pltpu.roll(u, half, 1) * high
        )

    def rotate_back(u):
        return (
            u * cosine
            - pltpu.roll(u, 2 * HD - half, 1) * low
            - pltpu.roll(u, half, 1) * high
        )

    def dot(a, b, a_dim, b_dim):
        return lax.dot_general(a, b, (((a_dim,), (b_dim,)), ((), ())), preferred_element_type=jnp.float32)

    zero = jnp.zeros((), jnp.bfloat16)
    for pair in range(width // (2 * HD)):
        lanes = pl.ds(pair * 2 * HD, 2 * HD)
        k_lanes = pl.ds(width + pair * 2 * HD, 2 * HD)
        v_lanes = pl.ds(2 * width + pair * 2 * HD, 2 * HD)
        q = rotate(fu_ref[:, lanes]).astype(jnp.bfloat16)
        k = rotate(fu_ref[:, k_lanes]).astype(jnp.bfloat16)
        v = fu_ref[:, v_lanes].astype(jnp.bfloat16)
        do = do_ref[:, lanes]
        o = dq = dk = dv = None
        for head in range(2):
            mine = (lane < HD) if head == 0 else (lane >= HD)
            qh = jnp.where(mine, q, zero)
            kh = jnp.where(mine, k, zero)
            vh = jnp.where(mine, v, zero)
            doh = jnp.where(mine, do, zero)
            scores = jnp.where(allowed, dot(qh, k, 1, 1) * scale, big_negative)
            row_max = jnp.max(scores, axis=1, keepdims=True)
            probs = jnp.where(allowed, jnp.exp(scores - row_max), 0.0)
            inverse = 1.0 / jnp.sum(probs, axis=1, keepdims=True)
            oh = dot(probs.astype(jnp.bfloat16), vh, 1, 0) * inverse
            delta = jnp.sum(
                doh.astype(jnp.float32) * oh.astype(jnp.bfloat16).astype(jnp.float32), axis=1, keepdims=True
            )
            probs = probs * inverse
            dvh = dot(probs.astype(jnp.bfloat16), doh, 0, 0)
            ds = (probs * (dot(doh, v, 1, 1) - delta) * scale).astype(jnp.bfloat16)
            dqh = dot(ds, kh, 1, 0)
            dkh = dot(ds, qh, 0, 0)
            if head == 0:
                o, dq, dk, dv = oh, dqh, dkh, dvh
            else:
                o, dq, dk, dv = o + oh, dq + dqh, dk + dkh, dv + dvh
        o_ref[:, lanes] = o.astype(jnp.bfloat16)
        dq = rotate_back(dq)
        dk = rotate_back(dk)
        for part, place in ((dq, lanes), (dk, k_lanes), (dv, v_lanes)):
            dcat_ref[:, place] = part.astype(jnp.bfloat16)
            sums_ref[0, :, place] = jnp.sum(part, axis=0, keepdims=True)
    dcat_ref[:, pl.ds(3 * width, du_ref.shape[1])] = du_ref[...]


def attention(fu, do, du, segments):
    count, rows = segments.shape
    width = do.shape[1]
    units = du.shape[1]
    tables = rotation_tables(rows)
    table_spec = pl.BlockSpec((rows, 2 * HD), lambda s: (0, 0))
    o, dcat, sums = pl.pallas_call(
        attention_kernel,
        grid=(count,),
        in_specs=[
            pl.BlockSpec((rows, 3 * width), lambda s: (s, 0)),
            pl.BlockSpec((rows, width), lambda s: (s, 0)),
            pl.BlockSpec((rows, units), lambda s: (s, 0)),
            pl.BlockSpec((rows, 1), lambda s: (s, 0)),
            pl.BlockSpec((1, 1, rows), lambda s: (s, 0, 0)),
            table_spec,
            table_spec,
            table_spec,
        ],
        out_specs=[
            pl.BlockSpec((rows, width), lambda s: (s, 0)),
            pl.BlockSpec((rows, 3 * width + units), lambda s: (s, 0)),
            pl.BlockSpec((1, 1, 3 * width), lambda s: (s, 0, 0)),
        ],
        out_shape=[
            jax.ShapeDtypeStruct((count * rows, width), jnp.bfloat16),
            jax.ShapeDtypeStruct((count * rows, 3 * width + units), jnp.bfloat16),
            jax.ShapeDtypeStruct((count, 1, 3 * width), jnp.float32),
        ],
        compiler_params=pltpu.CompilerParams(vmem_limit_bytes=56 << 20),
        cost_estimate=pl.CostEstimate(
            flops=count * (width // HD) * 10 * rows * rows * HD,
            bytes_accessed=count * rows * (width * 20 + units * 4),
            transcendentals=count * (width // HD) * rows * rows,
        ),
    )(fu, do, du, segments.reshape(count * rows, 1), segments.reshape(count, 1, rows), *tables)
    return o, dcat, jnp.sum(sums, axis=(0, 1))


def adam_values(weight, moment_one, moment_two, grad):
    first = beta_one * moment_one + (1.0 - beta_one) * grad
    second = beta_two * moment_two + (1.0 - beta_two) * grad * grad
    corrected = first * (1.0 / (1.0 - beta_one**STEP))
    divisor = jnp.sqrt(second * (1.0 / (1.0 - beta_two**STEP))) + adam_eps
    return weight - learn_rate * (corrected / divisor + weight_decay * weight), first, second


def owner_update_kernel(plan, small_plan, *refs):
    count = len(plan)
    small_ref = refs[2 * count]
    outs = refs[2 * count + 1 :]
    step = pl.program_id(0)
    lane = lax.broadcasted_iota(jnp.int32, (8, 128), 1)
    sub = lax.broadcasted_iota(jnp.int32, (8, 128), 0)
    lane_row = lax.broadcasted_iota(jnp.int32, (1, 128), 1)

    @pl.when(step == 0)
    def small():
        for source, row, low, high in small_plan:
            for entry in range(3):
                old = outs[entry][pl.ds(row, 1), :]
                new = small_ref[entry, pl.ds(source, 1), :]
                outs[entry][pl.ds(row, 1), :] = jnp.where((lane_row >= low) & (lane_row < high), new, old)

    for index, (rows, tiles, start, shifted) in enumerate(plan):
        state, grad = refs[2 * index], refs[2 * index + 1]
        for group in range(rows // 8):
            place = pl.ds(group * 8, 8)
            base = start + (step * (rows // 8) + group) * (8 * tiles)

            def values(column, state=state, grad=grad, place=place):
                lanes = pl.ds(pl.multiple_of(column * 128, 128), 128)
                return adam_values(
                    state[0, place, lanes], state[1, place, lanes], state[2, place, lanes], grad[place, lanes]
                )

            if not shifted:

                def plain(column, carry, base=base, tiles=tiles, values=values):
                    for out, value in zip(outs, values(column)):
                        out[pl.ds(base + column, 8, stride=tiles), :] = value
                    return carry

                lax.fori_loop(0, tiles, plain, 0, unroll=4)
                continue

            def turned(column, values=values):
                return tuple(pltpu.roll(value, 64, 1) for value in values(column))

            last = turned(tiles - 1)
            before = tuple(
                jnp.where(sub == 0, out[pl.ds(base, 1), :], pltpu.roll(value, 1, 0))
                for out, value in zip(outs, last)
            )

            def moved(column, carry, base=base, tiles=tiles, turned=turned):
                now = turned(column)
                for out, old, new in zip(outs, carry, now):
                    out[pl.ds(base + column, 8, stride=tiles), :] = jnp.where(lane < 64, old, new)
                return now

            lax.fori_loop(0, tiles, moved, before, unroll=4)
            for out, value in zip(outs, last):
                row = pl.ds(base + 8 * tiles, 1)
                out[row, :] = jnp.where(lane_row < 64, value[7:8], out[row, :])


def owner_update(states, grads, small_states, small_grads):
    steps = 8
    sizes = [state.shape[1] * state.shape[2] for state in states]
    small_sizes = [grad.size for grad in small_grads]
    order = [("m", 0), ("s", 0), ("m", 1), ("m", 2), ("s", 1), ("m", 3), ("s", 2)]
    offset = 0
    plan = [None] * 4
    small_plan = []
    pads = []
    small_row = 0
    for kind, index in order:
        if kind == "m":
            state = states[index]
            rows = state.shape[1] // steps
            plan[index] = (rows, state.shape[2] // 128, offset // 128, offset % 128 == 64)
            offset += sizes[index]
        else:
            size = small_sizes[index]
            front = offset % 128
            total = -(-(front + size) // 128)
            pads.append((front, total * 128 - front - size))
            for extra in range(total):
                low = front if extra == 0 else 0
                high = min(128, front + size - extra * 128)
                small_plan.append((small_row + extra, offset // 128 + extra, low, high))
            small_row += total
            offset += size
    entries = offset
    out_rows = -(-entries // 1024) * 8
    small_new = [
        adam_values(state[0].reshape(-1), state[1].reshape(-1), state[2].reshape(-1), grad.reshape(-1))
        for state, grad in zip(small_states, small_grads)
    ]
    small = jnp.stack(
        [
            jnp.concatenate([jnp.pad(new[entry], pad) for new, pad in zip(small_new, pads)])
            for entry in range(3)
        ]
    ).reshape(3, small_row, 128)
    in_specs = []
    operands = []
    for state, grad, (rows, tiles, start, shifted) in zip(states, grads, plan):
        in_specs.append(pl.BlockSpec((3, rows, tiles * 128), lambda s: (0, s, 0)))
        in_specs.append(pl.BlockSpec((rows, tiles * 128), lambda s: (s, 0)))
        operands += [state, grad]
    in_specs.append(pl.BlockSpec((3, small_row, 128), lambda s: (0, 0, 0)))
    outs = pl.pallas_call(
        partial(owner_update_kernel, plan, small_plan),
        grid=(steps,),
        in_specs=in_specs,
        out_specs=[pl.BlockSpec((out_rows, 128), lambda s: (0, 0), pipeline_mode=pl.Buffered(1))] * 3,
        out_shape=[jax.ShapeDtypeStruct((out_rows, 128), jnp.float32)] * 3,
        compiler_params=pltpu.CompilerParams(vmem_limit_bytes=56 << 20),
        cost_estimate=pl.CostEstimate(
            flops=20 * entries, bytes_accessed=28 * entries, transcendentals=2 * entries
        ),
    )(*operands, small)
    return tuple(out.reshape(1, 1, out_rows * 128)[:, :, :entries] for out in outs)


class Wires:
    def __init__(self, send_sems):
        self.send_sems, self.count, self.pending = send_sems, 0, []
        self.plane, self.core, self.shard = (
            lax.axis_index("plane"),
            lax.axis_index("core"),
            lax.axis_index("shard"),
        )
        self.shards = lax.axis_size("shard")
        self.group = lax.axis_size("core") * self.shards
        self.mine = self.core * self.shards + self.shard
        self.first = (self.plane ^ 1, self.core, self.shard)
        self.second = (self.plane ^ 2, self.core, self.shard)

    def member(self, index):
        return (self.plane, index // self.shards, index % self.shards)

    def barrier(self):
        barrier = pltpu.get_barrier_semaphore()
        partners = [self.member(self.mine ^ mask) for mask in range(1, self.group)]
        partners += [self.first, self.second]
        for partner in partners:
            pl.semaphore_signal(barrier, inc=1, device_id=partner, device_id_type=pl.DeviceIdType.MESH)
        pl.semaphore_wait(barrier, len(partners))

    def send(self, source, target, recv_sem, device, when=None):
        copy = pltpu.make_async_remote_copy(
            src_ref=source,
            dst_ref=target,
            send_sem=self.send_sems.at[self.count],
            recv_sem=recv_sem,
            device_id=device,
            device_id_type=pl.DeviceIdType.MESH,
        )
        self.count += 1
        self.pending.append((copy, when))
        if when is None:
            copy.start()
        else:
            pl.when(when)(copy.start)

    def arrived(self, place, recv_sem, when=None):
        copy = pltpu.make_async_remote_copy(
            src_ref=place,
            dst_ref=place,
            send_sem=self.send_sems.at[0],
            recv_sem=recv_sem,
            device_id=self.first,
            device_id_type=pl.DeviceIdType.MESH,
        )
        if when is None:
            copy.wait_recv()
        else:
            pl.when(when)(copy.wait_recv)

    def drain(self):
        for copy, when in self.pending:
            if when is None:
                copy.wait_send()
            else:
                pl.when(when)(copy.wait_send)


def gather_kernel(
    pieces, dense, down, tokens, cotangent, vectors,
    cat_out, dense_out, down_out, x_out, dy_out, vec_out,
    send_sems, group_sem, first_sem, second_sem, far_sem, up_sem, low_sem, core_sem, local_sem,
):
    net = Wires(send_sems)
    plane, core, shard, shards, group, mine = net.plane, net.core, net.shard, net.shards, net.group, net.mine
    order = sorted(range(group), key=lambda mask: (mask % shards, mask // shards))
    partner = (plane, 1 - core, shard)

    def cat_unit(mask):
        return lambda p: cat_out.at[p, mine ^ mask]

    def vec_unit(mask):
        return lambda p: vec_out.at[p, mine ^ mask]

    units = []
    down_rows = down.shape[0] // 4
    for part in range(4):
        rows = pl.ds(part * down_rows, down_rows)
        units.append((down.at[rows], lambda p, rows=rows: down_out.at[p, rows]))
    dense_rows = dense.shape[0] // 2
    for part in range(2):
        rows = pl.ds(part * dense_rows, dense_rows)
        units.append((dense.at[rows], lambda p, rows=rows: dense_out.at[p, rows]))
    own_units = list(range(len(units)))
    cat_units, vec_units = {}, {}
    for mask in order:
        cat_units[mask] = len(units)
        units.append((pieces.at[mine] if mask == 0 else None, cat_unit(mask)))
        vec_units[mask] = len(units)
        units.append((vectors if mask == 0 else None, vec_unit(mask)))

    def spread(index):
        source, place = units[index]
        source = place(plane) if source is None else source
        net.send(source, place(plane), first_sem.at[index], net.first)
        net.send(source, place(plane), second_sem.at[index], net.second)

    def hand_on(index):
        place = units[index][1]
        if relay_first[index]:
            net.arrived(place(plane ^ 1), first_sem.at[index])
            net.send(place(plane ^ 1), place(plane ^ 1), far_sem.at[index], net.second)
        else:
            net.arrived(place(plane ^ 2), second_sem.at[index])
            net.send(place(plane ^ 2), place(plane ^ 2), far_sem.at[index], net.first)

    relay_first = {}
    for position, index in enumerate(own_units):
        relay_first[index] = position % 2 == 0
    for position, mask in enumerate(order):
        relay_first[cat_units[mask]] = position % 2 == 0
        relay_first[vec_units[mask]] = position % 2 == 1

    net.barrier()

    locals_ = [
        (pieces.at[mine], cat_out.at[plane, mine]),
        (dense, dense_out.at[plane]),
        (down, down_out.at[plane]),
        (tokens, x_out.at[mine]),
        (cotangent, dy_out.at[mine]),
        (vectors, vec_out.at[plane, mine]),
    ]
    copies = [
        pltpu.make_async_copy(source, target, local_sem.at[index])
        for index, (source, target) in enumerate(locals_)
    ]
    for mask in order[1:]:
        target = net.member(mine ^ mask)
        net.send(vectors, vec_out.at[plane, mine], group_sem.at[1, mask], target)
        net.send(pieces.at[mine ^ mask], cat_out.at[plane, mine], group_sem.at[0, mask], target)
    for index in own_units:
        spread(index)
    spread(cat_units[0])
    spread(vec_units[0])
    streams = ((tokens, x_out), (cotangent, dy_out))

    def block(stream, origin):
        return streams[stream][1].at[core * shards + origin]

    def to_core(stream, source, origin, slot, when=None):
        net.send(source, block(stream, origin), core_sem.at[stream, slot], partner, when)

    def hop(stream, distance):
        own = distance == 1
        for upward, sem in ((True, up_sem), (False, low_sem)):
            origin = shard - (distance - 1) if upward else shard + (distance - 1)
            there = shard + 1 if upward else shard - 1
            held = (origin >= 0) if upward else (origin < shards)
            inside = (there < shards) if upward else (there >= 0)
            near = jnp.clip(origin, 0, shards - 1)
            source = streams[stream][0] if own else block(stream, near)
            net.send(
                source,
                block(stream, near),
                sem.at[stream, distance],
                (plane, core, jnp.clip(there, 0, shards - 1)),
                inside & held,
            )

    def hop_arrived(stream, distance):
        for upward, sem in ((True, up_sem), (False, low_sem)):
            origin = shard - distance if upward else shard + distance
            held = (origin >= 0) if upward else (origin < shards)
            near = jnp.clip(origin, 0, shards - 1)
            net.arrived(block(stream, near), sem.at[stream, distance], held)
            slot = distance if upward else shards + distance
            to_core(stream, block(stream, near), near, slot, held)

    for stream in range(2):
        hop(stream, 1)
    for stream in range(2):
        to_core(stream, streams[stream][0], shard, 0)
    for copy in copies:
        copy.start()

    for position, mask in enumerate(order[1:]):
        net.arrived(vec_out.at[plane, mine ^ mask], group_sem.at[1, mask])
        spread(vec_units[mask])
        net.arrived(cat_out.at[plane, mine ^ mask], group_sem.at[0, mask])
        spread(cat_units[mask])
        if position == 2:
            for index in own_units:
                hand_on(index)
    hand_on(cat_units[0])
    hand_on(vec_units[0])
    for distance in range(1, shards):
        for stream in range(2):
            hop_arrived(stream, distance)
            if distance + 1 < shards:
                hop(stream, distance + 1)
        for mask in order[1 + (distance - 1) * 3 : 1 + distance * 3]:
            hand_on(vec_units[mask])
            hand_on(cat_units[mask])

    for index, (source, place) in enumerate(units):
        if relay_first[index]:
            net.arrived(place(plane ^ 2), second_sem.at[index])
        else:
            net.arrived(place(plane ^ 1), first_sem.at[index])
        net.arrived(place(plane ^ 3), far_sem.at[index])
    for stream in range(2):
        other = streams[stream][1]
        for slot in range(2 * shards):
            if slot == shards:
                continue
            origin = shard - slot if slot < shards else shard + (slot - shards)
            held = None if slot == 0 else ((origin >= 0) & (origin < shards))
            near = jnp.clip(origin, 0, shards - 1)
            net.arrived(other.at[(1 - core) * shards + near], core_sem.at[stream, slot], held)
    for copy in copies:
        copy.wait()
    net.drain()


def gather_wires(pieces, dense, down, tokens, cotangent, vectors):
    group, shards = lax.axis_size("core") * lax.axis_size("shard"), lax.axis_size("shard")
    planes = lax.axis_size("plane")
    units = 6 + 2 * group
    vmem = pl.BlockSpec(memory_space=pltpu.VMEM)
    hbm = pl.BlockSpec(memory_space=pl.ANY)

    def out(lead, value):
        return jax.ShapeDtypeStruct(lead + value.shape, value.dtype)

    dma = pltpu.SemaphoreType.DMA
    return pl.pallas_call(
        gather_kernel,
        in_specs=[vmem] * 6,
        out_specs=[hbm] * 6,
        out_shape=[
            out((planes,), pieces),
            out((planes,), dense),
            out((planes,), down),
            out((group,), tokens),
            out((group,), cotangent),
            out((planes, group), vectors),
        ],
        scratch_shapes=[
            dma((2 * (group - 1) + 3 * units + 2 * 2 * (shards - 1) + 2 * (2 * shards - 1),)),
            dma((2, group)),
            dma((units,)),
            dma((units,)),
            dma((units,)),
            dma((2, shards)),
            dma((2, shards)),
            dma((2, 2 * shards)),
            dma((6,)),
        ],
        compiler_params=pltpu.CompilerParams(
            collective_id=0, has_side_effects=True, vmem_limit_bytes=24 << 20
        ),
    )(pieces, dense, down, tokens, cotangent, vectors)


def add_rows(target, *sources):
    step = 16
    rows = target.shape[0]

    def body(index, carry):
        place = pl.ds(pl.multiple_of(index * step, step), step)
        total = sources[0][place, :].astype(jnp.float32)
        for source in sources[1:]:
            total = total + source[place, :].astype(jnp.float32)
        target[place, :] = total.astype(target.dtype)
        return carry

    lax.fori_loop(0, rows // step, body, 0)


def reduce_kernel(
    cat, dense, down, out_part, norm_part, sums,
    cat_out, dense_out, down_out, mixed_out, norm_out, sums_out,
    cat_buf, down_buf, dense_buf, token_buf, sum_buf,
    send_sems, near_sem, pass_sem, group_sem, core_sem, line_sem, sum_sem, local_sem,
):
    PASS_IN, PASS_OWN, PASS_OUT, KEEP_IN, KEEP_OWN, LAST_IN = range(6)
    net = Wires(send_sems)
    plane, core, shard, shards, group, mine = net.plane, net.core, net.shard, net.shards, net.group, net.mine
    partner = (plane, 1 - core, shard)
    order = sorted(range(group), key=lambda mask: (mask % shards, mask // shards), reverse=True)

    units = []
    for mask in order:
        units.append((lambda p, mask=mask: cat.at[p, mine ^ mask], cat_buf, mask))
    down_rows = down.shape[1] // 4
    for part in range(4):
        rows = pl.ds(part * down_rows, down_rows)
        units.append((lambda p, rows=rows: down.at[p, rows], down_buf, part))
    dense_rows = dense.shape[1] // 2
    for part in range(2):
        rows = pl.ds(part * dense_rows, dense_rows)
        units.append((lambda p, rows=rows: dense.at[p, rows], dense_buf, part))

    def ways(index):
        if index % 2 == 0:
            return net.first, net.second, plane ^ 1, plane ^ 2
        return net.second, net.first, plane ^ 2, plane ^ 1

    loads = {}

    def load(key, source, target):
        loads[key] = pltpu.make_async_copy(source, target, local_sem.at[len(loads)])
        loads[key].start()

    streams = (out_part, norm_part)
    finals = (mixed_out, norm_out)
    TOKEN_IN, TOKEN_OWN, TOKEN_SUM, TOKEN_LINE = range(4)

    for index, (part, buffers, slot) in enumerate(units):
        near, far, near_plane, far_plane = ways(index)
        load(("pass", index), part(far_plane), buffers.at[PASS_OWN, slot])
    for stream in range(2):
        for mask in range(shards):
            load(
                ("token", stream, mask),
                streams[stream].at[core * shards + (shard ^ mask)],
                token_buf.at[TOKEN_OWN, stream, mask],
            )
    for index, (part, buffers, slot) in enumerate(units):
        load(("keep", index), part(plane), buffers.at[KEEP_OWN, slot])

    net.barrier()

    net.send(sums, sum_buf.at[0], sum_sem.at[0], net.first)
    for stream in range(2):
        for mask in reversed(range(shards)):
            net.send(
                streams[stream].at[(1 - core) * shards + (shard ^ mask)],
                token_buf.at[TOKEN_IN, stream, mask],
                core_sem.at[stream, mask],
                partner,
            )
    for index, (part, buffers, slot) in enumerate(units):
        near, far, near_plane, far_plane = ways(index)
        net.send(part(plane ^ 3), buffers.at[PASS_IN, slot], pass_sem.at[0, index], near)
        net.send(part(near_plane), buffers.at[KEEP_IN, slot], near_sem.at[index], near)

    def token_sum(stream, mask):
        net.arrived(token_buf.at[TOKEN_IN, stream, mask], core_sem.at[stream, mask])
        loads["token", stream, mask].wait()
        add_rows(
            token_buf.at[TOKEN_SUM, stream, mask],
            token_buf.at[TOKEN_IN, stream, mask],
            token_buf.at[TOKEN_OWN, stream, mask],
        )
        if mask:
            net.send(
                token_buf.at[TOKEN_SUM, stream, mask],
                token_buf.at[TOKEN_LINE, stream, mask],
                line_sem.at[stream, mask],
                (plane, core, shard ^ mask),
            )

    def pass_on(index):
        part, buffers, slot = units[index]
        near, far, near_plane, far_plane = ways(index)
        net.arrived(buffers.at[PASS_IN, slot], pass_sem.at[0, index])
        loads["pass", index].wait()
        add_rows(buffers.at[PASS_OUT, slot], buffers.at[PASS_IN, slot], buffers.at[PASS_OWN, slot])
        net.send(buffers.at[PASS_OUT, slot], buffers.at[LAST_IN, slot], pass_sem.at[1, index], far)

    def finish(index):
        part, buffers, slot = units[index]
        net.arrived(buffers.at[KEEP_IN, slot], near_sem.at[index])
        loads["keep", index].wait()
        net.arrived(buffers.at[LAST_IN, slot], pass_sem.at[1, index])
        values = (buffers.at[KEEP_IN, slot], buffers.at[KEEP_OWN, slot], buffers.at[LAST_IN, slot])
        if index < group:
            add_rows(buffers.at[KEEP_OWN, slot], *values)
            if slot:
                net.send(
                    buffers.at[KEEP_OWN, slot],
                    cat_out.at[mine],
                    group_sem.at[0, slot],
                    net.member(mine ^ slot),
                )
            else:
                load("own", buffers.at[KEEP_OWN, slot], cat_out.at[mine])
        elif index < group + 4:
            add_rows(down_out.at[pl.ds(slot * down_rows, down_rows)], *values)
        else:
            add_rows(dense_out.at[pl.ds(slot * dense_rows, dense_rows)], *values)

    net.arrived(sum_buf.at[0], sum_sem.at[0])
    sum_buf[1] = sums[...] + sum_buf[0]
    net.send(sum_buf.at[1], sum_buf.at[2], sum_sem.at[1], net.second)
    for mask in reversed(range(shards)):
        token_sum(0, mask)
    net.arrived(sum_buf.at[2], sum_sem.at[1])
    sum_buf[3] = sum_buf[1] + sum_buf[2]
    for mask in range(1, group):
        net.send(sum_buf.at[3], sums_out.at[mine], group_sem.at[1, mask], net.member(mine ^ mask))
    load("sums", sum_buf.at[3], sums_out.at[mine])
    lag = 4
    for index in range(len(units) + lag):
        if index < len(units):
            pass_on(index)
        if index >= lag:
            finish(index - lag)
        if index == 1:
            for mask in reversed(range(shards)):
                token_sum(1, mask)
    for stream in range(2):
        for mask in range(1, shards):
            net.arrived(token_buf.at[TOKEN_LINE, stream, mask], line_sem.at[stream, mask])
        add_rows(
            finals[stream],
            token_buf.at[TOKEN_SUM, stream, 0],
            *[token_buf.at[TOKEN_LINE, stream, mask] for mask in range(1, shards)],
        )
    for mask in range(1, group):
        net.arrived(cat_out.at[mine ^ mask], group_sem.at[0, mask])
        net.arrived(sums_out.at[mine ^ mask], group_sem.at[1, mask])
    loads["own"].wait()
    loads["sums"].wait()
    net.drain()


def reduce_wires(cat, dense, down, out_part, norm_part, sums):
    shards = lax.axis_size("shard")
    group = lax.axis_size("core") * shards
    units = group + 6
    vmem = pl.BlockSpec(memory_space=pltpu.VMEM)
    hbm = pl.BlockSpec(memory_space=pl.ANY)
    dma = pltpu.SemaphoreType.DMA
    tokens = out_part.shape[1:]
    return pl.pallas_call(
        reduce_kernel,
        in_specs=[hbm] * 5 + [vmem],
        out_specs=[hbm] + [vmem] * 4 + [hbm],
        out_shape=[
            jax.ShapeDtypeStruct(cat.shape[1:], cat.dtype),
            jax.ShapeDtypeStruct(dense.shape[1:], jnp.float32),
            jax.ShapeDtypeStruct(down.shape[1:], jnp.float32),
            jax.ShapeDtypeStruct(tokens, jnp.float32),
            jax.ShapeDtypeStruct(tokens, jnp.float32),
            jax.ShapeDtypeStruct((group,) + sums.shape, sums.dtype),
        ],
        scratch_shapes=[
            pltpu.VMEM((6, group) + cat.shape[2:], cat.dtype),
            pltpu.VMEM((6, 4, down.shape[1] // 4, down.shape[2]), down.dtype),
            pltpu.VMEM((6, 2, dense.shape[1] // 2, dense.shape[2]), dense.dtype),
            pltpu.VMEM((4, 2, shards) + tokens, out_part.dtype),
            pltpu.VMEM((4,) + sums.shape, sums.dtype),
            dma((2 + 2 * shards + 2 * (shards - 1) + 3 * units + 2 * (group - 1),)),
            dma((units,)),
            dma((2, units)),
            dma((2, group)),
            dma((2, shards)),
            dma((2, shards)),
            dma((2,)),
            dma((2 * units + 2 * shards + 2,)),
        ],
        compiler_params=pltpu.CompilerParams(
            collective_id=1, has_side_effects=True, vmem_limit_bytes=58 << 20
        ),
    )(cat, dense, down, out_part, norm_part, sums)


def fast_body(
    hidden_in,
    segment_ids,
    out_grad,
    qkv_weight_state,
    qkv_bias_state,
    dense_weight_state,
    up_weight_state,
    up_bias_state,
    down_weight_state,
    vector_state,
):
    planes, cores, shards = lax.axis_size("plane"), lax.axis_size("core"), lax.axis_size("shard")
    plane, core, shard = lax.axis_index("plane"), lax.axis_index("core"), lax.axis_index("shard")
    group = cores * shards
    owner = (plane * cores + core) * shards + shard
    owners = planes * group
    model_rows = qkv_weight_state.shape[1]
    unit_rows = down_weight_state.shape[1]
    tokens_here = hidden_in.shape[1]
    head_width = planes * HD
    unit_width = planes * unit_rows
    qkv_count, upb_count = qkv_bias_state.shape[1], up_bias_state.shape[1]

    tokens, cotangent, q_seg = hidden_in[0], out_grad[0], segment_ids[0]
    qkv_pieces = (
        qkv_weight_state[0]
        .astype(jnp.bfloat16)
        .reshape(model_rows, 3, planes, cores, shards, HD)
        .transpose(3, 4, 0, 1, 2, 5)
        .reshape(group, model_rows, 3 * head_width)
    )
    up_pieces = (
        up_weight_state[0]
        .astype(jnp.bfloat16)
        .reshape(model_rows, planes, cores, shards, unit_rows)
        .transpose(2, 3, 0, 1, 4)
        .reshape(group, model_rows, unit_width)
    )
    pieces = jnp.concatenate([qkv_pieces, up_pieces], axis=2)
    dense_own = dense_weight_state[0].astype(jnp.bfloat16)
    down_own = down_weight_state[0].astype(jnp.bfloat16)
    vec_list = [
        qkv_bias_state[0],
        up_bias_state[0],
        vector_state[0].T.reshape(-1),
        q_seg.astype(jnp.float32),
    ]
    vec_sizes = [value.size for value in vec_list]
    vec_rows = -(-sum(vec_sizes) // 1024) * 8
    vec_own = jnp.pad(jnp.concatenate(vec_list), (0, vec_rows * 128 - sum(vec_sizes))).reshape(vec_rows, 128)

    cat_w, dense_w, down_w, x_all, dy_all, vec_all = gather_wires(
        pieces, dense_own, down_own, tokens, cotangent, vec_own
    )

    cat_w = cat_w.reshape(D, 3 * head_width + unit_width)
    dense_w = dense_w.reshape(head_width, D)
    down_w = down_w.reshape(unit_width, D)
    rows = group * tokens_here
    x_all = x_all.reshape(rows, D)
    dy_all = dy_all.reshape(rows, D)
    vec_flat = vec_all.reshape(planes, cores, shards, vec_rows * 128)
    at = [0]
    for size in vec_sizes:
        at.append(at[-1] + size)

    def rounded(value):
        return value.astype(jnp.bfloat16).astype(jnp.float32)

    qkv_bias = rounded(vec_flat[..., at[0] : at[1]]).reshape(3, planes, cores, shards, HD)
    qkv_bias = lax.dynamic_index_in_dim(
        qkv_bias.transpose(2, 3, 0, 1, 4).reshape(group, 3 * head_width), core * shards + shard, 0, False
    )
    up_bias = lax.dynamic_index_in_dim(
        rounded(vec_flat[..., at[1] : at[2]]).transpose(1, 2, 0, 3).reshape(group, unit_width),
        core * shards + shard,
        0,
        False,
    )
    vec_columns = (
        rounded(vec_flat[..., at[2] : at[3]])
        .reshape(owners, 4, model_rows)
        .transpose(1, 0, 2)
        .reshape(4, D)
    )
    norm_gain, norm_shift, dense_bias, down_bias = (vec_columns[index] for index in range(4))
    segments = lax.dynamic_index_in_dim(vec_flat[..., at[3] : at[4]], plane, 0, False)
    segments = segments.astype(jnp.int32).reshape(cores, shards * tokens_here)
    cat_bias = jnp.concatenate([qkv_bias, up_bias])

    x_float = x_all.astype(jnp.float32)
    center = x_float - jnp.mean(x_float, axis=-1, keepdims=True)
    inverse = lax.rsqrt(jnp.mean(center * center, axis=-1, keepdims=True) + norm_eps)
    x_hat = center * inverse
    norm_bf = (x_hat * norm_gain + norm_shift).astype(jnp.bfloat16)

    fu = jnp.dot(norm_bf, cat_w, preferred_element_type=jnp.float32) + cat_bias
    pre_act = fu[:, 3 * head_width :]
    hidden = gelu_tanh(pre_act).astype(jnp.bfloat16)
    grad_hidden = jnp.dot(dy_all, down_w.T, preferred_element_type=jnp.float32)
    grad_pre = jax.vjp(gelu_tanh, pre_act)[1](grad_hidden)[0]
    upb_part = jnp.sum(grad_pre, axis=0)
    grad_heads = jnp.dot(dy_all, dense_w.T, preferred_element_type=jnp.float32).astype(jnp.bfloat16)
    attn, dcat, qkvb_part = attention(fu, grad_heads, grad_pre.astype(jnp.bfloat16), segments)
    out_part = (
        jnp.dot(attn, dense_w, preferred_element_type=jnp.float32)
        + jnp.dot(hidden, down_w, preferred_element_type=jnp.float32)
    ).astype(jnp.bfloat16)
    down_grad = jnp.dot(hidden.T, dy_all, preferred_element_type=jnp.float32).astype(jnp.bfloat16)
    dense_grad = jnp.dot(attn.T, dy_all, preferred_element_type=jnp.float32).astype(jnp.bfloat16)
    cat_grad = jnp.dot(norm_bf.T, dcat, preferred_element_type=jnp.float32).astype(jnp.bfloat16)
    norm_part = jnp.dot(dcat, cat_w.T, preferred_element_type=jnp.float32)
    gain_part = jnp.sum(norm_part * x_hat, axis=0)
    shift_part = jnp.sum(norm_part, axis=0)
    bias_part = jnp.sum(cotangent.astype(jnp.float32), axis=0)
    sums = [qkvb_part, upb_part, gain_part, shift_part, bias_part]
    sum_sizes = [value.size for value in sums]
    sum_rows = -(-sum(sum_sizes) // 1024) * 8
    sums = jnp.pad(jnp.concatenate(sums), (0, sum_rows * 128 - sum(sum_sizes))).reshape(sum_rows, 128)

    cat_sum, dense_grad, down_grad, mixed, grad_norm, sums_all = reduce_wires(
        cat_grad.reshape(planes, group, model_rows, 3 * head_width + unit_width),
        dense_grad.reshape(planes, model_rows, D),
        down_grad.reshape(planes, unit_rows, D),
        out_part.reshape(group, tokens_here, D),
        norm_part.astype(jnp.bfloat16).reshape(group, tokens_here, D),
        sums,
    )

    cat_sum = cat_sum.astype(jnp.float32)
    qkv_grad = (
        cat_sum[:, :, : 3 * head_width]
        .reshape(cores, shards, model_rows, 3, planes, HD)
        .transpose(2, 3, 4, 0, 1, 5)
        .reshape(model_rows, 3 * D)
    )
    up_grad = (
        cat_sum[:, :, 3 * head_width :]
        .reshape(cores, shards, model_rows, planes, unit_rows)
        .transpose(2, 3, 0, 1, 4)
        .reshape(model_rows, FF)
    )
    sums_flat = sums_all.reshape(cores, shards, sum_rows * 128)
    at = [0]
    for size in sum_sizes:
        at.append(at[-1] + size)
    qkvb_grad = (
        sums_flat[..., : at[1]]
        .reshape(cores, shards, 3, planes, HD)
        .transpose(2, 3, 0, 1, 4)
        .reshape(owners, qkv_count)
    )
    qkvb_grad = lax.dynamic_index_in_dim(qkvb_grad, owner, 0, False)
    upb_grad = sums_flat[..., at[1] : at[2]].reshape(group, planes, upb_count)
    upb_grad = lax.dynamic_index_in_dim(
        lax.dynamic_index_in_dim(upb_grad, core * shards + shard, 0, False), plane, 0, False
    )
    vec_grad = jnp.sum(sums_flat[..., at[2] : at[5]], axis=(0, 1)).reshape(3, owners, model_rows)
    vec_grad = lax.dynamic_index_in_dim(vec_grad, owner, 1, False)
    vec_grad = jnp.stack([vec_grad[0], vec_grad[1], vec_grad[2], vec_grad[2]], axis=1)

    x_own = tokens.astype(jnp.float32)
    output = (x_own + (mixed.astype(jnp.float32) + dense_bias + down_bias)).astype(jnp.bfloat16)
    own_center = x_own - jnp.mean(x_own, axis=-1, keepdims=True)
    own_inverse = lax.rsqrt(jnp.mean(own_center * own_center, axis=-1, keepdims=True) + norm_eps)
    own_hat = own_center * own_inverse
    hat_grad = grad_norm.astype(jnp.float32) * norm_gain
    x_grad = own_inverse * (
        hat_grad
        - jnp.mean(hat_grad, axis=-1, keepdims=True)
        - own_hat * jnp.mean(hat_grad * own_hat, axis=-1, keepdims=True)
    )
    input_grad = cotangent.astype(jnp.float32) + x_grad

    new = owner_update(
        (qkv_weight_state, dense_weight_state, up_weight_state, down_weight_state),
        (qkv_grad, dense_grad, up_grad, down_grad),
        (qkv_bias_state, up_bias_state, vector_state),
        (qkvb_grad, upb_grad, vec_grad),
    )
    return (
        output[None],
        input_grad[None],
        qkv_grad,
        qkvb_grad,
        dense_grad,
        up_grad,
        upb_grad,
        down_grad,
        vec_grad,
        *new,
    )


def fast_solution(mesh):
    rep, shard = mesh.shape["rep"], mesh.shape["shard"]
    inner = Mesh(mesh.devices.reshape(rep // 2, 2, shard), ("plane", "core", "shard"))
    both = ("plane", "core")
    every = ("plane", "core", "shard")
    in_specs = (
        P(both, "shard", None),
        P(both, "shard"),
        P(both, "shard", None),
        P(None, every, None),
        P(None, every),
        P(None, every, None),
        P(None, every, None),
        P(None, every),
        P(None, every, None),
        P(None, every, None),
    )
    out_specs = (
        P(both, "shard", None),
        P(both, "shard", None),
        P(every, None),
        P(every),
        P(every, None),
        P(every, None),
        P(every),
        P(every, None),
        P(every, None),
        P(both, "shard", None),
        P(both, "shard", None),
        P(both, "shard", None),
    )
    return jax.shard_map(fast_body, mesh=inner, in_specs=in_specs, out_specs=out_specs, check_vma=False)


def solution(mesh):
    in_specs = (
        P("rep", "shard", None),
        P("rep", "shard"),
        P("rep", "shard", None),
        P(None, ("rep", "shard"), None),
        P(None, ("rep", "shard")),
        P(None, ("rep", "shard"), None),
        P(None, ("rep", "shard"), None),
        P(None, ("rep", "shard")),
        P(None, ("rep", "shard"), None),
        P(None, ("rep", "shard"), None),
    )
    out_specs = (
        P("rep", "shard", None),
        P("rep", "shard", None),
        P(("rep", "shard"), None),
        P(("rep", "shard")),
        P(("rep", "shard"), None),
        P(("rep", "shard"), None),
        P(("rep", "shard")),
        P(("rep", "shard"), None),
        P(("rep", "shard"), None),
        P("rep", "shard", None),
        P("rep", "shard", None),
        P("rep", "shard", None),
    )
    if whole_heads(mesh):
        return fast_solution(mesh)
    return jax.shard_map(body, mesh=mesh, in_specs=in_specs, out_specs=out_specs, check_vma=False)
```

```python
from functools import partial
import math

import jax
import jax.numpy as jnp
from jax import lax
from jax.experimental import pallas as pl
from jax.experimental.pallas import tpu as pltpu
from jax.sharding import Mesh
from jax.sharding import PartitionSpec as P

D = 2048
HD = 64
ROT = 32
FF = 8192
STEP = 5


learn_rate = 0.02
beta_one = 0.9
beta_two = 0.95
adam_eps = 1e-08
weight_decay = 0.1
norm_eps = 1e-05
big_negative = -1e30


def layer_norm(x, norm_gain, norm_shift):
    center = x - jnp.mean(x, axis=-1, keepdims=True)
    variance = jnp.mean(center * center, axis=-1, keepdims=True)
    return center * lax.rsqrt(variance + norm_eps) * norm_gain + norm_shift


def gelu_tanh(v):
    return 0.5 * v * (1.0 + jnp.tanh(0.7978845608028654 * (v + 0.044715 * v * v * v)))


def rotary(x, positions):
    half_rot = ROT // 2
    frequency = jnp.exp(jnp.arange(half_rot, dtype=jnp.float32) * (-2.0 * math.log(10000.0) / ROT))
    angles = positions.astype(jnp.float32)[:, None] * frequency[None, :]
    cosine = jnp.cos(angles)[:, None, :]
    sine_val = jnp.sin(angles)[:, None, :]
    lower_part = x[..., :half_rot]
    upper_part = x[..., half_rot:ROT]
    return jnp.concatenate(
        [
            lower_part * cosine - upper_part * sine_val,
            upper_part * cosine + lower_part * sine_val,
            x[..., ROT:],
        ],
        axis=-1,
    )


def adam_update(state, grad):
    moment_one = beta_one * state[1] + (1.0 - beta_one) * grad
    moment_two = beta_two * state[2] + (1.0 - beta_two) * grad * grad
    corrected = moment_one / (1.0 - beta_one**STEP)
    divisor = jnp.sqrt(moment_two / (1.0 - beta_two**STEP)) + adam_eps
    weight = state[0] - learn_rate * (corrected / divisor + weight_decay * state[0])
    return jnp.stack([weight, moment_one, moment_two])


def owner_entries(new_states, entry):
    return jnp.concatenate(
        [state_new[entry].reshape(-1) for state_new in new_states], axis=0
    ).reshape(1, 1, -1)


def block_mask(q_pos, q_seg, k_pos, k_seg):
    return (k_pos[None, :] <= q_pos[:, None]) & (k_seg[None, :] == q_seg[:, None])


def attend_keys(kv_all, seg_all, queries, q_pos, q_seg):
    key_count = kv_all.shape[0]
    width = kv_all.shape[1] // 2
    heads_here = queries.shape[1]
    query_rows = queries.shape[0]
    block_rows = math.gcd(key_count, 512)
    block_count = key_count // block_rows
    kv_blocks = kv_all.reshape(block_count, block_rows, 2 * width)
    seg_blocks = seg_all.reshape(block_count, block_rows)
    score_scale = 1.0 / math.sqrt(HD)

    def attend_step_block(carry, block_items):
        kv_rows, seg_rows, block_index = block_items
        row_max, totals, accumulated = carry
        key_rows = kv_rows[:, :width].reshape(block_rows, heads_here, HD)
        value_rows = kv_rows[:, width:].reshape(block_rows, heads_here, HD)
        k_pos = block_index * block_rows + jnp.arange(block_rows, dtype=jnp.int32)
        allowed = block_mask(q_pos, q_seg, k_pos, seg_rows)
        scores = (
            jnp.einsum("qhd,khd->hqk", queries, key_rows, preferred_element_type=jnp.float32)
            * score_scale
        )
        scores = jnp.where(allowed[None], scores, big_negative)
        new_max = jnp.maximum(row_max, jnp.max(scores, axis=-1))
        probabilities = jnp.where(allowed[None], jnp.exp(scores - new_max[..., None]), 0.0)
        factor = jnp.exp(row_max - new_max)
        totals = totals * factor + jnp.sum(probabilities, axis=-1)
        accumulated = accumulated * factor[..., None] + jnp.einsum(
            "hqk,khd->hqd",
            probabilities.astype(jnp.bfloat16),
            value_rows,
            preferred_element_type=jnp.float32,
        )
        return ((new_max, totals, accumulated), None)

    start_state = (
        jnp.full((heads_here, query_rows), big_negative, jnp.float32),
        jnp.zeros((heads_here, query_rows), jnp.float32),
        jnp.zeros((heads_here, query_rows, HD), jnp.float32),
    )
    running, unused = lax.scan(
        attend_step_block,
        start_state,
        (kv_blocks, seg_blocks, jnp.arange(block_count, dtype=jnp.int32)),
    )
    return running


def attention_grads(queries, kv_all, seg_all, q_pos, q_seg, grad_heads, delta_all, lse_all):
    key_count = kv_all.shape[0]
    width = kv_all.shape[1] // 2
    heads_here = queries.shape[1]
    query_rows = queries.shape[0]
    block_rows = math.gcd(key_count, 512)
    block_count = key_count // block_rows
    kv_blocks = kv_all.reshape(block_count, block_rows, 2 * width)
    seg_blocks = seg_all.reshape(block_count, block_rows)
    score_scale = 1.0 / math.sqrt(HD)

    def attention_step_block(query_grad, block_items):
        kv_rows, seg_rows, block_index = block_items
        key_rows = kv_rows[:, :width].reshape(block_rows, heads_here, HD)
        value_rows = kv_rows[:, width:].reshape(block_rows, heads_here, HD)
        k_pos = block_index * block_rows + jnp.arange(block_rows, dtype=jnp.int32)
        allowed = block_mask(q_pos, q_seg, k_pos, seg_rows)
        scores = (
            jnp.einsum("qhd,khd->hqk", queries, key_rows, preferred_element_type=jnp.float32)
            * score_scale
        )
        scores = jnp.where(allowed[None], scores, big_negative)
        probabilities = jnp.where(allowed[None], jnp.exp(scores - lse_all[..., None]), 0.0)
        value_grad = jnp.einsum(
            "hqk,qhd->khd",
            probabilities.astype(jnp.bfloat16),
            grad_heads,
            preferred_element_type=jnp.float32,
        )
        prob_grad = jnp.einsum(
            "qhd,khd->hqk", grad_heads, value_rows, preferred_element_type=jnp.float32
        )
        score_grad = (probabilities * (prob_grad - delta_all[..., None]) * score_scale).astype(
            jnp.bfloat16
        )
        query_grad = query_grad + jnp.einsum(
            "hqk,khd->hqd", score_grad, key_rows, preferred_element_type=jnp.float32
        )
        key_grad = jnp.einsum(
            "hqk,qhd->khd", score_grad, queries, preferred_element_type=jnp.float32
        )
        return (
            query_grad,
            jnp.concatenate(
                [key_grad.reshape(block_rows, width), value_grad.reshape(block_rows, width)], axis=1
            ),
        )

    query_grad, kv_grad_blocks = lax.scan(
        attention_step_block,
        jnp.zeros((heads_here, query_rows, HD), jnp.float32),
        (kv_blocks, seg_blocks, jnp.arange(block_count, dtype=jnp.int32)),
    )
    return (query_grad, kv_grad_blocks.reshape(key_count, 2 * width))


def gather_vectors(own_qkvb, own_upb, own_vec):
    return (
        lax.all_gather(own_qkvb, ("rep", "shard"), axis=0, tiled=True),
        lax.all_gather(own_upb, ("rep", "shard"), axis=0, tiled=True),
        lax.all_gather(own_vec, ("rep", "shard"), axis=0, tiled=True),
    )


def sum_vectors(qkvb_grad, upb_grad, vec_grad):
    return (
        lax.psum_scatter(qkvb_grad, ("rep", "shard"), scatter_dimension=0, tiled=True),
        lax.psum_scatter(upb_grad, ("rep", "shard"), scatter_dimension=0, tiled=True),
        lax.psum_scatter(vec_grad, ("rep", "shard"), scatter_dimension=0, tiled=True),
    )


def sum_positions(partial_rows):
    return lax.psum_scatter(partial_rows, "shard", scatter_dimension=0, tiled=True)


def attention_pass(norm_rows, qkv_w, qkv_b, positions, key_width):
    row_count = norm_rows.shape[0]
    heads_here = key_width // HD
    joined = jnp.dot(norm_rows, qkv_w, preferred_element_type=jnp.float32) + qkv_b
    q_pre = joined[:, :key_width].reshape(row_count, heads_here, HD)
    k_pre = joined[:, key_width : 2 * key_width].reshape(row_count, heads_here, HD)
    queries = rotary(q_pre, positions).astype(jnp.bfloat16)
    key_local = rotary(k_pre, positions).astype(jnp.bfloat16).reshape(row_count, key_width)
    value_local = joined[:, 2 * key_width :].astype(jnp.bfloat16)
    kv_local = jnp.concatenate([key_local, value_local], axis=1)
    return (q_pre, k_pre, queries, kv_local)


def finish_qkv_grad(q_pre, k_pre, positions, query_grad, kv_grad, key_width):
    row_count = q_pre.shape[0]
    heads_here = key_width // HD
    rotate_back = partial(rotary, positions=positions)
    query_pre = jax.vjp(rotate_back, q_pre)[1](query_grad.transpose(1, 0, 2))[0]
    key_pre = jax.vjp(rotate_back, k_pre)[1](
        kv_grad[:, :key_width].reshape(row_count, heads_here, HD)
    )[0]
    return jnp.concatenate(
        [
            query_pre.reshape(row_count, key_width),
            key_pre.reshape(row_count, key_width),
            kv_grad[:, key_width:],
        ],
        axis=1,
    )


def sliced_pass(norm_bf, q_seg, cotangent, own_mats, qkv_bb, up_bb):
    own_qkv, own_dense, own_up, own_down = own_mats
    inner_count = lax.axis_size("shard")
    outer_count = lax.axis_size("rep")
    stride = outer_count // inner_count
    place = lax.axis_index("shard")
    head_width = D // inner_count
    unit_width = FF // inner_count
    qkv_rows = own_qkv.shape[0]
    dense_rows = own_dense.shape[0]
    down_rows = own_down.shape[0]
    qkv_split = own_qkv.reshape(qkv_rows, 3, inner_count, head_width)
    up_split = own_up.reshape(qkv_rows, 1, inner_count, unit_width)
    qkv_cols, up_cols = (
        lax.all_to_all(qkv_split, "shard", split_axis=2, concat_axis=0, tiled=True),
        lax.all_to_all(up_split, "shard", split_axis=2, concat_axis=0, tiled=True),
    )
    qkv_rep, up_rep, dense_rep, down_rep = (
        lax.all_gather(qkv_cols, "rep", axis=0, tiled=True),
        lax.all_gather(up_cols, "rep", axis=0, tiled=True),
        lax.all_gather(own_dense[None], "rep", axis=0, tiled=True),
        lax.all_gather(own_down[None], "rep", axis=0, tiled=True),
    )
    dense_grid = dense_rep.reshape(inner_count, stride, 1, dense_rows, D)
    down_grid = down_rep.reshape(inner_count, stride, 1, down_rows, D)
    dense_moved, down_moved = (
        lax.all_to_all(dense_grid, "shard", split_axis=0, concat_axis=2, tiled=True),
        lax.all_to_all(down_grid, "shard", split_axis=0, concat_axis=2, tiled=True),
    )
    qkv_w = qkv_rep.reshape(D, 3 * head_width)
    up_w = up_rep.reshape(D, unit_width)
    dense_w = dense_moved.reshape(head_width, D)
    down_w = down_moved.reshape(unit_width, D)
    qkv_b = lax.dynamic_index_in_dim(
        qkv_bb.astype(jnp.float32).reshape(3, inner_count, head_width), place, 1, False
    ).reshape(3 * head_width)
    up_b = lax.dynamic_slice_in_dim(up_bb.astype(jnp.float32), place * unit_width, unit_width, 0)
    norm_seq, grad_seq, seg_seq = (
        lax.all_gather(norm_bf, "shard", axis=0, tiled=True),
        lax.all_gather(cotangent, "shard", axis=0, tiled=True),
        lax.all_gather(q_seg, "shard", axis=0, tiled=True),
    )
    seq_rows = norm_seq.shape[0]
    heads_here = head_width // HD
    positions = jnp.arange(seq_rows, dtype=jnp.int32)
    q_pre, k_pre, queries, kv_seq = attention_pass(norm_seq, qkv_w, qkv_b, positions, head_width)
    row_max, totals, accumulated = attend_keys(kv_seq, seg_seq, queries, positions, seg_seq)
    lse_all = row_max + jnp.log(totals)
    out_heads = (accumulated / totals[..., None]).transpose(1, 0, 2).astype(jnp.bfloat16)
    attn_bf = out_heads.reshape(seq_rows, head_width)
    pre_act = jnp.dot(norm_seq, up_w, preferred_element_type=jnp.float32) + up_b
    hidden = gelu_tanh(pre_act).astype(jnp.bfloat16)
    partial_out = jnp.dot(attn_bf, dense_w, preferred_element_type=jnp.float32) + jnp.dot(
        hidden, down_w, preferred_element_type=jnp.float32
    )
    mixed = sum_positions(partial_out)
    grad_down = jnp.dot(hidden.T, grad_seq, preferred_element_type=jnp.float32)
    grad_dense = jnp.dot(attn_bf.T, grad_seq, preferred_element_type=jnp.float32)
    grad_hidden = jnp.dot(grad_seq, down_w.T, preferred_element_type=jnp.float32)
    grad_pre = jax.vjp(gelu_tanh, pre_act)[1](grad_hidden)[0]
    grad_pre_bf = grad_pre.astype(jnp.bfloat16)
    grad_up = jnp.dot(norm_seq.T, grad_pre_bf, preferred_element_type=jnp.float32)
    upb_part = jnp.sum(grad_pre, axis=0)
    norm_part = jnp.dot(grad_pre_bf, up_w.T, preferred_element_type=jnp.float32)
    grad_heads = (
        jnp.dot(grad_seq, dense_w.T, preferred_element_type=jnp.float32)
        .astype(jnp.bfloat16)
        .reshape(seq_rows, heads_here, HD)
    )
    delta_all = jnp.sum(grad_heads.astype(jnp.float32) * out_heads.astype(jnp.float32), axis=-1).T
    query_grad, kv_grad = attention_grads(
        queries, kv_seq, seg_seq, positions, seg_seq, grad_heads, delta_all, lse_all
    )
    grad_joined = finish_qkv_grad(q_pre, k_pre, positions, query_grad, kv_grad, head_width)
    grad_joined_bf = grad_joined.astype(jnp.bfloat16)
    grad_qkv = jnp.dot(norm_seq.T, grad_joined_bf, preferred_element_type=jnp.float32)
    qkvb_part = jnp.sum(grad_joined, axis=0)
    norm_part = norm_part + jnp.dot(grad_joined_bf, qkv_w.T, preferred_element_type=jnp.float32)
    grad_norm = sum_positions(norm_part)
    dense_grid_grad = grad_dense.reshape(1, stride, inner_count, dense_rows, D)
    down_grid_grad = grad_down.reshape(1, stride, inner_count, down_rows, D)
    dense_back, down_back = (
        lax.all_to_all(dense_grid_grad, "shard", split_axis=2, concat_axis=0, tiled=True),
        lax.all_to_all(down_grid_grad, "shard", split_axis=2, concat_axis=0, tiled=True),
    )
    qkv_sum, up_sum, dense_sum, down_sum = (
        lax.psum_scatter(
            grad_qkv.reshape(D, 3, 1, head_width), "rep", scatter_dimension=0, tiled=True
        ),
        lax.psum_scatter(
            grad_up.reshape(D, 1, 1, unit_width), "rep", scatter_dimension=0, tiled=True
        ),
        lax.psum_scatter(
            dense_back.reshape(outer_count, dense_rows, D), "rep", scatter_dimension=0, tiled=True
        ),
        lax.psum_scatter(
            down_back.reshape(outer_count, down_rows, D), "rep", scatter_dimension=0, tiled=True
        ),
    )
    qkv_home, up_home = (
        lax.all_to_all(qkv_sum, "shard", split_axis=0, concat_axis=2, tiled=True),
        lax.all_to_all(up_sum, "shard", split_axis=0, concat_axis=2, tiled=True),
    )
    qkv_own = qkv_home.reshape(qkv_rows, 3 * D)
    up_own = up_home.reshape(qkv_rows, FF)
    dense_own = dense_sum.reshape(dense_rows, D)
    down_own = down_sum.reshape(down_rows, D)
    selector = (jnp.arange(inner_count, dtype=jnp.int32) == place).astype(jnp.float32)
    qkvb_grad = (selector[None, :, None] * qkvb_part.reshape(3, 1, head_width)).reshape(3 * D)
    upb_grad = (selector[:, None] * upb_part[None, :]).reshape(FF)
    return (mixed, grad_norm, (qkv_own, dense_own, up_own, down_own), qkvb_grad, upb_grad)


def body(
    hidden_in,
    segment_ids,
    out_grad,
    qkv_weight_state,
    qkv_bias_state,
    dense_weight_state,
    up_weight_state,
    up_bias_state,
    down_weight_state,
    vector_state,
):
    own_mats = (
        qkv_weight_state[0].astype(jnp.bfloat16),
        dense_weight_state[0].astype(jnp.bfloat16),
        up_weight_state[0].astype(jnp.bfloat16),
        down_weight_state[0].astype(jnp.bfloat16),
    )
    qkv_bb, up_bb, vec_bf = gather_vectors(
        qkv_bias_state[0].astype(jnp.bfloat16),
        up_bias_state[0].astype(jnp.bfloat16),
        vector_state[0].astype(jnp.bfloat16),
    )
    vec_all = vec_bf.astype(jnp.float32)
    norm_gain = vec_all[:, 0]
    norm_shift = vec_all[:, 1]
    dense_bias = vec_all[:, 2]
    down_bias = vec_all[:, 3]
    tokens = hidden_in[0]
    q_seg = segment_ids[0]
    cotangent = out_grad[0]
    x_full = tokens.astype(jnp.float32)
    normed = layer_norm(x_full, norm_gain, norm_shift)
    norm_bf = normed.astype(jnp.bfloat16)
    mixed, grad_norm, owned, qkvb_grad, upb_grad = sliced_pass(
        norm_bf, q_seg, cotangent, own_mats, qkv_bb, up_bb
    )
    qkv_own, dense_own, up_own, down_own = owned
    output = (x_full + (mixed + dense_bias + down_bias)).astype(jnp.bfloat16)
    grad_x, grad_gain, grad_shift = jax.vjp(layer_norm, x_full, norm_gain, norm_shift)[1](grad_norm)
    out_bias_grad = jnp.sum(cotangent.astype(jnp.float32), axis=0)
    grad_vec = jnp.stack([grad_gain, grad_shift, out_bias_grad, out_bias_grad], axis=1)
    input_grad = cotangent.astype(jnp.float32) + grad_x
    qkvb_own, upb_own, vec_own = sum_vectors(qkvb_grad, upb_grad, grad_vec)
    new_states = (
        adam_update(qkv_weight_state, qkv_own),
        adam_update(qkv_bias_state, qkvb_own),
        adam_update(dense_weight_state, dense_own),
        adam_update(up_weight_state, up_own),
        adam_update(up_bias_state, upb_own),
        adam_update(down_weight_state, down_own),
        adam_update(vector_state, vec_own),
    )
    return (
        output[None],
        input_grad[None],
        qkv_own,
        qkvb_own,
        dense_own,
        up_own,
        upb_own,
        down_own,
        vec_own,
        owner_entries(new_states, 0),
        owner_entries(new_states, 1),
        owner_entries(new_states, 2),
    )


def whole_heads(mesh):
    owners = mesh.shape["rep"] * mesh.shape["shard"]
    return D % owners == 0 and D // owners == HD and mesh.shape["rep"] % 2 == 0


def rotation_tables(seq_rows):
    half_rot = ROT // 2
    lane = jnp.arange(2 * HD, dtype=jnp.int32) % HD
    frequency = jnp.exp((lane % half_rot).astype(jnp.float32) * (-2.0 * math.log(10000.0) / ROT))
    angles = jnp.arange(seq_rows, dtype=jnp.int32).astype(jnp.float32)[:, None] * frequency[None, :]
    sine = jnp.sin(angles)
    cosine = jnp.where(lane[None, :] < ROT, jnp.cos(angles), 1.0)
    low = jnp.where(lane[None, :] < half_rot, -sine, 0.0)
    high = jnp.where((lane[None, :] >= half_rot) & (lane[None, :] < ROT), sine, 0.0)
    return cosine, low, high


def attention_kernel(
    fu_ref, do_ref, du_ref, seg_col_ref, seg_row_ref, cos_ref, low_ref, high_ref, o_ref, dcat_ref, sums_ref
):
    rows, width = do_ref.shape
    scale = 1.0 / math.sqrt(HD)
    row_id = lax.broadcasted_iota(jnp.int32, (rows, rows), 0)
    col_id = lax.broadcasted_iota(jnp.int32, (rows, rows), 1)
    allowed = (col_id <= row_id) & (seg_col_ref[...] == seg_row_ref[0])
    cosine, low, high = cos_ref[...], low_ref[...], high_ref[...]
    half = ROT // 2
    lane = lax.broadcasted_iota(jnp.int32, (rows, 2 * HD), 1)

    def rotate(u):
        return (
            u * cosine
            + pltpu.roll(u, 2 * HD - half, 1) * low
            + pltpu.roll(u, half, 1) * high
        )

    def rotate_back(u):
        return (
            u * cosine
            - pltpu.roll(u, 2 * HD - half, 1) * low
            - pltpu.roll(u, half, 1) * high
        )

    def dot(a, b, a_dim, b_dim):
        return lax.dot_general(a, b, (((a_dim,), (b_dim,)), ((), ())), preferred_element_type=jnp.float32)

    zero = jnp.zeros((), jnp.bfloat16)
    for pair in range(width // (2 * HD)):
        lanes = pl.ds(pair * 2 * HD, 2 * HD)
        k_lanes = pl.ds(width + pair * 2 * HD, 2 * HD)
        v_lanes = pl.ds(2 * width + pair * 2 * HD, 2 * HD)
        q = rotate(fu_ref[:, lanes]).astype(jnp.bfloat16)
        k = rotate(fu_ref[:, k_lanes]).astype(jnp.bfloat16)
        v = fu_ref[:, v_lanes].astype(jnp.bfloat16)
        do = do_ref[:, lanes]
        o = dq = dk = dv = None
        for head in range(2):
            mine = (lane < HD) if head == 0 else (lane >= HD)
            qh = jnp.where(mine, q, zero)
            kh = jnp.where(mine, k, zero)
            vh = jnp.where(mine, v, zero)
            doh = jnp.where(mine, do, zero)
            scores = jnp.where(allowed, dot(qh, k, 1, 1) * scale, big_negative)
            row_max = jnp.max(scores, axis=1, keepdims=True)
            probs = jnp.where(allowed, jnp.exp(scores - row_max), 0.0)
            inverse = 1.0 / jnp.sum(probs, axis=1, keepdims=True)
            oh = dot(probs.astype(jnp.bfloat16), vh, 1, 0) * inverse
            delta = jnp.sum(
                doh.astype(jnp.float32) * oh.astype(jnp.bfloat16).astype(jnp.float32), axis=1, keepdims=True
            )
            probs = probs * inverse
            dvh = dot(probs.astype(jnp.bfloat16), doh, 0, 0)
            ds = (probs * (dot(doh, v, 1, 1) - delta) * scale).astype(jnp.bfloat16)
            dqh = dot(ds, kh, 1, 0)
            dkh = dot(ds, qh, 0, 0)
            if head == 0:
                o, dq, dk, dv = oh, dqh, dkh, dvh
            else:
                o, dq, dk, dv = o + oh, dq + dqh, dk + dkh, dv + dvh
        o_ref[:, lanes] = o.astype(jnp.bfloat16)
        dq = rotate_back(dq)
        dk = rotate_back(dk)
        for part, place in ((dq, lanes), (dk, k_lanes), (dv, v_lanes)):
            dcat_ref[:, place] = part.astype(jnp.bfloat16)
            sums_ref[0, :, place] = jnp.sum(part, axis=0, keepdims=True)
    dcat_ref[:, pl.ds(3 * width, du_ref.shape[1])] = du_ref[...]


def attention(fu, do, du, segments):
    count, rows = segments.shape
    width = do.shape[1]
    units = du.shape[1]
    tables = rotation_tables(rows)
    table_spec = pl.BlockSpec((rows, 2 * HD), lambda s: (0, 0))
    o, dcat, sums = pl.pallas_call(
        attention_kernel,
        grid=(count,),
        in_specs=[
            pl.BlockSpec((rows, 3 * width), lambda s: (s, 0)),
            pl.BlockSpec((rows, width), lambda s: (s, 0)),
            pl.BlockSpec((rows, units), lambda s: (s, 0)),
            pl.BlockSpec((rows, 1), lambda s: (s, 0)),
            pl.BlockSpec((1, 1, rows), lambda s: (s, 0, 0)),
            table_spec,
            table_spec,
            table_spec,
        ],
        out_specs=[
            pl.BlockSpec((rows, width), lambda s: (s, 0)),
            pl.BlockSpec((rows, 3 * width + units), lambda s: (s, 0)),
            pl.BlockSpec((1, 1, 3 * width), lambda s: (s, 0, 0)),
        ],
        out_shape=[
            jax.ShapeDtypeStruct((count * rows, width), jnp.bfloat16),
            jax.ShapeDtypeStruct((count * rows, 3 * width + units), jnp.bfloat16),
            jax.ShapeDtypeStruct((count, 1, 3 * width), jnp.float32),
        ],
        compiler_params=pltpu.CompilerParams(vmem_limit_bytes=56 << 20),
        cost_estimate=pl.CostEstimate(
            flops=count * (width // HD) * 10 * rows * rows * HD,
            bytes_accessed=count * rows * (width * 20 + units * 4),
            transcendentals=count * (width // HD) * rows * rows,
        ),
    )(fu, do, du, segments.reshape(count * rows, 1), segments.reshape(count, 1, rows), *tables)
    return o, dcat, jnp.sum(sums, axis=(0, 1))


def adam_values(weight, moment_one, moment_two, grad):
    first = beta_one * moment_one + (1.0 - beta_one) * grad
    second = beta_two * moment_two + (1.0 - beta_two) * grad * grad
    corrected = first * (1.0 / (1.0 - beta_one**STEP))
    divisor = jnp.sqrt(second * (1.0 / (1.0 - beta_two**STEP))) + adam_eps
    return weight - learn_rate * (corrected / divisor + weight_decay * weight), first, second


def owner_update_kernel(plan, small_plan, groups, *refs):
    planes, cores, shards = groups
    qkv_state, dense_state, up_state, down_state, cat_ref, dense_grad, down_grad, small_ref = refs[:8]
    outs = refs[8:11]
    qkv_out, up_out, cat_buf = refs[11:]
    step = pl.program_id(0)
    lane = lax.broadcasted_iota(jnp.int32, (8, 128), 1)
    sub = lax.broadcasted_iota(jnp.int32, (8, 128), 0)
    lane_row = lax.broadcasted_iota(jnp.int32, (1, 128), 1)
    wide = 1024

    @pl.when(step == 0)
    def small():
        for source, row, low, high in small_plan:
            for entry in range(3):
                old = outs[entry][pl.ds(row, 1), :]
                new = small_ref[entry, pl.ds(source, 1), :]
                outs[entry][pl.ds(row, 1), :] = jnp.where((lane_row >= low) & (lane_row < high), new, old)

    def widen(piece, carry):
        cat_buf[piece] = cat_ref[piece].astype(jnp.float32)
        return carry

    lax.fori_loop(0, cat_ref.shape[0], widen, 0)

    def place_rows(state, grad_of, rows, tiles, start, shifted, keep=None):
        chunk = min(wide, tiles * 128)

        def one_group(group, carry):
            place = pl.ds(pl.multiple_of(group * 8, 8), 8)
            base = start + (step * (rows // 8) + group) * (8 * tiles)

            def values(column, size):
                lanes = pl.ds(column, size)
                grad = grad_of(place, column, size)
                if keep is not None and size > 128:
                    keep[place, lanes] = grad
                return adam_values(
                    state[0, place, lanes], state[1, place, lanes], state[2, place, lanes], grad
                )

            if shifted:
                last = tuple(pltpu.roll(value, 64, 1) for value in values((tiles - 1) * 128, 128))
                before = tuple(
                    jnp.where(sub == 0, out[pl.ds(base, 1), :], pltpu.roll(value, 1, 0))
                    for out, value in zip(outs, last)
                )
            for column in range(0, tiles * 128, chunk):
                done = values(column, chunk)
                for entry, out in enumerate(outs):
                    for tile in range(chunk // 128):
                        value = done[entry][:, tile * 128 : (tile + 1) * 128]
                        if shifted:
                            value = pltpu.roll(value, 64, 1)
                            old = before[entry] if tile == 0 else now
                            now = value
                            value = jnp.where(lane < 64, old, value)
                        out[pl.ds(base + column // 128 + tile, 8, stride=tiles), :] = value
                    if shifted:
                        before = before[:entry] + (now,) + before[entry + 1 :]
            if shifted:
                for out, value in zip(outs, before):
                    row = pl.ds(base + 8 * tiles, 1)
                    out[row, :] = jnp.where(lane_row < 64, value[7:8], out[row, :])
            return carry

        lax.fori_loop(0, rows // 8, one_group, 0)

    def qkv_grad(place, column, size):
        tiles = []
        for start in range(column, column + size, 128):
            part, head = divmod(start // HD, planes * cores * shards)
            halves = []
            for side in range(2):
                plane, member = divmod(head + side, cores * shards)
                spot = (part * planes + plane) * HD
                half = cat_buf[member, place, pl.ds(spot // 128 * 128, 128)]
                halves.append(half if spot % 128 == side * HD else pltpu.roll(half, HD, 1))
            tiles.append(jnp.where(lane < HD, halves[0], halves[1]))
        return tiles[0] if len(tiles) == 1 else jnp.concatenate(tiles, axis=1)

    units = up_state.shape[2] // (planes * cores * shards)

    def up_grad(place, column, size):
        parts = []
        for start in range(column, column + size, min(units, size)):
            plane, member = divmod(start // units, cores * shards)
            spot = 3 * planes * HD + plane * units + start % units
            parts.append(cat_buf[member, place, pl.ds(spot, min(units, size))])
        return parts[0] if len(parts) == 1 else jnp.concatenate(parts, axis=1)

    def plain(grad):
        return lambda place, column, size: grad[place, pl.ds(column, size)]

    place_rows(qkv_state, qkv_grad, *plan[0], keep=qkv_out)
    place_rows(dense_state, plain(dense_grad), *plan[1])
    place_rows(up_state, up_grad, *plan[2], keep=up_out)
    place_rows(down_state, plain(down_grad), *plan[3])


def owner_update(states, cat_sum, grads, small_states, small_grads, groups):
    steps = 4
    sizes = [state.shape[1] * state.shape[2] for state in states]
    small_sizes = [grad.size for grad in small_grads]
    order = [("m", 0), ("s", 0), ("m", 1), ("m", 2), ("s", 1), ("m", 3), ("s", 2)]
    offset = 0
    plan = [None] * 4
    small_plan = []
    pads = []
    small_row = 0
    for kind, index in order:
        if kind == "m":
            state = states[index]
            rows = state.shape[1] // steps
            plan[index] = (rows, state.shape[2] // 128, offset // 128, offset % 128 == 64)
            offset += sizes[index]
        else:
            size = small_sizes[index]
            front = offset % 128
            total = -(-(front + size) // 128)
            pads.append((front, total * 128 - front - size))
            for extra in range(total):
                low = front if extra == 0 else 0
                high = min(128, front + size - extra * 128)
                small_plan.append((small_row + extra, offset // 128 + extra, low, high))
            small_row += total
            offset += size
    entries = offset
    out_rows = -(-entries // 1024) * 8
    small_new = [
        adam_values(state[0].reshape(-1), state[1].reshape(-1), state[2].reshape(-1), grad.reshape(-1))
        for state, grad in zip(small_states, small_grads)
    ]
    small = jnp.stack(
        [
            jnp.concatenate([jnp.pad(new[entry], pad) for new, pad in zip(small_new, pads)])
            for entry in range(3)
        ]
    ).reshape(3, small_row, 128)
    in_specs = [
        pl.BlockSpec((3, rows, tiles * 128), lambda s: (0, s, 0)) for rows, tiles, start, shifted in plan
    ]
    qkv_rows, up_rows = plan[0][0], plan[2][0]
    in_specs.append(pl.BlockSpec((cat_sum.shape[0], qkv_rows, cat_sum.shape[2]), lambda s: (0, s, 0)))
    in_specs.append(pl.BlockSpec((plan[1][0], plan[1][1] * 128), lambda s: (s, 0)))
    in_specs.append(pl.BlockSpec((plan[3][0], plan[3][1] * 128), lambda s: (s, 0)))
    in_specs.append(pl.BlockSpec((3, small_row, 128), lambda s: (0, 0, 0)))
    flat = [pl.BlockSpec((out_rows, 128), lambda s: (0, 0), pipeline_mode=pl.Buffered(1))] * 3
    *outs, qkv_grad, up_grad = pl.pallas_call(
        partial(owner_update_kernel, plan, small_plan, groups),
        grid=(steps,),
        in_specs=in_specs,
        out_specs=flat
        + [
            pl.BlockSpec((qkv_rows, plan[0][1] * 128), lambda s: (s, 0)),
            pl.BlockSpec((up_rows, plan[2][1] * 128), lambda s: (s, 0)),
        ],
        out_shape=[jax.ShapeDtypeStruct((out_rows, 128), jnp.float32)] * 3
        + [
            jax.ShapeDtypeStruct(states[0].shape[1:], jnp.float32),
            jax.ShapeDtypeStruct(states[2].shape[1:], jnp.float32),
        ],
        scratch_shapes=[pltpu.VMEM((cat_sum.shape[0], qkv_rows, cat_sum.shape[2]), jnp.float32)],
        compiler_params=pltpu.CompilerParams(vmem_limit_bytes=56 << 20),
        cost_estimate=pl.CostEstimate(
            flops=20 * entries, bytes_accessed=28 * entries, transcendentals=2 * entries
        ),
    )(*states, cat_sum, *grads, small)
    return tuple(out.reshape(1, 1, out_rows * 128)[:, :, :entries] for out in outs), qkv_grad, up_grad


class Wires:
    def __init__(self, send_sems):
        self.send_sems, self.count, self.pending = send_sems, 0, []
        self.plane, self.core, self.shard = (
            lax.axis_index("plane"),
            lax.axis_index("core"),
            lax.axis_index("shard"),
        )
        self.shards = lax.axis_size("shard")
        self.group = lax.axis_size("core") * self.shards
        self.mine = self.core * self.shards + self.shard
        self.first = (self.plane ^ 1, self.core, self.shard)
        self.second = (self.plane ^ 2, self.core, self.shard)

    def member(self, index):
        return (self.plane, index // self.shards, index % self.shards)

    def barrier(self):
        barrier = pltpu.get_barrier_semaphore()
        partners = [self.member(self.mine ^ mask) for mask in range(1, self.group)]
        partners += [self.first, self.second]
        for partner in partners:
            pl.semaphore_signal(barrier, inc=1, device_id=partner, device_id_type=pl.DeviceIdType.MESH)
        pl.semaphore_wait(barrier, len(partners))

    def send(self, source, target, recv_sem, device, when=None):
        copy = pltpu.make_async_remote_copy(
            src_ref=source,
            dst_ref=target,
            send_sem=self.send_sems.at[self.count],
            recv_sem=recv_sem,
            device_id=device,
            device_id_type=pl.DeviceIdType.MESH,
        )
        self.count += 1
        self.pending.append((copy, when))
        if when is None:
            copy.start()
        else:
            pl.when(when)(copy.start)

    def arrived(self, place, recv_sem, when=None):
        copy = pltpu.make_async_remote_copy(
            src_ref=place,
            dst_ref=place,
            send_sem=self.send_sems.at[0],
            recv_sem=recv_sem,
            device_id=self.first,
            device_id_type=pl.DeviceIdType.MESH,
        )
        if when is None:
            copy.wait_recv()
        else:
            pl.when(when)(copy.wait_recv)

    def drain(self):
        for copy, when in self.pending:
            if when is None:
                copy.wait_send()
            else:
                pl.when(when)(copy.wait_send)


def pack_pieces(qkv, up, pieces, planes, cores, shards):
    rows = qkv.shape[0]
    lane = lax.broadcasted_iota(jnp.int32, (rows, 128), 1)
    units = up.shape[1] // (planes * cores * shards)
    for core in range(cores):
        for shard in range(shards):
            piece = core * shards + shard
            for tile in range(3 * planes // 2):
                halves = []
                for side in range(2):
                    part, plane = divmod(2 * tile + side, planes)
                    head = (plane * cores + core) * shards + shard
                    start = part * planes * cores * shards * HD + head * HD
                    half = qkv[:, pl.ds(start // 128 * 128, 128)]
                    halves.append(half if start % 128 == side * HD else pltpu.roll(half, HD, 1))
                pieces[piece, :, pl.ds(tile * 128, 128)] = jnp.where(lane < HD, halves[0], halves[1]).astype(
                    jnp.bfloat16
                )
            for plane in range(planes):
                block = (plane * cores + core) * shards + shard
                pieces[piece, :, pl.ds(3 * planes * HD + plane * units, units)] = up[
                    :, pl.ds(block * units, units)
                ].astype(jnp.bfloat16)


def gather_kernel(
    qkv_state, up_state, dense_state, down_state, tokens, cotangent, vectors,
    cat_out, dense_out, down_out, x_out, dy_out, vec_out,
    qkv_buf, up_buf, dense_buf, down_buf, pieces, dense, down,
    load_sem, send_sems, group_sem, first_sem, second_sem, far_sem, up_sem, low_sem, core_sem, local_sem,
):
    net = Wires(send_sems)
    plane, core, shard, shards, group, mine = net.plane, net.core, net.shard, net.shards, net.group, net.mine
    order = sorted(range(group), key=lambda mask: (mask % shards, mask // shards))
    partner = (plane, 1 - core, shard)

    def cat_unit(mask):
        return lambda p: cat_out.at[p, mine ^ mask]

    def vec_unit(mask):
        return lambda p: vec_out.at[p, mine ^ mask]

    units = []
    down_rows = down.shape[0] // 4
    for part in range(4):
        rows = pl.ds(part * down_rows, down_rows)
        units.append((down.at[rows], lambda p, rows=rows: down_out.at[p, rows]))
    dense_rows = dense.shape[0] // 2
    for part in range(2):
        rows = pl.ds(part * dense_rows, dense_rows)
        units.append((dense.at[rows], lambda p, rows=rows: dense_out.at[p, rows]))
    own_units = list(range(len(units)))
    cat_units, vec_units = {}, {}
    for mask in order:
        cat_units[mask] = len(units)
        units.append((pieces.at[mine] if mask == 0 else None, cat_unit(mask)))
        vec_units[mask] = len(units)
        units.append((vectors if mask == 0 else None, vec_unit(mask)))

    def spread(index):
        source, place = units[index]
        source = place(plane) if source is None else source
        net.send(source, place(plane), first_sem.at[index], net.first)
        net.send(source, place(plane), second_sem.at[index], net.second)

    def hand_on(index):
        place = units[index][1]
        if relay_first[index]:
            net.arrived(place(plane ^ 1), first_sem.at[index])
            net.send(place(plane ^ 1), place(plane ^ 1), far_sem.at[index], net.second)
        else:
            net.arrived(place(plane ^ 2), second_sem.at[index])
            net.send(place(plane ^ 2), place(plane ^ 2), far_sem.at[index], net.first)

    relay_first = {}
    for position, index in enumerate(own_units):
        relay_first[index] = position % 2 == 0
    for position, mask in enumerate(order):
        relay_first[cat_units[mask]] = position % 2 == 0
        relay_first[vec_units[mask]] = position % 2 == 1

    loads = [
        pltpu.make_async_copy(state.at[0], buffer, load_sem.at[index])
        for index, (state, buffer) in enumerate(
            ((qkv_state, qkv_buf), (up_state, up_buf), (down_state, down_buf), (dense_state, dense_buf))
        )
    ]
    for load in loads:
        load.start()
    net.barrier()
    loads[0].wait()
    loads[1].wait()
    pack_pieces(qkv_buf, up_buf, pieces, cat_out.shape[0], group // shards, shards)

    locals_ = [
        (pieces.at[mine], cat_out.at[plane, mine]),
        (dense, dense_out.at[plane]),
        (down, down_out.at[plane]),
        (tokens, x_out.at[mine]),
        (cotangent, dy_out.at[mine]),
        (vectors, vec_out.at[plane, mine]),
    ]
    copies = [
        pltpu.make_async_copy(source, target, local_sem.at[index])
        for index, (source, target) in enumerate(locals_)
    ]
    for mask in order[1:]:
        target = net.member(mine ^ mask)
        net.send(vectors, vec_out.at[plane, mine], group_sem.at[1, mask], target)
        net.send(pieces.at[mine ^ mask], cat_out.at[plane, mine], group_sem.at[0, mask], target)
    loads[2].wait()
    down[...] = down_buf[...].astype(jnp.bfloat16)
    loads[3].wait()
    dense[...] = dense_buf[...].astype(jnp.bfloat16)
    for index in own_units:
        spread(index)
    spread(cat_units[0])
    spread(vec_units[0])
    streams = ((tokens, x_out), (cotangent, dy_out))

    def block(stream, origin):
        return streams[stream][1].at[core * shards + origin]

    def to_core(stream, source, origin, slot, when=None):
        net.send(source, block(stream, origin), core_sem.at[stream, slot], partner, when)

    def hop(stream, distance):
        own = distance == 1
        for upward, sem in ((True, up_sem), (False, low_sem)):
            origin = shard - (distance - 1) if upward else shard + (distance - 1)
            there = shard + 1 if upward else shard - 1
            held = (origin >= 0) if upward else (origin < shards)
            inside = (there < shards) if upward else (there >= 0)
            near = jnp.clip(origin, 0, shards - 1)
            source = streams[stream][0] if own else block(stream, near)
            net.send(
                source,
                block(stream, near),
                sem.at[stream, distance],
                (plane, core, jnp.clip(there, 0, shards - 1)),
                inside & held,
            )

    def hop_arrived(stream, distance):
        for upward, sem in ((True, up_sem), (False, low_sem)):
            origin = shard - distance if upward else shard + distance
            held = (origin >= 0) if upward else (origin < shards)
            near = jnp.clip(origin, 0, shards - 1)
            net.arrived(block(stream, near), sem.at[stream, distance], held)
            slot = distance if upward else shards + distance
            to_core(stream, block(stream, near), near, slot, held)

    for stream in range(2):
        hop(stream, 1)
    for stream in range(2):
        to_core(stream, streams[stream][0], shard, 0)
    for copy in copies:
        copy.start()

    for position, mask in enumerate(order[1:]):
        net.arrived(vec_out.at[plane, mine ^ mask], group_sem.at[1, mask])
        spread(vec_units[mask])
        net.arrived(cat_out.at[plane, mine ^ mask], group_sem.at[0, mask])
        spread(cat_units[mask])
        if position == 2:
            for index in own_units:
                hand_on(index)
    hand_on(cat_units[0])
    hand_on(vec_units[0])
    for distance in range(1, shards):
        for stream in range(2):
            hop_arrived(stream, distance)
            if distance + 1 < shards:
                hop(stream, distance + 1)
        for mask in order[1 + (distance - 1) * 3 : 1 + distance * 3]:
            hand_on(vec_units[mask])
            hand_on(cat_units[mask])

    for index, (source, place) in enumerate(units):
        if relay_first[index]:
            net.arrived(place(plane ^ 2), second_sem.at[index])
        else:
            net.arrived(place(plane ^ 1), first_sem.at[index])
        net.arrived(place(plane ^ 3), far_sem.at[index])
    for stream in range(2):
        other = streams[stream][1]
        for slot in range(2 * shards):
            if slot == shards:
                continue
            origin = shard - slot if slot < shards else shard + (slot - shards)
            held = None if slot == 0 else ((origin >= 0) & (origin < shards))
            near = jnp.clip(origin, 0, shards - 1)
            net.arrived(other.at[(1 - core) * shards + near], core_sem.at[stream, slot], held)
    for copy in copies:
        copy.wait()
    net.drain()


def gather_wires(qkv, up, dense, down, tokens, cotangent, vectors):
    group, shards = lax.axis_size("core") * lax.axis_size("shard"), lax.axis_size("shard")
    planes = lax.axis_size("plane")
    width = (qkv.shape[2] + up.shape[2]) // group
    units = 6 + 2 * group
    vmem = pl.BlockSpec(memory_space=pltpu.VMEM)
    hbm = pl.BlockSpec(memory_space=pl.ANY)

    def out(*shape, dtype=jnp.bfloat16):
        return jax.ShapeDtypeStruct(shape, dtype)

    dma = pltpu.SemaphoreType.DMA
    return pl.pallas_call(
        gather_kernel,
        in_specs=[hbm] * 4 + [vmem] * 3,
        out_specs=[hbm] * 6,
        out_shape=[
            out(planes, group, qkv.shape[1], width),
            out(planes, *dense.shape[1:]),
            out(planes, *down.shape[1:]),
            out(group, *tokens.shape),
            out(group, *cotangent.shape),
            out(planes, group, *vectors.shape, dtype=vectors.dtype),
        ],
        scratch_shapes=[
            pltpu.VMEM(qkv.shape[1:], qkv.dtype),
            pltpu.VMEM(up.shape[1:], up.dtype),
            pltpu.VMEM(dense.shape[1:], dense.dtype),
            pltpu.VMEM(down.shape[1:], down.dtype),
            pltpu.VMEM((group, qkv.shape[1], width), jnp.bfloat16),
            pltpu.VMEM(dense.shape[1:], jnp.bfloat16),
            pltpu.VMEM(down.shape[1:], jnp.bfloat16),
            dma((4,)),
            dma((2 * (group - 1) + 3 * units + 2 * 2 * (shards - 1) + 2 * (2 * shards - 1),)),
            dma((2, group)),
            dma((units,)),
            dma((units,)),
            dma((units,)),
            dma((2, shards)),
            dma((2, shards)),
            dma((2, 2 * shards)),
            dma((6,)),
        ],
        compiler_params=pltpu.CompilerParams(
            collective_id=0, has_side_effects=True, vmem_limit_bytes=24 << 20
        ),
    )(qkv, up, dense, down, tokens, cotangent, vectors)


def add_rows(target, *sources):
    step = 16
    rows = target.shape[0]

    def body(index, carry):
        place = pl.ds(pl.multiple_of(index * step, step), step)
        total = sources[0][place, :].astype(jnp.float32)
        for source in sources[1:]:
            total = total + source[place, :].astype(jnp.float32)
        target[place, :] = total.astype(target.dtype)
        return carry

    lax.fori_loop(0, rows // step, body, 0)


def reduce_kernel(
    cat, dense, down, out_part, norm_part, sums,
    cat_out, dense_out, down_out, mixed_out, norm_out, sums_out,
    cat_buf, down_buf, dense_buf, token_buf, sum_buf,
    send_sems, near_sem, pass_sem, group_sem, core_sem, line_sem, sum_sem, local_sem,
):
    PASS_IN, PASS_OWN, PASS_OUT, KEEP_IN, KEEP_OWN, LAST_IN = range(6)
    net = Wires(send_sems)
    plane, core, shard, shards, group, mine = net.plane, net.core, net.shard, net.shards, net.group, net.mine
    partner = (plane, 1 - core, shard)
    order = sorted(range(group), key=lambda mask: (mask % shards, mask // shards), reverse=True)

    units = []
    for mask in order:
        units.append((lambda p, mask=mask: cat.at[p, mine ^ mask], cat_buf, mask))
    down_rows = down.shape[1] // 4
    for part in range(4):
        rows = pl.ds(part * down_rows, down_rows)
        units.append((lambda p, rows=rows: down.at[p, rows], down_buf, part))
    dense_rows = dense.shape[1] // 2
    for part in range(2):
        rows = pl.ds(part * dense_rows, dense_rows)
        units.append((lambda p, rows=rows: dense.at[p, rows], dense_buf, part))

    def ways(index):
        if index % 2 == 0:
            return net.first, net.second, plane ^ 1, plane ^ 2
        return net.second, net.first, plane ^ 2, plane ^ 1

    loads = {}

    def load(key, source, target):
        loads[key] = pltpu.make_async_copy(source, target, local_sem.at[len(loads)])
        loads[key].start()

    streams = (out_part, norm_part)
    finals = (mixed_out, norm_out)
    TOKEN_IN, TOKEN_OWN, TOKEN_UP, TOKEN_LOW, TOKEN_SUM = range(5)

    for stream in range(2):
        for place in range(shards):
            load(
                ("token", stream, place),
                streams[stream].at[core * shards + place],
                token_buf.at[TOKEN_OWN, stream, place],
            )
    for index, (part, buffers, slot) in enumerate(units):
        near, far, near_plane, far_plane = ways(index)
        load(("pass", index), part(far_plane), buffers.at[PASS_OWN, slot])
    for index, (part, buffers, slot) in enumerate(units):
        load(("keep", index), part(plane), buffers.at[KEEP_OWN, slot])

    net.barrier()

    def start_unit(index):
        part, buffers, slot = units[index]
        near, far, near_plane, far_plane = ways(index)
        net.send(part(plane ^ 3), buffers.at[PASS_IN, slot], pass_sem.at[0, index], near)
        net.send(part(near_plane), buffers.at[KEEP_IN, slot], near_sem.at[index], near)

    net.send(sums, sum_buf.at[0], sum_sem.at[0], net.first)
    places = [place for rank in range(shards // 2) for place in (shards - 1 - rank, rank)]
    for place in places:
        for stream in range(2):
            net.send(
                streams[stream].at[(1 - core) * shards + place],
                token_buf.at[TOKEN_IN, stream, place],
                core_sem.at[stream, place],
                partner,
            )
    for index in range(group):
        start_unit(index)

    def chain(stream, hop, rank):
        for upward in (True, False):
            target = shards - 1 - rank if upward else rank
            here = hop if upward else shards - 1 - hop
            slot, sems = (TOKEN_UP, line_sem.at[0]) if upward else (TOKEN_LOW, line_sem.at[1])
            values = [token_buf.at[TOKEN_IN, stream, target], token_buf.at[TOKEN_OWN, stream, target]]
            came = token_buf.at[slot, stream, target]
            total = token_buf.at[TOKEN_SUM, stream, target]
            holds = shard == here
            if hop:
                net.arrived(came, sems.at[stream, target], holds)

            @pl.when(holds)
            def add(values=values, came=came, total=total):
                add_rows(total, *(values + ([came] if hop else [])))

            there = jnp.clip(shard + (1 if upward else -1), 0, shards - 1)
            net.send(total, came, sems.at[stream, target], (plane, core, there), holds)

    def final(stream):
        for place in range(shards):
            holds = shard == place
            values = [token_buf.at[TOKEN_IN, stream, place], token_buf.at[TOKEN_OWN, stream, place]]
            for slot, side, present in (
                (TOKEN_UP, line_sem.at[0], place > 0),
                (TOKEN_LOW, line_sem.at[1], place < shards - 1),
            ):
                if present:
                    values.append(token_buf.at[slot, stream, place])
                    net.arrived(token_buf.at[slot, stream, place], side.at[stream, place], holds)

            @pl.when(holds)
            def add(values=values):
                add_rows(finals[stream], *values)

    def pass_on(index):
        part, buffers, slot = units[index]
        near, far, near_plane, far_plane = ways(index)
        net.arrived(buffers.at[PASS_IN, slot], pass_sem.at[0, index])
        loads["pass", index].wait()
        add_rows(buffers.at[PASS_OUT, slot], buffers.at[PASS_IN, slot], buffers.at[PASS_OWN, slot])
        net.send(buffers.at[PASS_OUT, slot], buffers.at[LAST_IN, slot], pass_sem.at[1, index], far)

    def finish(index):
        part, buffers, slot = units[index]
        net.arrived(buffers.at[KEEP_IN, slot], near_sem.at[index])
        loads["keep", index].wait()
        net.arrived(buffers.at[LAST_IN, slot], pass_sem.at[1, index])
        values = (buffers.at[KEEP_IN, slot], buffers.at[KEEP_OWN, slot], buffers.at[LAST_IN, slot])
        if index < group:
            add_rows(buffers.at[KEEP_OWN, slot], *values)
            if slot:
                net.send(
                    buffers.at[KEEP_OWN, slot],
                    cat_out.at[mine],
                    group_sem.at[0, slot],
                    net.member(mine ^ slot),
                )
            else:
                load("own", buffers.at[KEEP_OWN, slot], cat_out.at[mine])
        elif index < group + 4:
            add_rows(down_out.at[pl.ds(slot * down_rows, down_rows)], *values)
        else:
            add_rows(dense_out.at[pl.ds(slot * dense_rows, dense_rows)], *values)

    for place in places:
        for stream in range(2):
            net.arrived(token_buf.at[TOKEN_IN, stream, place], core_sem.at[stream, place])
            loads["token", stream, place].wait()
    for rank in range(shards - 1):
        for stream in range(2):
            chain(stream, 0, rank)
    net.arrived(sum_buf.at[0], sum_sem.at[0])
    sum_buf[1] = sums[...] + sum_buf[0]
    net.send(sum_buf.at[1], sum_buf.at[2], sum_sem.at[1], net.second)
    later = [
        (stream, hop, rank)
        for hop, rank in sorted(
            ((hop, rank) for hop in range(1, shards - 1) for rank in range(shards - 1 - hop)),
            key=lambda pair: (pair[0] + 2 * pair[1], pair[0]),
        )
        for stream in range(2)
    ]
    cats, every = range(group), range(len(units))
    for index in cats:
        if index == group - 2:
            for other in every[group:]:
                start_unit(other)
        pass_on(index)
        if index % 2 and later:
            chain(*later.pop(0))
            if later and index > 1:
                chain(*later.pop(0))
    net.arrived(sum_buf.at[2], sum_sem.at[1])
    sum_buf[3] = sum_buf[1] + sum_buf[2]
    for mask in range(1, group):
        net.send(sum_buf.at[3], sums_out.at[mine], group_sem.at[1, mask], net.member(mine ^ mask))
    load("sums", sum_buf.at[3], sums_out.at[mine])
    for index in cats[: group - 2]:
        finish(index)
        if later:
            chain(*later.pop(0))
    for index in every[group:]:
        pass_on(index)
    for index in cats[group - 2 :]:
        finish(index)
    for stream in range(2):
        final(stream)
    for index in every[group:]:
        finish(index)
    for mask in range(1, group):
        net.arrived(cat_out.at[mine ^ mask], group_sem.at[0, mask])
        net.arrived(sums_out.at[mine ^ mask], group_sem.at[1, mask])
    loads["own"].wait()
    loads["sums"].wait()
    net.drain()


def reduce_wires(cat, dense, down, out_part, norm_part, sums):
    shards = lax.axis_size("shard")
    group = lax.axis_size("core") * shards
    units = group + 6
    vmem = pl.BlockSpec(memory_space=pltpu.VMEM)
    hbm = pl.BlockSpec(memory_space=pl.ANY)
    dma = pltpu.SemaphoreType.DMA
    tokens = out_part.shape[1:]
    return pl.pallas_call(
        reduce_kernel,
        in_specs=[hbm] * 5 + [vmem],
        out_specs=[hbm] + [vmem] * 4 + [hbm],
        out_shape=[
            jax.ShapeDtypeStruct(cat.shape[1:], cat.dtype),
            jax.ShapeDtypeStruct(dense.shape[1:], jnp.float32),
            jax.ShapeDtypeStruct(down.shape[1:], jnp.float32),
            jax.ShapeDtypeStruct(tokens, jnp.float32),
            jax.ShapeDtypeStruct(tokens, jnp.float32),
            jax.ShapeDtypeStruct((group,) + sums.shape, sums.dtype),
        ],
        scratch_shapes=[
            pltpu.VMEM((6, group) + cat.shape[2:], cat.dtype),
            pltpu.VMEM((6, 4, down.shape[1] // 4, down.shape[2]), down.dtype),
            pltpu.VMEM((6, 2, dense.shape[1] // 2, dense.shape[2]), dense.dtype),
            pltpu.VMEM((5, 2, shards) + tokens, out_part.dtype),
            pltpu.VMEM((4,) + sums.shape, sums.dtype),
            dma((2 + 2 * shards + 2 * shards * (shards - 1) + 3 * units + 2 * (group - 1),)),
            dma((units,)),
            dma((2, units)),
            dma((2, group)),
            dma((2, shards)),
            dma((2, 2, shards)),
            dma((2,)),
            dma((2 * units + 2 * shards + 2,)),
        ],
        compiler_params=pltpu.CompilerParams(
            collective_id=1, has_side_effects=True, vmem_limit_bytes=58 << 20
        ),
    )(cat, dense, down, out_part, norm_part, sums)


def fast_body(
    hidden_in,
    segment_ids,
    out_grad,
    qkv_weight_state,
    qkv_bias_state,
    dense_weight_state,
    up_weight_state,
    up_bias_state,
    down_weight_state,
    vector_state,
):
    planes, cores, shards = lax.axis_size("plane"), lax.axis_size("core"), lax.axis_size("shard")
    plane, core, shard = lax.axis_index("plane"), lax.axis_index("core"), lax.axis_index("shard")
    group = cores * shards
    owner = (plane * cores + core) * shards + shard
    owners = planes * group
    model_rows = qkv_weight_state.shape[1]
    unit_rows = down_weight_state.shape[1]
    tokens_here = hidden_in.shape[1]
    head_width = planes * HD
    unit_width = planes * unit_rows
    qkv_count, upb_count = qkv_bias_state.shape[1], up_bias_state.shape[1]

    tokens, cotangent, q_seg = hidden_in[0], out_grad[0], segment_ids[0]
    vec_list = [
        qkv_bias_state[0],
        up_bias_state[0],
        vector_state[0].T.reshape(-1),
        q_seg.astype(jnp.float32),
    ]
    vec_sizes = [value.size for value in vec_list]
    vec_rows = -(-sum(vec_sizes) // 1024) * 8
    vec_own = jnp.pad(jnp.concatenate(vec_list), (0, vec_rows * 128 - sum(vec_sizes))).reshape(vec_rows, 128)

    cat_w, dense_w, down_w, x_all, dy_all, vec_all = gather_wires(
        qkv_weight_state,
        up_weight_state,
        dense_weight_state,
        down_weight_state,
        tokens,
        cotangent,
        vec_own,
    )

    cat_w = cat_w.reshape(D, 3 * head_width + unit_width)
    dense_w = dense_w.reshape(head_width, D)
    down_w = down_w.reshape(unit_width, D)
    rows = group * tokens_here
    x_all = x_all.reshape(rows, D)
    dy_all = dy_all.reshape(rows, D)
    vec_flat = vec_all.reshape(planes, cores, shards, vec_rows * 128)
    at = [0]
    for size in vec_sizes:
        at.append(at[-1] + size)

    def rounded(value):
        return value.astype(jnp.bfloat16).astype(jnp.float32)

    qkv_bias = rounded(vec_flat[..., at[0] : at[1]]).reshape(3, planes, cores, shards, HD)
    qkv_bias = lax.dynamic_index_in_dim(
        qkv_bias.transpose(2, 3, 0, 1, 4).reshape(group, 3 * head_width), core * shards + shard, 0, False
    )
    up_bias = lax.dynamic_index_in_dim(
        rounded(vec_flat[..., at[1] : at[2]]).transpose(1, 2, 0, 3).reshape(group, unit_width),
        core * shards + shard,
        0,
        False,
    )
    vec_columns = (
        rounded(vec_flat[..., at[2] : at[3]])
        .reshape(owners, 4, model_rows)
        .transpose(1, 0, 2)
        .reshape(4, D)
    )
    norm_gain, norm_shift, dense_bias, down_bias = (vec_columns[index] for index in range(4))
    segments = lax.dynamic_index_in_dim(vec_flat[..., at[3] : at[4]], plane, 0, False)
    segments = segments.astype(jnp.int32).reshape(cores, shards * tokens_here)
    cat_bias = jnp.concatenate([qkv_bias, up_bias])

    x_float = x_all.astype(jnp.float32)
    center = x_float - jnp.mean(x_float, axis=-1, keepdims=True)
    inverse = lax.rsqrt(jnp.mean(center * center, axis=-1, keepdims=True) + norm_eps)
    x_hat = center * inverse
    norm_bf = (x_hat * norm_gain + norm_shift).astype(jnp.bfloat16)

    fu = jnp.dot(norm_bf, cat_w, preferred_element_type=jnp.float32) + cat_bias
    pre_act = fu[:, 3 * head_width :]
    hidden = gelu_tanh(pre_act).astype(jnp.bfloat16)
    grad_hidden = jnp.dot(dy_all, down_w.T, preferred_element_type=jnp.float32)
    grad_pre = jax.vjp(gelu_tanh, pre_act)[1](grad_hidden)[0]
    upb_part = jnp.sum(grad_pre, axis=0)
    grad_heads = jnp.dot(dy_all, dense_w.T, preferred_element_type=jnp.float32).astype(jnp.bfloat16)
    attn, dcat, qkvb_part = attention(fu, grad_heads, grad_pre.astype(jnp.bfloat16), segments)
    out_part = (
        jnp.dot(attn, dense_w, preferred_element_type=jnp.float32)
        + jnp.dot(hidden, down_w, preferred_element_type=jnp.float32)
    ).astype(jnp.bfloat16)
    down_grad = jnp.dot(hidden.T, dy_all, preferred_element_type=jnp.float32).astype(jnp.bfloat16)
    dense_grad = jnp.dot(attn.T, dy_all, preferred_element_type=jnp.float32).astype(jnp.bfloat16)
    cat_grad = jnp.dot(norm_bf.T, dcat, preferred_element_type=jnp.float32).astype(jnp.bfloat16)
    norm_part = jnp.dot(dcat, cat_w.T, preferred_element_type=jnp.float32)
    gain_part = jnp.sum(norm_part * x_hat, axis=0)
    shift_part = jnp.sum(norm_part, axis=0)
    bias_part = jnp.sum(cotangent.astype(jnp.float32), axis=0)
    sums = [qkvb_part, upb_part, gain_part, shift_part, bias_part]
    sum_sizes = [value.size for value in sums]
    sum_rows = -(-sum(sum_sizes) // 1024) * 8
    sums = jnp.pad(jnp.concatenate(sums), (0, sum_rows * 128 - sum(sum_sizes))).reshape(sum_rows, 128)

    cat_sum, dense_grad, down_grad, mixed, grad_norm, sums_all = reduce_wires(
        cat_grad.reshape(planes, group, model_rows, 3 * head_width + unit_width),
        dense_grad.reshape(planes, model_rows, D),
        down_grad.reshape(planes, unit_rows, D),
        out_part.reshape(group, tokens_here, D),
        norm_part.astype(jnp.bfloat16).reshape(group, tokens_here, D),
        sums,
    )

    sums_flat = sums_all.reshape(cores, shards, sum_rows * 128)
    at = [0]
    for size in sum_sizes:
        at.append(at[-1] + size)
    qkvb_grad = (
        sums_flat[..., : at[1]]
        .reshape(cores, shards, 3, planes, HD)
        .transpose(2, 3, 0, 1, 4)
        .reshape(owners, qkv_count)
    )
    qkvb_grad = lax.dynamic_index_in_dim(qkvb_grad, owner, 0, False)
    upb_grad = sums_flat[..., at[1] : at[2]].reshape(group, planes, upb_count)
    upb_grad = lax.dynamic_index_in_dim(
        lax.dynamic_index_in_dim(upb_grad, core * shards + shard, 0, False), plane, 0, False
    )
    vec_grad = jnp.sum(sums_flat[..., at[2] : at[5]], axis=(0, 1)).reshape(3, owners, model_rows)
    vec_grad = lax.dynamic_index_in_dim(vec_grad, owner, 1, False)
    vec_grad = jnp.stack([vec_grad[0], vec_grad[1], vec_grad[2], vec_grad[2]], axis=1)

    x_own = tokens.astype(jnp.float32)
    output = (x_own + (mixed.astype(jnp.float32) + dense_bias + down_bias)).astype(jnp.bfloat16)
    own_center = x_own - jnp.mean(x_own, axis=-1, keepdims=True)
    own_inverse = lax.rsqrt(jnp.mean(own_center * own_center, axis=-1, keepdims=True) + norm_eps)
    own_hat = own_center * own_inverse
    hat_grad = grad_norm.astype(jnp.float32) * norm_gain
    x_grad = own_inverse * (
        hat_grad
        - jnp.mean(hat_grad, axis=-1, keepdims=True)
        - own_hat * jnp.mean(hat_grad * own_hat, axis=-1, keepdims=True)
    )
    input_grad = cotangent.astype(jnp.float32) + x_grad

    new, qkv_grad, up_grad = owner_update(
        (qkv_weight_state, dense_weight_state, up_weight_state, down_weight_state),
        cat_sum,
        (dense_grad, down_grad),
        (qkv_bias_state, up_bias_state, vector_state),
        (qkvb_grad, upb_grad, vec_grad),
        (planes, cores, shards),
    )
    return (
        output[None],
        input_grad[None],
        qkv_grad,
        qkvb_grad,
        dense_grad,
        up_grad,
        upb_grad,
        down_grad,
        vec_grad,
        *new,
    )


def fast_solution(mesh):
    rep, shard = mesh.shape["rep"], mesh.shape["shard"]
    inner = Mesh(mesh.devices.reshape(rep // 2, 2, shard), ("plane", "core", "shard"))
    both = ("plane", "core")
    every = ("plane", "core", "shard")
    in_specs = (
        P(both, "shard", None),
        P(both, "shard"),
        P(both, "shard", None),
        P(None, every, None),
        P(None, every),
        P(None, every, None),
        P(None, every, None),
        P(None, every),
        P(None, every, None),
        P(None, every, None),
    )
    out_specs = (
        P(both, "shard", None),
        P(both, "shard", None),
        P(every, None),
        P(every),
        P(every, None),
        P(every, None),
        P(every),
        P(every, None),
        P(every, None),
        P(both, "shard", None),
        P(both, "shard", None),
        P(both, "shard", None),
    )
    return jax.shard_map(fast_body, mesh=inner, in_specs=in_specs, out_specs=out_specs, check_vma=False)


def solution(mesh):
    in_specs = (
        P("rep", "shard", None),
        P("rep", "shard"),
        P("rep", "shard", None),
        P(None, ("rep", "shard"), None),
        P(None, ("rep", "shard")),
        P(None, ("rep", "shard"), None),
        P(None, ("rep", "shard"), None),
        P(None, ("rep", "shard")),
        P(None, ("rep", "shard"), None),
        P(None, ("rep", "shard"), None),
    )
    out_specs = (
        P("rep", "shard", None),
        P("rep", "shard", None),
        P(("rep", "shard"), None),
        P(("rep", "shard")),
        P(("rep", "shard"), None),
        P(("rep", "shard"), None),
        P(("rep", "shard")),
        P(("rep", "shard"), None),
        P(("rep", "shard"), None),
        P("rep", "shard", None),
        P("rep", "shard", None),
        P("rep", "shard", None),
    )
    if whole_heads(mesh):
        return fast_solution(mesh)
    return jax.shard_map(body, mesh=mesh, in_specs=in_specs, out_specs=out_specs, check_vma=False)
```

```python
from functools import partial
import math

import jax
import jax.numpy as jnp
from jax import lax
from jax.experimental import pallas as pl
from jax.experimental.pallas import tpu as pltpu
from jax.sharding import Mesh
from jax.sharding import PartitionSpec as P

D = 2048
HD = 64
ROT = 32
FF = 8192
STEP = 5


learn_rate = 0.02
beta_one = 0.9
beta_two = 0.95
adam_eps = 1e-08
weight_decay = 0.1
norm_eps = 1e-05
big_negative = -1e30


def layer_norm(x, norm_gain, norm_shift):
    center = x - jnp.mean(x, axis=-1, keepdims=True)
    variance = jnp.mean(center * center, axis=-1, keepdims=True)
    return center * lax.rsqrt(variance + norm_eps) * norm_gain + norm_shift


def gelu_tanh(v):
    return 0.5 * v * (1.0 + jnp.tanh(0.7978845608028654 * (v + 0.044715 * v * v * v)))


def rotary(x, positions):
    half_rot = ROT // 2
    frequency = jnp.exp(jnp.arange(half_rot, dtype=jnp.float32) * (-2.0 * math.log(10000.0) / ROT))
    angles = positions.astype(jnp.float32)[:, None] * frequency[None, :]
    cosine = jnp.cos(angles)[:, None, :]
    sine_val = jnp.sin(angles)[:, None, :]
    lower_part = x[..., :half_rot]
    upper_part = x[..., half_rot:ROT]
    return jnp.concatenate(
        [
            lower_part * cosine - upper_part * sine_val,
            upper_part * cosine + lower_part * sine_val,
            x[..., ROT:],
        ],
        axis=-1,
    )


def adam_update(state, grad):
    moment_one = beta_one * state[1] + (1.0 - beta_one) * grad
    moment_two = beta_two * state[2] + (1.0 - beta_two) * grad * grad
    corrected = moment_one / (1.0 - beta_one**STEP)
    divisor = jnp.sqrt(moment_two / (1.0 - beta_two**STEP)) + adam_eps
    weight = state[0] - learn_rate * (corrected / divisor + weight_decay * state[0])
    return jnp.stack([weight, moment_one, moment_two])


def owner_entries(new_states, entry):
    return jnp.concatenate(
        [state_new[entry].reshape(-1) for state_new in new_states], axis=0
    ).reshape(1, 1, -1)


def block_mask(q_pos, q_seg, k_pos, k_seg):
    return (k_pos[None, :] <= q_pos[:, None]) & (k_seg[None, :] == q_seg[:, None])


def attend_keys(kv_all, seg_all, queries, q_pos, q_seg):
    key_count = kv_all.shape[0]
    width = kv_all.shape[1] // 2
    heads_here = queries.shape[1]
    query_rows = queries.shape[0]
    block_rows = math.gcd(key_count, 512)
    block_count = key_count // block_rows
    kv_blocks = kv_all.reshape(block_count, block_rows, 2 * width)
    seg_blocks = seg_all.reshape(block_count, block_rows)
    score_scale = 1.0 / math.sqrt(HD)

    def attend_step_block(carry, block_items):
        kv_rows, seg_rows, block_index = block_items
        row_max, totals, accumulated = carry
        key_rows = kv_rows[:, :width].reshape(block_rows, heads_here, HD)
        value_rows = kv_rows[:, width:].reshape(block_rows, heads_here, HD)
        k_pos = block_index * block_rows + jnp.arange(block_rows, dtype=jnp.int32)
        allowed = block_mask(q_pos, q_seg, k_pos, seg_rows)
        scores = (
            jnp.einsum("qhd,khd->hqk", queries, key_rows, preferred_element_type=jnp.float32)
            * score_scale
        )
        scores = jnp.where(allowed[None], scores, big_negative)
        new_max = jnp.maximum(row_max, jnp.max(scores, axis=-1))
        probabilities = jnp.where(allowed[None], jnp.exp(scores - new_max[..., None]), 0.0)
        factor = jnp.exp(row_max - new_max)
        totals = totals * factor + jnp.sum(probabilities, axis=-1)
        accumulated = accumulated * factor[..., None] + jnp.einsum(
            "hqk,khd->hqd",
            probabilities.astype(jnp.bfloat16),
            value_rows,
            preferred_element_type=jnp.float32,
        )
        return ((new_max, totals, accumulated), None)

    start_state = (
        jnp.full((heads_here, query_rows), big_negative, jnp.float32),
        jnp.zeros((heads_here, query_rows), jnp.float32),
        jnp.zeros((heads_here, query_rows, HD), jnp.float32),
    )
    running, unused = lax.scan(
        attend_step_block,
        start_state,
        (kv_blocks, seg_blocks, jnp.arange(block_count, dtype=jnp.int32)),
    )
    return running


def attention_grads(queries, kv_all, seg_all, q_pos, q_seg, grad_heads, delta_all, lse_all):
    key_count = kv_all.shape[0]
    width = kv_all.shape[1] // 2
    heads_here = queries.shape[1]
    query_rows = queries.shape[0]
    block_rows = math.gcd(key_count, 512)
    block_count = key_count // block_rows
    kv_blocks = kv_all.reshape(block_count, block_rows, 2 * width)
    seg_blocks = seg_all.reshape(block_count, block_rows)
    score_scale = 1.0 / math.sqrt(HD)

    def attention_step_block(query_grad, block_items):
        kv_rows, seg_rows, block_index = block_items
        key_rows = kv_rows[:, :width].reshape(block_rows, heads_here, HD)
        value_rows = kv_rows[:, width:].reshape(block_rows, heads_here, HD)
        k_pos = block_index * block_rows + jnp.arange(block_rows, dtype=jnp.int32)
        allowed = block_mask(q_pos, q_seg, k_pos, seg_rows)
        scores = (
            jnp.einsum("qhd,khd->hqk", queries, key_rows, preferred_element_type=jnp.float32)
            * score_scale
        )
        scores = jnp.where(allowed[None], scores, big_negative)
        probabilities = jnp.where(allowed[None], jnp.exp(scores - lse_all[..., None]), 0.0)
        value_grad = jnp.einsum(
            "hqk,qhd->khd",
            probabilities.astype(jnp.bfloat16),
            grad_heads,
            preferred_element_type=jnp.float32,
        )
        prob_grad = jnp.einsum(
            "qhd,khd->hqk", grad_heads, value_rows, preferred_element_type=jnp.float32
        )
        score_grad = (probabilities * (prob_grad - delta_all[..., None]) * score_scale).astype(
            jnp.bfloat16
        )
        query_grad = query_grad + jnp.einsum(
            "hqk,khd->hqd", score_grad, key_rows, preferred_element_type=jnp.float32
        )
        key_grad = jnp.einsum(
            "hqk,qhd->khd", score_grad, queries, preferred_element_type=jnp.float32
        )
        return (
            query_grad,
            jnp.concatenate(
                [key_grad.reshape(block_rows, width), value_grad.reshape(block_rows, width)], axis=1
            ),
        )

    query_grad, kv_grad_blocks = lax.scan(
        attention_step_block,
        jnp.zeros((heads_here, query_rows, HD), jnp.float32),
        (kv_blocks, seg_blocks, jnp.arange(block_count, dtype=jnp.int32)),
    )
    return (query_grad, kv_grad_blocks.reshape(key_count, 2 * width))


def gather_vectors(own_qkvb, own_upb, own_vec):
    return (
        lax.all_gather(own_qkvb, ("rep", "shard"), axis=0, tiled=True),
        lax.all_gather(own_upb, ("rep", "shard"), axis=0, tiled=True),
        lax.all_gather(own_vec, ("rep", "shard"), axis=0, tiled=True),
    )


def sum_vectors(qkvb_grad, upb_grad, vec_grad):
    return (
        lax.psum_scatter(qkvb_grad, ("rep", "shard"), scatter_dimension=0, tiled=True),
        lax.psum_scatter(upb_grad, ("rep", "shard"), scatter_dimension=0, tiled=True),
        lax.psum_scatter(vec_grad, ("rep", "shard"), scatter_dimension=0, tiled=True),
    )


def sum_positions(partial_rows):
    return lax.psum_scatter(partial_rows, "shard", scatter_dimension=0, tiled=True)


def attention_pass(norm_rows, qkv_w, qkv_b, positions, key_width):
    row_count = norm_rows.shape[0]
    heads_here = key_width // HD
    joined = jnp.dot(norm_rows, qkv_w, preferred_element_type=jnp.float32) + qkv_b
    q_pre = joined[:, :key_width].reshape(row_count, heads_here, HD)
    k_pre = joined[:, key_width : 2 * key_width].reshape(row_count, heads_here, HD)
    queries = rotary(q_pre, positions).astype(jnp.bfloat16)
    key_local = rotary(k_pre, positions).astype(jnp.bfloat16).reshape(row_count, key_width)
    value_local = joined[:, 2 * key_width :].astype(jnp.bfloat16)
    kv_local = jnp.concatenate([key_local, value_local], axis=1)
    return (q_pre, k_pre, queries, kv_local)


def finish_qkv_grad(q_pre, k_pre, positions, query_grad, kv_grad, key_width):
    row_count = q_pre.shape[0]
    heads_here = key_width // HD
    rotate_back = partial(rotary, positions=positions)
    query_pre = jax.vjp(rotate_back, q_pre)[1](query_grad.transpose(1, 0, 2))[0]
    key_pre = jax.vjp(rotate_back, k_pre)[1](
        kv_grad[:, :key_width].reshape(row_count, heads_here, HD)
    )[0]
    return jnp.concatenate(
        [
            query_pre.reshape(row_count, key_width),
            key_pre.reshape(row_count, key_width),
            kv_grad[:, key_width:],
        ],
        axis=1,
    )


def sliced_pass(norm_bf, q_seg, cotangent, own_mats, qkv_bb, up_bb):
    own_qkv, own_dense, own_up, own_down = own_mats
    inner_count = lax.axis_size("shard")
    outer_count = lax.axis_size("rep")
    stride = outer_count // inner_count
    place = lax.axis_index("shard")
    head_width = D // inner_count
    unit_width = FF // inner_count
    qkv_rows = own_qkv.shape[0]
    dense_rows = own_dense.shape[0]
    down_rows = own_down.shape[0]
    qkv_split = own_qkv.reshape(qkv_rows, 3, inner_count, head_width)
    up_split = own_up.reshape(qkv_rows, 1, inner_count, unit_width)
    qkv_cols, up_cols = (
        lax.all_to_all(qkv_split, "shard", split_axis=2, concat_axis=0, tiled=True),
        lax.all_to_all(up_split, "shard", split_axis=2, concat_axis=0, tiled=True),
    )
    qkv_rep, up_rep, dense_rep, down_rep = (
        lax.all_gather(qkv_cols, "rep", axis=0, tiled=True),
        lax.all_gather(up_cols, "rep", axis=0, tiled=True),
        lax.all_gather(own_dense[None], "rep", axis=0, tiled=True),
        lax.all_gather(own_down[None], "rep", axis=0, tiled=True),
    )
    dense_grid = dense_rep.reshape(inner_count, stride, 1, dense_rows, D)
    down_grid = down_rep.reshape(inner_count, stride, 1, down_rows, D)
    dense_moved, down_moved = (
        lax.all_to_all(dense_grid, "shard", split_axis=0, concat_axis=2, tiled=True),
        lax.all_to_all(down_grid, "shard", split_axis=0, concat_axis=2, tiled=True),
    )
    qkv_w = qkv_rep.reshape(D, 3 * head_width)
    up_w = up_rep.reshape(D, unit_width)
    dense_w = dense_moved.reshape(head_width, D)
    down_w = down_moved.reshape(unit_width, D)
    qkv_b = lax.dynamic_index_in_dim(
        qkv_bb.astype(jnp.float32).reshape(3, inner_count, head_width), place, 1, False
    ).reshape(3 * head_width)
    up_b = lax.dynamic_slice_in_dim(up_bb.astype(jnp.float32), place * unit_width, unit_width, 0)
    norm_seq, grad_seq, seg_seq = (
        lax.all_gather(norm_bf, "shard", axis=0, tiled=True),
        lax.all_gather(cotangent, "shard", axis=0, tiled=True),
        lax.all_gather(q_seg, "shard", axis=0, tiled=True),
    )
    seq_rows = norm_seq.shape[0]
    heads_here = head_width // HD
    positions = jnp.arange(seq_rows, dtype=jnp.int32)
    q_pre, k_pre, queries, kv_seq = attention_pass(norm_seq, qkv_w, qkv_b, positions, head_width)
    row_max, totals, accumulated = attend_keys(kv_seq, seg_seq, queries, positions, seg_seq)
    lse_all = row_max + jnp.log(totals)
    out_heads = (accumulated / totals[..., None]).transpose(1, 0, 2).astype(jnp.bfloat16)
    attn_bf = out_heads.reshape(seq_rows, head_width)
    pre_act = jnp.dot(norm_seq, up_w, preferred_element_type=jnp.float32) + up_b
    hidden = gelu_tanh(pre_act).astype(jnp.bfloat16)
    partial_out = jnp.dot(attn_bf, dense_w, preferred_element_type=jnp.float32) + jnp.dot(
        hidden, down_w, preferred_element_type=jnp.float32
    )
    mixed = sum_positions(partial_out)
    grad_down = jnp.dot(hidden.T, grad_seq, preferred_element_type=jnp.float32)
    grad_dense = jnp.dot(attn_bf.T, grad_seq, preferred_element_type=jnp.float32)
    grad_hidden = jnp.dot(grad_seq, down_w.T, preferred_element_type=jnp.float32)
    grad_pre = jax.vjp(gelu_tanh, pre_act)[1](grad_hidden)[0]
    grad_pre_bf = grad_pre.astype(jnp.bfloat16)
    grad_up = jnp.dot(norm_seq.T, grad_pre_bf, preferred_element_type=jnp.float32)
    upb_part = jnp.sum(grad_pre, axis=0)
    norm_part = jnp.dot(grad_pre_bf, up_w.T, preferred_element_type=jnp.float32)
    grad_heads = (
        jnp.dot(grad_seq, dense_w.T, preferred_element_type=jnp.float32)
        .astype(jnp.bfloat16)
        .reshape(seq_rows, heads_here, HD)
    )
    delta_all = jnp.sum(grad_heads.astype(jnp.float32) * out_heads.astype(jnp.float32), axis=-1).T
    query_grad, kv_grad = attention_grads(
        queries, kv_seq, seg_seq, positions, seg_seq, grad_heads, delta_all, lse_all
    )
    grad_joined = finish_qkv_grad(q_pre, k_pre, positions, query_grad, kv_grad, head_width)
    grad_joined_bf = grad_joined.astype(jnp.bfloat16)
    grad_qkv = jnp.dot(norm_seq.T, grad_joined_bf, preferred_element_type=jnp.float32)
    qkvb_part = jnp.sum(grad_joined, axis=0)
    norm_part = norm_part + jnp.dot(grad_joined_bf, qkv_w.T, preferred_element_type=jnp.float32)
    grad_norm = sum_positions(norm_part)
    dense_grid_grad = grad_dense.reshape(1, stride, inner_count, dense_rows, D)
    down_grid_grad = grad_down.reshape(1, stride, inner_count, down_rows, D)
    dense_back, down_back = (
        lax.all_to_all(dense_grid_grad, "shard", split_axis=2, concat_axis=0, tiled=True),
        lax.all_to_all(down_grid_grad, "shard", split_axis=2, concat_axis=0, tiled=True),
    )
    qkv_sum, up_sum, dense_sum, down_sum = (
        lax.psum_scatter(
            grad_qkv.reshape(D, 3, 1, head_width), "rep", scatter_dimension=0, tiled=True
        ),
        lax.psum_scatter(
            grad_up.reshape(D, 1, 1, unit_width), "rep", scatter_dimension=0, tiled=True
        ),
        lax.psum_scatter(
            dense_back.reshape(outer_count, dense_rows, D), "rep", scatter_dimension=0, tiled=True
        ),
        lax.psum_scatter(
            down_back.reshape(outer_count, down_rows, D), "rep", scatter_dimension=0, tiled=True
        ),
    )
    qkv_home, up_home = (
        lax.all_to_all(qkv_sum, "shard", split_axis=0, concat_axis=2, tiled=True),
        lax.all_to_all(up_sum, "shard", split_axis=0, concat_axis=2, tiled=True),
    )
    qkv_own = qkv_home.reshape(qkv_rows, 3 * D)
    up_own = up_home.reshape(qkv_rows, FF)
    dense_own = dense_sum.reshape(dense_rows, D)
    down_own = down_sum.reshape(down_rows, D)
    selector = (jnp.arange(inner_count, dtype=jnp.int32) == place).astype(jnp.float32)
    qkvb_grad = (selector[None, :, None] * qkvb_part.reshape(3, 1, head_width)).reshape(3 * D)
    upb_grad = (selector[:, None] * upb_part[None, :]).reshape(FF)
    return (mixed, grad_norm, (qkv_own, dense_own, up_own, down_own), qkvb_grad, upb_grad)


def body(
    hidden_in,
    segment_ids,
    out_grad,
    qkv_weight_state,
    qkv_bias_state,
    dense_weight_state,
    up_weight_state,
    up_bias_state,
    down_weight_state,
    vector_state,
):
    own_mats = (
        qkv_weight_state[0].astype(jnp.bfloat16),
        dense_weight_state[0].astype(jnp.bfloat16),
        up_weight_state[0].astype(jnp.bfloat16),
        down_weight_state[0].astype(jnp.bfloat16),
    )
    qkv_bb, up_bb, vec_bf = gather_vectors(
        qkv_bias_state[0].astype(jnp.bfloat16),
        up_bias_state[0].astype(jnp.bfloat16),
        vector_state[0].astype(jnp.bfloat16),
    )
    vec_all = vec_bf.astype(jnp.float32)
    norm_gain = vec_all[:, 0]
    norm_shift = vec_all[:, 1]
    dense_bias = vec_all[:, 2]
    down_bias = vec_all[:, 3]
    tokens = hidden_in[0]
    q_seg = segment_ids[0]
    cotangent = out_grad[0]
    x_full = tokens.astype(jnp.float32)
    normed = layer_norm(x_full, norm_gain, norm_shift)
    norm_bf = normed.astype(jnp.bfloat16)
    mixed, grad_norm, owned, qkvb_grad, upb_grad = sliced_pass(
        norm_bf, q_seg, cotangent, own_mats, qkv_bb, up_bb
    )
    qkv_own, dense_own, up_own, down_own = owned
    output = (x_full + (mixed + dense_bias + down_bias)).astype(jnp.bfloat16)
    grad_x, grad_gain, grad_shift = jax.vjp(layer_norm, x_full, norm_gain, norm_shift)[1](grad_norm)
    out_bias_grad = jnp.sum(cotangent.astype(jnp.float32), axis=0)
    grad_vec = jnp.stack([grad_gain, grad_shift, out_bias_grad, out_bias_grad], axis=1)
    input_grad = cotangent.astype(jnp.float32) + grad_x
    qkvb_own, upb_own, vec_own = sum_vectors(qkvb_grad, upb_grad, grad_vec)
    new_states = (
        adam_update(qkv_weight_state, qkv_own),
        adam_update(qkv_bias_state, qkvb_own),
        adam_update(dense_weight_state, dense_own),
        adam_update(up_weight_state, up_own),
        adam_update(up_bias_state, upb_own),
        adam_update(down_weight_state, down_own),
        adam_update(vector_state, vec_own),
    )
    return (
        output[None],
        input_grad[None],
        qkv_own,
        qkvb_own,
        dense_own,
        up_own,
        upb_own,
        down_own,
        vec_own,
        owner_entries(new_states, 0),
        owner_entries(new_states, 1),
        owner_entries(new_states, 2),
    )


def whole_heads(mesh):
    owners = mesh.shape["rep"] * mesh.shape["shard"]
    return D % owners == 0 and D // owners == HD and mesh.shape["rep"] % 2 == 0


def rotation_tables(seq_rows):
    half_rot = ROT // 2
    lane = jnp.arange(2 * HD, dtype=jnp.int32) % HD
    frequency = jnp.exp((lane % half_rot).astype(jnp.float32) * (-2.0 * math.log(10000.0) / ROT))
    angles = jnp.arange(seq_rows, dtype=jnp.int32).astype(jnp.float32)[:, None] * frequency[None, :]
    sine = jnp.sin(angles)
    cosine = jnp.where(lane[None, :] < ROT, jnp.cos(angles), 1.0)
    low = jnp.where(lane[None, :] < half_rot, -sine, 0.0)
    high = jnp.where((lane[None, :] >= half_rot) & (lane[None, :] < ROT), sine, 0.0)
    return cosine, low, high


def attention_kernel(
    fu_ref, do_ref, du_ref, seg_col_ref, seg_row_ref, cos_ref, low_ref, high_ref, o_ref, dcat_ref, sums_ref
):
    rows, width = do_ref.shape
    scale = 1.0 / math.sqrt(HD)
    row_id = lax.broadcasted_iota(jnp.int32, (rows, rows), 0)
    col_id = lax.broadcasted_iota(jnp.int32, (rows, rows), 1)
    allowed = (col_id <= row_id) & (seg_col_ref[...] == seg_row_ref[0])
    cosine, low, high = cos_ref[...], low_ref[...], high_ref[...]
    half = ROT // 2
    lane = lax.broadcasted_iota(jnp.int32, (rows, 2 * HD), 1)

    def rotate(u):
        return (
            u * cosine
            + pltpu.roll(u, 2 * HD - half, 1) * low
            + pltpu.roll(u, half, 1) * high
        )

    def rotate_back(u):
        return (
            u * cosine
            - pltpu.roll(u, 2 * HD - half, 1) * low
            - pltpu.roll(u, half, 1) * high
        )

    def dot(a, b, a_dim, b_dim):
        return lax.dot_general(a, b, (((a_dim,), (b_dim,)), ((), ())), preferred_element_type=jnp.float32)

    zero = jnp.zeros((), jnp.bfloat16)
    for pair in range(width // (2 * HD)):
        lanes = pl.ds(pair * 2 * HD, 2 * HD)
        k_lanes = pl.ds(width + pair * 2 * HD, 2 * HD)
        v_lanes = pl.ds(2 * width + pair * 2 * HD, 2 * HD)
        q = rotate(fu_ref[:, lanes]).astype(jnp.bfloat16)
        k = rotate(fu_ref[:, k_lanes]).astype(jnp.bfloat16)
        v = fu_ref[:, v_lanes].astype(jnp.bfloat16)
        do = do_ref[:, lanes]
        o = dq = dk = dv = None
        for head in range(2):
            mine = (lane < HD) if head == 0 else (lane >= HD)
            qh = jnp.where(mine, q, zero)
            kh = jnp.where(mine, k, zero)
            vh = jnp.where(mine, v, zero)
            doh = jnp.where(mine, do, zero)
            scores = jnp.where(allowed, dot(qh, k, 1, 1) * scale, big_negative)
            row_max = jnp.max(scores, axis=1, keepdims=True)
            probs = jnp.where(allowed, jnp.exp(scores - row_max), 0.0)
            inverse = 1.0 / jnp.sum(probs, axis=1, keepdims=True)
            oh = dot(probs.astype(jnp.bfloat16), vh, 1, 0) * inverse
            delta = jnp.sum(
                doh.astype(jnp.float32) * oh.astype(jnp.bfloat16).astype(jnp.float32), axis=1, keepdims=True
            )
            probs = probs * inverse
            dvh = dot(probs.astype(jnp.bfloat16), doh, 0, 0)
            ds = (probs * (dot(doh, v, 1, 1) - delta) * scale).astype(jnp.bfloat16)
            dqh = dot(ds, kh, 1, 0)
            dkh = dot(ds, qh, 0, 0)
            if head == 0:
                o, dq, dk, dv = oh, dqh, dkh, dvh
            else:
                o, dq, dk, dv = o + oh, dq + dqh, dk + dkh, dv + dvh
        o_ref[:, lanes] = o.astype(jnp.bfloat16)
        dq = rotate_back(dq)
        dk = rotate_back(dk)
        for part, place in ((dq, lanes), (dk, k_lanes), (dv, v_lanes)):
            dcat_ref[:, place] = part.astype(jnp.bfloat16)
            sums_ref[0, :, place] = jnp.sum(part, axis=0, keepdims=True)
    dcat_ref[:, pl.ds(3 * width, du_ref.shape[1])] = du_ref[...]


def attention(fu, do, du, segments):
    count, rows = segments.shape
    width = do.shape[1]
    units = du.shape[1]
    tables = rotation_tables(rows)
    table_spec = pl.BlockSpec((rows, 2 * HD), lambda s: (0, 0))
    o, dcat, sums = pl.pallas_call(
        attention_kernel,
        grid=(count,),
        in_specs=[
            pl.BlockSpec((rows, 3 * width), lambda s: (s, 0)),
            pl.BlockSpec((rows, width), lambda s: (s, 0)),
            pl.BlockSpec((rows, units), lambda s: (s, 0)),
            pl.BlockSpec((rows, 1), lambda s: (s, 0)),
            pl.BlockSpec((1, 1, rows), lambda s: (s, 0, 0)),
            table_spec,
            table_spec,
            table_spec,
        ],
        out_specs=[
            pl.BlockSpec((rows, width), lambda s: (s, 0)),
            pl.BlockSpec((rows, 3 * width + units), lambda s: (s, 0)),
            pl.BlockSpec((1, 1, 3 * width), lambda s: (s, 0, 0)),
        ],
        out_shape=[
            jax.ShapeDtypeStruct((count * rows, width), jnp.bfloat16),
            jax.ShapeDtypeStruct((count * rows, 3 * width + units), jnp.bfloat16),
            jax.ShapeDtypeStruct((count, 1, 3 * width), jnp.float32),
        ],
        compiler_params=pltpu.CompilerParams(vmem_limit_bytes=56 << 20),
        cost_estimate=pl.CostEstimate(
            flops=count * (width // HD) * 10 * rows * rows * HD,
            bytes_accessed=count * rows * (width * 20 + units * 4),
            transcendentals=count * (width // HD) * rows * rows,
        ),
    )(fu, do, du, segments.reshape(count * rows, 1), segments.reshape(count, 1, rows), *tables)
    return o, dcat, jnp.sum(sums, axis=(0, 1))


def adam_values(weight, moment_one, moment_two, grad):
    first = beta_one * moment_one + (1.0 - beta_one) * grad
    second = beta_two * moment_two + (1.0 - beta_two) * grad * grad
    corrected = first * (1.0 / (1.0 - beta_one**STEP))
    divisor = jnp.sqrt(second * (1.0 / (1.0 - beta_two**STEP))) + adam_eps
    return weight - learn_rate * (corrected / divisor + weight_decay * weight), first, second


def owner_update_kernel(plan, small_plan, groups, *refs):
    planes, cores, shards = groups
    qkv_state, dense_state, up_state, down_state, cat_ref, dense_grad, down_grad, small_ref = refs[:8]
    outs = refs[8:11]
    qkv_out, up_out, cat_buf = refs[11:]
    step = pl.program_id(0)
    lane = lax.broadcasted_iota(jnp.int32, (8, 128), 1)
    sub = lax.broadcasted_iota(jnp.int32, (8, 128), 0)
    lane_row = lax.broadcasted_iota(jnp.int32, (1, 128), 1)
    wide = 1024

    @pl.when(step == 0)
    def small():
        for source, row, low, high in small_plan:
            for entry in range(3):
                old = outs[entry][pl.ds(row, 1), :]
                new = small_ref[entry, pl.ds(source, 1), :]
                outs[entry][pl.ds(row, 1), :] = jnp.where((lane_row >= low) & (lane_row < high), new, old)

    def widen(piece, carry):
        cat_buf[piece] = cat_ref[piece].astype(jnp.float32)
        return carry

    lax.fori_loop(0, cat_ref.shape[0], widen, 0)

    def place_rows(state, grad_of, rows, tiles, start, shifted, keep=None):
        chunk = min(wide, tiles * 128)

        def one_group(group, carry):
            place = pl.ds(pl.multiple_of(group * 8, 8), 8)
            base = start + (step * (rows // 8) + group) * (8 * tiles)

            def values(column, size):
                lanes = pl.ds(column, size)
                grad = grad_of(place, column, size)
                if keep is not None and size > 128:
                    keep[place, lanes] = grad
                return adam_values(
                    state[0, place, lanes], state[1, place, lanes], state[2, place, lanes], grad
                )

            if shifted:
                last = tuple(pltpu.roll(value, 64, 1) for value in values((tiles - 1) * 128, 128))
                before = tuple(
                    jnp.where(sub == 0, out[pl.ds(base, 1), :], pltpu.roll(value, 1, 0))
                    for out, value in zip(outs, last)
                )
            for column in range(0, tiles * 128, chunk):
                done = values(column, chunk)
                for entry, out in enumerate(outs):
                    for tile in range(chunk // 128):
                        value = done[entry][:, tile * 128 : (tile + 1) * 128]
                        if shifted:
                            value = pltpu.roll(value, 64, 1)
                            old = before[entry] if tile == 0 else now
                            now = value
                            value = jnp.where(lane < 64, old, value)
                        out[pl.ds(base + column // 128 + tile, 8, stride=tiles), :] = value
                    if shifted:
                        before = before[:entry] + (now,) + before[entry + 1 :]
            if shifted:
                for out, value in zip(outs, before):
                    row = pl.ds(base + 8 * tiles, 1)
                    out[row, :] = jnp.where(lane_row < 64, value[7:8], out[row, :])
            return carry

        lax.fori_loop(0, rows // 8, one_group, 0)

    def qkv_grad(place, column, size):
        tiles = []
        for start in range(column, column + size, 128):
            part, head = divmod(start // HD, planes * cores * shards)
            halves = []
            for side in range(2):
                plane, member = divmod(head + side, cores * shards)
                spot = (part * planes + plane) * HD
                half = cat_buf[member, place, pl.ds(spot // 128 * 128, 128)]
                halves.append(half if spot % 128 == side * HD else pltpu.roll(half, HD, 1))
            tiles.append(jnp.where(lane < HD, halves[0], halves[1]))
        return tiles[0] if len(tiles) == 1 else jnp.concatenate(tiles, axis=1)

    units = up_state.shape[2] // (planes * cores * shards)

    def up_grad(place, column, size):
        parts = []
        for start in range(column, column + size, min(units, size)):
            plane, member = divmod(start // units, cores * shards)
            spot = 3 * planes * HD + plane * units + start % units
            parts.append(cat_buf[member, place, pl.ds(spot, min(units, size))])
        return parts[0] if len(parts) == 1 else jnp.concatenate(parts, axis=1)

    def plain(grad):
        return lambda place, column, size: grad[place, pl.ds(column, size)]

    place_rows(qkv_state, qkv_grad, *plan[0], keep=qkv_out)
    place_rows(dense_state, plain(dense_grad), *plan[1])
    place_rows(up_state, up_grad, *plan[2], keep=up_out)
    place_rows(down_state, plain(down_grad), *plan[3])


def owner_update(states, cat_sum, grads, small_states, small_grads, groups):
    steps = 4
    sizes = [state.shape[1] * state.shape[2] for state in states]
    small_sizes = [grad.size for grad in small_grads]
    order = [("m", 0), ("s", 0), ("m", 1), ("m", 2), ("s", 1), ("m", 3), ("s", 2)]
    offset = 0
    plan = [None] * 4
    small_plan = []
    pads = []
    small_row = 0
    for kind, index in order:
        if kind == "m":
            state = states[index]
            rows = state.shape[1] // steps
            plan[index] = (rows, state.shape[2] // 128, offset // 128, offset % 128 == 64)
            offset += sizes[index]
        else:
            size = small_sizes[index]
            front = offset % 128
            total = -(-(front + size) // 128)
            pads.append((front, total * 128 - front - size))
            for extra in range(total):
                low = front if extra == 0 else 0
                high = min(128, front + size - extra * 128)
                small_plan.append((small_row + extra, offset // 128 + extra, low, high))
            small_row += total
            offset += size
    entries = offset
    out_rows = -(-entries // 1024) * 8
    small_new = [
        adam_values(state[0].reshape(-1), state[1].reshape(-1), state[2].reshape(-1), grad.reshape(-1))
        for state, grad in zip(small_states, small_grads)
    ]
    small = jnp.stack(
        [
            jnp.concatenate([jnp.pad(new[entry], pad) for new, pad in zip(small_new, pads)])
            for entry in range(3)
        ]
    ).reshape(3, small_row, 128)
    in_specs = [
        pl.BlockSpec((3, rows, tiles * 128), lambda s: (0, s, 0)) for rows, tiles, start, shifted in plan
    ]
    qkv_rows, up_rows = plan[0][0], plan[2][0]
    in_specs.append(pl.BlockSpec((cat_sum.shape[0], qkv_rows, cat_sum.shape[2]), lambda s: (0, s, 0)))
    in_specs.append(pl.BlockSpec((plan[1][0], plan[1][1] * 128), lambda s: (s, 0)))
    in_specs.append(pl.BlockSpec((plan[3][0], plan[3][1] * 128), lambda s: (s, 0)))
    in_specs.append(pl.BlockSpec((3, small_row, 128), lambda s: (0, 0, 0)))
    flat = [pl.BlockSpec((out_rows, 128), lambda s: (0, 0), pipeline_mode=pl.Buffered(1))] * 3
    *outs, qkv_grad, up_grad = pl.pallas_call(
        partial(owner_update_kernel, plan, small_plan, groups),
        grid=(steps,),
        in_specs=in_specs,
        out_specs=flat
        + [
            pl.BlockSpec((qkv_rows, plan[0][1] * 128), lambda s: (s, 0)),
            pl.BlockSpec((up_rows, plan[2][1] * 128), lambda s: (s, 0)),
        ],
        out_shape=[jax.ShapeDtypeStruct((out_rows, 128), jnp.float32)] * 3
        + [
            jax.ShapeDtypeStruct(states[0].shape[1:], jnp.float32),
            jax.ShapeDtypeStruct(states[2].shape[1:], jnp.float32),
        ],
        scratch_shapes=[pltpu.VMEM((cat_sum.shape[0], qkv_rows, cat_sum.shape[2]), jnp.float32)],
        compiler_params=pltpu.CompilerParams(vmem_limit_bytes=56 << 20),
        cost_estimate=pl.CostEstimate(
            flops=20 * entries, bytes_accessed=28 * entries, transcendentals=2 * entries
        ),
    )(*states, cat_sum, *grads, small)
    return tuple(out.reshape(1, 1, out_rows * 128)[:, :, :entries] for out in outs), qkv_grad, up_grad


class Wires:
    def __init__(self, send_sems):
        self.send_sems, self.count, self.pending = send_sems, 0, []
        self.plane, self.core, self.shard = (
            lax.axis_index("plane"),
            lax.axis_index("core"),
            lax.axis_index("shard"),
        )
        self.shards = lax.axis_size("shard")
        self.group = lax.axis_size("core") * self.shards
        self.mine = self.core * self.shards + self.shard
        self.first = (self.plane ^ 1, self.core, self.shard)
        self.second = (self.plane ^ 2, self.core, self.shard)

    def member(self, index):
        return (self.plane, index // self.shards, index % self.shards)

    def barrier(self):
        barrier = pltpu.get_barrier_semaphore()
        partners = [self.member(self.mine ^ mask) for mask in range(1, self.group)]
        partners += [self.first, self.second]
        for partner in partners:
            pl.semaphore_signal(barrier, inc=1, device_id=partner, device_id_type=pl.DeviceIdType.MESH)
        pl.semaphore_wait(barrier, len(partners))

    def send(self, source, target, recv_sem, device, when=None):
        copy = pltpu.make_async_remote_copy(
            src_ref=source,
            dst_ref=target,
            send_sem=self.send_sems.at[self.count],
            recv_sem=recv_sem,
            device_id=device,
            device_id_type=pl.DeviceIdType.MESH,
        )
        self.count += 1
        self.pending.append((copy, when))
        if when is None:
            copy.start()
        else:
            pl.when(when)(copy.start)

    def arrived(self, place, recv_sem, when=None):
        copy = pltpu.make_async_remote_copy(
            src_ref=place,
            dst_ref=place,
            send_sem=self.send_sems.at[0],
            recv_sem=recv_sem,
            device_id=self.first,
            device_id_type=pl.DeviceIdType.MESH,
        )
        if when is None:
            copy.wait_recv()
        else:
            pl.when(when)(copy.wait_recv)

    def drain(self):
        for copy, when in self.pending:
            if when is None:
                copy.wait_send()
            else:
                pl.when(when)(copy.wait_send)


def pack_pieces(qkv, up, pieces, planes, cores, shards):
    rows = qkv.shape[0]
    lane = lax.broadcasted_iota(jnp.int32, (rows, 128), 1)
    units = up.shape[1] // (planes * cores * shards)
    for core in range(cores):
        for shard in range(shards):
            piece = core * shards + shard
            for tile in range(3 * planes // 2):
                halves = []
                for side in range(2):
                    part, plane = divmod(2 * tile + side, planes)
                    head = (plane * cores + core) * shards + shard
                    start = part * planes * cores * shards * HD + head * HD
                    half = qkv[:, pl.ds(start // 128 * 128, 128)]
                    halves.append(half if start % 128 == side * HD else pltpu.roll(half, HD, 1))
                pieces[piece, :, pl.ds(tile * 128, 128)] = jnp.where(lane < HD, halves[0], halves[1]).astype(
                    jnp.bfloat16
                )
            for plane in range(planes):
                block = (plane * cores + core) * shards + shard
                pieces[piece, :, pl.ds(3 * planes * HD + plane * units, units)] = up[
                    :, pl.ds(block * units, units)
                ].astype(jnp.bfloat16)


def gather_kernel(
    qkv_state, up_state, dense_state, down_state, tokens, cotangent, vectors,
    cat_out, dense_out, down_out, x_out, dy_out, vec_out,
    qkv_buf, up_buf, dense_buf, down_buf, pieces, dense, down,
    load_sem, send_sems, group_sem, first_sem, second_sem, far_sem, up_sem, low_sem, core_sem, local_sem,
):
    net = Wires(send_sems)
    plane, core, shard, shards, group, mine = net.plane, net.core, net.shard, net.shards, net.group, net.mine
    order = sorted(range(group), key=lambda mask: (mask % shards, mask // shards))
    partner = (plane, 1 - core, shard)

    def cat_unit(mask):
        return lambda p: cat_out.at[p, mine ^ mask]

    def vec_unit(mask):
        return lambda p: vec_out.at[p, mine ^ mask]

    units = []
    down_rows = down.shape[0] // 4
    for part in range(4):
        rows = pl.ds(part * down_rows, down_rows)
        units.append((down.at[rows], lambda p, rows=rows: down_out.at[p, rows]))
    dense_rows = dense.shape[0] // 2
    for part in range(2):
        rows = pl.ds(part * dense_rows, dense_rows)
        units.append((dense.at[rows], lambda p, rows=rows: dense_out.at[p, rows]))
    own_units = list(range(len(units)))
    cat_units, vec_units = {}, {}
    for mask in order:
        cat_units[mask] = len(units)
        units.append((pieces.at[mine] if mask == 0 else None, cat_unit(mask)))
        vec_units[mask] = len(units)
        units.append((vectors if mask == 0 else None, vec_unit(mask)))

    def spread(index):
        source, place = units[index]
        source = place(plane) if source is None else source
        net.send(source, place(plane), first_sem.at[index], net.first)
        net.send(source, place(plane), second_sem.at[index], net.second)

    def hand_on(index):
        place = units[index][1]
        if relay_first[index]:
            net.arrived(place(plane ^ 1), first_sem.at[index])
            net.send(place(plane ^ 1), place(plane ^ 1), far_sem.at[index], net.second)
        else:
            net.arrived(place(plane ^ 2), second_sem.at[index])
            net.send(place(plane ^ 2), place(plane ^ 2), far_sem.at[index], net.first)

    relay_first = {}
    for position, index in enumerate(own_units):
        relay_first[index] = position % 2 == 0
    for position, mask in enumerate(order):
        relay_first[cat_units[mask]] = position % 2 == 0
        relay_first[vec_units[mask]] = position % 2 == 1

    loads = [
        pltpu.make_async_copy(state.at[0], buffer, load_sem.at[index])
        for index, (state, buffer) in enumerate(
            ((qkv_state, qkv_buf), (up_state, up_buf), (down_state, down_buf), (dense_state, dense_buf))
        )
    ]
    for load in loads:
        load.start()
    net.barrier()
    loads[0].wait()
    loads[1].wait()
    pack_pieces(qkv_buf, up_buf, pieces, cat_out.shape[0], group // shards, shards)

    locals_ = [
        (pieces.at[mine], cat_out.at[plane, mine]),
        (dense, dense_out.at[plane]),
        (down, down_out.at[plane]),
        (tokens, x_out.at[mine]),
        (cotangent, dy_out.at[mine]),
        (vectors, vec_out.at[plane, mine]),
    ]
    copies = [
        pltpu.make_async_copy(source, target, local_sem.at[index])
        for index, (source, target) in enumerate(locals_)
    ]
    for mask in order[1:]:
        target = net.member(mine ^ mask)
        net.send(vectors, vec_out.at[plane, mine], group_sem.at[1, mask], target)
        net.send(pieces.at[mine ^ mask], cat_out.at[plane, mine], group_sem.at[0, mask], target)
    loads[2].wait()
    down[...] = down_buf[...].astype(jnp.bfloat16)
    loads[3].wait()
    dense[...] = dense_buf[...].astype(jnp.bfloat16)
    for index in own_units:
        spread(index)
    spread(cat_units[0])
    spread(vec_units[0])
    streams = ((tokens, x_out), (cotangent, dy_out))

    def block(stream, origin):
        return streams[stream][1].at[core * shards + origin]

    def to_core(stream, source, origin, slot, when=None):
        net.send(source, block(stream, origin), core_sem.at[stream, slot], partner, when)

    def hop(stream, distance):
        own = distance == 1
        for upward, sem in ((True, up_sem), (False, low_sem)):
            origin = shard - (distance - 1) if upward else shard + (distance - 1)
            there = shard + 1 if upward else shard - 1
            held = (origin >= 0) if upward else (origin < shards)
            inside = (there < shards) if upward else (there >= 0)
            near = jnp.clip(origin, 0, shards - 1)
            source = streams[stream][0] if own else block(stream, near)
            net.send(
                source,
                block(stream, near),
                sem.at[stream, distance],
                (plane, core, jnp.clip(there, 0, shards - 1)),
                inside & held,
            )

    def hop_arrived(stream, distance):
        for upward, sem in ((True, up_sem), (False, low_sem)):
            origin = shard - distance if upward else shard + distance
            held = (origin >= 0) if upward else (origin < shards)
            near = jnp.clip(origin, 0, shards - 1)
            net.arrived(block(stream, near), sem.at[stream, distance], held)
            slot = distance if upward else shards + distance
            to_core(stream, block(stream, near), near, slot, held)

    for stream in range(2):
        hop(stream, 1)
    for stream in range(2):
        to_core(stream, streams[stream][0], shard, 0)
    for copy in copies:
        copy.start()

    for position, mask in enumerate(order[1:]):
        net.arrived(vec_out.at[plane, mine ^ mask], group_sem.at[1, mask])
        spread(vec_units[mask])
        net.arrived(cat_out.at[plane, mine ^ mask], group_sem.at[0, mask])
        spread(cat_units[mask])
        if position == 2:
            for index in own_units:
                hand_on(index)
    hand_on(cat_units[0])
    hand_on(vec_units[0])
    for distance in range(1, shards):
        for stream in range(2):
            hop_arrived(stream, distance)
            if distance + 1 < shards:
                hop(stream, distance + 1)
        for mask in order[1 + (distance - 1) * 3 : 1 + distance * 3]:
            hand_on(vec_units[mask])
            hand_on(cat_units[mask])

    for index, (source, place) in enumerate(units):
        if relay_first[index]:
            net.arrived(place(plane ^ 2), second_sem.at[index])
        else:
            net.arrived(place(plane ^ 1), first_sem.at[index])
        net.arrived(place(plane ^ 3), far_sem.at[index])
    for stream in range(2):
        other = streams[stream][1]
        for slot in range(2 * shards):
            if slot == shards:
                continue
            origin = shard - slot if slot < shards else shard + (slot - shards)
            held = None if slot == 0 else ((origin >= 0) & (origin < shards))
            near = jnp.clip(origin, 0, shards - 1)
            net.arrived(other.at[(1 - core) * shards + near], core_sem.at[stream, slot], held)
    for copy in copies:
        copy.wait()
    net.drain()


def gather_wires(qkv, up, dense, down, tokens, cotangent, vectors):
    group, shards = lax.axis_size("core") * lax.axis_size("shard"), lax.axis_size("shard")
    planes = lax.axis_size("plane")
    width = (qkv.shape[2] + up.shape[2]) // group
    units = 6 + 2 * group
    vmem = pl.BlockSpec(memory_space=pltpu.VMEM)
    hbm = pl.BlockSpec(memory_space=pl.ANY)

    def out(*shape, dtype=jnp.bfloat16):
        return jax.ShapeDtypeStruct(shape, dtype)

    dma = pltpu.SemaphoreType.DMA
    return pl.pallas_call(
        gather_kernel,
        in_specs=[hbm] * 4 + [vmem] * 3,
        out_specs=[hbm] * 6,
        out_shape=[
            out(planes, group, qkv.shape[1], width),
            out(planes, *dense.shape[1:]),
            out(planes, *down.shape[1:]),
            out(group, *tokens.shape),
            out(group, *cotangent.shape),
            out(planes, group, *vectors.shape, dtype=vectors.dtype),
        ],
        scratch_shapes=[
            pltpu.VMEM(qkv.shape[1:], qkv.dtype),
            pltpu.VMEM(up.shape[1:], up.dtype),
            pltpu.VMEM(dense.shape[1:], dense.dtype),
            pltpu.VMEM(down.shape[1:], down.dtype),
            pltpu.VMEM((group, qkv.shape[1], width), jnp.bfloat16),
            pltpu.VMEM(dense.shape[1:], jnp.bfloat16),
            pltpu.VMEM(down.shape[1:], jnp.bfloat16),
            dma((4,)),
            dma((2 * (group - 1) + 3 * units + 2 * 2 * (shards - 1) + 2 * (2 * shards - 1),)),
            dma((2, group)),
            dma((units,)),
            dma((units,)),
            dma((units,)),
            dma((2, shards)),
            dma((2, shards)),
            dma((2, 2 * shards)),
            dma((6,)),
        ],
        compiler_params=pltpu.CompilerParams(
            collective_id=0, has_side_effects=True, vmem_limit_bytes=67043328
        ),
    )(qkv, up, dense, down, tokens, cotangent, vectors)


def add_rows(target, *sources):
    step = 16
    rows = target.shape[0]

    def body(index, carry):
        place = pl.ds(pl.multiple_of(index * step, step), step)
        total = sources[0][place, :].astype(jnp.float32)
        for source in sources[1:]:
            total = total + source[place, :].astype(jnp.float32)
        target[place, :] = total.astype(target.dtype)
        return carry

    lax.fori_loop(0, rows // step, body, 0)


def chunked(first, last, copies_of, body):
    for copy in copies_of(first, first % 2):
        copy.start()

    def step(n, carry):
        slot = lax.rem(n, 2)

        @pl.when(n + 1 < last)
        def ahead():
            for copy in copies_of(n + 1, 1 - slot):
                copy.start()

        for copy in copies_of(n, slot):
            copy.wait()
        body(n, slot)
        return carry

    lax.fori_loop(first, last, step, 0)


def reduce_kernel(
    norm, dcat, x_all, mean, inverse, attn, hidden, dy, cat_w, dense_w, down_w, sums,
    cat_out, dense_out, down_out, mixed_out, norm_out, sums_out,
    cat_part, down_part, dense_part, cat_in, down_in, dense_in,
    tokens, token_in, token_line, token_last, sum_buf,
    wide, attn_turned, norm_chunk, norm_turned, cat_chunk, x_chunk, down_chunk, dense_chunk, dy_chunk,
    send_sems, near_sem, pass_sem, group_sem, core_sem, line_sem, sum_sem, local_sem, chunk_sem,
):
    PASS, KEEP, LAST = range(3)
    net = Wires(send_sems)
    plane, core, shard, shards, group, mine = net.plane, net.core, net.shard, net.shards, net.group, net.mine
    planes = cat_part.shape[0]
    partner = (plane, 1 - core, shard)
    order = sorted(range(group), key=lambda mask: (mask % shards, mask // shards), reverse=True)
    rows, width = dcat.shape
    model = norm.shape[1]
    block = cat_part.shape[2]
    token_rows = tokens.shape[2]
    units_here = hidden.shape[1]
    heads_here = attn.shape[1]
    lane = 256

    def dot(a, b, a_dim=1, b_dim=0):
        return lax.dot_general(a, b, (((a_dim,), (b_dim,)), ((), ())), preferred_element_type=jnp.float32)

    def columns(n):
        return pl.ds(pl.multiple_of(n * lane, lane), lane)

    units = [(cat_part, cat_in, mask) for mask in order]
    units += [(down_part, down_in, part) for part in range(down_part.shape[1])]
    units += [(dense_part, dense_in, part) for part in range(dense_part.shape[1])]
    down_rows, dense_rows = down_part.shape[2], dense_part.shape[2]

    def ways(index):
        return (net.first, net.second, 1, 2) if index % 2 == 0 else (net.second, net.first, 2, 1)

    def send_pass(index):
        parts, came, slot = units[index]
        net.send(parts.at[3, slot], came.at[PASS, slot], pass_sem.at[0, index], ways(index)[0])

    def send_keep(index):
        parts, came, slot = units[index]
        near, far, near_mask, far_mask = ways(index)
        net.send(parts.at[near_mask, slot], came.at[KEEP, slot], near_sem.at[index], near)

    locals_ = {}

    def local(key, source, target):
        locals_[key] = pltpu.make_async_copy(source, target, local_sem.at[len(locals_)])
        locals_[key].start()

    local("dcat", dcat, wide.at[:, pl.ds(0, width)])
    net.barrier()

    plane_rows = group * block

    def norm_copy(turn, distance):
        place = pl.ds(pl.multiple_of((plane ^ distance) * plane_rows, plane_rows), plane_rows)
        return pltpu.make_async_copy(
            norm.at[:, place], norm_chunk.at[turn % 2], chunk_sem.at[0, turn % 2]
        )

    cats, every = range(group), range(len(units))
    turns = (3, 1, 2, 0)
    norm_copy(0, turns[0]).start()
    locals_["dcat"].wait()
    for turn, distance in enumerate(turns):
        if turn + 1 < planes:
            norm_copy(turn + 1, turns[turn + 1]).start()
        norm_copy(turn, distance).wait()
        norm_turned[...] = norm_chunk[turn % 2].T

        def cat_step(n, carry, distance=distance):
            total = dot(norm_turned[...], wide[:, columns(n)]).astype(jnp.bfloat16)
            for member in range(group):
                cat_part[distance, mine ^ member, :, columns(n)] = total[member * block : (member + 1) * block]
            return carry

        lax.fori_loop(0, width // lane, cat_step, 0)
        for index in cats:
            if distance == 3:
                send_pass(index)
            elif distance == ways(index)[2]:
                send_keep(index)

    sum_buf[4] = sums[...]
    gain_row = width // 128

    def norm_copies(n, slot):
        return [
            pltpu.make_async_copy(cat_w.at[columns(n), :], cat_chunk.at[slot], chunk_sem.at[1, slot]),
            pltpu.make_async_copy(x_all.at[:, columns(n)], x_chunk.at[slot], chunk_sem.at[2, slot]),
        ]

    def norm_step(n, slot):
        total = dot(wide[:, pl.ds(0, width)], cat_chunk[slot], 1, 1)
        x_hat = (x_chunk[slot].astype(jnp.float32) - mean[...]) * inverse[...]
        gain = jnp.sum(total * x_hat, axis=0, keepdims=True)
        shift = jnp.sum(total, axis=0, keepdims=True)
        for half in range(lane // 128):
            row = gain_row + n * (lane // 128) + half
            sum_buf[4, pl.ds(row, 1), :] = gain[:, half * 128 : (half + 1) * 128]
            sum_buf[4, pl.ds(row + model // 128, 1), :] = shift[:, half * 128 : (half + 1) * 128]
        for member in range(group):
            tokens[1, member, :, columns(n)] = total[member * token_rows : (member + 1) * token_rows].astype(
                jnp.bfloat16
            )

    chunked(0, model // lane, norm_copies, norm_step)

    places = [place for rank in range(shards // 2) for place in (shards - 1 - rank, rank)]

    def to_partner(stream):
        for place in places:
            net.send(
                tokens.at[stream, (1 - core) * shards + place],
                token_in.at[stream, place],
                core_sem.at[stream, place],
                partner,
            )

    net.send(sum_buf.at[4], sum_buf.at[0], sum_sem.at[0], net.first)
    to_partner(1)

    local("hidden", hidden, wide.at[:, pl.ds(0, units_here)])
    local("attn", attn, wide.at[:, pl.ds(2 * units_here, heads_here)])

    def own(stream, place):
        return tokens.at[stream, core * shards + place]

    def chain(stream, hop, rank):
        for upward in (True, False):
            target = shards - 1 - rank if upward else rank
            here = hop if upward else shards - 1 - hop
            sems = line_sem.at[0 if upward else 1]
            came = token_line.at[stream, target]
            total = own(stream, target)
            holds = shard == here
            if hop:
                net.arrived(came, sems.at[stream, target], holds)

            @pl.when(holds)
            def add(target=target, came=came, total=total):
                add_rows(total, total, token_in.at[stream, target], *([came] if hop else []))

            there = jnp.clip(shard + (1 if upward else -1), 0, shards - 1)
            ends = (not upward) and rank == shards - 2 - hop
            landing = token_last.at[stream] if ends else came
            net.send(total, landing, sems.at[stream, target], (plane, core, there), holds)

    def final(stream):
        for place in range(shards):
            holds = shard == place
            values = [own(stream, place), token_in.at[stream, place]]
            for landing, side, present in (
                (token_line.at[stream, place], line_sem.at[0], place > 0),
                (token_last.at[stream], line_sem.at[1], place < shards - 1),
            ):
                if present:
                    values.append(landing)
                    net.arrived(landing, side.at[stream, place], holds)

            @pl.when(holds)
            def add(values=values):
                add_rows((mixed_out, norm_out)[stream], *values)

    locals_["hidden"].wait()
    locals_["attn"].wait()
    turned = pl.ds(units_here, rows)
    wide[:, turned] = wide[:, pl.ds(0, units_here)].T
    attn_turned[...] = wide[:, pl.ds(2 * units_here, heads_here)].T

    def out_copies(n, slot):
        return [
            pltpu.make_async_copy(down_w.at[:, columns(n)], down_chunk.at[slot], chunk_sem.at[3, slot]),
            pltpu.make_async_copy(dense_w.at[:, columns(n)], dense_chunk.at[slot], chunk_sem.at[4, slot]),
            pltpu.make_async_copy(dy.at[:, columns(n)], dy_chunk.at[slot], chunk_sem.at[5, slot]),
        ]

    def out_step(n, slot):
        total = dot(wide[:, pl.ds(0, units_here)], down_chunk[slot]) + dot(
            wide[:, pl.ds(2 * units_here, heads_here)], dense_chunk[slot]
        )
        for member in range(group):
            tokens[0, member, :, columns(n)] = total[member * token_rows : (member + 1) * token_rows].astype(
                jnp.bfloat16
            )
        for parts, left in ((down_part, wide[:, turned]), (dense_part, attn_turned[...])):
            grad = dot(left, dy_chunk[slot]).astype(jnp.bfloat16)
            pieces, size = parts.shape[1], parts.shape[2]
            for q in range(planes):
                for piece in range(pieces):
                    start = (q * pieces + piece) * size
                    parts[plane ^ q, piece, :, columns(n)] = grad[start : start + size]

    half = model // lane // 2
    chunked(0, half, out_copies, out_step)
    for place in places:
        net.arrived(token_in.at[1, place], core_sem.at[1, place])
    for rank in range(shards - 1):
        chain(1, 0, rank)
    chunked(half, 2 * half, out_copies, out_step)
    to_partner(0)

    def pass_on(index):
        parts, came, slot = units[index]
        near, far, near_mask, far_mask = ways(index)
        total = parts.at[far_mask, slot]
        net.arrived(came.at[PASS, slot], pass_sem.at[0, index])
        add_rows(total, total, came.at[PASS, slot])
        net.send(total, came.at[LAST, slot], pass_sem.at[1, index], far)

    def finish(index):
        parts, came, slot = units[index]
        total = parts.at[0, slot]
        net.arrived(came.at[KEEP, slot], near_sem.at[index])
        net.arrived(came.at[LAST, slot], pass_sem.at[1, index])
        values = (total, came.at[KEEP, slot], came.at[LAST, slot])
        if index < group:
            add_rows(total, *values)
            if slot:
                net.send(total, cat_out.at[mine], group_sem.at[0, slot], net.member(mine ^ slot))
            else:
                local("own", total, cat_out.at[mine])
        elif parts is down_part:
            add_rows(down_out.at[pl.ds(slot * down_rows, down_rows)], *values)
        else:
            add_rows(dense_out.at[pl.ds(slot * dense_rows, dense_rows)], *values)

    for index in every[group:]:
        send_pass(index)
        send_keep(index)
    net.arrived(sum_buf.at[0], sum_sem.at[0])
    sum_buf[1] = sum_buf[4] + sum_buf[0]
    net.send(sum_buf.at[1], sum_buf.at[2], sum_sem.at[1], net.second)
    for index in cats[:2]:
        pass_on(index)
    for place in places:
        net.arrived(token_in.at[0, place], core_sem.at[0, place])
    for rank in range(shards - 1):
        chain(0, 0, rank)
    later = [
        (stream, hop, rank)
        for hop, rank in sorted(
            ((hop, rank) for hop in range(1, shards - 1) for rank in range(shards - 1 - hop)),
            key=lambda pair: (pair[0] + 2 * pair[1], pair[0]),
        )
        for stream in (1, 0)
    ]
    later.sort(key=lambda item: -item[0])
    for index in cats[2:]:
        pass_on(index)
        if index % 2 and later:
            chain(*later.pop(0))
    net.arrived(sum_buf.at[2], sum_sem.at[1])
    sum_buf[3] = sum_buf[1] + sum_buf[2]
    for mask in range(1, group):
        net.send(sum_buf.at[3], sums_out.at[mine], group_sem.at[1, mask], net.member(mine ^ mask))
    local("sums", sum_buf.at[3], sums_out.at[mine])
    for index in cats[: group - 2]:
        finish(index)
        if later:
            chain(*later.pop(0))
    while later:
        chain(*later.pop(0))
    for index in every[group:]:
        pass_on(index)
    for index in cats[group - 2 :]:
        finish(index)
    for stream in (1, 0):
        final(stream)
    for index in every[group:]:
        finish(index)
    for mask in range(1, group):
        net.arrived(cat_out.at[mine ^ mask], group_sem.at[0, mask])
        net.arrived(sums_out.at[mine ^ mask], group_sem.at[1, mask])
    locals_["own"].wait()
    locals_["sums"].wait()
    net.drain()


def reduce_wires(norm, dcat, x_all, mean, inverse, attn, hidden, dy, cat_w, dense_w, down_w, sums):
    planes, shards = lax.axis_size("plane"), lax.axis_size("shard")
    group = lax.axis_size("core") * shards
    units = group + 6
    rows, width = dcat.shape
    model = norm.shape[1]
    block = model // (planes * group)
    unit_rows, head_rows = down_w.shape[0] // planes, dense_w.shape[0] // planes
    token_rows = rows // group
    vmem = pl.BlockSpec(memory_space=pltpu.VMEM)
    hbm = pl.BlockSpec(memory_space=pl.ANY)
    dma = pltpu.SemaphoreType.DMA
    lane = 256

    def scratch(*shape, dtype=jnp.bfloat16):
        return pltpu.VMEM(shape, dtype)

    return pl.pallas_call(
        reduce_kernel,
        in_specs=[hbm] * 3 + [vmem] * 2 + [hbm] * 6 + [vmem],
        out_specs=[hbm] + [vmem] * 4 + [hbm],
        out_shape=[
            jax.ShapeDtypeStruct((group, block, width), jnp.bfloat16),
            jax.ShapeDtypeStruct((head_rows, model), jnp.float32),
            jax.ShapeDtypeStruct((unit_rows, model), jnp.float32),
            jax.ShapeDtypeStruct((token_rows, model), jnp.float32),
            jax.ShapeDtypeStruct((token_rows, model), jnp.float32),
            jax.ShapeDtypeStruct((group,) + sums.shape, sums.dtype),
        ],
        scratch_shapes=[
            scratch(planes, group, block, width),
            scratch(planes, 4, unit_rows // 4, model),
            scratch(planes, 2, head_rows // 2, model),
            scratch(3, group, block, width),
            scratch(3, 4, unit_rows // 4, model),
            scratch(3, 2, head_rows // 2, model),
            scratch(2, group, token_rows, model),
            scratch(2, shards, token_rows, model),
            scratch(2, shards, token_rows, model),
            scratch(2, token_rows, model),
            scratch(5, *sums.shape, dtype=jnp.float32),
            scratch(rows, hidden.shape[1] + rows + attn.shape[1]),
            scratch(attn.shape[1], rows),
            scratch(2, rows, group * block),
            scratch(group * block, rows),
            scratch(2, lane, width),
            scratch(2, rows, lane),
            scratch(2, hidden.shape[1], lane),
            scratch(2, attn.shape[1], lane),
            scratch(2, rows, lane),
            dma((2 + 2 * shards + 2 * shards * (shards - 1) + 3 * units + 2 * (group - 1),)),
            dma((units,)),
            dma((2, units)),
            dma((2, group)),
            dma((2, shards)),
            dma((2, 2, shards)),
            dma((2,)),
            dma((5,)),
            dma((6, 2)),
        ],
        compiler_params=pltpu.CompilerParams(
            collective_id=1, has_side_effects=True, vmem_limit_bytes=67043328
        ),
    )(norm, dcat, x_all, mean, inverse, attn, hidden, dy, cat_w, dense_w, down_w, sums)


def fast_body(
    hidden_in,
    segment_ids,
    out_grad,
    qkv_weight_state,
    qkv_bias_state,
    dense_weight_state,
    up_weight_state,
    up_bias_state,
    down_weight_state,
    vector_state,
):
    planes, cores, shards = lax.axis_size("plane"), lax.axis_size("core"), lax.axis_size("shard")
    plane, core, shard = lax.axis_index("plane"), lax.axis_index("core"), lax.axis_index("shard")
    group = cores * shards
    owner = (plane * cores + core) * shards + shard
    owners = planes * group
    model_rows = qkv_weight_state.shape[1]
    unit_rows = down_weight_state.shape[1]
    tokens_here = hidden_in.shape[1]
    head_width = planes * HD
    unit_width = planes * unit_rows
    qkv_count, upb_count = qkv_bias_state.shape[1], up_bias_state.shape[1]

    tokens, cotangent, q_seg = hidden_in[0], out_grad[0], segment_ids[0]
    vec_list = [
        qkv_bias_state[0],
        up_bias_state[0],
        vector_state[0].T.reshape(-1),
        q_seg.astype(jnp.float32),
    ]
    vec_sizes = [value.size for value in vec_list]
    vec_rows = -(-sum(vec_sizes) // 1024) * 8
    vec_own = jnp.pad(jnp.concatenate(vec_list), (0, vec_rows * 128 - sum(vec_sizes))).reshape(vec_rows, 128)

    cat_w, dense_w, down_w, x_all, dy_all, vec_all = gather_wires(
        qkv_weight_state,
        up_weight_state,
        dense_weight_state,
        down_weight_state,
        tokens,
        cotangent,
        vec_own,
    )

    cat_w = cat_w.reshape(D, 3 * head_width + unit_width)
    dense_w = dense_w.reshape(head_width, D)
    down_w = down_w.reshape(unit_width, D)
    rows = group * tokens_here
    x_all = x_all.reshape(rows, D)
    dy_all = dy_all.reshape(rows, D)
    vec_flat = vec_all.reshape(planes, cores, shards, vec_rows * 128)
    at = [0]
    for size in vec_sizes:
        at.append(at[-1] + size)

    def rounded(value):
        return value.astype(jnp.bfloat16).astype(jnp.float32)

    qkv_bias = rounded(vec_flat[..., at[0] : at[1]]).reshape(3, planes, cores, shards, HD)
    qkv_bias = lax.dynamic_index_in_dim(
        qkv_bias.transpose(2, 3, 0, 1, 4).reshape(group, 3 * head_width), core * shards + shard, 0, False
    )
    up_bias = lax.dynamic_index_in_dim(
        rounded(vec_flat[..., at[1] : at[2]]).transpose(1, 2, 0, 3).reshape(group, unit_width),
        core * shards + shard,
        0,
        False,
    )
    vec_columns = (
        rounded(vec_flat[..., at[2] : at[3]])
        .reshape(owners, 4, model_rows)
        .transpose(1, 0, 2)
        .reshape(4, D)
    )
    norm_gain, norm_shift, dense_bias, down_bias = (vec_columns[index] for index in range(4))
    segments = lax.dynamic_index_in_dim(vec_flat[..., at[3] : at[4]], plane, 0, False)
    segments = segments.astype(jnp.int32).reshape(cores, shards * tokens_here)
    cat_bias = jnp.concatenate([qkv_bias, up_bias])

    x_float = x_all.astype(jnp.float32)
    x_mean = jnp.mean(x_float, axis=-1, keepdims=True)
    center = x_float - x_mean
    inverse = lax.rsqrt(jnp.mean(center * center, axis=-1, keepdims=True) + norm_eps)
    x_hat = center * inverse
    norm_bf = (x_hat * norm_gain + norm_shift).astype(jnp.bfloat16)

    fu = jnp.dot(norm_bf, cat_w, preferred_element_type=jnp.float32) + cat_bias
    pre_act = fu[:, 3 * head_width :]
    hidden = gelu_tanh(pre_act).astype(jnp.bfloat16)
    grad_hidden = jnp.dot(dy_all, down_w.T, preferred_element_type=jnp.float32)
    grad_pre = jax.vjp(gelu_tanh, pre_act)[1](grad_hidden)[0]
    upb_part = jnp.sum(grad_pre, axis=0)
    grad_heads = jnp.dot(dy_all, dense_w.T, preferred_element_type=jnp.float32).astype(jnp.bfloat16)
    attn, dcat, qkvb_part = attention(fu, grad_heads, grad_pre.astype(jnp.bfloat16), segments)
    bias_part = jnp.sum(cotangent.astype(jnp.float32), axis=0)
    nothing = jnp.zeros((D,), jnp.float32)
    sums = [qkvb_part, upb_part, nothing, nothing, bias_part]
    sum_sizes = [value.size for value in sums]
    sum_rows = -(-sum(sum_sizes) // 1024) * 8
    sums = jnp.pad(jnp.concatenate(sums), (0, sum_rows * 128 - sum(sum_sizes))).reshape(sum_rows, 128)

    cat_sum, dense_grad, down_grad, mixed, grad_norm, sums_all = reduce_wires(
        norm_bf,
        dcat,
        x_all,
        x_mean,
        inverse,
        attn,
        hidden,
        dy_all,
        cat_w,
        dense_w,
        down_w,
        sums,
    )

    sums_flat = sums_all.reshape(cores, shards, sum_rows * 128)
    at = [0]
    for size in sum_sizes:
        at.append(at[-1] + size)
    qkvb_grad = (
        sums_flat[..., : at[1]]
        .reshape(cores, shards, 3, planes, HD)
        .transpose(2, 3, 0, 1, 4)
        .reshape(owners, qkv_count)
    )
    qkvb_grad = lax.dynamic_index_in_dim(qkvb_grad, owner, 0, False)
    upb_grad = sums_flat[..., at[1] : at[2]].reshape(group, planes, upb_count)
    upb_grad = lax.dynamic_index_in_dim(
        lax.dynamic_index_in_dim(upb_grad, core * shards + shard, 0, False), plane, 0, False
    )
    vec_grad = jnp.sum(sums_flat[..., at[2] : at[5]], axis=(0, 1)).reshape(3, owners, model_rows)
    vec_grad = lax.dynamic_index_in_dim(vec_grad, owner, 1, False)
    vec_grad = jnp.stack([vec_grad[0], vec_grad[1], vec_grad[2], vec_grad[2]], axis=1)

    x_own = tokens.astype(jnp.float32)
    output = (x_own + (mixed.astype(jnp.float32) + dense_bias + down_bias)).astype(jnp.bfloat16)
    own_center = x_own - jnp.mean(x_own, axis=-1, keepdims=True)
    own_inverse = lax.rsqrt(jnp.mean(own_center * own_center, axis=-1, keepdims=True) + norm_eps)
    own_hat = own_center * own_inverse
    hat_grad = grad_norm.astype(jnp.float32) * norm_gain
    x_grad = own_inverse * (
        hat_grad
        - jnp.mean(hat_grad, axis=-1, keepdims=True)
        - own_hat * jnp.mean(hat_grad * own_hat, axis=-1, keepdims=True)
    )
    input_grad = cotangent.astype(jnp.float32) + x_grad

    new, qkv_grad, up_grad = owner_update(
        (qkv_weight_state, dense_weight_state, up_weight_state, down_weight_state),
        cat_sum,
        (dense_grad, down_grad),
        (qkv_bias_state, up_bias_state, vector_state),
        (qkvb_grad, upb_grad, vec_grad),
        (planes, cores, shards),
    )
    return (
        output[None],
        input_grad[None],
        qkv_grad,
        qkvb_grad,
        dense_grad,
        up_grad,
        upb_grad,
        down_grad,
        vec_grad,
        *new,
    )


def fast_solution(mesh):
    rep, shard = mesh.shape["rep"], mesh.shape["shard"]
    inner = Mesh(mesh.devices.reshape(rep // 2, 2, shard), ("plane", "core", "shard"))
    both = ("plane", "core")
    every = ("plane", "core", "shard")
    in_specs = (
        P(both, "shard", None),
        P(both, "shard"),
        P(both, "shard", None),
        P(None, every, None),
        P(None, every),
        P(None, every, None),
        P(None, every, None),
        P(None, every),
        P(None, every, None),
        P(None, every, None),
    )
    out_specs = (
        P(both, "shard", None),
        P(both, "shard", None),
        P(every, None),
        P(every),
        P(every, None),
        P(every, None),
        P(every),
        P(every, None),
        P(every, None),
        P(both, "shard", None),
        P(both, "shard", None),
        P(both, "shard", None),
    )
    return jax.shard_map(fast_body, mesh=inner, in_specs=in_specs, out_specs=out_specs, check_vma=False)


def solution(mesh):
    in_specs = (
        P("rep", "shard", None),
        P("rep", "shard"),
        P("rep", "shard", None),
        P(None, ("rep", "shard"), None),
        P(None, ("rep", "shard")),
        P(None, ("rep", "shard"), None),
        P(None, ("rep", "shard"), None),
        P(None, ("rep", "shard")),
        P(None, ("rep", "shard"), None),
        P(None, ("rep", "shard"), None),
    )
    out_specs = (
        P("rep", "shard", None),
        P("rep", "shard", None),
        P(("rep", "shard"), None),
        P(("rep", "shard")),
        P(("rep", "shard"), None),
        P(("rep", "shard"), None),
        P(("rep", "shard")),
        P(("rep", "shard"), None),
        P(("rep", "shard"), None),
        P("rep", "shard", None),
        P("rep", "shard", None),
        P("rep", "shard", None),
    )
    if whole_heads(mesh):
        return fast_solution(mesh)
    return jax.shard_map(body, mesh=mesh, in_specs=in_specs, out_specs=out_specs, check_vma=False)
```

```python
from functools import partial
import math

import jax
import jax.numpy as jnp
from jax import lax
from jax.experimental import pallas as pl
from jax.experimental.pallas import tpu as pltpu
from jax.sharding import Mesh
from jax.sharding import PartitionSpec as P

D = 2048
HD = 64
ROT = 32
FF = 8192
STEP = 5


learn_rate = 0.02
beta_one = 0.9
beta_two = 0.95
adam_eps = 1e-08
weight_decay = 0.1
norm_eps = 1e-05
big_negative = -1e30


def layer_norm(x, norm_gain, norm_shift):
    center = x - jnp.mean(x, axis=-1, keepdims=True)
    variance = jnp.mean(center * center, axis=-1, keepdims=True)
    return center * lax.rsqrt(variance + norm_eps) * norm_gain + norm_shift


def gelu_tanh(v):
    return 0.5 * v * (1.0 + jnp.tanh(0.7978845608028654 * (v + 0.044715 * v * v * v)))


def rotary(x, positions):
    half_rot = ROT // 2
    frequency = jnp.exp(jnp.arange(half_rot, dtype=jnp.float32) * (-2.0 * math.log(10000.0) / ROT))
    angles = positions.astype(jnp.float32)[:, None] * frequency[None, :]
    cosine = jnp.cos(angles)[:, None, :]
    sine_val = jnp.sin(angles)[:, None, :]
    lower_part = x[..., :half_rot]
    upper_part = x[..., half_rot:ROT]
    return jnp.concatenate(
        [
            lower_part * cosine - upper_part * sine_val,
            upper_part * cosine + lower_part * sine_val,
            x[..., ROT:],
        ],
        axis=-1,
    )


def adam_update(state, grad):
    moment_one = beta_one * state[1] + (1.0 - beta_one) * grad
    moment_two = beta_two * state[2] + (1.0 - beta_two) * grad * grad
    corrected = moment_one / (1.0 - beta_one**STEP)
    divisor = jnp.sqrt(moment_two / (1.0 - beta_two**STEP)) + adam_eps
    weight = state[0] - learn_rate * (corrected / divisor + weight_decay * state[0])
    return jnp.stack([weight, moment_one, moment_two])


def owner_entries(new_states, entry):
    return jnp.concatenate(
        [state_new[entry].reshape(-1) for state_new in new_states], axis=0
    ).reshape(1, 1, -1)


def block_mask(q_pos, q_seg, k_pos, k_seg):
    return (k_pos[None, :] <= q_pos[:, None]) & (k_seg[None, :] == q_seg[:, None])


def attend_keys(kv_all, seg_all, queries, q_pos, q_seg):
    key_count = kv_all.shape[0]
    width = kv_all.shape[1] // 2
    heads_here = queries.shape[1]
    query_rows = queries.shape[0]
    block_rows = math.gcd(key_count, 512)
    block_count = key_count // block_rows
    kv_blocks = kv_all.reshape(block_count, block_rows, 2 * width)
    seg_blocks = seg_all.reshape(block_count, block_rows)
    score_scale = 1.0 / math.sqrt(HD)

    def attend_step_block(carry, block_items):
        kv_rows, seg_rows, block_index = block_items
        row_max, totals, accumulated = carry
        key_rows = kv_rows[:, :width].reshape(block_rows, heads_here, HD)
        value_rows = kv_rows[:, width:].reshape(block_rows, heads_here, HD)
        k_pos = block_index * block_rows + jnp.arange(block_rows, dtype=jnp.int32)
        allowed = block_mask(q_pos, q_seg, k_pos, seg_rows)
        scores = (
            jnp.einsum("qhd,khd->hqk", queries, key_rows, preferred_element_type=jnp.float32)
            * score_scale
        )
        scores = jnp.where(allowed[None], scores, big_negative)
        new_max = jnp.maximum(row_max, jnp.max(scores, axis=-1))
        probabilities = jnp.where(allowed[None], jnp.exp(scores - new_max[..., None]), 0.0)
        factor = jnp.exp(row_max - new_max)
        totals = totals * factor + jnp.sum(probabilities, axis=-1)
        accumulated = accumulated * factor[..., None] + jnp.einsum(
            "hqk,khd->hqd",
            probabilities.astype(jnp.bfloat16),
            value_rows,
            preferred_element_type=jnp.float32,
        )
        return ((new_max, totals, accumulated), None)

    start_state = (
        jnp.full((heads_here, query_rows), big_negative, jnp.float32),
        jnp.zeros((heads_here, query_rows), jnp.float32),
        jnp.zeros((heads_here, query_rows, HD), jnp.float32),
    )
    running, unused = lax.scan(
        attend_step_block,
        start_state,
        (kv_blocks, seg_blocks, jnp.arange(block_count, dtype=jnp.int32)),
    )
    return running


def attention_grads(queries, kv_all, seg_all, q_pos, q_seg, grad_heads, delta_all, lse_all):
    key_count = kv_all.shape[0]
    width = kv_all.shape[1] // 2
    heads_here = queries.shape[1]
    query_rows = queries.shape[0]
    block_rows = math.gcd(key_count, 512)
    block_count = key_count // block_rows
    kv_blocks = kv_all.reshape(block_count, block_rows, 2 * width)
    seg_blocks = seg_all.reshape(block_count, block_rows)
    score_scale = 1.0 / math.sqrt(HD)

    def attention_step_block(query_grad, block_items):
        kv_rows, seg_rows, block_index = block_items
        key_rows = kv_rows[:, :width].reshape(block_rows, heads_here, HD)
        value_rows = kv_rows[:, width:].reshape(block_rows, heads_here, HD)
        k_pos = block_index * block_rows + jnp.arange(block_rows, dtype=jnp.int32)
        allowed = block_mask(q_pos, q_seg, k_pos, seg_rows)
        scores = (
            jnp.einsum("qhd,khd->hqk", queries, key_rows, preferred_element_type=jnp.float32)
            * score_scale
        )
        scores = jnp.where(allowed[None], scores, big_negative)
        probabilities = jnp.where(allowed[None], jnp.exp(scores - lse_all[..., None]), 0.0)
        value_grad = jnp.einsum(
            "hqk,qhd->khd",
            probabilities.astype(jnp.bfloat16),
            grad_heads,
            preferred_element_type=jnp.float32,
        )
        prob_grad = jnp.einsum(
            "qhd,khd->hqk", grad_heads, value_rows, preferred_element_type=jnp.float32
        )
        score_grad = (probabilities * (prob_grad - delta_all[..., None]) * score_scale).astype(
            jnp.bfloat16
        )
        query_grad = query_grad + jnp.einsum(
            "hqk,khd->hqd", score_grad, key_rows, preferred_element_type=jnp.float32
        )
        key_grad = jnp.einsum(
            "hqk,qhd->khd", score_grad, queries, preferred_element_type=jnp.float32
        )
        return (
            query_grad,
            jnp.concatenate(
                [key_grad.reshape(block_rows, width), value_grad.reshape(block_rows, width)], axis=1
            ),
        )

    query_grad, kv_grad_blocks = lax.scan(
        attention_step_block,
        jnp.zeros((heads_here, query_rows, HD), jnp.float32),
        (kv_blocks, seg_blocks, jnp.arange(block_count, dtype=jnp.int32)),
    )
    return (query_grad, kv_grad_blocks.reshape(key_count, 2 * width))


def gather_vectors(own_qkvb, own_upb, own_vec):
    return (
        lax.all_gather(own_qkvb, ("rep", "shard"), axis=0, tiled=True),
        lax.all_gather(own_upb, ("rep", "shard"), axis=0, tiled=True),
        lax.all_gather(own_vec, ("rep", "shard"), axis=0, tiled=True),
    )


def sum_vectors(qkvb_grad, upb_grad, vec_grad):
    return (
        lax.psum_scatter(qkvb_grad, ("rep", "shard"), scatter_dimension=0, tiled=True),
        lax.psum_scatter(upb_grad, ("rep", "shard"), scatter_dimension=0, tiled=True),
        lax.psum_scatter(vec_grad, ("rep", "shard"), scatter_dimension=0, tiled=True),
    )


def sum_positions(partial_rows):
    return lax.psum_scatter(partial_rows, "shard", scatter_dimension=0, tiled=True)


def attention_pass(norm_rows, qkv_w, qkv_b, positions, key_width):
    row_count = norm_rows.shape[0]
    heads_here = key_width // HD
    joined = jnp.dot(norm_rows, qkv_w, preferred_element_type=jnp.float32) + qkv_b
    q_pre = joined[:, :key_width].reshape(row_count, heads_here, HD)
    k_pre = joined[:, key_width : 2 * key_width].reshape(row_count, heads_here, HD)
    queries = rotary(q_pre, positions).astype(jnp.bfloat16)
    key_local = rotary(k_pre, positions).astype(jnp.bfloat16).reshape(row_count, key_width)
    value_local = joined[:, 2 * key_width :].astype(jnp.bfloat16)
    kv_local = jnp.concatenate([key_local, value_local], axis=1)
    return (q_pre, k_pre, queries, kv_local)


def finish_qkv_grad(q_pre, k_pre, positions, query_grad, kv_grad, key_width):
    row_count = q_pre.shape[0]
    heads_here = key_width // HD
    rotate_back = partial(rotary, positions=positions)
    query_pre = jax.vjp(rotate_back, q_pre)[1](query_grad.transpose(1, 0, 2))[0]
    key_pre = jax.vjp(rotate_back, k_pre)[1](
        kv_grad[:, :key_width].reshape(row_count, heads_here, HD)
    )[0]
    return jnp.concatenate(
        [
            query_pre.reshape(row_count, key_width),
            key_pre.reshape(row_count, key_width),
            kv_grad[:, key_width:],
        ],
        axis=1,
    )


def sliced_pass(norm_bf, q_seg, cotangent, own_mats, qkv_bb, up_bb):
    own_qkv, own_dense, own_up, own_down = own_mats
    inner_count = lax.axis_size("shard")
    outer_count = lax.axis_size("rep")
    stride = outer_count // inner_count
    place = lax.axis_index("shard")
    head_width = D // inner_count
    unit_width = FF // inner_count
    qkv_rows = own_qkv.shape[0]
    dense_rows = own_dense.shape[0]
    down_rows = own_down.shape[0]
    qkv_split = own_qkv.reshape(qkv_rows, 3, inner_count, head_width)
    up_split = own_up.reshape(qkv_rows, 1, inner_count, unit_width)
    qkv_cols, up_cols = (
        lax.all_to_all(qkv_split, "shard", split_axis=2, concat_axis=0, tiled=True),
        lax.all_to_all(up_split, "shard", split_axis=2, concat_axis=0, tiled=True),
    )
    qkv_rep, up_rep, dense_rep, down_rep = (
        lax.all_gather(qkv_cols, "rep", axis=0, tiled=True),
        lax.all_gather(up_cols, "rep", axis=0, tiled=True),
        lax.all_gather(own_dense[None], "rep", axis=0, tiled=True),
        lax.all_gather(own_down[None], "rep", axis=0, tiled=True),
    )
    dense_grid = dense_rep.reshape(inner_count, stride, 1, dense_rows, D)
    down_grid = down_rep.reshape(inner_count, stride, 1, down_rows, D)
    dense_moved, down_moved = (
        lax.all_to_all(dense_grid, "shard", split_axis=0, concat_axis=2, tiled=True),
        lax.all_to_all(down_grid, "shard", split_axis=0, concat_axis=2, tiled=True),
    )
    qkv_w = qkv_rep.reshape(D, 3 * head_width)
    up_w = up_rep.reshape(D, unit_width)
    dense_w = dense_moved.reshape(head_width, D)
    down_w = down_moved.reshape(unit_width, D)
    qkv_b = lax.dynamic_index_in_dim(
        qkv_bb.astype(jnp.float32).reshape(3, inner_count, head_width), place, 1, False
    ).reshape(3 * head_width)
    up_b = lax.dynamic_slice_in_dim(up_bb.astype(jnp.float32), place * unit_width, unit_width, 0)
    norm_seq, grad_seq, seg_seq = (
        lax.all_gather(norm_bf, "shard", axis=0, tiled=True),
        lax.all_gather(cotangent, "shard", axis=0, tiled=True),
        lax.all_gather(q_seg, "shard", axis=0, tiled=True),
    )
    seq_rows = norm_seq.shape[0]
    heads_here = head_width // HD
    positions = jnp.arange(seq_rows, dtype=jnp.int32)
    q_pre, k_pre, queries, kv_seq = attention_pass(norm_seq, qkv_w, qkv_b, positions, head_width)
    row_max, totals, accumulated = attend_keys(kv_seq, seg_seq, queries, positions, seg_seq)
    lse_all = row_max + jnp.log(totals)
    out_heads = (accumulated / totals[..., None]).transpose(1, 0, 2).astype(jnp.bfloat16)
    attn_bf = out_heads.reshape(seq_rows, head_width)
    pre_act = jnp.dot(norm_seq, up_w, preferred_element_type=jnp.float32) + up_b
    hidden = gelu_tanh(pre_act).astype(jnp.bfloat16)
    partial_out = jnp.dot(attn_bf, dense_w, preferred_element_type=jnp.float32) + jnp.dot(
        hidden, down_w, preferred_element_type=jnp.float32
    )
    mixed = sum_positions(partial_out)
    grad_down = jnp.dot(hidden.T, grad_seq, preferred_element_type=jnp.float32)
    grad_dense = jnp.dot(attn_bf.T, grad_seq, preferred_element_type=jnp.float32)
    grad_hidden = jnp.dot(grad_seq, down_w.T, preferred_element_type=jnp.float32)
    grad_pre = jax.vjp(gelu_tanh, pre_act)[1](grad_hidden)[0]
    grad_pre_bf = grad_pre.astype(jnp.bfloat16)
    grad_up = jnp.dot(norm_seq.T, grad_pre_bf, preferred_element_type=jnp.float32)
    upb_part = jnp.sum(grad_pre, axis=0)
    norm_part = jnp.dot(grad_pre_bf, up_w.T, preferred_element_type=jnp.float32)
    grad_heads = (
        jnp.dot(grad_seq, dense_w.T, preferred_element_type=jnp.float32)
        .astype(jnp.bfloat16)
        .reshape(seq_rows, heads_here, HD)
    )
    delta_all = jnp.sum(grad_heads.astype(jnp.float32) * out_heads.astype(jnp.float32), axis=-1).T
    query_grad, kv_grad = attention_grads(
        queries, kv_seq, seg_seq, positions, seg_seq, grad_heads, delta_all, lse_all
    )
    grad_joined = finish_qkv_grad(q_pre, k_pre, positions, query_grad, kv_grad, head_width)
    grad_joined_bf = grad_joined.astype(jnp.bfloat16)
    grad_qkv = jnp.dot(norm_seq.T, grad_joined_bf, preferred_element_type=jnp.float32)
    qkvb_part = jnp.sum(grad_joined, axis=0)
    norm_part = norm_part + jnp.dot(grad_joined_bf, qkv_w.T, preferred_element_type=jnp.float32)
    grad_norm = sum_positions(norm_part)
    dense_grid_grad = grad_dense.reshape(1, stride, inner_count, dense_rows, D)
    down_grid_grad = grad_down.reshape(1, stride, inner_count, down_rows, D)
    dense_back, down_back = (
        lax.all_to_all(dense_grid_grad, "shard", split_axis=2, concat_axis=0, tiled=True),
        lax.all_to_all(down_grid_grad, "shard", split_axis=2, concat_axis=0, tiled=True),
    )
    qkv_sum, up_sum, dense_sum, down_sum = (
        lax.psum_scatter(
            grad_qkv.reshape(D, 3, 1, head_width), "rep", scatter_dimension=0, tiled=True
        ),
        lax.psum_scatter(
            grad_up.reshape(D, 1, 1, unit_width), "rep", scatter_dimension=0, tiled=True
        ),
        lax.psum_scatter(
            dense_back.reshape(outer_count, dense_rows, D), "rep", scatter_dimension=0, tiled=True
        ),
        lax.psum_scatter(
            down_back.reshape(outer_count, down_rows, D), "rep", scatter_dimension=0, tiled=True
        ),
    )
    qkv_home, up_home = (
        lax.all_to_all(qkv_sum, "shard", split_axis=0, concat_axis=2, tiled=True),
        lax.all_to_all(up_sum, "shard", split_axis=0, concat_axis=2, tiled=True),
    )
    qkv_own = qkv_home.reshape(qkv_rows, 3 * D)
    up_own = up_home.reshape(qkv_rows, FF)
    dense_own = dense_sum.reshape(dense_rows, D)
    down_own = down_sum.reshape(down_rows, D)
    selector = (jnp.arange(inner_count, dtype=jnp.int32) == place).astype(jnp.float32)
    qkvb_grad = (selector[None, :, None] * qkvb_part.reshape(3, 1, head_width)).reshape(3 * D)
    upb_grad = (selector[:, None] * upb_part[None, :]).reshape(FF)
    return (mixed, grad_norm, (qkv_own, dense_own, up_own, down_own), qkvb_grad, upb_grad)


def body(
    hidden_in,
    segment_ids,
    out_grad,
    qkv_weight_state,
    qkv_bias_state,
    dense_weight_state,
    up_weight_state,
    up_bias_state,
    down_weight_state,
    vector_state,
):
    own_mats = (
        qkv_weight_state[0].astype(jnp.bfloat16),
        dense_weight_state[0].astype(jnp.bfloat16),
        up_weight_state[0].astype(jnp.bfloat16),
        down_weight_state[0].astype(jnp.bfloat16),
    )
    qkv_bb, up_bb, vec_bf = gather_vectors(
        qkv_bias_state[0].astype(jnp.bfloat16),
        up_bias_state[0].astype(jnp.bfloat16),
        vector_state[0].astype(jnp.bfloat16),
    )
    vec_all = vec_bf.astype(jnp.float32)
    norm_gain = vec_all[:, 0]
    norm_shift = vec_all[:, 1]
    dense_bias = vec_all[:, 2]
    down_bias = vec_all[:, 3]
    tokens = hidden_in[0]
    q_seg = segment_ids[0]
    cotangent = out_grad[0]
    x_full = tokens.astype(jnp.float32)
    normed = layer_norm(x_full, norm_gain, norm_shift)
    norm_bf = normed.astype(jnp.bfloat16)
    mixed, grad_norm, owned, qkvb_grad, upb_grad = sliced_pass(
        norm_bf, q_seg, cotangent, own_mats, qkv_bb, up_bb
    )
    qkv_own, dense_own, up_own, down_own = owned
    output = (x_full + (mixed + dense_bias + down_bias)).astype(jnp.bfloat16)
    grad_x, grad_gain, grad_shift = jax.vjp(layer_norm, x_full, norm_gain, norm_shift)[1](grad_norm)
    out_bias_grad = jnp.sum(cotangent.astype(jnp.float32), axis=0)
    grad_vec = jnp.stack([grad_gain, grad_shift, out_bias_grad, out_bias_grad], axis=1)
    input_grad = cotangent.astype(jnp.float32) + grad_x
    qkvb_own, upb_own, vec_own = sum_vectors(qkvb_grad, upb_grad, grad_vec)
    new_states = (
        adam_update(qkv_weight_state, qkv_own),
        adam_update(qkv_bias_state, qkvb_own),
        adam_update(dense_weight_state, dense_own),
        adam_update(up_weight_state, up_own),
        adam_update(up_bias_state, upb_own),
        adam_update(down_weight_state, down_own),
        adam_update(vector_state, vec_own),
    )
    return (
        output[None],
        input_grad[None],
        qkv_own,
        qkvb_own,
        dense_own,
        up_own,
        upb_own,
        down_own,
        vec_own,
        owner_entries(new_states, 0),
        owner_entries(new_states, 1),
        owner_entries(new_states, 2),
    )


def whole_heads(mesh):
    owners = mesh.shape["rep"] * mesh.shape["shard"]
    return D % owners == 0 and D // owners == HD and mesh.shape["rep"] % 2 == 0


def rotation_tables(seq_rows):
    half_rot = ROT // 2
    lane = jnp.arange(2 * HD, dtype=jnp.int32) % HD
    frequency = jnp.exp((lane % half_rot).astype(jnp.float32) * (-2.0 * math.log(10000.0) / ROT))
    angles = jnp.arange(seq_rows, dtype=jnp.int32).astype(jnp.float32)[:, None] * frequency[None, :]
    sine = jnp.sin(angles)
    cosine = jnp.where(lane[None, :] < ROT, jnp.cos(angles), 1.0)
    low = jnp.where(lane[None, :] < half_rot, -sine, 0.0)
    high = jnp.where((lane[None, :] >= half_rot) & (lane[None, :] < ROT), sine, 0.0)
    return cosine, low, high


def attention_kernel(
    fu_ref, do_ref, du_ref, seg_col_ref, seg_row_ref, cos_ref, low_ref, high_ref, o_ref, dcat_ref, sums_ref
):
    rows, width = do_ref.shape
    scale = 1.0 / math.sqrt(HD)
    row_id = lax.broadcasted_iota(jnp.int32, (rows, rows), 0)
    col_id = lax.broadcasted_iota(jnp.int32, (rows, rows), 1)
    allowed = (col_id <= row_id) & (seg_col_ref[...] == seg_row_ref[0])
    cosine, low, high = cos_ref[...], low_ref[...], high_ref[...]
    half = ROT // 2
    lane = lax.broadcasted_iota(jnp.int32, (rows, 2 * HD), 1)

    def rotate(u):
        return (
            u * cosine
            + pltpu.roll(u, 2 * HD - half, 1) * low
            + pltpu.roll(u, half, 1) * high
        )

    def rotate_back(u):
        return (
            u * cosine
            - pltpu.roll(u, 2 * HD - half, 1) * low
            - pltpu.roll(u, half, 1) * high
        )

    def dot(a, b, a_dim, b_dim):
        return lax.dot_general(a, b, (((a_dim,), (b_dim,)), ((), ())), preferred_element_type=jnp.float32)

    zero = jnp.zeros((), jnp.bfloat16)
    for pair in range(width // (2 * HD)):
        lanes = pl.ds(pair * 2 * HD, 2 * HD)
        k_lanes = pl.ds(width + pair * 2 * HD, 2 * HD)
        v_lanes = pl.ds(2 * width + pair * 2 * HD, 2 * HD)
        q = rotate(fu_ref[:, lanes]).astype(jnp.bfloat16)
        k = rotate(fu_ref[:, k_lanes]).astype(jnp.bfloat16)
        v = fu_ref[:, v_lanes].astype(jnp.bfloat16)
        do = do_ref[:, lanes]
        o = dq = dk = dv = None
        for head in range(2):
            mine = (lane < HD) if head == 0 else (lane >= HD)
            qh = jnp.where(mine, q, zero)
            kh = jnp.where(mine, k, zero)
            vh = jnp.where(mine, v, zero)
            doh = jnp.where(mine, do, zero)
            scores = jnp.where(allowed, dot(qh, k, 1, 1) * scale, big_negative)
            row_max = jnp.max(scores, axis=1, keepdims=True)
            probs = jnp.where(allowed, jnp.exp(scores - row_max), 0.0)
            inverse = 1.0 / jnp.sum(probs, axis=1, keepdims=True)
            oh = dot(probs.astype(jnp.bfloat16), vh, 1, 0) * inverse
            delta = jnp.sum(
                doh.astype(jnp.float32) * oh.astype(jnp.bfloat16).astype(jnp.float32), axis=1, keepdims=True
            )
            probs = probs * inverse
            dvh = dot(probs.astype(jnp.bfloat16), doh, 0, 0)
            ds = (probs * (dot(doh, v, 1, 1) - delta) * scale).astype(jnp.bfloat16)
            dqh = dot(ds, kh, 1, 0)
            dkh = dot(ds, qh, 0, 0)
            if head == 0:
                o, dq, dk, dv = oh, dqh, dkh, dvh
            else:
                o, dq, dk, dv = o + oh, dq + dqh, dk + dkh, dv + dvh
        o_ref[:, lanes] = o.astype(jnp.bfloat16)
        dq = rotate_back(dq)
        dk = rotate_back(dk)
        for part, place in ((dq, lanes), (dk, k_lanes), (dv, v_lanes)):
            dcat_ref[:, place] = part.astype(jnp.bfloat16)
            sums_ref[0, :, place] = jnp.sum(part, axis=0, keepdims=True)
    dcat_ref[:, pl.ds(3 * width, du_ref.shape[1])] = du_ref[...]


def attention(fu, do, du, segments):
    count, rows = segments.shape
    width = do.shape[1]
    units = du.shape[1]
    tables = rotation_tables(rows)
    table_spec = pl.BlockSpec((rows, 2 * HD), lambda s: (0, 0))
    o, dcat, sums = pl.pallas_call(
        attention_kernel,
        grid=(count,),
        in_specs=[
            pl.BlockSpec((rows, 3 * width), lambda s: (s, 0)),
            pl.BlockSpec((rows, width), lambda s: (s, 0)),
            pl.BlockSpec((rows, units), lambda s: (s, 0)),
            pl.BlockSpec((rows, 1), lambda s: (s, 0)),
            pl.BlockSpec((1, 1, rows), lambda s: (s, 0, 0)),
            table_spec,
            table_spec,
            table_spec,
        ],
        out_specs=[
            pl.BlockSpec((rows, width), lambda s: (s, 0)),
            pl.BlockSpec((rows, 3 * width + units), lambda s: (s, 0)),
            pl.BlockSpec((1, 1, 3 * width), lambda s: (s, 0, 0)),
        ],
        out_shape=[
            jax.ShapeDtypeStruct((count * rows, width), jnp.bfloat16),
            jax.ShapeDtypeStruct((count * rows, 3 * width + units), jnp.bfloat16),
            jax.ShapeDtypeStruct((count, 1, 3 * width), jnp.float32),
        ],
        compiler_params=pltpu.CompilerParams(vmem_limit_bytes=56 << 20),
        cost_estimate=pl.CostEstimate(
            flops=count * (width // HD) * 10 * rows * rows * HD,
            bytes_accessed=count * rows * (width * 20 + units * 4),
            transcendentals=count * (width // HD) * rows * rows,
        ),
    )(fu, do, du, segments.reshape(count * rows, 1), segments.reshape(count, 1, rows), *tables)
    return o, dcat, jnp.sum(sums, axis=(0, 1))


def adam_values(weight, moment_one, moment_two, grad):
    first = beta_one * moment_one + (1.0 - beta_one) * grad
    second = beta_two * moment_two + (1.0 - beta_two) * grad * grad
    corrected = first * (1.0 / (1.0 - beta_one**STEP))
    divisor = jnp.sqrt(second * (1.0 / (1.0 - beta_two**STEP))) + adam_eps
    return weight - learn_rate * (corrected / divisor + weight_decay * weight), first, second


def owner_update_kernel(plan, small_plan, groups, steps, whole_rows, *refs):
    planes, cores, shards = groups
    qkv_state, dense_state, up_state, down_state, cat_ref, dense_grad, down_grad, small_ref = refs[:8]
    flat = refs[8:11]
    qkv_out, up_out, cat_buf = refs[11:14]
    outs = refs[14:17]
    step_sem, rest_sem = refs[17:]
    step = pl.program_id(0)
    lane = lax.broadcasted_iota(jnp.int32, (8, 128), 1)
    sub = lax.broadcasted_iota(jnp.int32, (8, 128), 0)
    lane_row = lax.broadcasted_iota(jnp.int32, (1, 128), 1)
    wide = 1024

    @pl.when(step == 0)
    def small():
        for source, row, low, high in small_plan:
            for entry in range(3):
                old = outs[entry][pl.ds(row, 1), :]
                new = small_ref[entry, pl.ds(source, 1), :]
                outs[entry][pl.ds(row, 1), :] = jnp.where((lane_row >= low) & (lane_row < high), new, old)

    def widen(piece, carry):
        cat_buf[piece] = cat_ref[piece].astype(jnp.float32)
        return carry

    lax.fori_loop(0, cat_ref.shape[0], widen, 0)

    def place_rows(state, grad_of, rows, tiles, start, shifted, keep=None):
        chunk = min(wide, tiles * 128)

        def one_group(group, carry):
            place = pl.ds(pl.multiple_of(group * 8, 8), 8)
            base = start + (step * (rows // 8) + group) * (8 * tiles)

            def values(column, size):
                lanes = pl.ds(column, size)
                grad = grad_of(place, column, size)
                if keep is not None and size > 128:
                    keep[place, lanes] = grad
                return adam_values(
                    state[0, place, lanes], state[1, place, lanes], state[2, place, lanes], grad
                )

            if shifted:
                last = tuple(pltpu.roll(value, 64, 1) for value in values((tiles - 1) * 128, 128))
                before = tuple(
                    jnp.where(sub == 0, out[pl.ds(base, 1), :], pltpu.roll(value, 1, 0))
                    for out, value in zip(outs, last)
                )
            for column in range(0, tiles * 128, chunk):
                done = values(column, chunk)
                for entry, out in enumerate(outs):
                    for tile in range(chunk // 128):
                        value = done[entry][:, tile * 128 : (tile + 1) * 128]
                        if shifted:
                            value = pltpu.roll(value, 64, 1)
                            old = before[entry] if tile == 0 else now
                            now = value
                            value = jnp.where(lane < 64, old, value)
                        out[pl.ds(base + column // 128 + tile, 8, stride=tiles), :] = value
                    if shifted:
                        before = before[:entry] + (now,) + before[entry + 1 :]
            if shifted:
                for out, value in zip(outs, before):
                    row = pl.ds(base + 8 * tiles, 1)
                    out[row, :] = jnp.where(lane_row < 64, value[7:8], out[row, :])
            return carry

        lax.fori_loop(0, rows // 8, one_group, 0)

    def qkv_grad(place, column, size):
        tiles = []
        for start in range(column, column + size, 128):
            part, head = divmod(start // HD, planes * cores * shards)
            halves = []
            for side in range(2):
                plane, member = divmod(head + side, cores * shards)
                spot = (part * planes + plane) * HD
                half = cat_buf[member, place, pl.ds(spot // 128 * 128, 128)]
                halves.append(half if spot % 128 == side * HD else pltpu.roll(half, HD, 1))
            tiles.append(jnp.where(lane < HD, halves[0], halves[1]))
        return tiles[0] if len(tiles) == 1 else jnp.concatenate(tiles, axis=1)

    units = up_state.shape[2] // (planes * cores * shards)

    def up_grad(place, column, size):
        parts = []
        for start in range(column, column + size, min(units, size)):
            plane, member = divmod(start // units, cores * shards)
            spot = 3 * planes * HD + plane * units + start % units
            parts.append(cat_buf[member, place, pl.ds(spot, min(units, size))])
        return parts[0] if len(parts) == 1 else jnp.concatenate(parts, axis=1)

    def plain(grad):
        return lambda place, column, size: grad[place, pl.ds(column, size)]

    place_rows(qkv_state, qkv_grad, *plan[0], keep=qkv_out)
    place_rows(dense_state, plain(dense_grad), *plan[1])
    place_rows(up_state, up_grad, *plan[2], keep=up_out)
    place_rows(down_state, plain(down_grad), *plan[3])

    def flush(entry, row, count, sem):
        place = pl.ds(pl.multiple_of(row * 128, 128), count * 128)
        source = outs[entry].reshape(1, 1, outs[entry].shape[0] * 128)
        return pltpu.make_async_copy(source.at[:, :, place], flat[entry].at[:, :, place], sem)

    def step_copies(at):
        copies = []
        for index, (rows, tiles, start, shifted) in enumerate(plan):
            count = rows * tiles
            skip = 1 if shifted and at == 0 else 0
            for entry in range(3):
                copies.append(
                    flush(entry, start + at * count + skip, count - skip, step_sem.at[entry, index, at])
                )
        return copies

    for at in range(steps):

        @pl.when(step == at)
        def begin(at=at):
            for copy in step_copies(at):
                copy.start()

    @pl.when(step == steps - 1)
    def end():
        covered = set()
        for rows, tiles, start, shifted in plan:
            covered |= set(range(start + (1 if shifted else 0), start + steps * rows * tiles))
        left = [row for row in range(whole_rows) if row not in covered]
        rest = [
            flush(entry, row, 1, rest_sem.at[entry, index]) for index, row in enumerate(left) for entry in range(3)
        ]
        for copy in rest:
            copy.start()
        for at in range(steps):
            for copy in step_copies(at):
                copy.wait()
        for copy in rest:
            copy.wait()


def owner_update(states, cat_sum, grads, small_states, small_grads, groups):
    steps = 4
    sizes = [state.shape[1] * state.shape[2] for state in states]
    small_sizes = [grad.size for grad in small_grads]
    order = [("m", 0), ("s", 0), ("m", 1), ("m", 2), ("s", 1), ("m", 3), ("s", 2)]
    offset = 0
    plan = [None] * 4
    small_plan = []
    pads = []
    small_row = 0
    for kind, index in order:
        if kind == "m":
            state = states[index]
            rows = state.shape[1] // steps
            plan[index] = (rows, state.shape[2] // 128, offset // 128, offset % 128 == 64)
            offset += sizes[index]
        else:
            size = small_sizes[index]
            front = offset % 128
            total = -(-(front + size) // 128)
            pads.append((front, total * 128 - front - size))
            for extra in range(total):
                low = front if extra == 0 else 0
                high = min(128, front + size - extra * 128)
                small_plan.append((small_row + extra, offset // 128 + extra, low, high))
            small_row += total
            offset += size
    entries = offset
    out_rows = -(-entries // 1024) * 8
    small_new = [
        adam_values(state[0].reshape(-1), state[1].reshape(-1), state[2].reshape(-1), grad.reshape(-1))
        for state, grad in zip(small_states, small_grads)
    ]
    small = jnp.stack(
        [
            jnp.concatenate([jnp.pad(new[entry], pad) for new, pad in zip(small_new, pads)])
            for entry in range(3)
        ]
    ).reshape(3, small_row, 128)
    in_specs = [
        pl.BlockSpec((3, rows, tiles * 128), lambda s: (0, s, 0)) for rows, tiles, start, shifted in plan
    ]
    qkv_rows, up_rows = plan[0][0], plan[2][0]
    in_specs.append(pl.BlockSpec((cat_sum.shape[0], qkv_rows, cat_sum.shape[2]), lambda s: (0, s, 0)))
    in_specs.append(pl.BlockSpec((plan[1][0], plan[1][1] * 128), lambda s: (s, 0)))
    in_specs.append(pl.BlockSpec((plan[3][0], plan[3][1] * 128), lambda s: (s, 0)))
    in_specs.append(pl.BlockSpec((3, small_row, 128), lambda s: (0, 0, 0)))
    whole_rows = entries // 128
    *outs, qkv_grad, up_grad = pl.pallas_call(
        partial(owner_update_kernel, plan, small_plan, groups, steps, whole_rows),
        grid=(steps,),
        in_specs=in_specs,
        out_specs=[pl.BlockSpec(memory_space=pl.ANY)] * 3
        + [
            pl.BlockSpec((qkv_rows, plan[0][1] * 128), lambda s: (s, 0)),
            pl.BlockSpec((up_rows, plan[2][1] * 128), lambda s: (s, 0)),
        ],
        out_shape=[jax.ShapeDtypeStruct((1, 1, entries), jnp.float32)] * 3
        + [
            jax.ShapeDtypeStruct(states[0].shape[1:], jnp.float32),
            jax.ShapeDtypeStruct(states[2].shape[1:], jnp.float32),
        ],
        scratch_shapes=[pltpu.VMEM((cat_sum.shape[0], qkv_rows, cat_sum.shape[2]), jnp.float32)]
        + [pltpu.VMEM((out_rows, 128), jnp.float32)] * 3
        + [pltpu.SemaphoreType.DMA((3, 4, steps)), pltpu.SemaphoreType.DMA((3, 16))],
        compiler_params=pltpu.CompilerParams(vmem_limit_bytes=56 << 20),
        cost_estimate=pl.CostEstimate(
            flops=20 * entries, bytes_accessed=28 * entries, transcendentals=2 * entries
        ),
    )(*states, cat_sum, *grads, small)
    tail = entries - whole_rows * 128
    if tail:
        outs = [
            lax.dynamic_update_slice(out, new[entries_of][-tail:].reshape(1, 1, tail), (0, 0, whole_rows * 128))
            for out, (new, entries_of) in zip(outs, ((small_new[-1], entry) for entry in range(3)))
        ]
    return tuple(outs), qkv_grad, up_grad


class Wires:
    def __init__(self, send_sems):
        self.send_sems, self.count, self.pending = send_sems, 0, []
        self.plane, self.core, self.shard = (
            lax.axis_index("plane"),
            lax.axis_index("core"),
            lax.axis_index("shard"),
        )
        self.shards = lax.axis_size("shard")
        self.group = lax.axis_size("core") * self.shards
        self.mine = self.core * self.shards + self.shard
        self.first = (self.plane ^ 1, self.core, self.shard)
        self.second = (self.plane ^ 2, self.core, self.shard)

    def member(self, index):
        return (self.plane, index // self.shards, index % self.shards)

    def barrier(self):
        barrier = pltpu.get_barrier_semaphore()
        partners = [self.member(self.mine ^ mask) for mask in range(1, self.group)]
        partners += [self.first, self.second]
        for partner in partners:
            pl.semaphore_signal(barrier, inc=1, device_id=partner, device_id_type=pl.DeviceIdType.MESH)
        pl.semaphore_wait(barrier, len(partners))

    def send(self, source, target, recv_sem, device, when=None):
        copy = pltpu.make_async_remote_copy(
            src_ref=source,
            dst_ref=target,
            send_sem=self.send_sems.at[self.count],
            recv_sem=recv_sem,
            device_id=device,
            device_id_type=pl.DeviceIdType.MESH,
        )
        self.count += 1
        self.pending.append((copy, when))
        if when is None:
            copy.start()
        else:
            pl.when(when)(copy.start)

    def arrived(self, place, recv_sem, when=None):
        copy = pltpu.make_async_remote_copy(
            src_ref=place,
            dst_ref=place,
            send_sem=self.send_sems.at[0],
            recv_sem=recv_sem,
            device_id=self.first,
            device_id_type=pl.DeviceIdType.MESH,
        )
        if when is None:
            copy.wait_recv()
        else:
            pl.when(when)(copy.wait_recv)

    def drain(self):
        for copy, when in self.pending:
            if when is None:
                copy.wait_send()
            else:
                pl.when(when)(copy.wait_send)


def pack_pieces(qkv, up, pieces, planes, cores, shards):
    rows = qkv.shape[0]
    lane = lax.broadcasted_iota(jnp.int32, (rows, 128), 1)
    units = up.shape[1] // (planes * cores * shards)
    for core in range(cores):
        for shard in range(shards):
            piece = core * shards + shard
            for tile in range(3 * planes // 2):
                halves = []
                for side in range(2):
                    part, plane = divmod(2 * tile + side, planes)
                    head = (plane * cores + core) * shards + shard
                    start = part * planes * cores * shards * HD + head * HD
                    half = qkv[:, pl.ds(start // 128 * 128, 128)]
                    halves.append(half if start % 128 == side * HD else pltpu.roll(half, HD, 1))
                pieces[piece, :, pl.ds(tile * 128, 128)] = jnp.where(lane < HD, halves[0], halves[1]).astype(
                    jnp.bfloat16
                )
            for plane in range(planes):
                block = (plane * cores + core) * shards + shard
                pieces[piece, :, pl.ds(3 * planes * HD + plane * units, units)] = up[
                    :, pl.ds(block * units, units)
                ].astype(jnp.bfloat16)


def gather_kernel(
    qkv_state, up_state, dense_state, down_state, tokens, cotangent, vectors,
    cat_out, dense_out, down_out, x_out, dy_out, vec_out,
    qkv_buf, up_buf, dense_buf, down_buf, pieces, dense, down,
    load_sem, send_sems, group_sem, first_sem, second_sem, far_sem, up_sem, low_sem, core_sem, local_sem,
):
    net = Wires(send_sems)
    plane, core, shard, shards, group, mine = net.plane, net.core, net.shard, net.shards, net.group, net.mine
    order = sorted(range(group), key=lambda mask: (mask % shards, mask // shards))
    partner = (plane, 1 - core, shard)

    def cat_unit(mask):
        return lambda p: cat_out.at[p, mine ^ mask]

    def vec_unit(mask):
        return lambda p: vec_out.at[p, mine ^ mask]

    units = []
    down_rows = down.shape[0] // 4
    for part in range(4):
        rows = pl.ds(part * down_rows, down_rows)
        units.append((down.at[rows], lambda p, rows=rows: down_out.at[p, rows]))
    dense_rows = dense.shape[0] // 2
    for part in range(2):
        rows = pl.ds(part * dense_rows, dense_rows)
        units.append((dense.at[rows], lambda p, rows=rows: dense_out.at[p, rows]))
    own_units = list(range(len(units)))
    cat_units, vec_units = {}, {}
    for mask in order:
        cat_units[mask] = len(units)
        units.append((pieces.at[mine] if mask == 0 else None, cat_unit(mask)))
        vec_units[mask] = len(units)
        units.append((vectors if mask == 0 else None, vec_unit(mask)))

    def spread(index):
        source, place = units[index]
        source = place(plane) if source is None else source
        net.send(source, place(plane), first_sem.at[index], net.first)
        net.send(source, place(plane), second_sem.at[index], net.second)

    def hand_on(index):
        place = units[index][1]
        if relay_first[index]:
            net.arrived(place(plane ^ 1), first_sem.at[index])
            net.send(place(plane ^ 1), place(plane ^ 1), far_sem.at[index], net.second)
        else:
            net.arrived(place(plane ^ 2), second_sem.at[index])
            net.send(place(plane ^ 2), place(plane ^ 2), far_sem.at[index], net.first)

    relay_first = {}
    for position, index in enumerate(own_units):
        relay_first[index] = position % 2 == 0
    for position, mask in enumerate(order):
        relay_first[cat_units[mask]] = position % 2 == 0
        relay_first[vec_units[mask]] = position % 2 == 1

    loads = [
        pltpu.make_async_copy(state.at[0], buffer, load_sem.at[index])
        for index, (state, buffer) in enumerate(
            ((qkv_state, qkv_buf), (up_state, up_buf), (down_state, down_buf), (dense_state, dense_buf))
        )
    ]
    for index in (2, 3, 0, 1):
        loads[index].start()
    net.barrier()
    loads[2].wait()
    down[...] = down_buf[...].astype(jnp.bfloat16)
    loads[3].wait()
    dense[...] = dense_buf[...].astype(jnp.bfloat16)
    for index in own_units:
        spread(index)
    loads[0].wait()
    loads[1].wait()
    pack_pieces(qkv_buf, up_buf, pieces, cat_out.shape[0], group // shards, shards)

    locals_ = [
        (pieces.at[mine], cat_out.at[plane, mine]),
        (dense, dense_out.at[plane]),
        (down, down_out.at[plane]),
        (tokens, x_out.at[mine]),
        (cotangent, dy_out.at[mine]),
        (vectors, vec_out.at[plane, mine]),
    ]
    copies = [
        pltpu.make_async_copy(source, target, local_sem.at[index])
        for index, (source, target) in enumerate(locals_)
    ]
    for mask in order[1:]:
        target = net.member(mine ^ mask)
        net.send(vectors, vec_out.at[plane, mine], group_sem.at[1, mask], target)
        net.send(pieces.at[mine ^ mask], cat_out.at[plane, mine], group_sem.at[0, mask], target)
    spread(cat_units[0])
    spread(vec_units[0])
    streams = ((tokens, x_out), (cotangent, dy_out))

    def block(stream, origin):
        return streams[stream][1].at[core * shards + origin]

    def to_core(stream, source, origin, slot, when=None):
        net.send(source, block(stream, origin), core_sem.at[stream, slot], partner, when)

    def hop(stream, distance):
        own = distance == 1
        for upward, sem in ((True, up_sem), (False, low_sem)):
            origin = shard - (distance - 1) if upward else shard + (distance - 1)
            there = shard + 1 if upward else shard - 1
            held = (origin >= 0) if upward else (origin < shards)
            inside = (there < shards) if upward else (there >= 0)
            near = jnp.clip(origin, 0, shards - 1)
            source = streams[stream][0] if own else block(stream, near)
            net.send(
                source,
                block(stream, near),
                sem.at[stream, distance],
                (plane, core, jnp.clip(there, 0, shards - 1)),
                inside & held,
            )

    def hop_arrived(stream, distance):
        for upward, sem in ((True, up_sem), (False, low_sem)):
            origin = shard - distance if upward else shard + distance
            held = (origin >= 0) if upward else (origin < shards)
            near = jnp.clip(origin, 0, shards - 1)
            net.arrived(block(stream, near), sem.at[stream, distance], held)
            slot = distance if upward else shards + distance
            to_core(stream, block(stream, near), near, slot, held)

    for stream in range(2):
        hop(stream, 1)
    for stream in range(2):
        to_core(stream, streams[stream][0], shard, 0)
    for copy in copies:
        copy.start()

    for position, mask in enumerate(order[1:]):
        net.arrived(vec_out.at[plane, mine ^ mask], group_sem.at[1, mask])
        spread(vec_units[mask])
        net.arrived(cat_out.at[plane, mine ^ mask], group_sem.at[0, mask])
        spread(cat_units[mask])
        if position == 2:
            for index in own_units:
                hand_on(index)
    hand_on(cat_units[0])
    hand_on(vec_units[0])
    for distance in range(1, shards):
        for stream in range(2):
            hop_arrived(stream, distance)
            if distance + 1 < shards:
                hop(stream, distance + 1)
        for mask in order[1 + (distance - 1) * 3 : 1 + distance * 3]:
            hand_on(vec_units[mask])
            hand_on(cat_units[mask])

    for index, (source, place) in enumerate(units):
        if relay_first[index]:
            net.arrived(place(plane ^ 2), second_sem.at[index])
        else:
            net.arrived(place(plane ^ 1), first_sem.at[index])
        net.arrived(place(plane ^ 3), far_sem.at[index])
    for stream in range(2):
        other = streams[stream][1]
        for slot in range(2 * shards):
            if slot == shards:
                continue
            origin = shard - slot if slot < shards else shard + (slot - shards)
            held = None if slot == 0 else ((origin >= 0) & (origin < shards))
            near = jnp.clip(origin, 0, shards - 1)
            net.arrived(other.at[(1 - core) * shards + near], core_sem.at[stream, slot], held)
    for copy in copies:
        copy.wait()
    net.drain()


def gather_wires(qkv, up, dense, down, tokens, cotangent, vectors):
    group, shards = lax.axis_size("core") * lax.axis_size("shard"), lax.axis_size("shard")
    planes = lax.axis_size("plane")
    width = (qkv.shape[2] + up.shape[2]) // group
    units = 6 + 2 * group
    vmem = pl.BlockSpec(memory_space=pltpu.VMEM)
    hbm = pl.BlockSpec(memory_space=pl.ANY)

    def out(*shape, dtype=jnp.bfloat16):
        return jax.ShapeDtypeStruct(shape, dtype)

    dma = pltpu.SemaphoreType.DMA
    return pl.pallas_call(
        gather_kernel,
        in_specs=[hbm] * 4 + [vmem] * 3,
        out_specs=[hbm] * 6,
        out_shape=[
            out(planes, group, qkv.shape[1], width),
            out(planes, *dense.shape[1:]),
            out(planes, *down.shape[1:]),
            out(group, *tokens.shape),
            out(group, *cotangent.shape),
            out(planes, group, *vectors.shape, dtype=vectors.dtype),
        ],
        scratch_shapes=[
            pltpu.VMEM(qkv.shape[1:], qkv.dtype),
            pltpu.VMEM(up.shape[1:], up.dtype),
            pltpu.VMEM(dense.shape[1:], dense.dtype),
            pltpu.VMEM(down.shape[1:], down.dtype),
            pltpu.VMEM((group, qkv.shape[1], width), jnp.bfloat16),
            pltpu.VMEM(dense.shape[1:], jnp.bfloat16),
            pltpu.VMEM(down.shape[1:], jnp.bfloat16),
            dma((4,)),
            dma((2 * (group - 1) + 3 * units + 2 * 2 * (shards - 1) + 2 * (2 * shards - 1),)),
            dma((2, group)),
            dma((units,)),
            dma((units,)),
            dma((units,)),
            dma((2, shards)),
            dma((2, shards)),
            dma((2, 2 * shards)),
            dma((6,)),
        ],
        compiler_params=pltpu.CompilerParams(
            collective_id=0, has_side_effects=True, vmem_limit_bytes=67043328
        ),
    )(qkv, up, dense, down, tokens, cotangent, vectors)


def add_rows(target, *sources):
    step = 16
    rows = target.shape[0]

    def body(index, carry):
        place = pl.ds(pl.multiple_of(index * step, step), step)
        total = sources[0][place, :].astype(jnp.float32)
        for source in sources[1:]:
            total = total + source[place, :].astype(jnp.float32)
        target[place, :] = total.astype(target.dtype)
        return carry

    lax.fori_loop(0, rows // step, body, 0)


def chunked(first, last, copies_of, body):
    for copy in copies_of(first, first % 2):
        copy.start()

    def step(n, carry):
        slot = lax.rem(n, 2)

        @pl.when(n + 1 < last)
        def ahead():
            for copy in copies_of(n + 1, 1 - slot):
                copy.start()

        for copy in copies_of(n, slot):
            copy.wait()
        body(n, slot)
        return carry

    lax.fori_loop(first, last, step, 0)


def reduce_kernel(
    norm, dcat, x_all, mean, inverse, attn, hidden, dy, cat_w, dense_w, down_w, sums,
    cat_out, dense_out, down_out, mixed_out, norm_out, sums_out,
    cat_part, down_part, dense_part, cat_in, down_in, dense_in,
    tokens, token_in, token_line, token_last, sum_buf,
    wide, attn_turned, norm_chunk, norm_turned, cat_chunk, x_chunk, down_chunk, dense_chunk, dy_chunk,
    send_sems, near_sem, pass_sem, group_sem, core_sem, line_sem, sum_sem, local_sem, chunk_sem,
):
    PASS, KEEP, LAST = range(3)
    net = Wires(send_sems)
    plane, core, shard, shards, group, mine = net.plane, net.core, net.shard, net.shards, net.group, net.mine
    planes = cat_part.shape[0]
    partner = (plane, 1 - core, shard)
    order = sorted(range(group), key=lambda mask: (mask % shards, mask // shards), reverse=True)
    rows, width = dcat.shape
    model = norm.shape[1]
    block = cat_part.shape[2]
    token_rows = tokens.shape[2]
    units_here = hidden.shape[1]
    heads_here = attn.shape[1]
    lane = 256

    def dot(a, b, a_dim=1, b_dim=0):
        return lax.dot_general(a, b, (((a_dim,), (b_dim,)), ((), ())), preferred_element_type=jnp.float32)

    def columns(n):
        return pl.ds(pl.multiple_of(n * lane, lane), lane)

    units = [(cat_part, cat_in, mask) for mask in order]
    units += [(down_part, down_in, part) for part in range(down_part.shape[1])]
    units += [(dense_part, dense_in, part) for part in range(dense_part.shape[1])]
    down_rows, dense_rows = down_part.shape[2], dense_part.shape[2]

    def ways(index):
        return (net.first, net.second, 1, 2) if index % 2 == 0 else (net.second, net.first, 2, 1)

    def send_pass(index):
        parts, came, slot = units[index]
        net.send(parts.at[3, slot], came.at[PASS, slot], pass_sem.at[0, index], ways(index)[0])

    def send_keep(index):
        parts, came, slot = units[index]
        near, far, near_mask, far_mask = ways(index)
        net.send(parts.at[near_mask, slot], came.at[KEEP, slot], near_sem.at[index], near)

    locals_ = {}

    def local(key, source, target):
        locals_[key] = pltpu.make_async_copy(source, target, local_sem.at[len(locals_)])
        locals_[key].start()

    local("dcat", dcat, wide.at[:, pl.ds(0, width)])
    net.barrier()

    plane_rows = group * block

    def norm_copy(turn, distance):
        place = pl.ds(pl.multiple_of((plane ^ distance) * plane_rows, plane_rows), plane_rows)
        return pltpu.make_async_copy(
            norm.at[:, place], norm_chunk.at[turn % 2], chunk_sem.at[0, turn % 2]
        )

    cats, every = range(group), range(len(units))
    turns = (3, 1, 2, 0)
    norm_copy(0, turns[0]).start()
    locals_["dcat"].wait()

    def cat_turn(turn):
        distance = turns[turn]
        if turn + 1 < planes:
            norm_copy(turn + 1, turns[turn + 1]).start()
        norm_copy(turn, distance).wait()
        norm_turned[...] = norm_chunk[turn % 2].T

        def cat_step(n, carry):
            total = dot(norm_turned[...], wide[:, columns(n)]).astype(jnp.bfloat16)
            for member in range(group):
                cat_part[distance, mine ^ member, :, columns(n)] = total[member * block : (member + 1) * block]
            return carry

        lax.fori_loop(0, width // lane, cat_step, 0)
        for index in cats:
            if distance == 3:
                send_pass(index)
            elif distance == ways(index)[2]:
                send_keep(index)

    cat_turn(0)

    sum_buf[4] = sums[...]
    gain_row = width // 128

    def norm_copies(n, slot):
        return [
            pltpu.make_async_copy(cat_w.at[columns(n), :], cat_chunk.at[slot], chunk_sem.at[1, slot]),
            pltpu.make_async_copy(x_all.at[:, columns(n)], x_chunk.at[slot], chunk_sem.at[2, slot]),
        ]

    def norm_step(n, slot):
        total = dot(wide[:, pl.ds(0, width)], cat_chunk[slot], 1, 1)
        x_hat = (x_chunk[slot].astype(jnp.float32) - mean[...]) * inverse[...]
        gain = jnp.sum(total * x_hat, axis=0, keepdims=True)
        shift = jnp.sum(total, axis=0, keepdims=True)
        for half in range(lane // 128):
            row = gain_row + n * (lane // 128) + half
            sum_buf[4, pl.ds(row, 1), :] = gain[:, half * 128 : (half + 1) * 128]
            sum_buf[4, pl.ds(row + model // 128, 1), :] = shift[:, half * 128 : (half + 1) * 128]
        for member in range(group):
            tokens[1, member, :, columns(n)] = total[member * token_rows : (member + 1) * token_rows].astype(
                jnp.bfloat16
            )

    chunked(0, model // lane, norm_copies, norm_step)

    places = [place for rank in range(shards // 2) for place in (shards - 1 - rank, rank)]

    def to_partner(stream):
        for place in places:
            net.send(
                tokens.at[stream, (1 - core) * shards + place],
                token_in.at[stream, place],
                core_sem.at[stream, place],
                partner,
            )

    net.send(sum_buf.at[4], sum_buf.at[0], sum_sem.at[0], net.first)
    to_partner(1)
    cat_turn(1)

    def own(stream, place):
        return tokens.at[stream, core * shards + place]

    def chain(stream, hop, rank):
        for upward in (True, False):
            target = shards - 1 - rank if upward else rank
            here = hop if upward else shards - 1 - hop
            sems = line_sem.at[0 if upward else 1]
            came = token_line.at[stream, target]
            total = own(stream, target)
            holds = shard == here
            if hop:
                net.arrived(came, sems.at[stream, target], holds)

            @pl.when(holds)
            def add(target=target, came=came, total=total):
                add_rows(total, total, token_in.at[stream, target], *([came] if hop else []))

            there = jnp.clip(shard + (1 if upward else -1), 0, shards - 1)
            ends = (not upward) and rank == shards - 2 - hop
            landing = token_last.at[stream] if ends else came
            net.send(total, landing, sems.at[stream, target], (plane, core, there), holds)

    def final(stream):
        for place in range(shards):
            holds = shard == place
            values = [own(stream, place), token_in.at[stream, place]]
            for landing, side, present in (
                (token_line.at[stream, place], line_sem.at[0], place > 0),
                (token_last.at[stream], line_sem.at[1], place < shards - 1),
            ):
                if present:
                    values.append(landing)
                    net.arrived(landing, side.at[stream, place], holds)

            @pl.when(holds)
            def add(values=values):
                add_rows((mixed_out, norm_out)[stream], *values)

    def first_sums(stream):
        for place in places:
            net.arrived(token_in.at[stream, place], core_sem.at[stream, place])
        for rank in range(shards - 1):
            chain(stream, 0, rank)

    def pass_on(index):
        parts, came, slot = units[index]
        near, far, near_mask, far_mask = ways(index)
        total = parts.at[far_mask, slot]
        net.arrived(came.at[PASS, slot], pass_sem.at[0, index])
        add_rows(total, total, came.at[PASS, slot])
        net.send(total, came.at[LAST, slot], pass_sem.at[1, index], far)

    first_sums(1)
    cat_turn(2)
    net.arrived(sum_buf.at[0], sum_sem.at[0])
    sum_buf[1] = sum_buf[4] + sum_buf[0]
    net.send(sum_buf.at[1], sum_buf.at[2], sum_sem.at[1], net.second)
    for index in cats:
        pass_on(index)
    cat_turn(3)
    local("hidden", hidden, wide.at[:, pl.ds(0, units_here)])
    local("attn", attn, wide.at[:, pl.ds(2 * units_here, heads_here)])
    steps = [
        (hop, rank)
        for hop, rank in sorted(
            ((hop, rank) for hop in range(1, shards - 1) for rank in range(shards - 1 - hop)),
            key=lambda pair: (pair[0] + 2 * pair[1], pair[0]),
        )
    ]
    later = [(stream, hop, rank) for stream in (1, 0) for hop, rank in steps]

    locals_["hidden"].wait()
    locals_["attn"].wait()
    turned = pl.ds(units_here, rows)
    wide[:, turned] = wide[:, pl.ds(0, units_here)].T
    attn_turned[...] = wide[:, pl.ds(2 * units_here, heads_here)].T

    def out_copies(n, slot):
        return [
            pltpu.make_async_copy(down_w.at[:, columns(n)], down_chunk.at[slot], chunk_sem.at[3, slot]),
            pltpu.make_async_copy(dense_w.at[:, columns(n)], dense_chunk.at[slot], chunk_sem.at[4, slot]),
            pltpu.make_async_copy(dy.at[:, columns(n)], dy_chunk.at[slot], chunk_sem.at[5, slot]),
        ]

    def out_step(n, slot):
        total = dot(wide[:, pl.ds(0, units_here)], down_chunk[slot]) + dot(
            wide[:, pl.ds(2 * units_here, heads_here)], dense_chunk[slot]
        )
        for member in range(group):
            tokens[0, member, :, columns(n)] = total[member * token_rows : (member + 1) * token_rows].astype(
                jnp.bfloat16
            )
        for parts, left in ((down_part, wide[:, turned]), (dense_part, attn_turned[...])):
            grad = dot(left, dy_chunk[slot]).astype(jnp.bfloat16)
            pieces, size = parts.shape[1], parts.shape[2]
            for q in range(planes):
                for piece in range(pieces):
                    start = (q * pieces + piece) * size
                    parts[plane ^ q, piece, :, columns(n)] = grad[start : start + size]

    half = model // lane // 2
    chunked(0, half, out_copies, out_step)
    chain(*later.pop(0))
    chunked(half, 2 * half, out_copies, out_step)
    to_partner(0)
    for index in every[group:]:
        send_pass(index)
        send_keep(index)
    chain(*later.pop(0))
    first_sums(0)

    def finish(index):
        parts, came, slot = units[index]
        total = parts.at[0, slot]
        net.arrived(came.at[KEEP, slot], near_sem.at[index])
        net.arrived(came.at[LAST, slot], pass_sem.at[1, index])
        values = (total, came.at[KEEP, slot], came.at[LAST, slot])
        if index < group:
            add_rows(total, *values)
            if slot:
                net.send(total, cat_out.at[mine], group_sem.at[0, slot], net.member(mine ^ slot))
            else:
                local("own", total, cat_out.at[mine])
        elif parts is down_part:
            add_rows(down_out.at[pl.ds(slot * down_rows, down_rows)], *values)
        else:
            add_rows(dense_out.at[pl.ds(slot * dense_rows, dense_rows)], *values)

    net.arrived(sum_buf.at[2], sum_sem.at[1])
    sum_buf[3] = sum_buf[1] + sum_buf[2]
    for mask in range(1, group):
        net.send(sum_buf.at[3], sums_out.at[mine], group_sem.at[1, mask], net.member(mine ^ mask))
    local("sums", sum_buf.at[3], sums_out.at[mine])
    for index in cats[: group - 2]:
        finish(index)
        if later:
            chain(*later.pop(0))
    while later:
        chain(*later.pop(0))
    for index in every[group:]:
        pass_on(index)
    for index in cats[group - 2 :]:
        finish(index)
    for stream in (1, 0):
        final(stream)
    for index in every[group:]:
        finish(index)
    for mask in range(1, group):
        net.arrived(cat_out.at[mine ^ mask], group_sem.at[0, mask])
        net.arrived(sums_out.at[mine ^ mask], group_sem.at[1, mask])
    locals_["own"].wait()
    locals_["sums"].wait()
    net.drain()


def reduce_wires(norm, dcat, x_all, mean, inverse, attn, hidden, dy, cat_w, dense_w, down_w, sums):
    planes, shards = lax.axis_size("plane"), lax.axis_size("shard")
    group = lax.axis_size("core") * shards
    units = group + 6
    rows, width = dcat.shape
    model = norm.shape[1]
    block = model // (planes * group)
    unit_rows, head_rows = down_w.shape[0] // planes, dense_w.shape[0] // planes
    token_rows = rows // group
    vmem = pl.BlockSpec(memory_space=pltpu.VMEM)
    hbm = pl.BlockSpec(memory_space=pl.ANY)
    dma = pltpu.SemaphoreType.DMA
    lane = 256

    def scratch(*shape, dtype=jnp.bfloat16):
        return pltpu.VMEM(shape, dtype)

    return pl.pallas_call(
        reduce_kernel,
        in_specs=[hbm] * 3 + [vmem] * 2 + [hbm] * 6 + [vmem],
        out_specs=[hbm] + [vmem] * 4 + [hbm],
        out_shape=[
            jax.ShapeDtypeStruct((group, block, width), jnp.bfloat16),
            jax.ShapeDtypeStruct((head_rows, model), jnp.float32),
            jax.ShapeDtypeStruct((unit_rows, model), jnp.float32),
            jax.ShapeDtypeStruct((token_rows, model), jnp.float32),
            jax.ShapeDtypeStruct((token_rows, model), jnp.float32),
            jax.ShapeDtypeStruct((group,) + sums.shape, sums.dtype),
        ],
        scratch_shapes=[
            scratch(planes, group, block, width),
            scratch(planes, 4, unit_rows // 4, model),
            scratch(planes, 2, head_rows // 2, model),
            scratch(3, group, block, width),
            scratch(3, 4, unit_rows // 4, model),
            scratch(3, 2, head_rows // 2, model),
            scratch(2, group, token_rows, model),
            scratch(2, shards, token_rows, model),
            scratch(2, shards, token_rows, model),
            scratch(2, token_rows, model),
            scratch(5, *sums.shape, dtype=jnp.float32),
            scratch(rows, hidden.shape[1] + rows + attn.shape[1]),
            scratch(attn.shape[1], rows),
            scratch(2, rows, group * block),
            scratch(group * block, rows),
            scratch(2, lane, width),
            scratch(2, rows, lane),
            scratch(2, hidden.shape[1], lane),
            scratch(2, attn.shape[1], lane),
            scratch(2, rows, lane),
            dma((2 + 2 * shards + 2 * shards * (shards - 1) + 3 * units + 2 * (group - 1),)),
            dma((units,)),
            dma((2, units)),
            dma((2, group)),
            dma((2, shards)),
            dma((2, 2, shards)),
            dma((2,)),
            dma((5,)),
            dma((6, 2)),
        ],
        compiler_params=pltpu.CompilerParams(
            collective_id=1, has_side_effects=True, vmem_limit_bytes=67043328
        ),
    )(norm, dcat, x_all, mean, inverse, attn, hidden, dy, cat_w, dense_w, down_w, sums)


def fast_body(
    hidden_in,
    segment_ids,
    out_grad,
    qkv_weight_state,
    qkv_bias_state,
    dense_weight_state,
    up_weight_state,
    up_bias_state,
    down_weight_state,
    vector_state,
):
    planes, cores, shards = lax.axis_size("plane"), lax.axis_size("core"), lax.axis_size("shard")
    plane, core, shard = lax.axis_index("plane"), lax.axis_index("core"), lax.axis_index("shard")
    group = cores * shards
    owner = (plane * cores + core) * shards + shard
    owners = planes * group
    model_rows = qkv_weight_state.shape[1]
    unit_rows = down_weight_state.shape[1]
    tokens_here = hidden_in.shape[1]
    head_width = planes * HD
    unit_width = planes * unit_rows
    qkv_count, upb_count = qkv_bias_state.shape[1], up_bias_state.shape[1]

    tokens, cotangent, q_seg = hidden_in[0], out_grad[0], segment_ids[0]
    vec_list = [
        qkv_bias_state[0],
        up_bias_state[0],
        vector_state[0].T.reshape(-1),
        q_seg.astype(jnp.float32),
    ]
    vec_sizes = [value.size for value in vec_list]
    vec_rows = -(-sum(vec_sizes) // 1024) * 8
    vec_own = jnp.pad(jnp.concatenate(vec_list), (0, vec_rows * 128 - sum(vec_sizes))).reshape(vec_rows, 128)

    cat_w, dense_w, down_w, x_all, dy_all, vec_all = gather_wires(
        qkv_weight_state,
        up_weight_state,
        dense_weight_state,
        down_weight_state,
        tokens,
        cotangent,
        vec_own,
    )

    cat_w = cat_w.reshape(D, 3 * head_width + unit_width)
    dense_w = dense_w.reshape(head_width, D)
    down_w = down_w.reshape(unit_width, D)
    rows = group * tokens_here
    x_all = x_all.reshape(rows, D)
    dy_all = dy_all.reshape(rows, D)
    vec_flat = vec_all.reshape(planes, cores, shards, vec_rows * 128)
    at = [0]
    for size in vec_sizes:
        at.append(at[-1] + size)

    def rounded(value):
        return value.astype(jnp.bfloat16).astype(jnp.float32)

    qkv_bias = rounded(vec_flat[..., at[0] : at[1]]).reshape(3, planes, cores, shards, HD)
    qkv_bias = lax.dynamic_index_in_dim(
        qkv_bias.transpose(2, 3, 0, 1, 4).reshape(group, 3 * head_width), core * shards + shard, 0, False
    )
    up_bias = lax.dynamic_index_in_dim(
        rounded(vec_flat[..., at[1] : at[2]]).transpose(1, 2, 0, 3).reshape(group, unit_width),
        core * shards + shard,
        0,
        False,
    )
    vec_columns = (
        rounded(vec_flat[..., at[2] : at[3]])
        .reshape(owners, 4, model_rows)
        .transpose(1, 0, 2)
        .reshape(4, D)
    )
    norm_gain, norm_shift, dense_bias, down_bias = (vec_columns[index] for index in range(4))
    segments = lax.dynamic_index_in_dim(vec_flat[..., at[3] : at[4]], plane, 0, False)
    segments = segments.astype(jnp.int32).reshape(cores, shards * tokens_here)
    cat_bias = jnp.concatenate([qkv_bias, up_bias])

    x_float = x_all.astype(jnp.float32)
    x_mean = jnp.mean(x_float, axis=-1, keepdims=True)
    center = x_float - x_mean
    inverse = lax.rsqrt(jnp.mean(center * center, axis=-1, keepdims=True) + norm_eps)
    x_hat = center * inverse
    norm_bf = lax.optimization_barrier((x_hat * norm_gain + norm_shift).astype(jnp.bfloat16))

    fu = jnp.dot(norm_bf, cat_w, preferred_element_type=jnp.float32) + cat_bias
    pre_act = fu[:, 3 * head_width :]
    hidden = gelu_tanh(pre_act).astype(jnp.bfloat16)
    grad_hidden = jnp.dot(dy_all, down_w.T, preferred_element_type=jnp.float32)
    grad_pre = jax.vjp(gelu_tanh, pre_act)[1](grad_hidden)[0]
    upb_part = jnp.sum(grad_pre, axis=0)
    grad_heads = jnp.dot(dy_all, dense_w.T, preferred_element_type=jnp.float32).astype(jnp.bfloat16)
    attn, dcat, qkvb_part = attention(fu, grad_heads, grad_pre.astype(jnp.bfloat16), segments)
    bias_part = jnp.sum(cotangent.astype(jnp.float32), axis=0)
    nothing = jnp.zeros((D,), jnp.float32)
    sums = [qkvb_part, upb_part, nothing, nothing, bias_part]
    sum_sizes = [value.size for value in sums]
    sum_rows = -(-sum(sum_sizes) // 1024) * 8
    sums = jnp.pad(jnp.concatenate(sums), (0, sum_rows * 128 - sum(sum_sizes))).reshape(sum_rows, 128)

    cat_sum, dense_grad, down_grad, mixed, grad_norm, sums_all = reduce_wires(
        norm_bf,
        dcat,
        x_all,
        x_mean,
        inverse,
        attn,
        hidden,
        dy_all,
        cat_w,
        dense_w,
        down_w,
        sums,
    )

    sums_flat = sums_all.reshape(cores, shards, sum_rows * 128)
    at = [0]
    for size in sum_sizes:
        at.append(at[-1] + size)
    qkvb_grad = (
        sums_flat[..., : at[1]]
        .reshape(cores, shards, 3, planes, HD)
        .transpose(2, 3, 0, 1, 4)
        .reshape(owners, qkv_count)
    )
    qkvb_grad = lax.dynamic_index_in_dim(qkvb_grad, owner, 0, False)
    upb_grad = sums_flat[..., at[1] : at[2]].reshape(group, planes, upb_count)
    upb_grad = lax.dynamic_index_in_dim(
        lax.dynamic_index_in_dim(upb_grad, core * shards + shard, 0, False), plane, 0, False
    )
    vec_grad = jnp.sum(sums_flat[..., at[2] : at[5]], axis=(0, 1)).reshape(3, owners, model_rows)
    vec_grad = lax.dynamic_index_in_dim(vec_grad, owner, 1, False)
    vec_grad = jnp.stack([vec_grad[0], vec_grad[1], vec_grad[2], vec_grad[2]], axis=1)

    x_own = tokens.astype(jnp.float32)
    output = (x_own + (mixed.astype(jnp.float32) + dense_bias + down_bias)).astype(jnp.bfloat16)
    own_center = x_own - jnp.mean(x_own, axis=-1, keepdims=True)
    own_inverse = lax.rsqrt(jnp.mean(own_center * own_center, axis=-1, keepdims=True) + norm_eps)
    own_hat = own_center * own_inverse
    hat_grad = grad_norm.astype(jnp.float32) * norm_gain
    x_grad = own_inverse * (
        hat_grad
        - jnp.mean(hat_grad, axis=-1, keepdims=True)
        - own_hat * jnp.mean(hat_grad * own_hat, axis=-1, keepdims=True)
    )
    input_grad = cotangent.astype(jnp.float32) + x_grad

    new, qkv_grad, up_grad = owner_update(
        (qkv_weight_state, dense_weight_state, up_weight_state, down_weight_state),
        cat_sum,
        (dense_grad, down_grad),
        (qkv_bias_state, up_bias_state, vector_state),
        (qkvb_grad, upb_grad, vec_grad),
        (planes, cores, shards),
    )
    return (
        output[None],
        input_grad[None],
        qkv_grad,
        qkvb_grad,
        dense_grad,
        up_grad,
        upb_grad,
        down_grad,
        vec_grad,
        *new,
    )


def fast_solution(mesh):
    rep, shard = mesh.shape["rep"], mesh.shape["shard"]
    inner = Mesh(mesh.devices.reshape(rep // 2, 2, shard), ("plane", "core", "shard"))
    both = ("plane", "core")
    every = ("plane", "core", "shard")
    in_specs = (
        P(both, "shard", None),
        P(both, "shard"),
        P(both, "shard", None),
        P(None, every, None),
        P(None, every),
        P(None, every, None),
        P(None, every, None),
        P(None, every),
        P(None, every, None),
        P(None, every, None),
    )
    out_specs = (
        P(both, "shard", None),
        P(both, "shard", None),
        P(every, None),
        P(every),
        P(every, None),
        P(every, None),
        P(every),
        P(every, None),
        P(every, None),
        P(both, "shard", None),
        P(both, "shard", None),
        P(both, "shard", None),
    )
    return jax.shard_map(fast_body, mesh=inner, in_specs=in_specs, out_specs=out_specs, check_vma=False)


def solution(mesh):
    in_specs = (
        P("rep", "shard", None),
        P("rep", "shard"),
        P("rep", "shard", None),
        P(None, ("rep", "shard"), None),
        P(None, ("rep", "shard")),
        P(None, ("rep", "shard"), None),
        P(None, ("rep", "shard"), None),
        P(None, ("rep", "shard")),
        P(None, ("rep", "shard"), None),
        P(None, ("rep", "shard"), None),
    )
    out_specs = (
        P("rep", "shard", None),
        P("rep", "shard", None),
        P(("rep", "shard"), None),
        P(("rep", "shard")),
        P(("rep", "shard"), None),
        P(("rep", "shard"), None),
        P(("rep", "shard")),
        P(("rep", "shard"), None),
        P(("rep", "shard"), None),
        P("rep", "shard", None),
        P("rep", "shard", None),
        P("rep", "shard", None),
    )
    if whole_heads(mesh):
        return fast_solution(mesh)
    return jax.shard_map(body, mesh=mesh, in_specs=in_specs, out_specs=out_specs, check_vma=False)
```

```python
from functools import partial
import math

import jax
import jax.numpy as jnp
from jax import lax
from jax.experimental import pallas as pl
from jax.experimental.pallas import tpu as pltpu
from jax.sharding import Mesh
from jax.sharding import PartitionSpec as P

D = 2048
HD = 64
ROT = 32
FF = 8192
STEP = 5


learn_rate = 0.02
beta_one = 0.9
beta_two = 0.95
adam_eps = 1e-08
weight_decay = 0.1
norm_eps = 1e-05
big_negative = -1e30


def layer_norm(x, norm_gain, norm_shift):
    center = x - jnp.mean(x, axis=-1, keepdims=True)
    variance = jnp.mean(center * center, axis=-1, keepdims=True)
    return center * lax.rsqrt(variance + norm_eps) * norm_gain + norm_shift


def gelu_tanh(v):
    return 0.5 * v * (1.0 + jnp.tanh(0.7978845608028654 * (v + 0.044715 * v * v * v)))


def rotary(x, positions):
    half_rot = ROT // 2
    frequency = jnp.exp(jnp.arange(half_rot, dtype=jnp.float32) * (-2.0 * math.log(10000.0) / ROT))
    angles = positions.astype(jnp.float32)[:, None] * frequency[None, :]
    cosine = jnp.cos(angles)[:, None, :]
    sine_val = jnp.sin(angles)[:, None, :]
    lower_part = x[..., :half_rot]
    upper_part = x[..., half_rot:ROT]
    return jnp.concatenate(
        [
            lower_part * cosine - upper_part * sine_val,
            upper_part * cosine + lower_part * sine_val,
            x[..., ROT:],
        ],
        axis=-1,
    )


def adam_update(state, grad):
    moment_one = beta_one * state[1] + (1.0 - beta_one) * grad
    moment_two = beta_two * state[2] + (1.0 - beta_two) * grad * grad
    corrected = moment_one / (1.0 - beta_one**STEP)
    divisor = jnp.sqrt(moment_two / (1.0 - beta_two**STEP)) + adam_eps
    weight = state[0] - learn_rate * (corrected / divisor + weight_decay * state[0])
    return jnp.stack([weight, moment_one, moment_two])


def owner_entries(new_states, entry):
    return jnp.concatenate(
        [state_new[entry].reshape(-1) for state_new in new_states], axis=0
    ).reshape(1, 1, -1)


def block_mask(q_pos, q_seg, k_pos, k_seg):
    return (k_pos[None, :] <= q_pos[:, None]) & (k_seg[None, :] == q_seg[:, None])


def attend_keys(kv_all, seg_all, queries, q_pos, q_seg):
    key_count = kv_all.shape[0]
    width = kv_all.shape[1] // 2
    heads_here = queries.shape[1]
    query_rows = queries.shape[0]
    block_rows = math.gcd(key_count, 512)
    block_count = key_count // block_rows
    kv_blocks = kv_all.reshape(block_count, block_rows, 2 * width)
    seg_blocks = seg_all.reshape(block_count, block_rows)
    score_scale = 1.0 / math.sqrt(HD)

    def attend_step_block(carry, block_items):
        kv_rows, seg_rows, block_index = block_items
        row_max, totals, accumulated = carry
        key_rows = kv_rows[:, :width].reshape(block_rows, heads_here, HD)
        value_rows = kv_rows[:, width:].reshape(block_rows, heads_here, HD)
        k_pos = block_index * block_rows + jnp.arange(block_rows, dtype=jnp.int32)
        allowed = block_mask(q_pos, q_seg, k_pos, seg_rows)
        scores = (
            jnp.einsum("qhd,khd->hqk", queries, key_rows, preferred_element_type=jnp.float32)
            * score_scale
        )
        scores = jnp.where(allowed[None], scores, big_negative)
        new_max = jnp.maximum(row_max, jnp.max(scores, axis=-1))
        probabilities = jnp.where(allowed[None], jnp.exp(scores - new_max[..., None]), 0.0)
        factor = jnp.exp(row_max - new_max)
        totals = totals * factor + jnp.sum(probabilities, axis=-1)
        accumulated = accumulated * factor[..., None] + jnp.einsum(
            "hqk,khd->hqd",
            probabilities.astype(jnp.bfloat16),
            value_rows,
            preferred_element_type=jnp.float32,
        )
        return ((new_max, totals, accumulated), None)

    start_state = (
        jnp.full((heads_here, query_rows), big_negative, jnp.float32),
        jnp.zeros((heads_here, query_rows), jnp.float32),
        jnp.zeros((heads_here, query_rows, HD), jnp.float32),
    )
    running, unused = lax.scan(
        attend_step_block,
        start_state,
        (kv_blocks, seg_blocks, jnp.arange(block_count, dtype=jnp.int32)),
    )
    return running


def attention_grads(queries, kv_all, seg_all, q_pos, q_seg, grad_heads, delta_all, lse_all):
    key_count = kv_all.shape[0]
    width = kv_all.shape[1] // 2
    heads_here = queries.shape[1]
    query_rows = queries.shape[0]
    block_rows = math.gcd(key_count, 512)
    block_count = key_count // block_rows
    kv_blocks = kv_all.reshape(block_count, block_rows, 2 * width)
    seg_blocks = seg_all.reshape(block_count, block_rows)
    score_scale = 1.0 / math.sqrt(HD)

    def attention_step_block(query_grad, block_items):
        kv_rows, seg_rows, block_index = block_items
        key_rows = kv_rows[:, :width].reshape(block_rows, heads_here, HD)
        value_rows = kv_rows[:, width:].reshape(block_rows, heads_here, HD)
        k_pos = block_index * block_rows + jnp.arange(block_rows, dtype=jnp.int32)
        allowed = block_mask(q_pos, q_seg, k_pos, seg_rows)
        scores = (
            jnp.einsum("qhd,khd->hqk", queries, key_rows, preferred_element_type=jnp.float32)
            * score_scale
        )
        scores = jnp.where(allowed[None], scores, big_negative)
        probabilities = jnp.where(allowed[None], jnp.exp(scores - lse_all[..., None]), 0.0)
        value_grad = jnp.einsum(
            "hqk,qhd->khd",
            probabilities.astype(jnp.bfloat16),
            grad_heads,
            preferred_element_type=jnp.float32,
        )
        prob_grad = jnp.einsum(
            "qhd,khd->hqk", grad_heads, value_rows, preferred_element_type=jnp.float32
        )
        score_grad = (probabilities * (prob_grad - delta_all[..., None]) * score_scale).astype(
            jnp.bfloat16
        )
        query_grad = query_grad + jnp.einsum(
            "hqk,khd->hqd", score_grad, key_rows, preferred_element_type=jnp.float32
        )
        key_grad = jnp.einsum(
            "hqk,qhd->khd", score_grad, queries, preferred_element_type=jnp.float32
        )
        return (
            query_grad,
            jnp.concatenate(
                [key_grad.reshape(block_rows, width), value_grad.reshape(block_rows, width)], axis=1
            ),
        )

    query_grad, kv_grad_blocks = lax.scan(
        attention_step_block,
        jnp.zeros((heads_here, query_rows, HD), jnp.float32),
        (kv_blocks, seg_blocks, jnp.arange(block_count, dtype=jnp.int32)),
    )
    return (query_grad, kv_grad_blocks.reshape(key_count, 2 * width))


def gather_vectors(own_qkvb, own_upb, own_vec):
    return (
        lax.all_gather(own_qkvb, ("rep", "shard"), axis=0, tiled=True),
        lax.all_gather(own_upb, ("rep", "shard"), axis=0, tiled=True),
        lax.all_gather(own_vec, ("rep", "shard"), axis=0, tiled=True),
    )


def sum_vectors(qkvb_grad, upb_grad, vec_grad):
    return (
        lax.psum_scatter(qkvb_grad, ("rep", "shard"), scatter_dimension=0, tiled=True),
        lax.psum_scatter(upb_grad, ("rep", "shard"), scatter_dimension=0, tiled=True),
        lax.psum_scatter(vec_grad, ("rep", "shard"), scatter_dimension=0, tiled=True),
    )


def sum_positions(partial_rows):
    return lax.psum_scatter(partial_rows, "shard", scatter_dimension=0, tiled=True)


def attention_pass(norm_rows, qkv_w, qkv_b, positions, key_width):
    row_count = norm_rows.shape[0]
    heads_here = key_width // HD
    joined = jnp.dot(norm_rows, qkv_w, preferred_element_type=jnp.float32) + qkv_b
    q_pre = joined[:, :key_width].reshape(row_count, heads_here, HD)
    k_pre = joined[:, key_width : 2 * key_width].reshape(row_count, heads_here, HD)
    queries = rotary(q_pre, positions).astype(jnp.bfloat16)
    key_local = rotary(k_pre, positions).astype(jnp.bfloat16).reshape(row_count, key_width)
    value_local = joined[:, 2 * key_width :].astype(jnp.bfloat16)
    kv_local = jnp.concatenate([key_local, value_local], axis=1)
    return (q_pre, k_pre, queries, kv_local)


def finish_qkv_grad(q_pre, k_pre, positions, query_grad, kv_grad, key_width):
    row_count = q_pre.shape[0]
    heads_here = key_width // HD
    rotate_back = partial(rotary, positions=positions)
    query_pre = jax.vjp(rotate_back, q_pre)[1](query_grad.transpose(1, 0, 2))[0]
    key_pre = jax.vjp(rotate_back, k_pre)[1](
        kv_grad[:, :key_width].reshape(row_count, heads_here, HD)
    )[0]
    return jnp.concatenate(
        [
            query_pre.reshape(row_count, key_width),
            key_pre.reshape(row_count, key_width),
            kv_grad[:, key_width:],
        ],
        axis=1,
    )


def sliced_pass(norm_bf, q_seg, cotangent, own_mats, qkv_bb, up_bb):
    own_qkv, own_dense, own_up, own_down = own_mats
    inner_count = lax.axis_size("shard")
    outer_count = lax.axis_size("rep")
    stride = outer_count // inner_count
    place = lax.axis_index("shard")
    head_width = D // inner_count
    unit_width = FF // inner_count
    qkv_rows = own_qkv.shape[0]
    dense_rows = own_dense.shape[0]
    down_rows = own_down.shape[0]
    qkv_split = own_qkv.reshape(qkv_rows, 3, inner_count, head_width)
    up_split = own_up.reshape(qkv_rows, 1, inner_count, unit_width)
    qkv_cols, up_cols = (
        lax.all_to_all(qkv_split, "shard", split_axis=2, concat_axis=0, tiled=True),
        lax.all_to_all(up_split, "shard", split_axis=2, concat_axis=0, tiled=True),
    )
    qkv_rep, up_rep, dense_rep, down_rep = (
        lax.all_gather(qkv_cols, "rep", axis=0, tiled=True),
        lax.all_gather(up_cols, "rep", axis=0, tiled=True),
        lax.all_gather(own_dense[None], "rep", axis=0, tiled=True),
        lax.all_gather(own_down[None], "rep", axis=0, tiled=True),
    )
    dense_grid = dense_rep.reshape(inner_count, stride, 1, dense_rows, D)
    down_grid = down_rep.reshape(inner_count, stride, 1, down_rows, D)
    dense_moved, down_moved = (
        lax.all_to_all(dense_grid, "shard", split_axis=0, concat_axis=2, tiled=True),
        lax.all_to_all(down_grid, "shard", split_axis=0, concat_axis=2, tiled=True),
    )
    qkv_w = qkv_rep.reshape(D, 3 * head_width)
    up_w = up_rep.reshape(D, unit_width)
    dense_w = dense_moved.reshape(head_width, D)
    down_w = down_moved.reshape(unit_width, D)
    qkv_b = lax.dynamic_index_in_dim(
        qkv_bb.astype(jnp.float32).reshape(3, inner_count, head_width), place, 1, False
    ).reshape(3 * head_width)
    up_b = lax.dynamic_slice_in_dim(up_bb.astype(jnp.float32), place * unit_width, unit_width, 0)
    norm_seq, grad_seq, seg_seq = (
        lax.all_gather(norm_bf, "shard", axis=0, tiled=True),
        lax.all_gather(cotangent, "shard", axis=0, tiled=True),
        lax.all_gather(q_seg, "shard", axis=0, tiled=True),
    )
    seq_rows = norm_seq.shape[0]
    heads_here = head_width // HD
    positions = jnp.arange(seq_rows, dtype=jnp.int32)
    q_pre, k_pre, queries, kv_seq = attention_pass(norm_seq, qkv_w, qkv_b, positions, head_width)
    row_max, totals, accumulated = attend_keys(kv_seq, seg_seq, queries, positions, seg_seq)
    lse_all = row_max + jnp.log(totals)
    out_heads = (accumulated / totals[..., None]).transpose(1, 0, 2).astype(jnp.bfloat16)
    attn_bf = out_heads.reshape(seq_rows, head_width)
    pre_act = jnp.dot(norm_seq, up_w, preferred_element_type=jnp.float32) + up_b
    hidden = gelu_tanh(pre_act).astype(jnp.bfloat16)
    partial_out = jnp.dot(attn_bf, dense_w, preferred_element_type=jnp.float32) + jnp.dot(
        hidden, down_w, preferred_element_type=jnp.float32
    )
    mixed = sum_positions(partial_out)
    grad_down = jnp.dot(hidden.T, grad_seq, preferred_element_type=jnp.float32)
    grad_dense = jnp.dot(attn_bf.T, grad_seq, preferred_element_type=jnp.float32)
    grad_hidden = jnp.dot(grad_seq, down_w.T, preferred_element_type=jnp.float32)
    grad_pre = jax.vjp(gelu_tanh, pre_act)[1](grad_hidden)[0]
    grad_pre_bf = grad_pre.astype(jnp.bfloat16)
    grad_up = jnp.dot(norm_seq.T, grad_pre_bf, preferred_element_type=jnp.float32)
    upb_part = jnp.sum(grad_pre, axis=0)
    norm_part = jnp.dot(grad_pre_bf, up_w.T, preferred_element_type=jnp.float32)
    grad_heads = (
        jnp.dot(grad_seq, dense_w.T, preferred_element_type=jnp.float32)
        .astype(jnp.bfloat16)
        .reshape(seq_rows, heads_here, HD)
    )
    delta_all = jnp.sum(grad_heads.astype(jnp.float32) * out_heads.astype(jnp.float32), axis=-1).T
    query_grad, kv_grad = attention_grads(
        queries, kv_seq, seg_seq, positions, seg_seq, grad_heads, delta_all, lse_all
    )
    grad_joined = finish_qkv_grad(q_pre, k_pre, positions, query_grad, kv_grad, head_width)
    grad_joined_bf = grad_joined.astype(jnp.bfloat16)
    grad_qkv = jnp.dot(norm_seq.T, grad_joined_bf, preferred_element_type=jnp.float32)
    qkvb_part = jnp.sum(grad_joined, axis=0)
    norm_part = norm_part + jnp.dot(grad_joined_bf, qkv_w.T, preferred_element_type=jnp.float32)
    grad_norm = sum_positions(norm_part)
    dense_grid_grad = grad_dense.reshape(1, stride, inner_count, dense_rows, D)
    down_grid_grad = grad_down.reshape(1, stride, inner_count, down_rows, D)
    dense_back, down_back = (
        lax.all_to_all(dense_grid_grad, "shard", split_axis=2, concat_axis=0, tiled=True),
        lax.all_to_all(down_grid_grad, "shard", split_axis=2, concat_axis=0, tiled=True),
    )
    qkv_sum, up_sum, dense_sum, down_sum = (
        lax.psum_scatter(
            grad_qkv.reshape(D, 3, 1, head_width), "rep", scatter_dimension=0, tiled=True
        ),
        lax.psum_scatter(
            grad_up.reshape(D, 1, 1, unit_width), "rep", scatter_dimension=0, tiled=True
        ),
        lax.psum_scatter(
            dense_back.reshape(outer_count, dense_rows, D), "rep", scatter_dimension=0, tiled=True
        ),
        lax.psum_scatter(
            down_back.reshape(outer_count, down_rows, D), "rep", scatter_dimension=0, tiled=True
        ),
    )
    qkv_home, up_home = (
        lax.all_to_all(qkv_sum, "shard", split_axis=0, concat_axis=2, tiled=True),
        lax.all_to_all(up_sum, "shard", split_axis=0, concat_axis=2, tiled=True),
    )
    qkv_own = qkv_home.reshape(qkv_rows, 3 * D)
    up_own = up_home.reshape(qkv_rows, FF)
    dense_own = dense_sum.reshape(dense_rows, D)
    down_own = down_sum.reshape(down_rows, D)
    selector = (jnp.arange(inner_count, dtype=jnp.int32) == place).astype(jnp.float32)
    qkvb_grad = (selector[None, :, None] * qkvb_part.reshape(3, 1, head_width)).reshape(3 * D)
    upb_grad = (selector[:, None] * upb_part[None, :]).reshape(FF)
    return (mixed, grad_norm, (qkv_own, dense_own, up_own, down_own), qkvb_grad, upb_grad)


def body(
    hidden_in,
    segment_ids,
    out_grad,
    qkv_weight_state,
    qkv_bias_state,
    dense_weight_state,
    up_weight_state,
    up_bias_state,
    down_weight_state,
    vector_state,
):
    own_mats = (
        qkv_weight_state[0].astype(jnp.bfloat16),
        dense_weight_state[0].astype(jnp.bfloat16),
        up_weight_state[0].astype(jnp.bfloat16),
        down_weight_state[0].astype(jnp.bfloat16),
    )
    qkv_bb, up_bb, vec_bf = gather_vectors(
        qkv_bias_state[0].astype(jnp.bfloat16),
        up_bias_state[0].astype(jnp.bfloat16),
        vector_state[0].astype(jnp.bfloat16),
    )
    vec_all = vec_bf.astype(jnp.float32)
    norm_gain = vec_all[:, 0]
    norm_shift = vec_all[:, 1]
    dense_bias = vec_all[:, 2]
    down_bias = vec_all[:, 3]
    tokens = hidden_in[0]
    q_seg = segment_ids[0]
    cotangent = out_grad[0]
    x_full = tokens.astype(jnp.float32)
    normed = layer_norm(x_full, norm_gain, norm_shift)
    norm_bf = normed.astype(jnp.bfloat16)
    mixed, grad_norm, owned, qkvb_grad, upb_grad = sliced_pass(
        norm_bf, q_seg, cotangent, own_mats, qkv_bb, up_bb
    )
    qkv_own, dense_own, up_own, down_own = owned
    output = (x_full + (mixed + dense_bias + down_bias)).astype(jnp.bfloat16)
    grad_x, grad_gain, grad_shift = jax.vjp(layer_norm, x_full, norm_gain, norm_shift)[1](grad_norm)
    out_bias_grad = jnp.sum(cotangent.astype(jnp.float32), axis=0)
    grad_vec = jnp.stack([grad_gain, grad_shift, out_bias_grad, out_bias_grad], axis=1)
    input_grad = cotangent.astype(jnp.float32) + grad_x
    qkvb_own, upb_own, vec_own = sum_vectors(qkvb_grad, upb_grad, grad_vec)
    new_states = (
        adam_update(qkv_weight_state, qkv_own),
        adam_update(qkv_bias_state, qkvb_own),
        adam_update(dense_weight_state, dense_own),
        adam_update(up_weight_state, up_own),
        adam_update(up_bias_state, upb_own),
        adam_update(down_weight_state, down_own),
        adam_update(vector_state, vec_own),
    )
    return (
        output[None],
        input_grad[None],
        qkv_own,
        qkvb_own,
        dense_own,
        up_own,
        upb_own,
        down_own,
        vec_own,
        owner_entries(new_states, 0),
        owner_entries(new_states, 1),
        owner_entries(new_states, 2),
    )


def whole_heads(mesh):
    owners = mesh.shape["rep"] * mesh.shape["shard"]
    return D % owners == 0 and D // owners == HD and mesh.shape["rep"] % 2 == 0


def rotation_tables(seq_rows):
    half_rot = ROT // 2
    lane = jnp.arange(2 * HD, dtype=jnp.int32) % HD
    frequency = jnp.exp((lane % half_rot).astype(jnp.float32) * (-2.0 * math.log(10000.0) / ROT))
    angles = jnp.arange(seq_rows, dtype=jnp.int32).astype(jnp.float32)[:, None] * frequency[None, :]
    sine = jnp.sin(angles)
    cosine = jnp.where(lane[None, :] < ROT, jnp.cos(angles), 1.0)
    low = jnp.where(lane[None, :] < half_rot, -sine, 0.0)
    high = jnp.where((lane[None, :] >= half_rot) & (lane[None, :] < ROT), sine, 0.0)
    return cosine, low, high


def attention_kernel(
    fu_ref, do_ref, du_ref, seg_col_ref, seg_row_ref, cos_ref, low_ref, high_ref, o_ref, dcat_ref, sums_ref
):
    rows, width = do_ref.shape
    scale = 1.0 / math.sqrt(HD)
    row_id = lax.broadcasted_iota(jnp.int32, (rows, rows), 0)
    col_id = lax.broadcasted_iota(jnp.int32, (rows, rows), 1)
    allowed = (col_id <= row_id) & (seg_col_ref[...] == seg_row_ref[0])
    cosine, low, high = cos_ref[...], low_ref[...], high_ref[...]
    half = ROT // 2
    lane = lax.broadcasted_iota(jnp.int32, (rows, 2 * HD), 1)

    def rotate(u):
        return (
            u * cosine
            + pltpu.roll(u, 2 * HD - half, 1) * low
            + pltpu.roll(u, half, 1) * high
        )

    def rotate_back(u):
        return (
            u * cosine
            - pltpu.roll(u, 2 * HD - half, 1) * low
            - pltpu.roll(u, half, 1) * high
        )

    def dot(a, b, a_dim, b_dim):
        return lax.dot_general(a, b, (((a_dim,), (b_dim,)), ((), ())), preferred_element_type=jnp.float32)

    zero = jnp.zeros((), jnp.bfloat16)
    for pair in range(width // (2 * HD)):
        lanes = pl.ds(pair * 2 * HD, 2 * HD)
        k_lanes = pl.ds(width + pair * 2 * HD, 2 * HD)
        v_lanes = pl.ds(2 * width + pair * 2 * HD, 2 * HD)
        q = rotate(fu_ref[:, lanes]).astype(jnp.bfloat16)
        k = rotate(fu_ref[:, k_lanes]).astype(jnp.bfloat16)
        v = fu_ref[:, v_lanes].astype(jnp.bfloat16)
        do = do_ref[:, lanes]
        o = dq = dk = dv = None
        for head in range(2):
            mine = (lane < HD) if head == 0 else (lane >= HD)
            qh = jnp.where(mine, q, zero)
            kh = jnp.where(mine, k, zero)
            vh = jnp.where(mine, v, zero)
            doh = jnp.where(mine, do, zero)
            scores = jnp.where(allowed, dot(qh, k, 1, 1) * scale, big_negative)
            row_max = jnp.max(scores, axis=1, keepdims=True)
            probs = jnp.where(allowed, jnp.exp(scores - row_max), 0.0)
            inverse = 1.0 / jnp.sum(probs, axis=1, keepdims=True)
            oh = dot(probs.astype(jnp.bfloat16), vh, 1, 0) * inverse
            delta = jnp.sum(
                doh.astype(jnp.float32) * oh.astype(jnp.bfloat16).astype(jnp.float32), axis=1, keepdims=True
            )
            probs = probs * inverse
            dvh = dot(probs.astype(jnp.bfloat16), doh, 0, 0)
            ds = (probs * (dot(doh, v, 1, 1) - delta) * scale).astype(jnp.bfloat16)
            dqh = dot(ds, kh, 1, 0)
            dkh = dot(ds, qh, 0, 0)
            if head == 0:
                o, dq, dk, dv = oh, dqh, dkh, dvh
            else:
                o, dq, dk, dv = o + oh, dq + dqh, dk + dkh, dv + dvh
        o_ref[:, lanes] = o.astype(jnp.bfloat16)
        dq = rotate_back(dq)
        dk = rotate_back(dk)
        for part, place in ((dq, lanes), (dk, k_lanes), (dv, v_lanes)):
            dcat_ref[:, place] = part.astype(jnp.bfloat16)
            sums_ref[0, :, place] = jnp.sum(part, axis=0, keepdims=True)
    dcat_ref[:, pl.ds(3 * width, du_ref.shape[1])] = du_ref[...]


def attention(fu, do, du, segments):
    count, rows = segments.shape
    width = do.shape[1]
    units = du.shape[1]
    tables = rotation_tables(rows)
    table_spec = pl.BlockSpec((rows, 2 * HD), lambda s: (0, 0))
    o, dcat, sums = pl.pallas_call(
        attention_kernel,
        grid=(count,),
        in_specs=[
            pl.BlockSpec((rows, 3 * width), lambda s: (s, 0)),
            pl.BlockSpec((rows, width), lambda s: (s, 0)),
            pl.BlockSpec((rows, units), lambda s: (s, 0)),
            pl.BlockSpec((rows, 1), lambda s: (s, 0)),
            pl.BlockSpec((1, 1, rows), lambda s: (s, 0, 0)),
            table_spec,
            table_spec,
            table_spec,
        ],
        out_specs=[
            pl.BlockSpec((rows, width), lambda s: (s, 0)),
            pl.BlockSpec((rows, 3 * width + units), lambda s: (s, 0)),
            pl.BlockSpec((1, 1, 3 * width), lambda s: (s, 0, 0)),
        ],
        out_shape=[
            jax.ShapeDtypeStruct((count * rows, width), jnp.bfloat16),
            jax.ShapeDtypeStruct((count * rows, 3 * width + units), jnp.bfloat16),
            jax.ShapeDtypeStruct((count, 1, 3 * width), jnp.float32),
        ],
        compiler_params=pltpu.CompilerParams(vmem_limit_bytes=56 << 20),
        cost_estimate=pl.CostEstimate(
            flops=count * (width // HD) * 10 * rows * rows * HD,
            bytes_accessed=count * rows * (width * 20 + units * 4),
            transcendentals=count * (width // HD) * rows * rows,
        ),
    )(fu, do, du, segments.reshape(count * rows, 1), segments.reshape(count, 1, rows), *tables)
    return o, dcat, jnp.sum(sums, axis=(0, 1))


def adam_values(weight, moment_one, moment_two, grad):
    first = beta_one * moment_one + (1.0 - beta_one) * grad
    second = beta_two * moment_two + (1.0 - beta_two) * grad * grad
    corrected = first * (1.0 / (1.0 - beta_one**STEP))
    divisor = jnp.sqrt(second * (1.0 / (1.0 - beta_two**STEP))) + adam_eps
    return weight - learn_rate * (corrected / divisor + weight_decay * weight), first, second


def owner_update_kernel(plan, small_plan, groups, steps, whole_rows, *refs):
    planes, cores, shards = groups
    qkv_state, dense_state, up_state, down_state, cat_ref, dense_grad, down_grad, small_ref = refs[:8]
    flat = refs[8:11]
    qkv_out, up_out, cat_buf = refs[11:14]
    outs = refs[14:17]
    step_sem, rest_sem = refs[17:]
    step = pl.program_id(0)
    lane = lax.broadcasted_iota(jnp.int32, (8, 128), 1)
    sub = lax.broadcasted_iota(jnp.int32, (8, 128), 0)
    lane_row = lax.broadcasted_iota(jnp.int32, (1, 128), 1)
    wide = 1024

    @pl.when(step == 0)
    def small():
        for source, row, low, high in small_plan:
            for entry in range(3):
                old = outs[entry][pl.ds(row, 1), :]
                new = small_ref[entry, pl.ds(source, 1), :]
                outs[entry][pl.ds(row, 1), :] = jnp.where((lane_row >= low) & (lane_row < high), new, old)

    def widen(piece, carry):
        cat_buf[piece] = cat_ref[piece].astype(jnp.float32)
        return carry

    lax.fori_loop(0, cat_ref.shape[0], widen, 0)

    def place_rows(state, grad_of, rows, tiles, start, shifted, keep=None):
        chunk = min(wide, tiles * 128)

        def one_group(group, carry):
            place = pl.ds(pl.multiple_of(group * 8, 8), 8)
            base = start + (step * (rows // 8) + group) * (8 * tiles)

            def values(column, size):
                lanes = pl.ds(column, size)
                grad = grad_of(place, column, size)
                if keep is not None and size > 128:
                    keep[place, lanes] = grad
                return adam_values(
                    state[0, place, lanes], state[1, place, lanes], state[2, place, lanes], grad
                )

            if shifted:
                last = tuple(pltpu.roll(value, 64, 1) for value in values((tiles - 1) * 128, 128))
                before = tuple(
                    jnp.where(sub == 0, out[pl.ds(base, 1), :], pltpu.roll(value, 1, 0))
                    for out, value in zip(outs, last)
                )
            for column in range(0, tiles * 128, chunk):
                done = values(column, chunk)
                for entry, out in enumerate(outs):
                    for tile in range(chunk // 128):
                        value = done[entry][:, tile * 128 : (tile + 1) * 128]
                        if shifted:
                            value = pltpu.roll(value, 64, 1)
                            old = before[entry] if tile == 0 else now
                            now = value
                            value = jnp.where(lane < 64, old, value)
                        out[pl.ds(base + column // 128 + tile, 8, stride=tiles), :] = value
                    if shifted:
                        before = before[:entry] + (now,) + before[entry + 1 :]
            if shifted:
                for out, value in zip(outs, before):
                    row = pl.ds(base + 8 * tiles, 1)
                    out[row, :] = jnp.where(lane_row < 64, value[7:8], out[row, :])
            return carry

        lax.fori_loop(0, rows // 8, one_group, 0)

    def qkv_grad(place, column, size):
        tiles = []
        for start in range(column, column + size, 128):
            part, head = divmod(start // HD, planes * cores * shards)
            halves = []
            for side in range(2):
                plane, member = divmod(head + side, cores * shards)
                spot = (part * planes + plane) * HD
                half = cat_buf[member, place, pl.ds(spot // 128 * 128, 128)]
                halves.append(half if spot % 128 == side * HD else pltpu.roll(half, HD, 1))
            tiles.append(jnp.where(lane < HD, halves[0], halves[1]))
        return tiles[0] if len(tiles) == 1 else jnp.concatenate(tiles, axis=1)

    units = up_state.shape[2] // (planes * cores * shards)

    def up_grad(place, column, size):
        parts = []
        for start in range(column, column + size, min(units, size)):
            plane, member = divmod(start // units, cores * shards)
            spot = 3 * planes * HD + plane * units + start % units
            parts.append(cat_buf[member, place, pl.ds(spot, min(units, size))])
        return parts[0] if len(parts) == 1 else jnp.concatenate(parts, axis=1)

    def plain(grad):
        return lambda place, column, size: grad[place, pl.ds(column, size)]

    place_rows(qkv_state, qkv_grad, *plan[0], keep=qkv_out)
    place_rows(dense_state, plain(dense_grad), *plan[1])
    place_rows(up_state, up_grad, *plan[2], keep=up_out)
    place_rows(down_state, plain(down_grad), *plan[3])

    def flush(entry, row, count, sem):
        place = pl.ds(pl.multiple_of(row * 128, 128), count * 128)
        source = outs[entry].reshape(1, 1, outs[entry].shape[0] * 128)
        return pltpu.make_async_copy(source.at[:, :, place], flat[entry].at[:, :, place], sem)

    def step_copies(at):
        copies = []
        for index, (rows, tiles, start, shifted) in enumerate(plan):
            count = rows * tiles
            skip = 1 if shifted and at == 0 else 0
            for entry in range(3):
                copies.append(
                    flush(entry, start + at * count + skip, count - skip, step_sem.at[entry, index, at])
                )
        return copies

    for at in range(steps):

        @pl.when(step == at)
        def begin(at=at):
            for copy in step_copies(at):
                copy.start()

    @pl.when(step == steps - 1)
    def end():
        covered = set()
        for rows, tiles, start, shifted in plan:
            covered |= set(range(start + (1 if shifted else 0), start + steps * rows * tiles))
        left = [row for row in range(whole_rows) if row not in covered]
        rest = [
            flush(entry, row, 1, rest_sem.at[entry, index]) for index, row in enumerate(left) for entry in range(3)
        ]
        for copy in rest:
            copy.start()
        for at in range(steps):
            for copy in step_copies(at):
                copy.wait()
        for copy in rest:
            copy.wait()


def owner_update(states, cat_sum, grads, small_states, small_grads, groups):
    steps = 4
    sizes = [state.shape[1] * state.shape[2] for state in states]
    small_sizes = [grad.size for grad in small_grads]
    order = [("m", 0), ("s", 0), ("m", 1), ("m", 2), ("s", 1), ("m", 3), ("s", 2)]
    offset = 0
    plan = [None] * 4
    small_plan = []
    pads = []
    small_row = 0
    for kind, index in order:
        if kind == "m":
            state = states[index]
            rows = state.shape[1] // steps
            plan[index] = (rows, state.shape[2] // 128, offset // 128, offset % 128 == 64)
            offset += sizes[index]
        else:
            size = small_sizes[index]
            front = offset % 128
            total = -(-(front + size) // 128)
            pads.append((front, total * 128 - front - size))
            for extra in range(total):
                low = front if extra == 0 else 0
                high = min(128, front + size - extra * 128)
                small_plan.append((small_row + extra, offset // 128 + extra, low, high))
            small_row += total
            offset += size
    entries = offset
    out_rows = -(-entries // 1024) * 8
    small_new = [
        adam_values(state[0].reshape(-1), state[1].reshape(-1), state[2].reshape(-1), grad.reshape(-1))
        for state, grad in zip(small_states, small_grads)
    ]
    small = jnp.stack(
        [
            jnp.concatenate([jnp.pad(new[entry], pad) for new, pad in zip(small_new, pads)])
            for entry in range(3)
        ]
    ).reshape(3, small_row, 128)
    in_specs = [
        pl.BlockSpec((3, rows, tiles * 128), lambda s: (0, s, 0)) for rows, tiles, start, shifted in plan
    ]
    qkv_rows, up_rows = plan[0][0], plan[2][0]
    in_specs.append(pl.BlockSpec((cat_sum.shape[0], qkv_rows, cat_sum.shape[2]), lambda s: (0, s, 0)))
    in_specs.append(pl.BlockSpec((plan[1][0], plan[1][1] * 128), lambda s: (s, 0)))
    in_specs.append(pl.BlockSpec((plan[3][0], plan[3][1] * 128), lambda s: (s, 0)))
    in_specs.append(pl.BlockSpec((3, small_row, 128), lambda s: (0, 0, 0)))
    whole_rows = entries // 128
    *outs, qkv_grad, up_grad = pl.pallas_call(
        partial(owner_update_kernel, plan, small_plan, groups, steps, whole_rows),
        grid=(steps,),
        in_specs=in_specs,
        out_specs=[pl.BlockSpec(memory_space=pl.ANY)] * 3
        + [
            pl.BlockSpec((qkv_rows, plan[0][1] * 128), lambda s: (s, 0)),
            pl.BlockSpec((up_rows, plan[2][1] * 128), lambda s: (s, 0)),
        ],
        out_shape=[jax.ShapeDtypeStruct((1, 1, entries), jnp.float32)] * 3
        + [
            jax.ShapeDtypeStruct(states[0].shape[1:], jnp.float32),
            jax.ShapeDtypeStruct(states[2].shape[1:], jnp.float32),
        ],
        scratch_shapes=[pltpu.VMEM((cat_sum.shape[0], qkv_rows, cat_sum.shape[2]), jnp.float32)]
        + [pltpu.VMEM((out_rows, 128), jnp.float32)] * 3
        + [pltpu.SemaphoreType.DMA((3, 4, steps)), pltpu.SemaphoreType.DMA((3, 16))],
        compiler_params=pltpu.CompilerParams(vmem_limit_bytes=56 << 20),
        cost_estimate=pl.CostEstimate(
            flops=20 * entries, bytes_accessed=28 * entries, transcendentals=2 * entries
        ),
    )(*states, cat_sum, *grads, small)
    tail = entries - whole_rows * 128
    if tail:
        outs = [
            lax.dynamic_update_slice(out, new[entries_of][-tail:].reshape(1, 1, tail), (0, 0, whole_rows * 128))
            for out, (new, entries_of) in zip(outs, ((small_new[-1], entry) for entry in range(3)))
        ]
    return tuple(outs), qkv_grad, up_grad


class Wires:
    def __init__(self, send_sems):
        self.send_sems, self.count, self.pending = send_sems, 0, []
        self.plane, self.core, self.shard = (
            lax.axis_index("plane"),
            lax.axis_index("core"),
            lax.axis_index("shard"),
        )
        self.shards = lax.axis_size("shard")
        self.group = lax.axis_size("core") * self.shards
        self.mine = self.core * self.shards + self.shard
        self.first = (self.plane ^ 1, self.core, self.shard)
        self.second = (self.plane ^ 2, self.core, self.shard)

    def member(self, index):
        return (self.plane, index // self.shards, index % self.shards)

    def barrier(self):
        barrier = pltpu.get_barrier_semaphore()
        partners = [self.member(self.mine ^ mask) for mask in range(1, self.group)]
        partners += [self.first, self.second]
        for partner in partners:
            pl.semaphore_signal(barrier, inc=1, device_id=partner, device_id_type=pl.DeviceIdType.MESH)
        pl.semaphore_wait(barrier, len(partners))

    def send(self, source, target, recv_sem, device, when=None):
        copy = pltpu.make_async_remote_copy(
            src_ref=source,
            dst_ref=target,
            send_sem=self.send_sems.at[self.count],
            recv_sem=recv_sem,
            device_id=device,
            device_id_type=pl.DeviceIdType.MESH,
        )
        self.count += 1
        self.pending.append((copy, when))
        if when is None:
            copy.start()
        else:
            pl.when(when)(copy.start)

    def arrived(self, place, recv_sem, when=None):
        copy = pltpu.make_async_remote_copy(
            src_ref=place,
            dst_ref=place,
            send_sem=self.send_sems.at[0],
            recv_sem=recv_sem,
            device_id=self.first,
            device_id_type=pl.DeviceIdType.MESH,
        )
        if when is None:
            copy.wait_recv()
        else:
            pl.when(when)(copy.wait_recv)

    def drain(self):
        for copy, when in self.pending:
            if when is None:
                copy.wait_send()
            else:
                pl.when(when)(copy.wait_send)


def pack_pieces(qkv, up, pieces, planes, cores, shards):
    rows = qkv.shape[0]
    lane = lax.broadcasted_iota(jnp.int32, (rows, 128), 1)
    units = up.shape[1] // (planes * cores * shards)
    for core in range(cores):
        for shard in range(shards):
            piece = core * shards + shard
            for tile in range(3 * planes // 2):
                halves = []
                for side in range(2):
                    part, plane = divmod(2 * tile + side, planes)
                    head = (plane * cores + core) * shards + shard
                    start = part * planes * cores * shards * HD + head * HD
                    half = qkv[:, pl.ds(start // 128 * 128, 128)]
                    halves.append(half if start % 128 == side * HD else pltpu.roll(half, HD, 1))
                pieces[piece, :, pl.ds(tile * 128, 128)] = jnp.where(lane < HD, halves[0], halves[1]).astype(
                    jnp.bfloat16
                )
            for plane in range(planes):
                block = (plane * cores + core) * shards + shard
                pieces[piece, :, pl.ds(3 * planes * HD + plane * units, units)] = up[
                    :, pl.ds(block * units, units)
                ].astype(jnp.bfloat16)


def gather_kernel(
    qkv_state, up_state, dense_state, down_state, tokens, cotangent, vectors,
    cat_out, dense_out, down_out, x_out, dy_out, vec_out,
    qkv_buf, up_buf, dense_buf, down_buf, pieces, dense, down,
    load_sem, send_sems, group_sem, first_sem, second_sem, far_sem, up_sem, low_sem, core_sem, local_sem,
):
    net = Wires(send_sems)
    plane, core, shard, shards, group, mine = net.plane, net.core, net.shard, net.shards, net.group, net.mine
    order = sorted(range(group), key=lambda mask: (mask % shards, mask // shards))
    partner = (plane, 1 - core, shard)

    def cat_unit(mask):
        return lambda p: cat_out.at[p, mine ^ mask]

    def vec_unit(mask):
        return lambda p: vec_out.at[p, mine ^ mask]

    units = []
    down_rows = down.shape[0] // 4
    for part in range(4):
        rows = pl.ds(part * down_rows, down_rows)
        units.append((down.at[rows], lambda p, rows=rows: down_out.at[p, rows]))
    dense_rows = dense.shape[0] // 2
    for part in range(2):
        rows = pl.ds(part * dense_rows, dense_rows)
        units.append((dense.at[rows], lambda p, rows=rows: dense_out.at[p, rows]))
    own_units = list(range(len(units)))
    cat_units, vec_units = {}, {}
    for mask in order:
        cat_units[mask] = len(units)
        units.append((pieces.at[mine] if mask == 0 else None, cat_unit(mask)))
        vec_units[mask] = len(units)
        units.append((vectors if mask == 0 else None, vec_unit(mask)))

    def spread(index):
        source, place = units[index]
        source = place(plane) if source is None else source
        net.send(source, place(plane), first_sem.at[index], net.first)
        net.send(source, place(plane), second_sem.at[index], net.second)

    def hand_on(index):
        place = units[index][1]
        if relay_first[index]:
            net.arrived(place(plane ^ 1), first_sem.at[index])
            net.send(place(plane ^ 1), place(plane ^ 1), far_sem.at[index], net.second)
        else:
            net.arrived(place(plane ^ 2), second_sem.at[index])
            net.send(place(plane ^ 2), place(plane ^ 2), far_sem.at[index], net.first)

    relay_first = {}
    for position, index in enumerate(own_units):
        relay_first[index] = position % 2 == 0
    for position, mask in enumerate(order):
        relay_first[cat_units[mask]] = position % 2 == 0
        relay_first[vec_units[mask]] = position % 2 == 1

    loads = [
        pltpu.make_async_copy(state.at[0], buffer, load_sem.at[index])
        for index, (state, buffer) in enumerate(
            ((qkv_state, qkv_buf), (up_state, up_buf), (down_state, down_buf), (dense_state, dense_buf))
        )
    ]
    for index in (2, 3, 0, 1):
        loads[index].start()
    net.barrier()
    loads[2].wait()
    down[...] = down_buf[...].astype(jnp.bfloat16)
    loads[3].wait()
    dense[...] = dense_buf[...].astype(jnp.bfloat16)
    for index in own_units:
        spread(index)
    loads[0].wait()
    loads[1].wait()
    pack_pieces(qkv_buf, up_buf, pieces, cat_out.shape[0], group // shards, shards)

    locals_ = [
        (pieces.at[mine], cat_out.at[plane, mine]),
        (dense, dense_out.at[plane]),
        (down, down_out.at[plane]),
        (tokens, x_out.at[mine]),
        (cotangent, dy_out.at[mine]),
        (vectors, vec_out.at[plane, mine]),
    ]
    copies = [
        pltpu.make_async_copy(source, target, local_sem.at[index])
        for index, (source, target) in enumerate(locals_)
    ]
    for mask in order[1:]:
        target = net.member(mine ^ mask)
        net.send(vectors, vec_out.at[plane, mine], group_sem.at[1, mask], target)
        net.send(pieces.at[mine ^ mask], cat_out.at[plane, mine], group_sem.at[0, mask], target)
    spread(cat_units[0])
    spread(vec_units[0])
    streams = ((tokens, x_out), (cotangent, dy_out))

    def block(stream, origin):
        return streams[stream][1].at[core * shards + origin]

    def to_core(stream, source, origin, slot, when=None):
        net.send(source, block(stream, origin), core_sem.at[stream, slot], partner, when)

    def hop(stream, distance):
        own = distance == 1
        for upward, sem in ((True, up_sem), (False, low_sem)):
            origin = shard - (distance - 1) if upward else shard + (distance - 1)
            there = shard + 1 if upward else shard - 1
            held = (origin >= 0) if upward else (origin < shards)
            inside = (there < shards) if upward else (there >= 0)
            near = jnp.clip(origin, 0, shards - 1)
            source = streams[stream][0] if own else block(stream, near)
            net.send(
                source,
                block(stream, near),
                sem.at[stream, distance],
                (plane, core, jnp.clip(there, 0, shards - 1)),
                inside & held,
            )

    def hop_arrived(stream, distance):
        for upward, sem in ((True, up_sem), (False, low_sem)):
            origin = shard - distance if upward else shard + distance
            held = (origin >= 0) if upward else (origin < shards)
            near = jnp.clip(origin, 0, shards - 1)
            net.arrived(block(stream, near), sem.at[stream, distance], held)
            slot = distance if upward else shards + distance
            to_core(stream, block(stream, near), near, slot, held)

    for stream in range(2):
        hop(stream, 1)
    for stream in range(2):
        to_core(stream, streams[stream][0], shard, 0)
    for copy in copies:
        copy.start()

    for position, mask in enumerate(order[1:]):
        net.arrived(vec_out.at[plane, mine ^ mask], group_sem.at[1, mask])
        spread(vec_units[mask])
        net.arrived(cat_out.at[plane, mine ^ mask], group_sem.at[0, mask])
        spread(cat_units[mask])
        if position == 2:
            for index in own_units:
                hand_on(index)
    hand_on(cat_units[0])
    hand_on(vec_units[0])
    for distance in range(1, shards):
        for stream in range(2):
            hop_arrived(stream, distance)
            if distance + 1 < shards:
                hop(stream, distance + 1)
        for mask in order[1 + (distance - 1) * 3 : 1 + distance * 3]:
            hand_on(vec_units[mask])
            hand_on(cat_units[mask])

    for index, (source, place) in enumerate(units):
        if relay_first[index]:
            net.arrived(place(plane ^ 2), second_sem.at[index])
        else:
            net.arrived(place(plane ^ 1), first_sem.at[index])
        net.arrived(place(plane ^ 3), far_sem.at[index])
    for stream in range(2):
        other = streams[stream][1]
        for slot in range(2 * shards):
            if slot == shards:
                continue
            origin = shard - slot if slot < shards else shard + (slot - shards)
            held = None if slot == 0 else ((origin >= 0) & (origin < shards))
            near = jnp.clip(origin, 0, shards - 1)
            net.arrived(other.at[(1 - core) * shards + near], core_sem.at[stream, slot], held)
    for copy in copies:
        copy.wait()
    net.drain()


def gather_wires(qkv, up, dense, down, tokens, cotangent, vectors):
    group, shards = lax.axis_size("core") * lax.axis_size("shard"), lax.axis_size("shard")
    planes = lax.axis_size("plane")
    width = (qkv.shape[2] + up.shape[2]) // group
    units = 6 + 2 * group
    vmem = pl.BlockSpec(memory_space=pltpu.VMEM)
    hbm = pl.BlockSpec(memory_space=pl.ANY)

    def out(*shape, dtype=jnp.bfloat16):
        return jax.ShapeDtypeStruct(shape, dtype)

    dma = pltpu.SemaphoreType.DMA
    return pl.pallas_call(
        gather_kernel,
        in_specs=[hbm] * 4 + [vmem] * 3,
        out_specs=[hbm] * 6,
        out_shape=[
            out(planes, group, qkv.shape[1], width),
            out(planes, *dense.shape[1:]),
            out(planes, *down.shape[1:]),
            out(group, *tokens.shape),
            out(group, *cotangent.shape),
            out(planes, group, *vectors.shape, dtype=vectors.dtype),
        ],
        scratch_shapes=[
            pltpu.VMEM(qkv.shape[1:], qkv.dtype),
            pltpu.VMEM(up.shape[1:], up.dtype),
            pltpu.VMEM(dense.shape[1:], dense.dtype),
            pltpu.VMEM(down.shape[1:], down.dtype),
            pltpu.VMEM((group, qkv.shape[1], width), jnp.bfloat16),
            pltpu.VMEM(dense.shape[1:], jnp.bfloat16),
            pltpu.VMEM(down.shape[1:], jnp.bfloat16),
            dma((4,)),
            dma((2 * (group - 1) + 3 * units + 2 * 2 * (shards - 1) + 2 * (2 * shards - 1),)),
            dma((2, group)),
            dma((units,)),
            dma((units,)),
            dma((units,)),
            dma((2, shards)),
            dma((2, shards)),
            dma((2, 2 * shards)),
            dma((6,)),
        ],
        compiler_params=pltpu.CompilerParams(
            collective_id=0, has_side_effects=True, vmem_limit_bytes=67043328
        ),
    )(qkv, up, dense, down, tokens, cotangent, vectors)


def add_rows(target, *sources):
    step = 16
    rows = target.shape[0]

    def body(index, carry):
        place = pl.ds(pl.multiple_of(index * step, step), step)
        total = sources[0][place, :].astype(jnp.float32)
        for source in sources[1:]:
            total = total + source[place, :].astype(jnp.float32)
        target[place, :] = total.astype(target.dtype)
        return carry

    lax.fori_loop(0, rows // step, body, 0)


def chunked(first, last, copies_of, body):
    for copy in copies_of(first, first % 2):
        copy.start()

    def step(n, carry):
        slot = lax.rem(n, 2)

        @pl.when(n + 1 < last)
        def ahead():
            for copy in copies_of(n + 1, 1 - slot):
                copy.start()

        for copy in copies_of(n, slot):
            copy.wait()
        body(n, slot)
        return carry

    lax.fori_loop(first, last, step, 0)


def reduce_kernel(
    norm, dcat, x_all, mean, inverse, attn, hidden, dy, cat_w, dense_w, down_w, sums,
    cat_out, dense_out, down_out, mixed_out, norm_out, sums_out,
    cat_part, down_part, dense_part, cat_in, down_in, dense_in,
    tokens, token_in, token_line, token_last, sum_buf,
    wide, hidden_turned, attn_turned, norm_chunk, norm_turned, cat_chunk, x_chunk, down_chunk, dense_chunk, dy_chunk,
    send_sems, near_sem, pass_sem, group_sem, core_sem, line_sem, sum_sem, local_sem, chunk_sem,
):
    PASS, KEEP, LAST = range(3)
    net = Wires(send_sems)
    plane, core, shard, shards, group, mine = net.plane, net.core, net.shard, net.shards, net.group, net.mine
    planes = cat_part.shape[0]
    partner = (plane, 1 - core, shard)
    order = sorted(range(group), key=lambda mask: (mask % shards, mask // shards), reverse=True)
    rows, width = dcat.shape
    model = norm.shape[1]
    block = cat_part.shape[2]
    token_rows = tokens.shape[2]
    units_here = hidden.shape[1]
    heads_here = attn.shape[1]
    lane = 256

    def dot(a, b, a_dim=1, b_dim=0):
        return lax.dot_general(a, b, (((a_dim,), (b_dim,)), ((), ())), preferred_element_type=jnp.float32)

    def columns(n):
        return pl.ds(pl.multiple_of(n * lane, lane), lane)

    units = [(cat_part, cat_in, mask) for mask in order]
    units += [(down_part, down_in, part) for part in range(down_part.shape[1])]
    units += [(dense_part, dense_in, part) for part in range(dense_part.shape[1])]
    down_rows, dense_rows = down_part.shape[2], dense_part.shape[2]

    def ways(index):
        return (net.first, net.second, 1, 2) if index % 2 == 0 else (net.second, net.first, 2, 1)

    def send_pass(index):
        parts, came, slot = units[index]
        net.send(parts.at[3, slot], came.at[PASS, slot], pass_sem.at[0, index], ways(index)[0])

    def send_keep(index):
        parts, came, slot = units[index]
        near, far, near_mask, far_mask = ways(index)
        net.send(parts.at[near_mask, slot], came.at[KEEP, slot], near_sem.at[index], near)

    locals_ = {}

    def local(key, source, target):
        locals_[key] = pltpu.make_async_copy(source, target, local_sem.at[len(locals_)])
        locals_[key].start()

    local("hidden", hidden, wide.at[:, pl.ds(0, units_here)])
    local("attn", attn, wide.at[:, pl.ds(units_here, heads_here)])
    net.barrier()

    places = [place for rank in range(shards // 2) for place in (shards - 1 - rank, rank)]

    def to_partner(stream):
        for place in places:
            net.send(
                tokens.at[stream, (1 - core) * shards + place],
                token_in.at[stream, place],
                core_sem.at[stream, place],
                partner,
            )

    def out_copies(n, slot):
        return [
            pltpu.make_async_copy(down_w.at[:, columns(n)], down_chunk.at[slot], chunk_sem.at[3, slot]),
            pltpu.make_async_copy(dense_w.at[:, columns(n)], dense_chunk.at[slot], chunk_sem.at[4, slot]),
        ]

    def out_step(n, slot):
        total = dot(wide[:, pl.ds(0, units_here)], down_chunk[slot]) + dot(
            wide[:, pl.ds(units_here, heads_here)], dense_chunk[slot]
        )
        for member in range(group):
            tokens[0, member, :, columns(n)] = total[member * token_rows : (member + 1) * token_rows].astype(
                jnp.bfloat16
            )

    locals_["hidden"].wait()
    locals_["attn"].wait()
    chunked(0, model // lane, out_copies, out_step)
    to_partner(0)
    hidden_turned[...] = wide[:, pl.ds(0, units_here)].T
    attn_turned[...] = wide[:, pl.ds(units_here, heads_here)].T
    local("dcat", dcat, wide.at[:, pl.ds(0, width)])

    plane_rows = group * block

    def norm_copy(turn, distance):
        place = pl.ds(pl.multiple_of((plane ^ distance) * plane_rows, plane_rows), plane_rows)
        return pltpu.make_async_copy(
            norm.at[:, place], norm_chunk.at[turn % 2], chunk_sem.at[0, turn % 2]
        )

    cats, every = range(group), range(len(units))
    chain_steps = sorted(
        ((hop, rank) for hop in range(1, shards - 1) for rank in range(shards - 1 - hop)),
        key=lambda pair: (pair[0] + 2 * pair[1], pair[0]),
    )
    turns = (3, 1, 2, 0)
    norm_copy(0, turns[0]).start()
    locals_["dcat"].wait()

    def cat_turn(turn):
        distance = turns[turn]
        if turn + 1 < planes:
            norm_copy(turn + 1, turns[turn + 1]).start()
        norm_copy(turn, distance).wait()
        norm_turned[...] = norm_chunk[turn % 2].T

        def cat_step(n, carry):
            total = dot(norm_turned[...], wide[:, columns(n)]).astype(jnp.bfloat16)
            for member in range(group):
                cat_part[distance, mine ^ member, :, columns(n)] = total[member * block : (member + 1) * block]
            return carry

        lax.fori_loop(0, width // lane, cat_step, 0)
        for index in cats:
            if distance == 3:
                send_pass(index)
            elif distance == ways(index)[2]:
                send_keep(index)

    def own(stream, place):
        return tokens.at[stream, core * shards + place]

    def chain(stream, hop, rank):
        for upward in (True, False):
            target = shards - 1 - rank if upward else rank
            here = hop if upward else shards - 1 - hop
            sems = line_sem.at[0 if upward else 1]
            came = token_line.at[stream, target]
            total = own(stream, target)
            holds = shard == here
            if hop:
                net.arrived(came, sems.at[stream, target], holds)

            @pl.when(holds)
            def add(target=target, came=came, total=total):
                add_rows(total, total, token_in.at[stream, target], *([came] if hop else []))

            there = jnp.clip(shard + (1 if upward else -1), 0, shards - 1)
            ends = (not upward) and rank == shards - 2 - hop
            landing = token_last.at[stream] if ends else came
            net.send(total, landing, sems.at[stream, target], (plane, core, there), holds)

    def final(stream):
        for place in range(shards):
            holds = shard == place
            values = [own(stream, place), token_in.at[stream, place]]
            for landing, side, present in (
                (token_line.at[stream, place], line_sem.at[0], place > 0),
                (token_last.at[stream], line_sem.at[1], place < shards - 1),
            ):
                if present:
                    values.append(landing)
                    net.arrived(landing, side.at[stream, place], holds)

            @pl.when(holds)
            def add(values=values):
                add_rows((mixed_out, norm_out)[stream], *values)

    def first_sums(stream):
        for place in places:
            net.arrived(token_in.at[stream, place], core_sem.at[stream, place])
        for rank in range(shards - 1):
            chain(stream, 0, rank)

    def pass_on(index):
        parts, came, slot = units[index]
        near, far, near_mask, far_mask = ways(index)
        total = parts.at[far_mask, slot]
        net.arrived(came.at[PASS, slot], pass_sem.at[0, index])
        add_rows(total, total, came.at[PASS, slot])
        net.send(total, came.at[LAST, slot], pass_sem.at[1, index], far)

    cat_turn(0)
    first_sums(0)

    sum_buf[4] = sums[...]
    gain_row = width // 128

    def norm_copies(n, slot):
        return [
            pltpu.make_async_copy(cat_w.at[columns(n), :], cat_chunk.at[slot], chunk_sem.at[1, slot]),
            pltpu.make_async_copy(x_all.at[:, columns(n)], x_chunk.at[slot], chunk_sem.at[2, slot]),
        ]

    def norm_step(n, slot):
        total = dot(wide[:, pl.ds(0, width)], cat_chunk[slot], 1, 1)
        x_hat = (x_chunk[slot].astype(jnp.float32) - mean[...]) * inverse[...]
        gain = jnp.sum(total * x_hat, axis=0, keepdims=True)
        shift = jnp.sum(total, axis=0, keepdims=True)
        for half in range(lane // 128):
            row = gain_row + n * (lane // 128) + half
            sum_buf[4, pl.ds(row, 1), :] = gain[:, half * 128 : (half + 1) * 128]
            sum_buf[4, pl.ds(row + model // 128, 1), :] = shift[:, half * 128 : (half + 1) * 128]
        for member in range(group):
            tokens[1, member, :, columns(n)] = total[member * token_rows : (member + 1) * token_rows].astype(
                jnp.bfloat16
            )

    chunked(0, model // lane, norm_copies, norm_step)

    net.send(sum_buf.at[4], sum_buf.at[0], sum_sem.at[0], net.first)
    to_partner(1)
    cat_turn(1)
    chain(0, 1, 0)
    first_sums(1)
    cat_turn(2)
    cat_turn(3)
    net.arrived(sum_buf.at[0], sum_sem.at[0])
    sum_buf[1] = sum_buf[4] + sum_buf[0]
    net.send(sum_buf.at[1], sum_buf.at[2], sum_sem.at[1], net.second)
    for index in cats:
        pass_on(index)

    def grad_copies(n, slot):
        return [pltpu.make_async_copy(dy.at[:, columns(n)], dy_chunk.at[slot], chunk_sem.at[5, slot])]

    def grad_step(n, slot):
        for parts, left in ((down_part, hidden_turned[...]), (dense_part, attn_turned[...])):
            grad = dot(left, dy_chunk[slot]).astype(jnp.bfloat16)
            pieces, size = parts.shape[1], parts.shape[2]
            for q in range(planes):
                for piece in range(pieces):
                    start = (q * pieces + piece) * size
                    parts[plane ^ q, piece, :, columns(n)] = grad[start : start + size]

    chunked(0, model // lane, grad_copies, grad_step)
    for index in every[group:]:
        send_pass(index)
        send_keep(index)
    for hop, rank in chain_steps[1:]:
        chain(0, hop, rank)

    def finish(index):
        parts, came, slot = units[index]
        total = parts.at[0, slot]
        net.arrived(came.at[KEEP, slot], near_sem.at[index])
        net.arrived(came.at[LAST, slot], pass_sem.at[1, index])
        values = (total, came.at[KEEP, slot], came.at[LAST, slot])
        if index < group:
            add_rows(total, *values)
            if slot:
                net.send(total, cat_out.at[mine], group_sem.at[0, slot], net.member(mine ^ slot))
            else:
                local("own", total, cat_out.at[mine])
        elif parts is down_part:
            add_rows(down_out.at[pl.ds(slot * down_rows, down_rows)], *values)
        else:
            add_rows(dense_out.at[pl.ds(slot * dense_rows, dense_rows)], *values)

    net.arrived(sum_buf.at[2], sum_sem.at[1])
    sum_buf[3] = sum_buf[1] + sum_buf[2]
    for mask in range(1, group):
        net.send(sum_buf.at[3], sums_out.at[mine], group_sem.at[1, mask], net.member(mine ^ mask))
    local("sums", sum_buf.at[3], sums_out.at[mine])
    for index in cats[: group // 2]:
        finish(index)
    chain(1, *chain_steps[0])
    for index in cats[group // 2 : group - 2]:
        finish(index)
    for hop, rank in chain_steps[1:]:
        chain(1, hop, rank)
    for index in cats[group - 2 :]:
        finish(index)
    for index in every[group:]:
        pass_on(index)
    final(0)
    for index in every[group:]:
        finish(index)
    final(1)
    for mask in range(1, group):
        net.arrived(cat_out.at[mine ^ mask], group_sem.at[0, mask])
        net.arrived(sums_out.at[mine ^ mask], group_sem.at[1, mask])
    locals_["own"].wait()
    locals_["sums"].wait()
    net.drain()


def reduce_wires(norm, dcat, x_all, mean, inverse, attn, hidden, dy, cat_w, dense_w, down_w, sums):
    planes, shards = lax.axis_size("plane"), lax.axis_size("shard")
    group = lax.axis_size("core") * shards
    units = group + 6
    rows, width = dcat.shape
    model = norm.shape[1]
    block = model // (planes * group)
    unit_rows, head_rows = down_w.shape[0] // planes, dense_w.shape[0] // planes
    token_rows = rows // group
    vmem = pl.BlockSpec(memory_space=pltpu.VMEM)
    hbm = pl.BlockSpec(memory_space=pl.ANY)
    dma = pltpu.SemaphoreType.DMA
    lane = 256

    def scratch(*shape, dtype=jnp.bfloat16):
        return pltpu.VMEM(shape, dtype)

    return pl.pallas_call(
        reduce_kernel,
        in_specs=[hbm] * 3 + [vmem] * 2 + [hbm] * 6 + [vmem],
        out_specs=[hbm] + [vmem] * 4 + [hbm],
        out_shape=[
            jax.ShapeDtypeStruct((group, block, width), jnp.bfloat16),
            jax.ShapeDtypeStruct((head_rows, model), jnp.float32),
            jax.ShapeDtypeStruct((unit_rows, model), jnp.float32),
            jax.ShapeDtypeStruct((token_rows, model), jnp.float32),
            jax.ShapeDtypeStruct((token_rows, model), jnp.float32),
            jax.ShapeDtypeStruct((group,) + sums.shape, sums.dtype),
        ],
        scratch_shapes=[
            scratch(planes, group, block, width),
            scratch(planes, 4, unit_rows // 4, model),
            scratch(planes, 2, head_rows // 2, model),
            scratch(3, group, block, width),
            scratch(3, 4, unit_rows // 4, model),
            scratch(3, 2, head_rows // 2, model),
            scratch(2, group, token_rows, model),
            scratch(2, shards, token_rows, model),
            scratch(2, shards, token_rows, model),
            scratch(2, token_rows, model),
            scratch(5, *sums.shape, dtype=jnp.float32),
            scratch(rows, max(width, hidden.shape[1] + attn.shape[1])),
            scratch(hidden.shape[1], rows),
            scratch(attn.shape[1], rows),
            scratch(2, rows, group * block),
            scratch(group * block, rows),
            scratch(2, lane, width),
            scratch(2, rows, lane),
            scratch(2, hidden.shape[1], lane),
            scratch(2, attn.shape[1], lane),
            scratch(2, rows, lane),
            dma((2 + 2 * shards + 2 * shards * (shards - 1) + 3 * units + 2 * (group - 1),)),
            dma((units,)),
            dma((2, units)),
            dma((2, group)),
            dma((2, shards)),
            dma((2, 2, shards)),
            dma((2,)),
            dma((5,)),
            dma((6, 2)),
        ],
        compiler_params=pltpu.CompilerParams(
            collective_id=1, has_side_effects=True, vmem_limit_bytes=67043328
        ),
    )(norm, dcat, x_all, mean, inverse, attn, hidden, dy, cat_w, dense_w, down_w, sums)


def fast_body(
    hidden_in,
    segment_ids,
    out_grad,
    qkv_weight_state,
    qkv_bias_state,
    dense_weight_state,
    up_weight_state,
    up_bias_state,
    down_weight_state,
    vector_state,
):
    planes, cores, shards = lax.axis_size("plane"), lax.axis_size("core"), lax.axis_size("shard")
    plane, core, shard = lax.axis_index("plane"), lax.axis_index("core"), lax.axis_index("shard")
    group = cores * shards
    owner = (plane * cores + core) * shards + shard
    owners = planes * group
    model_rows = qkv_weight_state.shape[1]
    unit_rows = down_weight_state.shape[1]
    tokens_here = hidden_in.shape[1]
    head_width = planes * HD
    unit_width = planes * unit_rows
    qkv_count, upb_count = qkv_bias_state.shape[1], up_bias_state.shape[1]

    tokens, cotangent, q_seg = hidden_in[0], out_grad[0], segment_ids[0]
    vec_list = [
        qkv_bias_state[0],
        up_bias_state[0],
        vector_state[0].T.reshape(-1),
        q_seg.astype(jnp.float32),
    ]
    vec_sizes = [value.size for value in vec_list]
    vec_rows = -(-sum(vec_sizes) // 1024) * 8
    vec_own = jnp.pad(jnp.concatenate(vec_list), (0, vec_rows * 128 - sum(vec_sizes))).reshape(vec_rows, 128)

    cat_w, dense_w, down_w, x_all, dy_all, vec_all = gather_wires(
        qkv_weight_state,
        up_weight_state,
        dense_weight_state,
        down_weight_state,
        tokens,
        cotangent,
        vec_own,
    )

    cat_w = cat_w.reshape(D, 3 * head_width + unit_width)
    dense_w = dense_w.reshape(head_width, D)
    down_w = down_w.reshape(unit_width, D)
    rows = group * tokens_here
    x_all = x_all.reshape(rows, D)
    dy_all = dy_all.reshape(rows, D)
    vec_flat = vec_all.reshape(planes, cores, shards, vec_rows * 128)
    at = [0]
    for size in vec_sizes:
        at.append(at[-1] + size)

    def rounded(value):
        return value.astype(jnp.bfloat16).astype(jnp.float32)

    qkv_bias = rounded(vec_flat[..., at[0] : at[1]]).reshape(3, planes, cores, shards, HD)
    qkv_bias = lax.dynamic_index_in_dim(
        qkv_bias.transpose(2, 3, 0, 1, 4).reshape(group, 3 * head_width), core * shards + shard, 0, False
    )
    up_bias = lax.dynamic_index_in_dim(
        rounded(vec_flat[..., at[1] : at[2]]).transpose(1, 2, 0, 3).reshape(group, unit_width),
        core * shards + shard,
        0,
        False,
    )
    vec_columns = (
        rounded(vec_flat[..., at[2] : at[3]])
        .reshape(owners, 4, model_rows)
        .transpose(1, 0, 2)
        .reshape(4, D)
    )
    norm_gain, norm_shift, dense_bias, down_bias = (vec_columns[index] for index in range(4))
    segments = lax.dynamic_index_in_dim(vec_flat[..., at[3] : at[4]], plane, 0, False)
    segments = segments.astype(jnp.int32).reshape(cores, shards * tokens_here)
    cat_bias = jnp.concatenate([qkv_bias, up_bias])

    x_float = x_all.astype(jnp.float32)
    x_mean = jnp.mean(x_float, axis=-1, keepdims=True)
    center = x_float - x_mean
    inverse = lax.rsqrt(jnp.mean(center * center, axis=-1, keepdims=True) + norm_eps)
    x_hat = center * inverse
    norm_bf = lax.optimization_barrier((x_hat * norm_gain + norm_shift).astype(jnp.bfloat16))

    fu = jnp.dot(norm_bf, cat_w, preferred_element_type=jnp.float32) + cat_bias
    pre_act = fu[:, 3 * head_width :]
    hidden = gelu_tanh(pre_act).astype(jnp.bfloat16)
    grad_hidden = jnp.dot(dy_all, down_w.T, preferred_element_type=jnp.float32)
    grad_pre = jax.vjp(gelu_tanh, pre_act)[1](grad_hidden)[0]
    upb_part = jnp.sum(grad_pre, axis=0)
    grad_heads = jnp.dot(dy_all, dense_w.T, preferred_element_type=jnp.float32).astype(jnp.bfloat16)
    attn, dcat, qkvb_part = attention(fu, grad_heads, grad_pre.astype(jnp.bfloat16), segments)
    bias_part = jnp.sum(cotangent.astype(jnp.float32), axis=0)
    nothing = jnp.zeros((D,), jnp.float32)
    sums = [qkvb_part, upb_part, nothing, nothing, bias_part]
    sum_sizes = [value.size for value in sums]
    sum_rows = -(-sum(sum_sizes) // 1024) * 8
    sums = jnp.pad(jnp.concatenate(sums), (0, sum_rows * 128 - sum(sum_sizes))).reshape(sum_rows, 128)

    cat_sum, dense_grad, down_grad, mixed, grad_norm, sums_all = reduce_wires(
        norm_bf,
        dcat,
        x_all,
        x_mean,
        inverse,
        attn,
        hidden,
        dy_all,
        cat_w,
        dense_w,
        down_w,
        sums,
    )

    sums_flat = sums_all.reshape(cores, shards, sum_rows * 128)
    at = [0]
    for size in sum_sizes:
        at.append(at[-1] + size)
    qkvb_grad = (
        sums_flat[..., : at[1]]
        .reshape(cores, shards, 3, planes, HD)
        .transpose(2, 3, 0, 1, 4)
        .reshape(owners, qkv_count)
    )
    qkvb_grad = lax.dynamic_index_in_dim(qkvb_grad, owner, 0, False)
    upb_grad = sums_flat[..., at[1] : at[2]].reshape(group, planes, upb_count)
    upb_grad = lax.dynamic_index_in_dim(
        lax.dynamic_index_in_dim(upb_grad, core * shards + shard, 0, False), plane, 0, False
    )
    vec_grad = jnp.sum(sums_flat[..., at[2] : at[5]], axis=(0, 1)).reshape(3, owners, model_rows)
    vec_grad = lax.dynamic_index_in_dim(vec_grad, owner, 1, False)
    vec_grad = jnp.stack([vec_grad[0], vec_grad[1], vec_grad[2], vec_grad[2]], axis=1)

    x_own = tokens.astype(jnp.float32)
    output = (x_own + (mixed.astype(jnp.float32) + dense_bias + down_bias)).astype(jnp.bfloat16)
    own_center = x_own - jnp.mean(x_own, axis=-1, keepdims=True)
    own_inverse = lax.rsqrt(jnp.mean(own_center * own_center, axis=-1, keepdims=True) + norm_eps)
    own_hat = own_center * own_inverse
    hat_grad = grad_norm.astype(jnp.float32) * norm_gain
    x_grad = own_inverse * (
        hat_grad
        - jnp.mean(hat_grad, axis=-1, keepdims=True)
        - own_hat * jnp.mean(hat_grad * own_hat, axis=-1, keepdims=True)
    )
    input_grad = cotangent.astype(jnp.float32) + x_grad

    new, qkv_grad, up_grad = owner_update(
        (qkv_weight_state, dense_weight_state, up_weight_state, down_weight_state),
        cat_sum,
        (dense_grad, down_grad),
        (qkv_bias_state, up_bias_state, vector_state),
        (qkvb_grad, upb_grad, vec_grad),
        (planes, cores, shards),
    )
    return (
        output[None],
        input_grad[None],
        qkv_grad,
        qkvb_grad,
        dense_grad,
        up_grad,
        upb_grad,
        down_grad,
        vec_grad,
        *new,
    )


def fast_solution(mesh):
    rep, shard = mesh.shape["rep"], mesh.shape["shard"]
    inner = Mesh(mesh.devices.reshape(rep // 2, 2, shard), ("plane", "core", "shard"))
    both = ("plane", "core")
    every = ("plane", "core", "shard")
    in_specs = (
        P(both, "shard", None),
        P(both, "shard"),
        P(both, "shard", None),
        P(None, every, None),
        P(None, every),
        P(None, every, None),
        P(None, every, None),
        P(None, every),
        P(None, every, None),
        P(None, every, None),
    )
    out_specs = (
        P(both, "shard", None),
        P(both, "shard", None),
        P(every, None),
        P(every),
        P(every, None),
        P(every, None),
        P(every),
        P(every, None),
        P(every, None),
        P(both, "shard", None),
        P(both, "shard", None),
        P(both, "shard", None),
    )
    return jax.shard_map(fast_body, mesh=inner, in_specs=in_specs, out_specs=out_specs, check_vma=False)


def solution(mesh):
    in_specs = (
        P("rep", "shard", None),
        P("rep", "shard"),
        P("rep", "shard", None),
        P(None, ("rep", "shard"), None),
        P(None, ("rep", "shard")),
        P(None, ("rep", "shard"), None),
        P(None, ("rep", "shard"), None),
        P(None, ("rep", "shard")),
        P(None, ("rep", "shard"), None),
        P(None, ("rep", "shard"), None),
    )
    out_specs = (
        P("rep", "shard", None),
        P("rep", "shard", None),
        P(("rep", "shard"), None),
        P(("rep", "shard")),
        P(("rep", "shard"), None),
        P(("rep", "shard"), None),
        P(("rep", "shard")),
        P(("rep", "shard"), None),
        P(("rep", "shard"), None),
        P("rep", "shard", None),
        P("rep", "shard", None),
        P("rep", "shard", None),
    )
    if whole_heads(mesh):
        return fast_solution(mesh)
    return jax.shard_map(body, mesh=mesh, in_specs=in_specs, out_specs=out_specs, check_vma=False)
```

```python
from functools import partial
import math

import jax
import jax.numpy as jnp
from jax import lax
from jax.experimental import pallas as pl
from jax.experimental.pallas import tpu as pltpu
from jax.sharding import Mesh
from jax.sharding import PartitionSpec as P

D = 2048
HD = 64
ROT = 32
FF = 8192
STEP = 5


learn_rate = 0.02
beta_one = 0.9
beta_two = 0.95
adam_eps = 1e-08
weight_decay = 0.1
norm_eps = 1e-05
big_negative = -1e30


def layer_norm(x, norm_gain, norm_shift):
    center = x - jnp.mean(x, axis=-1, keepdims=True)
    variance = jnp.mean(center * center, axis=-1, keepdims=True)
    return center * lax.rsqrt(variance + norm_eps) * norm_gain + norm_shift


def gelu_tanh(v):
    return 0.5 * v * (1.0 + jnp.tanh(0.7978845608028654 * (v + 0.044715 * v * v * v)))


def rotary(x, positions):
    half_rot = ROT // 2
    frequency = jnp.exp(jnp.arange(half_rot, dtype=jnp.float32) * (-2.0 * math.log(10000.0) / ROT))
    angles = positions.astype(jnp.float32)[:, None] * frequency[None, :]
    cosine = jnp.cos(angles)[:, None, :]
    sine_val = jnp.sin(angles)[:, None, :]
    lower_part = x[..., :half_rot]
    upper_part = x[..., half_rot:ROT]
    return jnp.concatenate(
        [
            lower_part * cosine - upper_part * sine_val,
            upper_part * cosine + lower_part * sine_val,
            x[..., ROT:],
        ],
        axis=-1,
    )


def adam_update(state, grad):
    moment_one = beta_one * state[1] + (1.0 - beta_one) * grad
    moment_two = beta_two * state[2] + (1.0 - beta_two) * grad * grad
    corrected = moment_one / (1.0 - beta_one**STEP)
    divisor = jnp.sqrt(moment_two / (1.0 - beta_two**STEP)) + adam_eps
    weight = state[0] - learn_rate * (corrected / divisor + weight_decay * state[0])
    return jnp.stack([weight, moment_one, moment_two])


def owner_entries(new_states, entry):
    return jnp.concatenate(
        [state_new[entry].reshape(-1) for state_new in new_states], axis=0
    ).reshape(1, 1, -1)


def block_mask(q_pos, q_seg, k_pos, k_seg):
    return (k_pos[None, :] <= q_pos[:, None]) & (k_seg[None, :] == q_seg[:, None])


def attend_keys(kv_all, seg_all, queries, q_pos, q_seg):
    key_count = kv_all.shape[0]
    width = kv_all.shape[1] // 2
    heads_here = queries.shape[1]
    query_rows = queries.shape[0]
    block_rows = math.gcd(key_count, 512)
    block_count = key_count // block_rows
    kv_blocks = kv_all.reshape(block_count, block_rows, 2 * width)
    seg_blocks = seg_all.reshape(block_count, block_rows)
    score_scale = 1.0 / math.sqrt(HD)

    def attend_step_block(carry, block_items):
        kv_rows, seg_rows, block_index = block_items
        row_max, totals, accumulated = carry
        key_rows = kv_rows[:, :width].reshape(block_rows, heads_here, HD)
        value_rows = kv_rows[:, width:].reshape(block_rows, heads_here, HD)
        k_pos = block_index * block_rows + jnp.arange(block_rows, dtype=jnp.int32)
        allowed = block_mask(q_pos, q_seg, k_pos, seg_rows)
        scores = (
            jnp.einsum("qhd,khd->hqk", queries, key_rows, preferred_element_type=jnp.float32)
            * score_scale
        )
        scores = jnp.where(allowed[None], scores, big_negative)
        new_max = jnp.maximum(row_max, jnp.max(scores, axis=-1))
        probabilities = jnp.where(allowed[None], jnp.exp(scores - new_max[..., None]), 0.0)
        factor = jnp.exp(row_max - new_max)
        totals = totals * factor + jnp.sum(probabilities, axis=-1)
        accumulated = accumulated * factor[..., None] + jnp.einsum(
            "hqk,khd->hqd",
            probabilities.astype(jnp.bfloat16),
            value_rows,
            preferred_element_type=jnp.float32,
        )
        return ((new_max, totals, accumulated), None)

    start_state = (
        jnp.full((heads_here, query_rows), big_negative, jnp.float32),
        jnp.zeros((heads_here, query_rows), jnp.float32),
        jnp.zeros((heads_here, query_rows, HD), jnp.float32),
    )
    running, unused = lax.scan(
        attend_step_block,
        start_state,
        (kv_blocks, seg_blocks, jnp.arange(block_count, dtype=jnp.int32)),
    )
    return running


def attention_grads(queries, kv_all, seg_all, q_pos, q_seg, grad_heads, delta_all, lse_all):
    key_count = kv_all.shape[0]
    width = kv_all.shape[1] // 2
    heads_here = queries.shape[1]
    query_rows = queries.shape[0]
    block_rows = math.gcd(key_count, 512)
    block_count = key_count // block_rows
    kv_blocks = kv_all.reshape(block_count, block_rows, 2 * width)
    seg_blocks = seg_all.reshape(block_count, block_rows)
    score_scale = 1.0 / math.sqrt(HD)

    def attention_step_block(query_grad, block_items):
        kv_rows, seg_rows, block_index = block_items
        key_rows = kv_rows[:, :width].reshape(block_rows, heads_here, HD)
        value_rows = kv_rows[:, width:].reshape(block_rows, heads_here, HD)
        k_pos = block_index * block_rows + jnp.arange(block_rows, dtype=jnp.int32)
        allowed = block_mask(q_pos, q_seg, k_pos, seg_rows)
        scores = (
            jnp.einsum("qhd,khd->hqk", queries, key_rows, preferred_element_type=jnp.float32)
            * score_scale
        )
        scores = jnp.where(allowed[None], scores, big_negative)
        probabilities = jnp.where(allowed[None], jnp.exp(scores - lse_all[..., None]), 0.0)
        value_grad = jnp.einsum(
            "hqk,qhd->khd",
            probabilities.astype(jnp.bfloat16),
            grad_heads,
            preferred_element_type=jnp.float32,
        )
        prob_grad = jnp.einsum(
            "qhd,khd->hqk", grad_heads, value_rows, preferred_element_type=jnp.float32
        )
        score_grad = (probabilities * (prob_grad - delta_all[..., None]) * score_scale).astype(
            jnp.bfloat16
        )
        query_grad = query_grad + jnp.einsum(
            "hqk,khd->hqd", score_grad, key_rows, preferred_element_type=jnp.float32
        )
        key_grad = jnp.einsum(
            "hqk,qhd->khd", score_grad, queries, preferred_element_type=jnp.float32
        )
        return (
            query_grad,
            jnp.concatenate(
                [key_grad.reshape(block_rows, width), value_grad.reshape(block_rows, width)], axis=1
            ),
        )

    query_grad, kv_grad_blocks = lax.scan(
        attention_step_block,
        jnp.zeros((heads_here, query_rows, HD), jnp.float32),
        (kv_blocks, seg_blocks, jnp.arange(block_count, dtype=jnp.int32)),
    )
    return (query_grad, kv_grad_blocks.reshape(key_count, 2 * width))


def gather_vectors(own_qkvb, own_upb, own_vec):
    return (
        lax.all_gather(own_qkvb, ("rep", "shard"), axis=0, tiled=True),
        lax.all_gather(own_upb, ("rep", "shard"), axis=0, tiled=True),
        lax.all_gather(own_vec, ("rep", "shard"), axis=0, tiled=True),
    )


def sum_vectors(qkvb_grad, upb_grad, vec_grad):
    return (
        lax.psum_scatter(qkvb_grad, ("rep", "shard"), scatter_dimension=0, tiled=True),
        lax.psum_scatter(upb_grad, ("rep", "shard"), scatter_dimension=0, tiled=True),
        lax.psum_scatter(vec_grad, ("rep", "shard"), scatter_dimension=0, tiled=True),
    )


def sum_positions(partial_rows):
    return lax.psum_scatter(partial_rows, "shard", scatter_dimension=0, tiled=True)


def attention_pass(norm_rows, qkv_w, qkv_b, positions, key_width):
    row_count = norm_rows.shape[0]
    heads_here = key_width // HD
    joined = jnp.dot(norm_rows, qkv_w, preferred_element_type=jnp.float32) + qkv_b
    q_pre = joined[:, :key_width].reshape(row_count, heads_here, HD)
    k_pre = joined[:, key_width : 2 * key_width].reshape(row_count, heads_here, HD)
    queries = rotary(q_pre, positions).astype(jnp.bfloat16)
    key_local = rotary(k_pre, positions).astype(jnp.bfloat16).reshape(row_count, key_width)
    value_local = joined[:, 2 * key_width :].astype(jnp.bfloat16)
    kv_local = jnp.concatenate([key_local, value_local], axis=1)
    return (q_pre, k_pre, queries, kv_local)


def finish_qkv_grad(q_pre, k_pre, positions, query_grad, kv_grad, key_width):
    row_count = q_pre.shape[0]
    heads_here = key_width // HD
    rotate_back = partial(rotary, positions=positions)
    query_pre = jax.vjp(rotate_back, q_pre)[1](query_grad.transpose(1, 0, 2))[0]
    key_pre = jax.vjp(rotate_back, k_pre)[1](
        kv_grad[:, :key_width].reshape(row_count, heads_here, HD)
    )[0]
    return jnp.concatenate(
        [
            query_pre.reshape(row_count, key_width),
            key_pre.reshape(row_count, key_width),
            kv_grad[:, key_width:],
        ],
        axis=1,
    )


def sliced_pass(norm_bf, q_seg, cotangent, own_mats, qkv_bb, up_bb):
    own_qkv, own_dense, own_up, own_down = own_mats
    inner_count = lax.axis_size("shard")
    outer_count = lax.axis_size("rep")
    stride = outer_count // inner_count
    place = lax.axis_index("shard")
    head_width = D // inner_count
    unit_width = FF // inner_count
    qkv_rows = own_qkv.shape[0]
    dense_rows = own_dense.shape[0]
    down_rows = own_down.shape[0]
    qkv_split = own_qkv.reshape(qkv_rows, 3, inner_count, head_width)
    up_split = own_up.reshape(qkv_rows, 1, inner_count, unit_width)
    qkv_cols, up_cols = (
        lax.all_to_all(qkv_split, "shard", split_axis=2, concat_axis=0, tiled=True),
        lax.all_to_all(up_split, "shard", split_axis=2, concat_axis=0, tiled=True),
    )
    qkv_rep, up_rep, dense_rep, down_rep = (
        lax.all_gather(qkv_cols, "rep", axis=0, tiled=True),
        lax.all_gather(up_cols, "rep", axis=0, tiled=True),
        lax.all_gather(own_dense[None], "rep", axis=0, tiled=True),
        lax.all_gather(own_down[None], "rep", axis=0, tiled=True),
    )
    dense_grid = dense_rep.reshape(inner_count, stride, 1, dense_rows, D)
    down_grid = down_rep.reshape(inner_count, stride, 1, down_rows, D)
    dense_moved, down_moved = (
        lax.all_to_all(dense_grid, "shard", split_axis=0, concat_axis=2, tiled=True),
        lax.all_to_all(down_grid, "shard", split_axis=0, concat_axis=2, tiled=True),
    )
    qkv_w = qkv_rep.reshape(D, 3 * head_width)
    up_w = up_rep.reshape(D, unit_width)
    dense_w = dense_moved.reshape(head_width, D)
    down_w = down_moved.reshape(unit_width, D)
    qkv_b = lax.dynamic_index_in_dim(
        qkv_bb.astype(jnp.float32).reshape(3, inner_count, head_width), place, 1, False
    ).reshape(3 * head_width)
    up_b = lax.dynamic_slice_in_dim(up_bb.astype(jnp.float32), place * unit_width, unit_width, 0)
    norm_seq, grad_seq, seg_seq = (
        lax.all_gather(norm_bf, "shard", axis=0, tiled=True),
        lax.all_gather(cotangent, "shard", axis=0, tiled=True),
        lax.all_gather(q_seg, "shard", axis=0, tiled=True),
    )
    seq_rows = norm_seq.shape[0]
    heads_here = head_width // HD
    positions = jnp.arange(seq_rows, dtype=jnp.int32)
    q_pre, k_pre, queries, kv_seq = attention_pass(norm_seq, qkv_w, qkv_b, positions, head_width)
    row_max, totals, accumulated = attend_keys(kv_seq, seg_seq, queries, positions, seg_seq)
    lse_all = row_max + jnp.log(totals)
    out_heads = (accumulated / totals[..., None]).transpose(1, 0, 2).astype(jnp.bfloat16)
    attn_bf = out_heads.reshape(seq_rows, head_width)
    pre_act = jnp.dot(norm_seq, up_w, preferred_element_type=jnp.float32) + up_b
    hidden = gelu_tanh(pre_act).astype(jnp.bfloat16)
    partial_out = jnp.dot(attn_bf, dense_w, preferred_element_type=jnp.float32) + jnp.dot(
        hidden, down_w, preferred_element_type=jnp.float32
    )
    mixed = sum_positions(partial_out)
    grad_down = jnp.dot(hidden.T, grad_seq, preferred_element_type=jnp.float32)
    grad_dense = jnp.dot(attn_bf.T, grad_seq, preferred_element_type=jnp.float32)
    grad_hidden = jnp.dot(grad_seq, down_w.T, preferred_element_type=jnp.float32)
    grad_pre = jax.vjp(gelu_tanh, pre_act)[1](grad_hidden)[0]
    grad_pre_bf = grad_pre.astype(jnp.bfloat16)
    grad_up = jnp.dot(norm_seq.T, grad_pre_bf, preferred_element_type=jnp.float32)
    upb_part = jnp.sum(grad_pre, axis=0)
    norm_part = jnp.dot(grad_pre_bf, up_w.T, preferred_element_type=jnp.float32)
    grad_heads = (
        jnp.dot(grad_seq, dense_w.T, preferred_element_type=jnp.float32)
        .astype(jnp.bfloat16)
        .reshape(seq_rows, heads_here, HD)
    )
    delta_all = jnp.sum(grad_heads.astype(jnp.float32) * out_heads.astype(jnp.float32), axis=-1).T
    query_grad, kv_grad = attention_grads(
        queries, kv_seq, seg_seq, positions, seg_seq, grad_heads, delta_all, lse_all
    )
    grad_joined = finish_qkv_grad(q_pre, k_pre, positions, query_grad, kv_grad, head_width)
    grad_joined_bf = grad_joined.astype(jnp.bfloat16)
    grad_qkv = jnp.dot(norm_seq.T, grad_joined_bf, preferred_element_type=jnp.float32)
    qkvb_part = jnp.sum(grad_joined, axis=0)
    norm_part = norm_part + jnp.dot(grad_joined_bf, qkv_w.T, preferred_element_type=jnp.float32)
    grad_norm = sum_positions(norm_part)
    dense_grid_grad = grad_dense.reshape(1, stride, inner_count, dense_rows, D)
    down_grid_grad = grad_down.reshape(1, stride, inner_count, down_rows, D)
    dense_back, down_back = (
        lax.all_to_all(dense_grid_grad, "shard", split_axis=2, concat_axis=0, tiled=True),
        lax.all_to_all(down_grid_grad, "shard", split_axis=2, concat_axis=0, tiled=True),
    )
    qkv_sum, up_sum, dense_sum, down_sum = (
        lax.psum_scatter(
            grad_qkv.reshape(D, 3, 1, head_width), "rep", scatter_dimension=0, tiled=True
        ),
        lax.psum_scatter(
            grad_up.reshape(D, 1, 1, unit_width), "rep", scatter_dimension=0, tiled=True
        ),
        lax.psum_scatter(
            dense_back.reshape(outer_count, dense_rows, D), "rep", scatter_dimension=0, tiled=True
        ),
        lax.psum_scatter(
            down_back.reshape(outer_count, down_rows, D), "rep", scatter_dimension=0, tiled=True
        ),
    )
    qkv_home, up_home = (
        lax.all_to_all(qkv_sum, "shard", split_axis=0, concat_axis=2, tiled=True),
        lax.all_to_all(up_sum, "shard", split_axis=0, concat_axis=2, tiled=True),
    )
    qkv_own = qkv_home.reshape(qkv_rows, 3 * D)
    up_own = up_home.reshape(qkv_rows, FF)
    dense_own = dense_sum.reshape(dense_rows, D)
    down_own = down_sum.reshape(down_rows, D)
    selector = (jnp.arange(inner_count, dtype=jnp.int32) == place).astype(jnp.float32)
    qkvb_grad = (selector[None, :, None] * qkvb_part.reshape(3, 1, head_width)).reshape(3 * D)
    upb_grad = (selector[:, None] * upb_part[None, :]).reshape(FF)
    return (mixed, grad_norm, (qkv_own, dense_own, up_own, down_own), qkvb_grad, upb_grad)


def body(
    hidden_in,
    segment_ids,
    out_grad,
    qkv_weight_state,
    qkv_bias_state,
    dense_weight_state,
    up_weight_state,
    up_bias_state,
    down_weight_state,
    vector_state,
):
    own_mats = (
        qkv_weight_state[0].astype(jnp.bfloat16),
        dense_weight_state[0].astype(jnp.bfloat16),
        up_weight_state[0].astype(jnp.bfloat16),
        down_weight_state[0].astype(jnp.bfloat16),
    )
    qkv_bb, up_bb, vec_bf = gather_vectors(
        qkv_bias_state[0].astype(jnp.bfloat16),
        up_bias_state[0].astype(jnp.bfloat16),
        vector_state[0].astype(jnp.bfloat16),
    )
    vec_all = vec_bf.astype(jnp.float32)
    norm_gain = vec_all[:, 0]
    norm_shift = vec_all[:, 1]
    dense_bias = vec_all[:, 2]
    down_bias = vec_all[:, 3]
    tokens = hidden_in[0]
    q_seg = segment_ids[0]
    cotangent = out_grad[0]
    x_full = tokens.astype(jnp.float32)
    normed = layer_norm(x_full, norm_gain, norm_shift)
    norm_bf = normed.astype(jnp.bfloat16)
    mixed, grad_norm, owned, qkvb_grad, upb_grad = sliced_pass(
        norm_bf, q_seg, cotangent, own_mats, qkv_bb, up_bb
    )
    qkv_own, dense_own, up_own, down_own = owned
    output = (x_full + (mixed + dense_bias + down_bias)).astype(jnp.bfloat16)
    grad_x, grad_gain, grad_shift = jax.vjp(layer_norm, x_full, norm_gain, norm_shift)[1](grad_norm)
    out_bias_grad = jnp.sum(cotangent.astype(jnp.float32), axis=0)
    grad_vec = jnp.stack([grad_gain, grad_shift, out_bias_grad, out_bias_grad], axis=1)
    input_grad = cotangent.astype(jnp.float32) + grad_x
    qkvb_own, upb_own, vec_own = sum_vectors(qkvb_grad, upb_grad, grad_vec)
    new_states = (
        adam_update(qkv_weight_state, qkv_own),
        adam_update(qkv_bias_state, qkvb_own),
        adam_update(dense_weight_state, dense_own),
        adam_update(up_weight_state, up_own),
        adam_update(up_bias_state, upb_own),
        adam_update(down_weight_state, down_own),
        adam_update(vector_state, vec_own),
    )
    return (
        output[None],
        input_grad[None],
        qkv_own,
        qkvb_own,
        dense_own,
        up_own,
        upb_own,
        down_own,
        vec_own,
        owner_entries(new_states, 0),
        owner_entries(new_states, 1),
        owner_entries(new_states, 2),
    )


def whole_heads(mesh):
    owners = mesh.shape["rep"] * mesh.shape["shard"]
    return D % owners == 0 and D // owners == HD and mesh.shape["rep"] % 2 == 0


def rotation_tables(seq_rows):
    half_rot = ROT // 2
    lane = jnp.arange(2 * HD, dtype=jnp.int32) % HD
    frequency = jnp.exp((lane % half_rot).astype(jnp.float32) * (-2.0 * math.log(10000.0) / ROT))
    angles = jnp.arange(seq_rows, dtype=jnp.int32).astype(jnp.float32)[:, None] * frequency[None, :]
    sine = jnp.sin(angles)
    cosine = jnp.where(lane[None, :] < ROT, jnp.cos(angles), 1.0)
    low = jnp.where(lane[None, :] < half_rot, -sine, 0.0)
    high = jnp.where((lane[None, :] >= half_rot) & (lane[None, :] < ROT), sine, 0.0)
    return cosine, low, high


def attention_kernel(
    fu_ref, do_ref, du_ref, seg_col_ref, seg_row_ref, cos_ref, low_ref, high_ref, o_ref, dcat_ref, sums_ref
):
    rows, width = do_ref.shape
    scale = 1.0 / math.sqrt(HD)
    row_id = lax.broadcasted_iota(jnp.int32, (rows, rows), 0)
    col_id = lax.broadcasted_iota(jnp.int32, (rows, rows), 1)
    allowed = (col_id <= row_id) & (seg_col_ref[...] == seg_row_ref[0])
    cosine, low, high = cos_ref[...], low_ref[...], high_ref[...]
    half = ROT // 2
    lane = lax.broadcasted_iota(jnp.int32, (rows, 2 * HD), 1)

    def rotate(u):
        return (
            u * cosine
            + pltpu.roll(u, 2 * HD - half, 1) * low
            + pltpu.roll(u, half, 1) * high
        )

    def rotate_back(u):
        return (
            u * cosine
            - pltpu.roll(u, 2 * HD - half, 1) * low
            - pltpu.roll(u, half, 1) * high
        )

    def dot(a, b, a_dim, b_dim):
        return lax.dot_general(a, b, (((a_dim,), (b_dim,)), ((), ())), preferred_element_type=jnp.float32)

    zero = jnp.zeros((), jnp.bfloat16)
    for pair in range(width // (2 * HD)):
        lanes = pl.ds(pair * 2 * HD, 2 * HD)
        k_lanes = pl.ds(width + pair * 2 * HD, 2 * HD)
        v_lanes = pl.ds(2 * width + pair * 2 * HD, 2 * HD)
        q = rotate(fu_ref[:, lanes]).astype(jnp.bfloat16)
        k = rotate(fu_ref[:, k_lanes]).astype(jnp.bfloat16)
        v = fu_ref[:, v_lanes].astype(jnp.bfloat16)
        do = do_ref[:, lanes]
        o = dq = dk = dv = None
        for head in range(2):
            mine = (lane < HD) if head == 0 else (lane >= HD)
            qh = jnp.where(mine, q, zero)
            kh = jnp.where(mine, k, zero)
            vh = jnp.where(mine, v, zero)
            doh = jnp.where(mine, do, zero)
            scores = jnp.where(allowed, dot(qh, k, 1, 1) * scale, big_negative)
            row_max = jnp.max(scores, axis=1, keepdims=True)
            probs = jnp.where(allowed, jnp.exp(scores - row_max), 0.0)
            inverse = 1.0 / jnp.sum(probs, axis=1, keepdims=True)
            oh = dot(probs.astype(jnp.bfloat16), vh, 1, 0) * inverse
            delta = jnp.sum(
                doh.astype(jnp.float32) * oh.astype(jnp.bfloat16).astype(jnp.float32), axis=1, keepdims=True
            )
            probs = probs * inverse
            dvh = dot(probs.astype(jnp.bfloat16), doh, 0, 0)
            ds = (probs * (dot(doh, v, 1, 1) - delta) * scale).astype(jnp.bfloat16)
            dqh = dot(ds, kh, 1, 0)
            dkh = dot(ds, qh, 0, 0)
            if head == 0:
                o, dq, dk, dv = oh, dqh, dkh, dvh
            else:
                o, dq, dk, dv = o + oh, dq + dqh, dk + dkh, dv + dvh
        o_ref[:, lanes] = o.astype(jnp.bfloat16)
        dq = rotate_back(dq)
        dk = rotate_back(dk)
        for part, place in ((dq, lanes), (dk, k_lanes), (dv, v_lanes)):
            dcat_ref[:, place] = part.astype(jnp.bfloat16)
            sums_ref[0, :, place] = jnp.sum(part, axis=0, keepdims=True)
    dcat_ref[:, pl.ds(3 * width, du_ref.shape[1])] = du_ref[...]


def attention(fu, do, du, segments):
    count, rows = segments.shape
    width = do.shape[1]
    units = du.shape[1]
    tables = rotation_tables(rows)
    table_spec = pl.BlockSpec((rows, 2 * HD), lambda s: (0, 0))
    o, dcat, sums = pl.pallas_call(
        attention_kernel,
        grid=(count,),
        in_specs=[
            pl.BlockSpec((rows, 3 * width), lambda s: (s, 0)),
            pl.BlockSpec((rows, width), lambda s: (s, 0)),
            pl.BlockSpec((rows, units), lambda s: (s, 0)),
            pl.BlockSpec((rows, 1), lambda s: (s, 0)),
            pl.BlockSpec((1, 1, rows), lambda s: (s, 0, 0)),
            table_spec,
            table_spec,
            table_spec,
        ],
        out_specs=[
            pl.BlockSpec((rows, width), lambda s: (s, 0)),
            pl.BlockSpec((rows, 3 * width + units), lambda s: (s, 0)),
            pl.BlockSpec((1, 1, 3 * width), lambda s: (s, 0, 0)),
        ],
        out_shape=[
            jax.ShapeDtypeStruct((count * rows, width), jnp.bfloat16),
            jax.ShapeDtypeStruct((count * rows, 3 * width + units), jnp.bfloat16),
            jax.ShapeDtypeStruct((count, 1, 3 * width), jnp.float32),
        ],
        compiler_params=pltpu.CompilerParams(vmem_limit_bytes=56 << 20),
        cost_estimate=pl.CostEstimate(
            flops=count * (width // HD) * 10 * rows * rows * HD,
            bytes_accessed=count * rows * (width * 20 + units * 4),
            transcendentals=count * (width // HD) * rows * rows,
        ),
    )(fu, do, du, segments.reshape(count * rows, 1), segments.reshape(count, 1, rows), *tables)
    return o, dcat, jnp.sum(sums, axis=(0, 1))


def adam_values(weight, moment_one, moment_two, grad):
    first = beta_one * moment_one + (1.0 - beta_one) * grad
    second = beta_two * moment_two + (1.0 - beta_two) * grad * grad
    corrected = first * (1.0 / (1.0 - beta_one**STEP))
    divisor = jnp.sqrt(second * (1.0 / (1.0 - beta_two**STEP))) + adam_eps
    return weight - learn_rate * (corrected / divisor + weight_decay * weight), first, second


def owner_update_kernel(plan, small_plan, groups, steps, whole_rows, *refs):
    planes, cores, shards = groups
    qkv_state, dense_state, up_state, down_state, cat_ref, dense_grad, down_grad, small_ref = refs[:8]
    flat = refs[8:11]
    qkv_out, dense_out, up_out, down_out, cat_buf = refs[11:16]
    outs = refs[16:19]
    step_sem, rest_sem = refs[19:]
    step = pl.program_id(0)
    lane = lax.broadcasted_iota(jnp.int32, (8, 128), 1)
    sub = lax.broadcasted_iota(jnp.int32, (8, 128), 0)
    lane_row = lax.broadcasted_iota(jnp.int32, (1, 128), 1)
    wide = 1024

    @pl.when(step == 0)
    def small():
        for source, row, low, high in small_plan:
            for entry in range(3):
                old = outs[entry][pl.ds(row, 1), :]
                new = small_ref[entry, pl.ds(source, 1), :]
                outs[entry][pl.ds(row, 1), :] = jnp.where((lane_row >= low) & (lane_row < high), new, old)

    def widen(piece, carry):
        cat_buf[piece] = cat_ref[piece].astype(jnp.float32)
        return carry

    lax.fori_loop(0, cat_ref.shape[0], widen, 0)

    def place_rows(state, grad_of, rows, tiles, start, shifted, keep=None):
        chunk = min(wide, tiles * 128)

        def one_group(group, carry):
            place = pl.ds(pl.multiple_of(group * 8, 8), 8)
            base = start + (step * (rows // 8) + group) * (8 * tiles)

            def values(column, size):
                lanes = pl.ds(column, size)
                grad = grad_of(place, column, size)
                if keep is not None and size > 128:
                    keep[place, lanes] = grad
                return adam_values(
                    state[0, place, lanes], state[1, place, lanes], state[2, place, lanes], grad
                )

            if shifted:
                last = tuple(pltpu.roll(value, 64, 1) for value in values((tiles - 1) * 128, 128))
                before = tuple(
                    jnp.where(sub == 0, out[pl.ds(base, 1), :], pltpu.roll(value, 1, 0))
                    for out, value in zip(outs, last)
                )
            for column in range(0, tiles * 128, chunk):
                done = values(column, chunk)
                for entry, out in enumerate(outs):
                    for tile in range(chunk // 128):
                        value = done[entry][:, tile * 128 : (tile + 1) * 128]
                        if shifted:
                            value = pltpu.roll(value, 64, 1)
                            old = before[entry] if tile == 0 else now
                            now = value
                            value = jnp.where(lane < 64, old, value)
                        out[pl.ds(base + column // 128 + tile, 8, stride=tiles), :] = value
                    if shifted:
                        before = before[:entry] + (now,) + before[entry + 1 :]
            if shifted:
                for out, value in zip(outs, before):
                    row = pl.ds(base + 8 * tiles, 1)
                    out[row, :] = jnp.where(lane_row < 64, value[7:8], out[row, :])
            return carry

        lax.fori_loop(0, rows // 8, one_group, 0)

    def qkv_grad(place, column, size):
        tiles = []
        for start in range(column, column + size, 128):
            part, head = divmod(start // HD, planes * cores * shards)
            halves = []
            for side in range(2):
                plane, member = divmod(head + side, cores * shards)
                spot = (part * planes + plane) * HD
                half = cat_buf[member, place, pl.ds(spot // 128 * 128, 128)]
                halves.append(half if spot % 128 == side * HD else pltpu.roll(half, HD, 1))
            tiles.append(jnp.where(lane < HD, halves[0], halves[1]))
        return tiles[0] if len(tiles) == 1 else jnp.concatenate(tiles, axis=1)

    units = up_state.shape[2] // (planes * cores * shards)

    def up_grad(place, column, size):
        parts = []
        for start in range(column, column + size, min(units, size)):
            plane, member = divmod(start // units, cores * shards)
            spot = 3 * planes * HD + plane * units + start % units
            parts.append(cat_buf[member, place, pl.ds(spot, min(units, size))])
        return parts[0] if len(parts) == 1 else jnp.concatenate(parts, axis=1)

    def plain(grad):
        return lambda place, column, size: grad[place, pl.ds(column, size)]

    place_rows(qkv_state, qkv_grad, *plan[0], keep=qkv_out)
    place_rows(dense_state, plain(dense_grad), *plan[1], keep=dense_out)
    place_rows(up_state, up_grad, *plan[2], keep=up_out)
    place_rows(down_state, plain(down_grad), *plan[3], keep=down_out)

    def flush(entry, row, count, sem):
        place = pl.ds(pl.multiple_of(row * 128, 128), count * 128)
        source = outs[entry].reshape(1, 1, outs[entry].shape[0] * 128)
        return pltpu.make_async_copy(source.at[:, :, place], flat[entry].at[:, :, place], sem)

    def step_copies(at):
        copies = []
        for index, (rows, tiles, start, shifted) in enumerate(plan):
            count = rows * tiles
            skip = 1 if shifted and at == 0 else 0
            for entry in range(3):
                copies.append(
                    flush(entry, start + at * count + skip, count - skip, step_sem.at[entry, index, at])
                )
        return copies

    for at in range(steps):

        @pl.when(step == at)
        def begin(at=at):
            for copy in step_copies(at):
                copy.start()

    @pl.when(step == steps - 1)
    def end():
        covered = set()
        for rows, tiles, start, shifted in plan:
            covered |= set(range(start + (1 if shifted else 0), start + steps * rows * tiles))
        left = [row for row in range(whole_rows) if row not in covered]
        rest = [
            flush(entry, row, 1, rest_sem.at[entry, index]) for index, row in enumerate(left) for entry in range(3)
        ]
        for copy in rest:
            copy.start()
        for at in range(steps):
            for copy in step_copies(at):
                copy.wait()
        for copy in rest:
            copy.wait()


def owner_update(states, cat_sum, grads, small_states, small_grads, groups):
    steps = 4
    sizes = [state.shape[1] * state.shape[2] for state in states]
    small_sizes = [grad.size for grad in small_grads]
    order = [("m", 0), ("s", 0), ("m", 1), ("m", 2), ("s", 1), ("m", 3), ("s", 2)]
    offset = 0
    plan = [None] * 4
    small_plan = []
    pads = []
    small_row = 0
    for kind, index in order:
        if kind == "m":
            state = states[index]
            rows = state.shape[1] // steps
            plan[index] = (rows, state.shape[2] // 128, offset // 128, offset % 128 == 64)
            offset += sizes[index]
        else:
            size = small_sizes[index]
            front = offset % 128
            total = -(-(front + size) // 128)
            pads.append((front, total * 128 - front - size))
            for extra in range(total):
                low = front if extra == 0 else 0
                high = min(128, front + size - extra * 128)
                small_plan.append((small_row + extra, offset // 128 + extra, low, high))
            small_row += total
            offset += size
    entries = offset
    out_rows = -(-entries // 1024) * 8
    small_new = [
        adam_values(state[0].reshape(-1), state[1].reshape(-1), state[2].reshape(-1), grad.reshape(-1))
        for state, grad in zip(small_states, small_grads)
    ]
    small = jnp.stack(
        [
            jnp.concatenate([jnp.pad(new[entry], pad) for new, pad in zip(small_new, pads)])
            for entry in range(3)
        ]
    ).reshape(3, small_row, 128)
    in_specs = [
        pl.BlockSpec((3, rows, tiles * 128), lambda s: (0, s, 0)) for rows, tiles, start, shifted in plan
    ]
    qkv_rows = plan[0][0]
    in_specs.append(pl.BlockSpec((cat_sum.shape[0], qkv_rows, cat_sum.shape[2]), lambda s: (0, s, 0)))
    in_specs.append(pl.BlockSpec((plan[1][0], plan[1][1] * 128), lambda s: (s, 0)))
    in_specs.append(pl.BlockSpec((plan[3][0], plan[3][1] * 128), lambda s: (s, 0)))
    in_specs.append(pl.BlockSpec((3, small_row, 128), lambda s: (0, 0, 0)))
    whole_rows = entries // 128
    *outs, qkv_grad, dense_grad, up_grad, down_grad = pl.pallas_call(
        partial(owner_update_kernel, plan, small_plan, groups, steps, whole_rows),
        grid=(steps,),
        in_specs=in_specs,
        out_specs=[pl.BlockSpec(memory_space=pl.ANY)] * 3
        + [
            pl.BlockSpec((rows, tiles * 128), lambda s: (s, 0)) for rows, tiles, start, shifted in plan
        ],
        out_shape=[jax.ShapeDtypeStruct((1, 1, entries), jnp.float32)] * 3
        + [
            jax.ShapeDtypeStruct(state.shape[1:], jnp.float32) for state in states
        ],
        scratch_shapes=[pltpu.VMEM((cat_sum.shape[0], qkv_rows, cat_sum.shape[2]), jnp.float32)]
        + [pltpu.VMEM((out_rows, 128), jnp.float32)] * 3
        + [pltpu.SemaphoreType.DMA((3, 4, steps)), pltpu.SemaphoreType.DMA((3, 16))],
        compiler_params=pltpu.CompilerParams(vmem_limit_bytes=56 << 20),
        cost_estimate=pl.CostEstimate(
            flops=20 * entries, bytes_accessed=28 * entries, transcendentals=2 * entries
        ),
    )(*states, cat_sum, *grads, small)
    tail = entries - whole_rows * 128
    if tail:
        outs = [
            lax.dynamic_update_slice(out, new[entries_of][-tail:].reshape(1, 1, tail), (0, 0, whole_rows * 128))
            for out, (new, entries_of) in zip(outs, ((small_new[-1], entry) for entry in range(3)))
        ]
    return tuple(outs), qkv_grad, dense_grad, up_grad, down_grad


class Wires:
    def __init__(self, send_sems):
        self.send_sems, self.count, self.pending = send_sems, 0, []
        self.plane, self.core, self.shard = (
            lax.axis_index("plane"),
            lax.axis_index("core"),
            lax.axis_index("shard"),
        )
        self.shards = lax.axis_size("shard")
        self.group = lax.axis_size("core") * self.shards
        self.mine = self.core * self.shards + self.shard
        self.first = (self.plane ^ 1, self.core, self.shard)
        self.second = (self.plane ^ 2, self.core, self.shard)

    def member(self, index):
        return (self.plane, index // self.shards, index % self.shards)

    def barrier(self):
        barrier = pltpu.get_barrier_semaphore()
        partners = [self.member(self.mine ^ mask) for mask in range(1, self.group)]
        partners += [self.first, self.second]
        for partner in partners:
            pl.semaphore_signal(barrier, inc=1, device_id=partner, device_id_type=pl.DeviceIdType.MESH)
        pl.semaphore_wait(barrier, len(partners))

    def send(self, source, target, recv_sem, device, when=None):
        copy = pltpu.make_async_remote_copy(
            src_ref=source,
            dst_ref=target,
            send_sem=self.send_sems.at[self.count],
            recv_sem=recv_sem,
            device_id=device,
            device_id_type=pl.DeviceIdType.MESH,
        )
        self.count += 1
        self.pending.append((copy, when))
        if when is None:
            copy.start()
        else:
            pl.when(when)(copy.start)

    def arrived(self, place, recv_sem, when=None):
        copy = pltpu.make_async_remote_copy(
            src_ref=place,
            dst_ref=place,
            send_sem=self.send_sems.at[0],
            recv_sem=recv_sem,
            device_id=self.first,
            device_id_type=pl.DeviceIdType.MESH,
        )
        if when is None:
            copy.wait_recv()
        else:
            pl.when(when)(copy.wait_recv)

    def drain(self):
        for copy, when in self.pending:
            if when is None:
                copy.wait_send()
            else:
                pl.when(when)(copy.wait_send)


def pack_pieces(qkv, up, pieces, planes, cores, shards):
    rows = qkv.shape[0]
    lane = lax.broadcasted_iota(jnp.int32, (rows, 128), 1)
    units = up.shape[1] // (planes * cores * shards)
    for core in range(cores):
        for shard in range(shards):
            piece = core * shards + shard
            for tile in range(3 * planes // 2):
                halves = []
                for side in range(2):
                    part, plane = divmod(2 * tile + side, planes)
                    head = (plane * cores + core) * shards + shard
                    start = part * planes * cores * shards * HD + head * HD
                    half = qkv[:, pl.ds(start // 128 * 128, 128)]
                    halves.append(half if start % 128 == side * HD else pltpu.roll(half, HD, 1))
                pieces[piece, :, pl.ds(tile * 128, 128)] = jnp.where(lane < HD, halves[0], halves[1]).astype(
                    jnp.bfloat16
                )
            for plane in range(planes):
                block = (plane * cores + core) * shards + shard
                pieces[piece, :, pl.ds(3 * planes * HD + plane * units, units)] = up[
                    :, pl.ds(block * units, units)
                ].astype(jnp.bfloat16)


def gather_kernel(
    vector_start, qkv_state, up_state, dense_state, down_state, tokens, cotangent, vectors,
    cat_out, dense_out, down_out, x_out, dy_out, vec_out, normed_out, mean_out, inverse_out,
    qkv_buf, up_buf, dense_buf, down_buf, pieces, dense, down, x_stage, vec_stage, gain_buf,
    load_sem, send_sems, group_sem, first_sem, second_sem, far_sem, up_sem, low_sem, core_sem, local_sem,
):
    net = Wires(send_sems)
    plane, core, shard, shards, group, mine = net.plane, net.core, net.shard, net.shards, net.group, net.mine
    order = sorted(range(group), key=lambda mask: (mask % shards, mask // shards))
    partner = (plane, 1 - core, shard)

    def cat_unit(mask):
        return lambda p: cat_out.at[p, mine ^ mask]

    def vec_unit(mask):
        return lambda p: vec_out.at[p, mine ^ mask]

    units = []
    down_rows = down.shape[0] // 4
    for part in range(4):
        rows = pl.ds(part * down_rows, down_rows)
        units.append((down.at[rows], lambda p, rows=rows: down_out.at[p, rows]))
    dense_rows = dense.shape[0] // 2
    for part in range(2):
        rows = pl.ds(part * dense_rows, dense_rows)
        units.append((dense.at[rows], lambda p, rows=rows: dense_out.at[p, rows]))
    own_units = list(range(len(units)))
    cat_units, vec_units = {}, {}
    for mask in order:
        cat_units[mask] = len(units)
        units.append((pieces.at[mine] if mask == 0 else None, cat_unit(mask)))
        vec_units[mask] = len(units)
        units.append((vectors if mask == 0 else None, vec_unit(mask)))

    def spread(index):
        source, place = units[index]
        source = place(plane) if source is None else source
        net.send(source, place(plane), first_sem.at[index], net.first)
        net.send(source, place(plane), second_sem.at[index], net.second)

    def hand_on(index):
        place = units[index][1]
        if relay_first[index]:
            net.arrived(place(plane ^ 1), first_sem.at[index])
            net.send(place(plane ^ 1), place(plane ^ 1), far_sem.at[index], net.second)
        else:
            net.arrived(place(plane ^ 2), second_sem.at[index])
            net.send(place(plane ^ 2), place(plane ^ 2), far_sem.at[index], net.first)

    relay_first = {}
    for position, index in enumerate(own_units):
        relay_first[index] = position % 2 == 0
    for position, mask in enumerate(order):
        relay_first[cat_units[mask]] = position % 2 == 0
        relay_first[vec_units[mask]] = position % 2 == 1

    loads = [
        pltpu.make_async_copy(state.at[0], buffer, load_sem.at[index])
        for index, (state, buffer) in enumerate(
            ((qkv_state, qkv_buf), (up_state, up_buf), (down_state, down_buf), (dense_state, dense_buf))
        )
    ]
    for index in (2, 3, 0, 1):
        loads[index].start()
    net.barrier()
    loads[2].wait()
    down[...] = down_buf[...].astype(jnp.bfloat16)
    loads[3].wait()
    dense[...] = dense_buf[...].astype(jnp.bfloat16)
    for index in own_units:
        spread(index)
    loads[0].wait()
    loads[1].wait()
    pack_pieces(qkv_buf, up_buf, pieces, cat_out.shape[0], group // shards, shards)

    locals_ = [
        (pieces.at[mine], cat_out.at[plane, mine]),
        (dense, dense_out.at[plane]),
        (down, down_out.at[plane]),
        (tokens, x_out.at[mine]),
        (cotangent, dy_out.at[mine]),
        (vectors, vec_out.at[plane, mine]),
    ]
    copies = [
        pltpu.make_async_copy(source, target, local_sem.at[index])
        for index, (source, target) in enumerate(locals_)
    ]
    for mask in order[1:]:
        target = net.member(mine ^ mask)
        net.send(vectors, vec_out.at[plane, mine], group_sem.at[1, mask], target)
        net.send(pieces.at[mine ^ mask], cat_out.at[plane, mine], group_sem.at[0, mask], target)
    spread(cat_units[0])
    spread(vec_units[0])
    streams = ((tokens, x_out), (cotangent, dy_out))

    def block(stream, origin):
        return streams[stream][1].at[core * shards + origin]

    def to_core(stream, source, origin, slot, when=None):
        net.send(source, block(stream, origin), core_sem.at[stream, slot], partner, when)

    def hop(stream, distance):
        own = distance == 1
        for upward, sem in ((True, up_sem), (False, low_sem)):
            origin = shard - (distance - 1) if upward else shard + (distance - 1)
            there = shard + 1 if upward else shard - 1
            held = (origin >= 0) if upward else (origin < shards)
            inside = (there < shards) if upward else (there >= 0)
            near = jnp.clip(origin, 0, shards - 1)
            source = streams[stream][0] if own else block(stream, near)
            net.send(
                source,
                block(stream, near),
                sem.at[stream, distance],
                (plane, core, jnp.clip(there, 0, shards - 1)),
                inside & held,
            )

    def hop_arrived(stream, distance):
        for upward, sem in ((True, up_sem), (False, low_sem)):
            origin = shard - distance if upward else shard + distance
            held = (origin >= 0) if upward else (origin < shards)
            near = jnp.clip(origin, 0, shards - 1)
            net.arrived(block(stream, near), sem.at[stream, distance], held)
            slot = distance if upward else shards + distance
            to_core(stream, block(stream, near), near, slot, held)

    for stream in range(2):
        hop(stream, 1)
    for stream in range(2):
        to_core(stream, streams[stream][0], shard, 0)
    for copy in copies:
        copy.start()

    for position, mask in enumerate(order[1:]):
        net.arrived(vec_out.at[plane, mine ^ mask], group_sem.at[1, mask])
        spread(vec_units[mask])
        net.arrived(cat_out.at[plane, mine ^ mask], group_sem.at[0, mask])
        spread(cat_units[mask])
        if position == 2:
            for index in own_units:
                hand_on(index)
    hand_on(cat_units[0])
    hand_on(vec_units[0])
    def unit_arrived(index):
        place = units[index][1]
        if relay_first[index]:
            net.arrived(place(plane ^ 2), second_sem.at[index])
        else:
            net.arrived(place(plane ^ 1), first_sem.at[index])
        net.arrived(place(plane ^ 3), far_sem.at[index])

    def norm_vectors():
        for mask in order:
            unit_arrived(vec_units[mask])
        copies[5].wait()
        fetch = pltpu.make_async_copy(vec_out, vec_stage, load_sem.at[4])
        fetch.start()
        fetch.wait()
        lane = lax.broadcasted_iota(jnp.int32, (1, 128), 1)
        for vector in range(2):
            row, low = divmod(vector_start + vector * HD, 128)
            for pair in range(vec_stage.shape[0] * group // 2):
                halves = []
                for side in range(2):
                    owner_plane, owner = divmod(2 * pair + side, group)
                    half = vec_stage[owner_plane, owner, pl.ds(row, 1), :]
                    halves.append(half if low == side * HD else pltpu.roll(half, HD, 1))
                value = jnp.where(lane < HD, halves[0], halves[1])
                gain_buf[pl.ds(vector, 1), pl.ds(pair * 128, 128)] = value.astype(jnp.bfloat16).astype(
                    jnp.float32
                )

    def normalize(source, index):
        step = 16

        def body(turn, carry):
            rows = pl.ds(pl.multiple_of(turn * step, step), step)
            x = source[rows, :].astype(jnp.float32)
            mean = jnp.mean(x, axis=1, keepdims=True)
            center = x - mean
            inverse = lax.rsqrt(jnp.mean(center * center, axis=1, keepdims=True) + norm_eps)
            normed = center * inverse * gain_buf[0:1, :] + gain_buf[1:2, :]
            normed_out[index, rows, :] = normed.astype(jnp.bfloat16)
            mean_out[index, rows, :] = mean
            inverse_out[index, rows, :] = inverse
            return carry

        lax.fori_loop(0, source.shape[0] // step, body, 0)

    def normalize_far(which, place, when):
        index = which * shards + place

        @pl.when(when)
        def there():
            fetch = pltpu.make_async_copy(x_out.at[index], x_stage, load_sem.at[4])
            fetch.start()
            fetch.wait()
            normalize(x_stage, index)

    def normalize_at(distance):
        for upward in (True, False):
            origin = shard - distance if upward else shard + distance
            held = (origin >= 0) if upward else (origin < shards)
            near = jnp.clip(origin, 0, shards - 1)
            normalize_far(core, near, held)

    def normalize_core(distance):
        for upward in (True, False):
            if distance == 0 and not upward:
                continue
            origin = shard - distance if upward else shard + distance
            held = (origin >= 0) & (origin < shards)
            near = jnp.clip(origin, 0, shards - 1)
            slot = distance if upward else shards + distance
            net.arrived(x_out.at[(1 - core) * shards + near], core_sem.at[0, slot], held)
            normalize_far(1 - core, near, held)

    for distance in range(1, shards):
        if distance == shards - 1:
            for mask in order[1 + (distance - 1) * 3 :]:
                hand_on(vec_units[mask])
                hand_on(cat_units[mask])
            norm_vectors()
            normalize(tokens, mine)
            normalize_core(0)
            for nearer in range(1, distance):
                normalize_at(nearer)
                normalize_core(nearer)
        for stream in range(2):
            hop_arrived(stream, distance)
            if distance + 1 < shards:
                hop(stream, distance + 1)
        if distance < shards - 1:
            for mask in order[1 + (distance - 1) * 3 : 1 + distance * 3]:
                hand_on(vec_units[mask])
                hand_on(cat_units[mask])
    normalize_at(shards - 1)
    normalize_core(shards - 1)

    for index in own_units:
        unit_arrived(index)
    for mask in order:
        unit_arrived(cat_units[mask])
    for slot in range(2 * shards):
        if slot == shards:
            continue
        origin = shard - slot if slot < shards else shard + (slot - shards)
        held = None if slot == 0 else ((origin >= 0) & (origin < shards))
        near = jnp.clip(origin, 0, shards - 1)
        net.arrived(dy_out.at[(1 - core) * shards + near], core_sem.at[1, slot], held)
    for copy in copies[:5]:
        copy.wait()
    net.drain()


def gather_wires(qkv, up, dense, down, tokens, cotangent, vectors, vector_start):
    group, shards = lax.axis_size("core") * lax.axis_size("shard"), lax.axis_size("shard")
    planes = lax.axis_size("plane")
    width = (qkv.shape[2] + up.shape[2]) // group
    units = 6 + 2 * group
    vmem = pl.BlockSpec(memory_space=pltpu.VMEM)
    hbm = pl.BlockSpec(memory_space=pl.ANY)

    def out(*shape, dtype=jnp.bfloat16):
        return jax.ShapeDtypeStruct(shape, dtype)

    dma = pltpu.SemaphoreType.DMA
    return pl.pallas_call(
        partial(gather_kernel, vector_start),
        in_specs=[hbm] * 4 + [vmem] * 3,
        out_specs=[hbm] * 6 + [vmem] * 3,
        out_shape=[
            out(planes, group, qkv.shape[1], width),
            out(planes, *dense.shape[1:]),
            out(planes, *down.shape[1:]),
            out(group, *tokens.shape),
            out(group, *cotangent.shape),
            out(planes, group, *vectors.shape, dtype=vectors.dtype),
            out(group, *tokens.shape),
            out(group, tokens.shape[0], 1, dtype=jnp.float32),
            out(group, tokens.shape[0], 1, dtype=jnp.float32),
        ],
        scratch_shapes=[
            pltpu.VMEM(qkv.shape[1:], qkv.dtype),
            pltpu.VMEM(up.shape[1:], up.dtype),
            pltpu.VMEM(dense.shape[1:], dense.dtype),
            pltpu.VMEM(down.shape[1:], down.dtype),
            pltpu.VMEM((group, qkv.shape[1], width), jnp.bfloat16),
            pltpu.VMEM(dense.shape[1:], jnp.bfloat16),
            pltpu.VMEM(down.shape[1:], jnp.bfloat16),
            pltpu.VMEM(tokens.shape, tokens.dtype),
            pltpu.VMEM((planes, group) + vectors.shape, vectors.dtype),
            pltpu.VMEM((8, tokens.shape[1]), jnp.float32),
            dma((5,)),
            dma((2 * (group - 1) + 3 * units + 2 * 2 * (shards - 1) + 2 * (2 * shards - 1),)),
            dma((2, group)),
            dma((units,)),
            dma((units,)),
            dma((units,)),
            dma((2, shards)),
            dma((2, shards)),
            dma((2, 2 * shards)),
            dma((6,)),
        ],
        compiler_params=pltpu.CompilerParams(
            collective_id=0, has_side_effects=True, vmem_limit_bytes=67043328
        ),
    )(qkv, up, dense, down, tokens, cotangent, vectors)


def add_rows(target, *sources):
    step = 16
    rows = target.shape[0]

    def body(index, carry):
        place = pl.ds(pl.multiple_of(index * step, step), step)
        total = sources[0][place, :].astype(jnp.float32)
        for source in sources[1:]:
            total = total + source[place, :].astype(jnp.float32)
        target[place, :] = total.astype(target.dtype)
        return carry

    lax.fori_loop(0, rows // step, body, 0)


def chunked(first, last, copies_of, body):
    for copy in copies_of(first, first % 2):
        copy.start()

    def step(n, carry):
        slot = lax.rem(n, 2)

        @pl.when(n + 1 < last)
        def ahead():
            for copy in copies_of(n + 1, 1 - slot):
                copy.start()

        for copy in copies_of(n, slot):
            copy.wait()
        body(n, slot)
        return carry

    lax.fori_loop(first, last, step, 0)


def reduce_kernel(
    norm, dcat, x_all, mean, inverse, attn, hidden, dy, cat_w, dense_w, down_w, sums,
    cat_out, dense_out, down_out, mixed_out, norm_out, sums_out,
    cat_part, down_part, dense_part, cat_in, down_in, dense_in,
    tokens, token_in, token_line, token_last, sum_buf,
    wide, hidden_turned, attn_turned, norm_chunk, norm_turned, cat_chunk, x_chunk, down_chunk, dense_chunk, dy_chunk,
    send_sems, near_sem, pass_sem, group_sem, core_sem, line_sem, sum_sem, local_sem, chunk_sem,
):
    PASS, KEEP, LAST = range(3)
    net = Wires(send_sems)
    plane, core, shard, shards, group, mine = net.plane, net.core, net.shard, net.shards, net.group, net.mine
    planes = cat_part.shape[0]
    partner = (plane, 1 - core, shard)
    order = sorted(range(group), key=lambda mask: (mask % shards, mask // shards), reverse=True)
    rows, width = dcat.shape
    model = norm.shape[1]
    block = cat_part.shape[2]
    token_rows = tokens.shape[2]
    units_here = hidden.shape[1]
    heads_here = attn.shape[1]
    lane = 256

    def dot(a, b, a_dim=1, b_dim=0):
        return lax.dot_general(a, b, (((a_dim,), (b_dim,)), ((), ())), preferred_element_type=jnp.float32)

    def columns(n):
        return pl.ds(pl.multiple_of(n * lane, lane), lane)

    units = [(cat_part, cat_in, mask) for mask in order]
    units += [(down_part, down_in, part) for part in range(down_part.shape[1])]
    units += [(dense_part, dense_in, part) for part in range(dense_part.shape[1])]
    down_rows, dense_rows = down_part.shape[2], dense_part.shape[2]

    def ways(index):
        return (net.first, net.second, 1, 2) if index % 2 == 0 else (net.second, net.first, 2, 1)

    def send_pass(index):
        parts, came, slot = units[index]
        net.send(parts.at[3, slot], came.at[PASS, slot], pass_sem.at[0, index], ways(index)[0])

    def send_keep(index):
        parts, came, slot = units[index]
        near, far, near_mask, far_mask = ways(index)
        net.send(parts.at[near_mask, slot], came.at[KEEP, slot], near_sem.at[index], near)

    locals_ = {}

    def local(key, source, target):
        locals_[key] = pltpu.make_async_copy(source, target, local_sem.at[len(locals_)])
        locals_[key].start()

    local("hidden", hidden, wide.at[:, pl.ds(0, units_here)])
    local("attn", attn, wide.at[:, pl.ds(units_here, heads_here)])
    net.barrier()

    places = [place for rank in range(shards // 2) for place in (shards - 1 - rank, rank)]

    def to_partner(stream):
        for place in places:
            net.send(
                tokens.at[stream, (1 - core) * shards + place],
                token_in.at[stream, place],
                core_sem.at[stream, place],
                partner,
            )

    def out_copies(n, slot):
        return [
            pltpu.make_async_copy(down_w.at[:, columns(n)], down_chunk.at[slot], chunk_sem.at[3, slot]),
            pltpu.make_async_copy(dense_w.at[:, columns(n)], dense_chunk.at[slot], chunk_sem.at[4, slot]),
        ]

    def out_step(n, slot):
        total = dot(wide[:, pl.ds(0, units_here)], down_chunk[slot]) + dot(
            wide[:, pl.ds(units_here, heads_here)], dense_chunk[slot]
        )
        for member in range(group):
            tokens[0, member, :, columns(n)] = total[member * token_rows : (member + 1) * token_rows].astype(
                jnp.bfloat16
            )

    locals_["hidden"].wait()
    locals_["attn"].wait()
    chunked(0, model // lane, out_copies, out_step)
    to_partner(0)
    hidden_turned[...] = wide[:, pl.ds(0, units_here)].T
    attn_turned[...] = wide[:, pl.ds(units_here, heads_here)].T
    local("dcat", dcat, wide.at[:, pl.ds(0, width)])

    plane_rows = group * block

    def norm_copy(turn, distance):
        place = pl.ds(pl.multiple_of((plane ^ distance) * plane_rows, plane_rows), plane_rows)
        return pltpu.make_async_copy(
            norm.at[:, place], norm_chunk.at[turn % 2], chunk_sem.at[0, turn % 2]
        )

    cats, every = range(group), range(len(units))
    chain_steps = sorted(
        ((hop, rank) for hop in range(1, shards - 1) for rank in range(shards - 1 - hop)),
        key=lambda pair: (pair[0] + 2 * pair[1], pair[0]),
    )
    turns = (3, 1, 2, 0)
    norm_copy(0, turns[0]).start()
    locals_["dcat"].wait()

    def cat_turn(turn):
        distance = turns[turn]
        if turn + 1 < planes:
            norm_copy(turn + 1, turns[turn + 1]).start()
        norm_copy(turn, distance).wait()
        norm_turned[...] = norm_chunk[turn % 2].T

        def cat_step(n, carry):
            total = dot(norm_turned[...], wide[:, columns(n)]).astype(jnp.bfloat16)
            for member in range(group):
                cat_part[distance, mine ^ member, :, columns(n)] = total[member * block : (member + 1) * block]
            return carry

        lax.fori_loop(0, width // lane, cat_step, 0)
        for index in cats:
            if distance == 3:
                send_pass(index)
            elif distance == ways(index)[2]:
                send_keep(index)

    def own(stream, place):
        return tokens.at[stream, core * shards + place]

    def chain(stream, hop, rank):
        for upward in (True, False):
            target = shards - 1 - rank if upward else rank
            here = hop if upward else shards - 1 - hop
            sems = line_sem.at[0 if upward else 1]
            came = token_line.at[stream, target]
            total = own(stream, target)
            holds = shard == here
            if hop:
                net.arrived(came, sems.at[stream, target], holds)

            @pl.when(holds)
            def add(target=target, came=came, total=total):
                add_rows(total, total, token_in.at[stream, target], *([came] if hop else []))

            there = jnp.clip(shard + (1 if upward else -1), 0, shards - 1)
            ends = (not upward) and rank == shards - 2 - hop
            landing = token_last.at[stream] if ends else came
            net.send(total, landing, sems.at[stream, target], (plane, core, there), holds)

    def final(stream):
        for place in range(shards):
            holds = shard == place
            values = [own(stream, place), token_in.at[stream, place]]
            for landing, side, present in (
                (token_line.at[stream, place], line_sem.at[0], place > 0),
                (token_last.at[stream], line_sem.at[1], place < shards - 1),
            ):
                if present:
                    values.append(landing)
                    net.arrived(landing, side.at[stream, place], holds)

            @pl.when(holds)
            def add(values=values):
                add_rows((mixed_out, norm_out)[stream], *values)

    def first_sums(stream):
        for place in places:
            net.arrived(token_in.at[stream, place], core_sem.at[stream, place])
        for rank in range(shards - 1):
            chain(stream, 0, rank)

    def pass_on(index):
        parts, came, slot = units[index]
        near, far, near_mask, far_mask = ways(index)
        total = parts.at[far_mask, slot]
        net.arrived(came.at[PASS, slot], pass_sem.at[0, index])
        add_rows(total, total, came.at[PASS, slot])
        net.send(total, came.at[LAST, slot], pass_sem.at[1, index], far)

    cat_turn(0)
    first_sums(0)

    sum_buf[4] = sums[...]
    gain_row = width // 128

    def norm_copies(n, slot):
        return [
            pltpu.make_async_copy(cat_w.at[columns(n), :], cat_chunk.at[slot], chunk_sem.at[1, slot]),
            pltpu.make_async_copy(x_all.at[:, columns(n)], x_chunk.at[slot], chunk_sem.at[2, slot]),
        ]

    def norm_step(n, slot):
        total = dot(wide[:, pl.ds(0, width)], cat_chunk[slot], 1, 1)
        x_hat = (x_chunk[slot].astype(jnp.float32) - mean[...]) * inverse[...]
        gain = jnp.sum(total * x_hat, axis=0, keepdims=True)
        shift = jnp.sum(total, axis=0, keepdims=True)
        for half in range(lane // 128):
            row = gain_row + n * (lane // 128) + half
            sum_buf[4, pl.ds(row, 1), :] = gain[:, half * 128 : (half + 1) * 128]
            sum_buf[4, pl.ds(row + model // 128, 1), :] = shift[:, half * 128 : (half + 1) * 128]
        for member in range(group):
            tokens[1, member, :, columns(n)] = total[member * token_rows : (member + 1) * token_rows].astype(
                jnp.bfloat16
            )

    chunked(0, model // lane, norm_copies, norm_step)

    net.send(sum_buf.at[4], sum_buf.at[0], sum_sem.at[0], net.first)
    to_partner(1)
    cat_turn(1)
    chain(0, 1, 0)
    first_sums(1)
    cat_turn(2)
    cat_turn(3)
    net.arrived(sum_buf.at[0], sum_sem.at[0])
    sum_buf[1] = sum_buf[4] + sum_buf[0]
    net.send(sum_buf.at[1], sum_buf.at[2], sum_sem.at[1], net.second)
    for index in cats:
        pass_on(index)

    def grad_copies(n, slot):
        return [pltpu.make_async_copy(dy.at[:, columns(n)], dy_chunk.at[slot], chunk_sem.at[5, slot])]

    def grad_step(n, slot):
        for parts, left in ((down_part, hidden_turned[...]), (dense_part, attn_turned[...])):
            grad = dot(left, dy_chunk[slot]).astype(jnp.bfloat16)
            pieces, size = parts.shape[1], parts.shape[2]
            for q in range(planes):
                for piece in range(pieces):
                    start = (q * pieces + piece) * size
                    parts[plane ^ q, piece, :, columns(n)] = grad[start : start + size]

    chunked(0, model // lane, grad_copies, grad_step)
    for index in every[group:]:
        send_pass(index)
        send_keep(index)
    for hop, rank in chain_steps[1:]:
        chain(0, hop, rank)

    def finish(index):
        parts, came, slot = units[index]
        total = parts.at[0, slot]
        net.arrived(came.at[KEEP, slot], near_sem.at[index])
        net.arrived(came.at[LAST, slot], pass_sem.at[1, index])
        values = (total, came.at[KEEP, slot], came.at[LAST, slot])
        if index < group:
            add_rows(total, *values)
            if slot:
                net.send(total, cat_out.at[mine], group_sem.at[0, slot], net.member(mine ^ slot))
            else:
                local("own", total, cat_out.at[mine])
        elif parts is down_part:
            add_rows(down_out.at[pl.ds(slot * down_rows, down_rows)], *values)
        else:
            add_rows(dense_out.at[pl.ds(slot * dense_rows, dense_rows)], *values)

    net.arrived(sum_buf.at[2], sum_sem.at[1])
    sum_buf[3] = sum_buf[1] + sum_buf[2]
    for mask in range(1, group):
        net.send(sum_buf.at[3], sums_out.at[mine], group_sem.at[1, mask], net.member(mine ^ mask))
    local("sums", sum_buf.at[3], sums_out.at[mine])
    for index in cats[: group // 2]:
        finish(index)
    chain(1, *chain_steps[0])
    for index in cats[group // 2 : group - 2]:
        finish(index)
    for hop, rank in chain_steps[1:]:
        chain(1, hop, rank)
    for index in cats[group - 2 :]:
        finish(index)
    for index in every[group:]:
        pass_on(index)
    final(0)
    for index in every[group:]:
        finish(index)
    final(1)
    for mask in range(1, group):
        net.arrived(cat_out.at[mine ^ mask], group_sem.at[0, mask])
        net.arrived(sums_out.at[mine ^ mask], group_sem.at[1, mask])
    locals_["own"].wait()
    locals_["sums"].wait()
    net.drain()


def reduce_wires(norm, dcat, x_all, mean, inverse, attn, hidden, dy, cat_w, dense_w, down_w, sums):
    planes, shards = lax.axis_size("plane"), lax.axis_size("shard")
    group = lax.axis_size("core") * shards
    units = group + 6
    rows, width = dcat.shape
    model = norm.shape[1]
    block = model // (planes * group)
    unit_rows, head_rows = down_w.shape[0] // planes, dense_w.shape[0] // planes
    token_rows = rows // group
    vmem = pl.BlockSpec(memory_space=pltpu.VMEM)
    hbm = pl.BlockSpec(memory_space=pl.ANY)
    dma = pltpu.SemaphoreType.DMA
    lane = 256

    def scratch(*shape, dtype=jnp.bfloat16):
        return pltpu.VMEM(shape, dtype)

    return pl.pallas_call(
        reduce_kernel,
        in_specs=[hbm] * 3 + [vmem] * 2 + [hbm] * 6 + [vmem],
        out_specs=[hbm] + [vmem] * 4 + [hbm],
        out_shape=[
            jax.ShapeDtypeStruct((group, block, width), jnp.bfloat16),
            jax.ShapeDtypeStruct((head_rows, model), jnp.float32),
            jax.ShapeDtypeStruct((unit_rows, model), jnp.float32),
            jax.ShapeDtypeStruct((token_rows, model), jnp.float32),
            jax.ShapeDtypeStruct((token_rows, model), jnp.float32),
            jax.ShapeDtypeStruct((group,) + sums.shape, sums.dtype),
        ],
        scratch_shapes=[
            scratch(planes, group, block, width),
            scratch(planes, 4, unit_rows // 4, model),
            scratch(planes, 2, head_rows // 2, model),
            scratch(3, group, block, width),
            scratch(3, 4, unit_rows // 4, model),
            scratch(3, 2, head_rows // 2, model),
            scratch(2, group, token_rows, model),
            scratch(2, shards, token_rows, model),
            scratch(2, shards, token_rows, model),
            scratch(2, token_rows, model),
            scratch(5, *sums.shape, dtype=jnp.float32),
            scratch(rows, max(width, hidden.shape[1] + attn.shape[1])),
            scratch(hidden.shape[1], rows),
            scratch(attn.shape[1], rows),
            scratch(2, rows, group * block),
            scratch(group * block, rows),
            scratch(2, lane, width),
            scratch(2, rows, lane),
            scratch(2, hidden.shape[1], lane),
            scratch(2, attn.shape[1], lane),
            scratch(2, rows, lane),
            dma((2 + 2 * shards + 2 * shards * (shards - 1) + 3 * units + 2 * (group - 1),)),
            dma((units,)),
            dma((2, units)),
            dma((2, group)),
            dma((2, shards)),
            dma((2, 2, shards)),
            dma((2,)),
            dma((5,)),
            dma((6, 2)),
        ],
        compiler_params=pltpu.CompilerParams(
            collective_id=1, has_side_effects=True, vmem_limit_bytes=67043328
        ),
    )(norm, dcat, x_all, mean, inverse, attn, hidden, dy, cat_w, dense_w, down_w, sums)


def fast_body(
    hidden_in,
    segment_ids,
    out_grad,
    qkv_weight_state,
    qkv_bias_state,
    dense_weight_state,
    up_weight_state,
    up_bias_state,
    down_weight_state,
    vector_state,
):
    planes, cores, shards = lax.axis_size("plane"), lax.axis_size("core"), lax.axis_size("shard")
    plane, core, shard = lax.axis_index("plane"), lax.axis_index("core"), lax.axis_index("shard")
    group = cores * shards
    owner = (plane * cores + core) * shards + shard
    owners = planes * group
    model_rows = qkv_weight_state.shape[1]
    unit_rows = down_weight_state.shape[1]
    tokens_here = hidden_in.shape[1]
    head_width = planes * HD
    unit_width = planes * unit_rows
    qkv_count, upb_count = qkv_bias_state.shape[1], up_bias_state.shape[1]

    tokens, cotangent, q_seg = hidden_in[0], out_grad[0], segment_ids[0]
    vec_list = [
        qkv_bias_state[0],
        up_bias_state[0],
        vector_state[0].T.reshape(-1),
        q_seg.astype(jnp.float32),
    ]
    vec_sizes = [value.size for value in vec_list]
    vec_rows = -(-sum(vec_sizes) // 1024) * 8
    vec_own = jnp.pad(jnp.concatenate(vec_list), (0, vec_rows * 128 - sum(vec_sizes))).reshape(vec_rows, 128)

    cat_w, dense_w, down_w, x_all, dy_all, vec_all, norm_bf, x_mean, inverse = gather_wires(
        qkv_weight_state,
        up_weight_state,
        dense_weight_state,
        down_weight_state,
        tokens,
        cotangent,
        vec_own,
        sum(vec_sizes[:2]),
    )

    cat_w = cat_w.reshape(D, 3 * head_width + unit_width)
    dense_w = dense_w.reshape(head_width, D)
    down_w = down_w.reshape(unit_width, D)
    rows = group * tokens_here
    x_all = x_all.reshape(rows, D)
    dy_all = dy_all.reshape(rows, D)
    vec_flat = vec_all.reshape(planes, cores, shards, vec_rows * 128)
    at = [0]
    for size in vec_sizes:
        at.append(at[-1] + size)

    def rounded(value):
        return value.astype(jnp.bfloat16).astype(jnp.float32)

    qkv_bias = rounded(vec_flat[..., at[0] : at[1]]).reshape(3, planes, cores, shards, HD)
    qkv_bias = lax.dynamic_index_in_dim(
        qkv_bias.transpose(2, 3, 0, 1, 4).reshape(group, 3 * head_width), core * shards + shard, 0, False
    )
    up_bias = lax.dynamic_index_in_dim(
        rounded(vec_flat[..., at[1] : at[2]]).transpose(1, 2, 0, 3).reshape(group, unit_width),
        core * shards + shard,
        0,
        False,
    )
    vec_columns = (
        rounded(vec_flat[..., at[2] : at[3]])
        .reshape(owners, 4, model_rows)
        .transpose(1, 0, 2)
        .reshape(4, D)
    )
    norm_gain, norm_shift, dense_bias, down_bias = (vec_columns[index] for index in range(4))
    segments = lax.dynamic_index_in_dim(vec_flat[..., at[3] : at[4]], plane, 0, False)
    segments = segments.astype(jnp.int32).reshape(cores, shards * tokens_here)
    cat_bias = jnp.concatenate([qkv_bias, up_bias])

    norm_bf = norm_bf.reshape(rows, D)
    x_mean = x_mean.reshape(rows, 1)
    inverse = inverse.reshape(rows, 1)

    fu = jnp.dot(norm_bf, cat_w, preferred_element_type=jnp.float32) + cat_bias
    pre_act = fu[:, 3 * head_width :]
    hidden = gelu_tanh(pre_act).astype(jnp.bfloat16)
    grad_hidden = jnp.dot(dy_all, down_w.T, preferred_element_type=jnp.float32)
    grad_pre = jax.vjp(gelu_tanh, pre_act)[1](grad_hidden)[0]
    upb_part = jnp.sum(grad_pre, axis=0)
    grad_heads = jnp.dot(dy_all, dense_w.T, preferred_element_type=jnp.float32).astype(jnp.bfloat16)
    attn, dcat, qkvb_part = attention(fu, grad_heads, grad_pre.astype(jnp.bfloat16), segments)
    bias_part = jnp.sum(cotangent.astype(jnp.float32), axis=0)
    nothing = jnp.zeros((D,), jnp.float32)
    sums = [qkvb_part, upb_part, nothing, nothing, bias_part]
    sum_sizes = [value.size for value in sums]
    sum_rows = -(-sum(sum_sizes) // 1024) * 8
    sums = jnp.pad(jnp.concatenate(sums), (0, sum_rows * 128 - sum(sum_sizes))).reshape(sum_rows, 128)

    cat_sum, dense_grad, down_grad, mixed, grad_norm, sums_all = reduce_wires(
        norm_bf,
        dcat,
        x_all,
        x_mean,
        inverse,
        attn,
        hidden,
        dy_all,
        cat_w,
        dense_w,
        down_w,
        sums,
    )

    sums_flat = sums_all.reshape(cores, shards, sum_rows * 128)
    at = [0]
    for size in sum_sizes:
        at.append(at[-1] + size)
    qkvb_grad = (
        sums_flat[..., : at[1]]
        .reshape(cores, shards, 3, planes, HD)
        .transpose(2, 3, 0, 1, 4)
        .reshape(owners, qkv_count)
    )
    qkvb_grad = lax.dynamic_index_in_dim(qkvb_grad, owner, 0, False)
    upb_grad = sums_flat[..., at[1] : at[2]].reshape(group, planes, upb_count)
    upb_grad = lax.dynamic_index_in_dim(
        lax.dynamic_index_in_dim(upb_grad, core * shards + shard, 0, False), plane, 0, False
    )
    vec_grad = jnp.sum(sums_flat[..., at[2] : at[5]], axis=(0, 1)).reshape(3, owners, model_rows)
    vec_grad = lax.dynamic_index_in_dim(vec_grad, owner, 1, False)
    vec_grad = jnp.stack([vec_grad[0], vec_grad[1], vec_grad[2], vec_grad[2]], axis=1)

    x_own = tokens.astype(jnp.float32)
    output = (x_own + (mixed.astype(jnp.float32) + dense_bias + down_bias)).astype(jnp.bfloat16)
    own_center = x_own - jnp.mean(x_own, axis=-1, keepdims=True)
    own_inverse = lax.rsqrt(jnp.mean(own_center * own_center, axis=-1, keepdims=True) + norm_eps)
    own_hat = own_center * own_inverse
    hat_grad = grad_norm.astype(jnp.float32) * norm_gain
    x_grad = own_inverse * (
        hat_grad
        - jnp.mean(hat_grad, axis=-1, keepdims=True)
        - own_hat * jnp.mean(hat_grad * own_hat, axis=-1, keepdims=True)
    )
    input_grad = cotangent.astype(jnp.float32) + x_grad

    new, qkv_grad, dense_grad, up_grad, down_grad = owner_update(
        (qkv_weight_state, dense_weight_state, up_weight_state, down_weight_state),
        cat_sum,
        (dense_grad, down_grad),
        (qkv_bias_state, up_bias_state, vector_state),
        (qkvb_grad, upb_grad, vec_grad),
        (planes, cores, shards),
    )
    return (
        output[None],
        input_grad[None],
        qkv_grad,
        qkvb_grad,
        dense_grad,
        up_grad,
        upb_grad,
        down_grad,
        vec_grad,
        *new,
    )


def fast_solution(mesh):
    rep, shard = mesh.shape["rep"], mesh.shape["shard"]
    inner = Mesh(mesh.devices.reshape(rep // 2, 2, shard), ("plane", "core", "shard"))
    both = ("plane", "core")
    every = ("plane", "core", "shard")
    in_specs = (
        P(both, "shard", None),
        P(both, "shard"),
        P(both, "shard", None),
        P(None, every, None),
        P(None, every),
        P(None, every, None),
        P(None, every, None),
        P(None, every),
        P(None, every, None),
        P(None, every, None),
    )
    out_specs = (
        P(both, "shard", None),
        P(both, "shard", None),
        P(every, None),
        P(every),
        P(every, None),
        P(every, None),
        P(every),
        P(every, None),
        P(every, None),
        P(both, "shard", None),
        P(both, "shard", None),
        P(both, "shard", None),
    )
    return jax.shard_map(fast_body, mesh=inner, in_specs=in_specs, out_specs=out_specs, check_vma=False)


def solution(mesh):
    in_specs = (
        P("rep", "shard", None),
        P("rep", "shard"),
        P("rep", "shard", None),
        P(None, ("rep", "shard"), None),
        P(None, ("rep", "shard")),
        P(None, ("rep", "shard"), None),
        P(None, ("rep", "shard"), None),
        P(None, ("rep", "shard")),
        P(None, ("rep", "shard"), None),
        P(None, ("rep", "shard"), None),
    )
    out_specs = (
        P("rep", "shard", None),
        P("rep", "shard", None),
        P(("rep", "shard"), None),
        P(("rep", "shard")),
        P(("rep", "shard"), None),
        P(("rep", "shard"), None),
        P(("rep", "shard")),
        P(("rep", "shard"), None),
        P(("rep", "shard"), None),
        P("rep", "shard", None),
        P("rep", "shard", None),
        P("rep", "shard", None),
    )
    if whole_heads(mesh):
        return fast_solution(mesh)
    return jax.shard_map(body, mesh=mesh, in_specs=in_specs, out_specs=out_specs, check_vma=False)
```

```python
from functools import partial
import math

import jax
import jax.numpy as jnp
from jax import lax
from jax.experimental import pallas as pl
from jax.experimental.pallas import tpu as pltpu
from jax.sharding import Mesh
from jax.sharding import PartitionSpec as P

D = 2048
HD = 64
ROT = 32
FF = 8192
STEP = 5


learn_rate = 0.02
beta_one = 0.9
beta_two = 0.95
adam_eps = 1e-08
weight_decay = 0.1
norm_eps = 1e-05
big_negative = -1e30


def layer_norm(x, norm_gain, norm_shift):
    center = x - jnp.mean(x, axis=-1, keepdims=True)
    variance = jnp.mean(center * center, axis=-1, keepdims=True)
    return center * lax.rsqrt(variance + norm_eps) * norm_gain + norm_shift


def gelu_tanh(v):
    return 0.5 * v * (1.0 + jnp.tanh(0.7978845608028654 * (v + 0.044715 * v * v * v)))


def rotary(x, positions):
    half_rot = ROT // 2
    frequency = jnp.exp(jnp.arange(half_rot, dtype=jnp.float32) * (-2.0 * math.log(10000.0) / ROT))
    angles = positions.astype(jnp.float32)[:, None] * frequency[None, :]
    cosine = jnp.cos(angles)[:, None, :]
    sine_val = jnp.sin(angles)[:, None, :]
    lower_part = x[..., :half_rot]
    upper_part = x[..., half_rot:ROT]
    return jnp.concatenate(
        [
            lower_part * cosine - upper_part * sine_val,
            upper_part * cosine + lower_part * sine_val,
            x[..., ROT:],
        ],
        axis=-1,
    )


def adam_update(state, grad):
    moment_one = beta_one * state[1] + (1.0 - beta_one) * grad
    moment_two = beta_two * state[2] + (1.0 - beta_two) * grad * grad
    corrected = moment_one / (1.0 - beta_one**STEP)
    divisor = jnp.sqrt(moment_two / (1.0 - beta_two**STEP)) + adam_eps
    weight = state[0] - learn_rate * (corrected / divisor + weight_decay * state[0])
    return jnp.stack([weight, moment_one, moment_two])


def owner_entries(new_states, entry):
    return jnp.concatenate(
        [state_new[entry].reshape(-1) for state_new in new_states], axis=0
    ).reshape(1, 1, -1)


def block_mask(q_pos, q_seg, k_pos, k_seg):
    return (k_pos[None, :] <= q_pos[:, None]) & (k_seg[None, :] == q_seg[:, None])


def attend_keys(kv_all, seg_all, queries, q_pos, q_seg):
    key_count = kv_all.shape[0]
    width = kv_all.shape[1] // 2
    heads_here = queries.shape[1]
    query_rows = queries.shape[0]
    block_rows = math.gcd(key_count, 512)
    block_count = key_count // block_rows
    kv_blocks = kv_all.reshape(block_count, block_rows, 2 * width)
    seg_blocks = seg_all.reshape(block_count, block_rows)
    score_scale = 1.0 / math.sqrt(HD)

    def attend_step_block(carry, block_items):
        kv_rows, seg_rows, block_index = block_items
        row_max, totals, accumulated = carry
        key_rows = kv_rows[:, :width].reshape(block_rows, heads_here, HD)
        value_rows = kv_rows[:, width:].reshape(block_rows, heads_here, HD)
        k_pos = block_index * block_rows + jnp.arange(block_rows, dtype=jnp.int32)
        allowed = block_mask(q_pos, q_seg, k_pos, seg_rows)
        scores = (
            jnp.einsum("qhd,khd->hqk", queries, key_rows, preferred_element_type=jnp.float32)
            * score_scale
        )
        scores = jnp.where(allowed[None], scores, big_negative)
        new_max = jnp.maximum(row_max, jnp.max(scores, axis=-1))
        probabilities = jnp.where(allowed[None], jnp.exp(scores - new_max[..., None]), 0.0)
        factor = jnp.exp(row_max - new_max)
        totals = totals * factor + jnp.sum(probabilities, axis=-1)
        accumulated = accumulated * factor[..., None] + jnp.einsum(
            "hqk,khd->hqd",
            probabilities.astype(jnp.bfloat16),
            value_rows,
            preferred_element_type=jnp.float32,
        )
        return ((new_max, totals, accumulated), None)

    start_state = (
        jnp.full((heads_here, query_rows), big_negative, jnp.float32),
        jnp.zeros((heads_here, query_rows), jnp.float32),
        jnp.zeros((heads_here, query_rows, HD), jnp.float32),
    )
    running, unused = lax.scan(
        attend_step_block,
        start_state,
        (kv_blocks, seg_blocks, jnp.arange(block_count, dtype=jnp.int32)),
    )
    return running


def attention_grads(queries, kv_all, seg_all, q_pos, q_seg, grad_heads, delta_all, lse_all):
    key_count = kv_all.shape[0]
    width = kv_all.shape[1] // 2
    heads_here = queries.shape[1]
    query_rows = queries.shape[0]
    block_rows = math.gcd(key_count, 512)
    block_count = key_count // block_rows
    kv_blocks = kv_all.reshape(block_count, block_rows, 2 * width)
    seg_blocks = seg_all.reshape(block_count, block_rows)
    score_scale = 1.0 / math.sqrt(HD)

    def attention_step_block(query_grad, block_items):
        kv_rows, seg_rows, block_index = block_items
        key_rows = kv_rows[:, :width].reshape(block_rows, heads_here, HD)
        value_rows = kv_rows[:, width:].reshape(block_rows, heads_here, HD)
        k_pos = block_index * block_rows + jnp.arange(block_rows, dtype=jnp.int32)
        allowed = block_mask(q_pos, q_seg, k_pos, seg_rows)
        scores = (
            jnp.einsum("qhd,khd->hqk", queries, key_rows, preferred_element_type=jnp.float32)
            * score_scale
        )
        scores = jnp.where(allowed[None], scores, big_negative)
        probabilities = jnp.where(allowed[None], jnp.exp(scores - lse_all[..., None]), 0.0)
        value_grad = jnp.einsum(
            "hqk,qhd->khd",
            probabilities.astype(jnp.bfloat16),
            grad_heads,
            preferred_element_type=jnp.float32,
        )
        prob_grad = jnp.einsum(
            "qhd,khd->hqk", grad_heads, value_rows, preferred_element_type=jnp.float32
        )
        score_grad = (probabilities * (prob_grad - delta_all[..., None]) * score_scale).astype(
            jnp.bfloat16
        )
        query_grad = query_grad + jnp.einsum(
            "hqk,khd->hqd", score_grad, key_rows, preferred_element_type=jnp.float32
        )
        key_grad = jnp.einsum(
            "hqk,qhd->khd", score_grad, queries, preferred_element_type=jnp.float32
        )
        return (
            query_grad,
            jnp.concatenate(
                [key_grad.reshape(block_rows, width), value_grad.reshape(block_rows, width)], axis=1
            ),
        )

    query_grad, kv_grad_blocks = lax.scan(
        attention_step_block,
        jnp.zeros((heads_here, query_rows, HD), jnp.float32),
        (kv_blocks, seg_blocks, jnp.arange(block_count, dtype=jnp.int32)),
    )
    return (query_grad, kv_grad_blocks.reshape(key_count, 2 * width))


def gather_vectors(own_qkvb, own_upb, own_vec):
    return (
        lax.all_gather(own_qkvb, ("rep", "shard"), axis=0, tiled=True),
        lax.all_gather(own_upb, ("rep", "shard"), axis=0, tiled=True),
        lax.all_gather(own_vec, ("rep", "shard"), axis=0, tiled=True),
    )


def sum_vectors(qkvb_grad, upb_grad, vec_grad):
    return (
        lax.psum_scatter(qkvb_grad, ("rep", "shard"), scatter_dimension=0, tiled=True),
        lax.psum_scatter(upb_grad, ("rep", "shard"), scatter_dimension=0, tiled=True),
        lax.psum_scatter(vec_grad, ("rep", "shard"), scatter_dimension=0, tiled=True),
    )


def sum_positions(partial_rows):
    return lax.psum_scatter(partial_rows, "shard", scatter_dimension=0, tiled=True)


def attention_pass(norm_rows, qkv_w, qkv_b, positions, key_width):
    row_count = norm_rows.shape[0]
    heads_here = key_width // HD
    joined = jnp.dot(norm_rows, qkv_w, preferred_element_type=jnp.float32) + qkv_b
    q_pre = joined[:, :key_width].reshape(row_count, heads_here, HD)
    k_pre = joined[:, key_width : 2 * key_width].reshape(row_count, heads_here, HD)
    queries = rotary(q_pre, positions).astype(jnp.bfloat16)
    key_local = rotary(k_pre, positions).astype(jnp.bfloat16).reshape(row_count, key_width)
    value_local = joined[:, 2 * key_width :].astype(jnp.bfloat16)
    kv_local = jnp.concatenate([key_local, value_local], axis=1)
    return (q_pre, k_pre, queries, kv_local)


def finish_qkv_grad(q_pre, k_pre, positions, query_grad, kv_grad, key_width):
    row_count = q_pre.shape[0]
    heads_here = key_width // HD
    rotate_back = partial(rotary, positions=positions)
    query_pre = jax.vjp(rotate_back, q_pre)[1](query_grad.transpose(1, 0, 2))[0]
    key_pre = jax.vjp(rotate_back, k_pre)[1](
        kv_grad[:, :key_width].reshape(row_count, heads_here, HD)
    )[0]
    return jnp.concatenate(
        [
            query_pre.reshape(row_count, key_width),
            key_pre.reshape(row_count, key_width),
            kv_grad[:, key_width:],
        ],
        axis=1,
    )


def sliced_pass(norm_bf, q_seg, cotangent, own_mats, qkv_bb, up_bb):
    own_qkv, own_dense, own_up, own_down = own_mats
    inner_count = lax.axis_size("shard")
    outer_count = lax.axis_size("rep")
    stride = outer_count // inner_count
    place = lax.axis_index("shard")
    head_width = D // inner_count
    unit_width = FF // inner_count
    qkv_rows = own_qkv.shape[0]
    dense_rows = own_dense.shape[0]
    down_rows = own_down.shape[0]
    qkv_split = own_qkv.reshape(qkv_rows, 3, inner_count, head_width)
    up_split = own_up.reshape(qkv_rows, 1, inner_count, unit_width)
    qkv_cols, up_cols = (
        lax.all_to_all(qkv_split, "shard", split_axis=2, concat_axis=0, tiled=True),
        lax.all_to_all(up_split, "shard", split_axis=2, concat_axis=0, tiled=True),
    )
    qkv_rep, up_rep, dense_rep, down_rep = (
        lax.all_gather(qkv_cols, "rep", axis=0, tiled=True),
        lax.all_gather(up_cols, "rep", axis=0, tiled=True),
        lax.all_gather(own_dense[None], "rep", axis=0, tiled=True),
        lax.all_gather(own_down[None], "rep", axis=0, tiled=True),
    )
    dense_grid = dense_rep.reshape(inner_count, stride, 1, dense_rows, D)
    down_grid = down_rep.reshape(inner_count, stride, 1, down_rows, D)
    dense_moved, down_moved = (
        lax.all_to_all(dense_grid, "shard", split_axis=0, concat_axis=2, tiled=True),
        lax.all_to_all(down_grid, "shard", split_axis=0, concat_axis=2, tiled=True),
    )
    qkv_w = qkv_rep.reshape(D, 3 * head_width)
    up_w = up_rep.reshape(D, unit_width)
    dense_w = dense_moved.reshape(head_width, D)
    down_w = down_moved.reshape(unit_width, D)
    qkv_b = lax.dynamic_index_in_dim(
        qkv_bb.astype(jnp.float32).reshape(3, inner_count, head_width), place, 1, False
    ).reshape(3 * head_width)
    up_b = lax.dynamic_slice_in_dim(up_bb.astype(jnp.float32), place * unit_width, unit_width, 0)
    norm_seq, grad_seq, seg_seq = (
        lax.all_gather(norm_bf, "shard", axis=0, tiled=True),
        lax.all_gather(cotangent, "shard", axis=0, tiled=True),
        lax.all_gather(q_seg, "shard", axis=0, tiled=True),
    )
    seq_rows = norm_seq.shape[0]
    heads_here = head_width // HD
    positions = jnp.arange(seq_rows, dtype=jnp.int32)
    q_pre, k_pre, queries, kv_seq = attention_pass(norm_seq, qkv_w, qkv_b, positions, head_width)
    row_max, totals, accumulated = attend_keys(kv_seq, seg_seq, queries, positions, seg_seq)
    lse_all = row_max + jnp.log(totals)
    out_heads = (accumulated / totals[..., None]).transpose(1, 0, 2).astype(jnp.bfloat16)
    attn_bf = out_heads.reshape(seq_rows, head_width)
    pre_act = jnp.dot(norm_seq, up_w, preferred_element_type=jnp.float32) + up_b
    hidden = gelu_tanh(pre_act).astype(jnp.bfloat16)
    partial_out = jnp.dot(attn_bf, dense_w, preferred_element_type=jnp.float32) + jnp.dot(
        hidden, down_w, preferred_element_type=jnp.float32
    )
    mixed = sum_positions(partial_out)
    grad_down = jnp.dot(hidden.T, grad_seq, preferred_element_type=jnp.float32)
    grad_dense = jnp.dot(attn_bf.T, grad_seq, preferred_element_type=jnp.float32)
    grad_hidden = jnp.dot(grad_seq, down_w.T, preferred_element_type=jnp.float32)
    grad_pre = jax.vjp(gelu_tanh, pre_act)[1](grad_hidden)[0]
    grad_pre_bf = grad_pre.astype(jnp.bfloat16)
    grad_up = jnp.dot(norm_seq.T, grad_pre_bf, preferred_element_type=jnp.float32)
    upb_part = jnp.sum(grad_pre, axis=0)
    norm_part = jnp.dot(grad_pre_bf, up_w.T, preferred_element_type=jnp.float32)
    grad_heads = (
        jnp.dot(grad_seq, dense_w.T, preferred_element_type=jnp.float32)
        .astype(jnp.bfloat16)
        .reshape(seq_rows, heads_here, HD)
    )
    delta_all = jnp.sum(grad_heads.astype(jnp.float32) * out_heads.astype(jnp.float32), axis=-1).T
    query_grad, kv_grad = attention_grads(
        queries, kv_seq, seg_seq, positions, seg_seq, grad_heads, delta_all, lse_all
    )
    grad_joined = finish_qkv_grad(q_pre, k_pre, positions, query_grad, kv_grad, head_width)
    grad_joined_bf = grad_joined.astype(jnp.bfloat16)
    grad_qkv = jnp.dot(norm_seq.T, grad_joined_bf, preferred_element_type=jnp.float32)
    qkvb_part = jnp.sum(grad_joined, axis=0)
    norm_part = norm_part + jnp.dot(grad_joined_bf, qkv_w.T, preferred_element_type=jnp.float32)
    grad_norm = sum_positions(norm_part)
    dense_grid_grad = grad_dense.reshape(1, stride, inner_count, dense_rows, D)
    down_grid_grad = grad_down.reshape(1, stride, inner_count, down_rows, D)
    dense_back, down_back = (
        lax.all_to_all(dense_grid_grad, "shard", split_axis=2, concat_axis=0, tiled=True),
        lax.all_to_all(down_grid_grad, "shard", split_axis=2, concat_axis=0, tiled=True),
    )
    qkv_sum, up_sum, dense_sum, down_sum = (
        lax.psum_scatter(
            grad_qkv.reshape(D, 3, 1, head_width), "rep", scatter_dimension=0, tiled=True
        ),
        lax.psum_scatter(
            grad_up.reshape(D, 1, 1, unit_width), "rep", scatter_dimension=0, tiled=True
        ),
        lax.psum_scatter(
            dense_back.reshape(outer_count, dense_rows, D), "rep", scatter_dimension=0, tiled=True
        ),
        lax.psum_scatter(
            down_back.reshape(outer_count, down_rows, D), "rep", scatter_dimension=0, tiled=True
        ),
    )
    qkv_home, up_home = (
        lax.all_to_all(qkv_sum, "shard", split_axis=0, concat_axis=2, tiled=True),
        lax.all_to_all(up_sum, "shard", split_axis=0, concat_axis=2, tiled=True),
    )
    qkv_own = qkv_home.reshape(qkv_rows, 3 * D)
    up_own = up_home.reshape(qkv_rows, FF)
    dense_own = dense_sum.reshape(dense_rows, D)
    down_own = down_sum.reshape(down_rows, D)
    selector = (jnp.arange(inner_count, dtype=jnp.int32) == place).astype(jnp.float32)
    qkvb_grad = (selector[None, :, None] * qkvb_part.reshape(3, 1, head_width)).reshape(3 * D)
    upb_grad = (selector[:, None] * upb_part[None, :]).reshape(FF)
    return (mixed, grad_norm, (qkv_own, dense_own, up_own, down_own), qkvb_grad, upb_grad)


def body(
    hidden_in,
    segment_ids,
    out_grad,
    qkv_weight_state,
    qkv_bias_state,
    dense_weight_state,
    up_weight_state,
    up_bias_state,
    down_weight_state,
    vector_state,
):
    own_mats = (
        qkv_weight_state[0].astype(jnp.bfloat16),
        dense_weight_state[0].astype(jnp.bfloat16),
        up_weight_state[0].astype(jnp.bfloat16),
        down_weight_state[0].astype(jnp.bfloat16),
    )
    qkv_bb, up_bb, vec_bf = gather_vectors(
        qkv_bias_state[0].astype(jnp.bfloat16),
        up_bias_state[0].astype(jnp.bfloat16),
        vector_state[0].astype(jnp.bfloat16),
    )
    vec_all = vec_bf.astype(jnp.float32)
    norm_gain = vec_all[:, 0]
    norm_shift = vec_all[:, 1]
    dense_bias = vec_all[:, 2]
    down_bias = vec_all[:, 3]
    tokens = hidden_in[0]
    q_seg = segment_ids[0]
    cotangent = out_grad[0]
    x_full = tokens.astype(jnp.float32)
    normed = layer_norm(x_full, norm_gain, norm_shift)
    norm_bf = normed.astype(jnp.bfloat16)
    mixed, grad_norm, owned, qkvb_grad, upb_grad = sliced_pass(
        norm_bf, q_seg, cotangent, own_mats, qkv_bb, up_bb
    )
    qkv_own, dense_own, up_own, down_own = owned
    output = (x_full + (mixed + dense_bias + down_bias)).astype(jnp.bfloat16)
    grad_x, grad_gain, grad_shift = jax.vjp(layer_norm, x_full, norm_gain, norm_shift)[1](grad_norm)
    out_bias_grad = jnp.sum(cotangent.astype(jnp.float32), axis=0)
    grad_vec = jnp.stack([grad_gain, grad_shift, out_bias_grad, out_bias_grad], axis=1)
    input_grad = cotangent.astype(jnp.float32) + grad_x
    qkvb_own, upb_own, vec_own = sum_vectors(qkvb_grad, upb_grad, grad_vec)
    new_states = (
        adam_update(qkv_weight_state, qkv_own),
        adam_update(qkv_bias_state, qkvb_own),
        adam_update(dense_weight_state, dense_own),
        adam_update(up_weight_state, up_own),
        adam_update(up_bias_state, upb_own),
        adam_update(down_weight_state, down_own),
        adam_update(vector_state, vec_own),
    )
    return (
        output[None],
        input_grad[None],
        qkv_own,
        qkvb_own,
        dense_own,
        up_own,
        upb_own,
        down_own,
        vec_own,
        owner_entries(new_states, 0),
        owner_entries(new_states, 1),
        owner_entries(new_states, 2),
    )


def whole_heads(mesh):
    owners = mesh.shape["rep"] * mesh.shape["shard"]
    return D % owners == 0 and D // owners == HD and mesh.shape["rep"] % 2 == 0


def rotation_tables(seq_rows):
    half_rot = ROT // 2
    lane = jnp.arange(2 * HD, dtype=jnp.int32) % HD
    frequency = jnp.exp((lane % half_rot).astype(jnp.float32) * (-2.0 * math.log(10000.0) / ROT))
    angles = jnp.arange(seq_rows, dtype=jnp.int32).astype(jnp.float32)[:, None] * frequency[None, :]
    sine = jnp.sin(angles)
    cosine = jnp.where(lane[None, :] < ROT, jnp.cos(angles), 1.0)
    low = jnp.where(lane[None, :] < half_rot, -sine, 0.0)
    high = jnp.where((lane[None, :] >= half_rot) & (lane[None, :] < ROT), sine, 0.0)
    return cosine, low, high


def attention_kernel(
    fu_ref, do_ref, du_ref, seg_col_ref, seg_row_ref, cos_ref, low_ref, high_ref, o_ref, dcat_ref, sums_ref
):
    rows, width = do_ref.shape
    scale = 1.0 / math.sqrt(HD)
    row_id = lax.broadcasted_iota(jnp.int32, (rows, rows), 0)
    col_id = lax.broadcasted_iota(jnp.int32, (rows, rows), 1)
    allowed = (col_id <= row_id) & (seg_col_ref[...] == seg_row_ref[0])
    cosine, low, high = cos_ref[...], low_ref[...], high_ref[...]
    half = ROT // 2
    lane = lax.broadcasted_iota(jnp.int32, (rows, 2 * HD), 1)

    def rotate(u):
        return (
            u * cosine
            + pltpu.roll(u, 2 * HD - half, 1) * low
            + pltpu.roll(u, half, 1) * high
        )

    def rotate_back(u):
        return (
            u * cosine
            - pltpu.roll(u, 2 * HD - half, 1) * low
            - pltpu.roll(u, half, 1) * high
        )

    def dot(a, b, a_dim, b_dim):
        return lax.dot_general(a, b, (((a_dim,), (b_dim,)), ((), ())), preferred_element_type=jnp.float32)

    zero = jnp.zeros((), jnp.bfloat16)
    for pair in range(width // (2 * HD)):
        lanes = pl.ds(pair * 2 * HD, 2 * HD)
        k_lanes = pl.ds(width + pair * 2 * HD, 2 * HD)
        v_lanes = pl.ds(2 * width + pair * 2 * HD, 2 * HD)
        q = rotate(fu_ref[:, lanes]).astype(jnp.bfloat16)
        k = rotate(fu_ref[:, k_lanes]).astype(jnp.bfloat16)
        v = fu_ref[:, v_lanes].astype(jnp.bfloat16)
        do = do_ref[:, lanes]
        o = dq = dk = dv = None
        for head in range(2):
            mine = (lane < HD) if head == 0 else (lane >= HD)
            qh = jnp.where(mine, q, zero)
            kh = jnp.where(mine, k, zero)
            vh = jnp.where(mine, v, zero)
            doh = jnp.where(mine, do, zero)
            scores = jnp.where(allowed, dot(qh, k, 1, 1) * scale, big_negative)
            row_max = jnp.max(scores, axis=1, keepdims=True)
            probs = jnp.where(allowed, jnp.exp(scores - row_max), 0.0)
            inverse = 1.0 / jnp.sum(probs, axis=1, keepdims=True)
            oh = dot(probs.astype(jnp.bfloat16), vh, 1, 0) * inverse
            delta = jnp.sum(
                doh.astype(jnp.float32) * oh.astype(jnp.bfloat16).astype(jnp.float32), axis=1, keepdims=True
            )
            probs = probs * inverse
            dvh = dot(probs.astype(jnp.bfloat16), doh, 0, 0)
            ds = (probs * (dot(doh, v, 1, 1) - delta) * scale).astype(jnp.bfloat16)
            dqh = dot(ds, kh, 1, 0)
            dkh = dot(ds, qh, 0, 0)
            if head == 0:
                o, dq, dk, dv = oh, dqh, dkh, dvh
            else:
                o, dq, dk, dv = o + oh, dq + dqh, dk + dkh, dv + dvh
        o_ref[:, lanes] = o.astype(jnp.bfloat16)
        dq = rotate_back(dq)
        dk = rotate_back(dk)
        for part, place in ((dq, lanes), (dk, k_lanes), (dv, v_lanes)):
            dcat_ref[:, place] = part.astype(jnp.bfloat16)
            sums_ref[0, :, place] = jnp.sum(part, axis=0, keepdims=True)
    dcat_ref[:, pl.ds(3 * width, du_ref.shape[1])] = du_ref[...]


def attention(fu, do, du, segments):
    count, rows = segments.shape
    width = do.shape[1]
    units = du.shape[1]
    tables = rotation_tables(rows)
    table_spec = pl.BlockSpec((rows, 2 * HD), lambda s: (0, 0))
    o, dcat, sums = pl.pallas_call(
        attention_kernel,
        grid=(count,),
        in_specs=[
            pl.BlockSpec((rows, 3 * width), lambda s: (s, 0)),
            pl.BlockSpec((rows, width), lambda s: (s, 0)),
            pl.BlockSpec((rows, units), lambda s: (s, 0)),
            pl.BlockSpec((rows, 1), lambda s: (s, 0)),
            pl.BlockSpec((1, 1, rows), lambda s: (s, 0, 0)),
            table_spec,
            table_spec,
            table_spec,
        ],
        out_specs=[
            pl.BlockSpec((rows, width), lambda s: (s, 0)),
            pl.BlockSpec((rows, 3 * width + units), lambda s: (s, 0)),
            pl.BlockSpec((1, 1, 3 * width), lambda s: (s, 0, 0)),
        ],
        out_shape=[
            jax.ShapeDtypeStruct((count * rows, width), jnp.bfloat16),
            jax.ShapeDtypeStruct((count * rows, 3 * width + units), jnp.bfloat16),
            jax.ShapeDtypeStruct((count, 1, 3 * width), jnp.float32),
        ],
        compiler_params=pltpu.CompilerParams(vmem_limit_bytes=56 << 20),
        cost_estimate=pl.CostEstimate(
            flops=count * (width // HD) * 10 * rows * rows * HD,
            bytes_accessed=count * rows * (width * 20 + units * 4),
            transcendentals=count * (width // HD) * rows * rows,
        ),
    )(fu, do, du, segments.reshape(count * rows, 1), segments.reshape(count, 1, rows), *tables)
    return o, dcat, jnp.sum(sums, axis=(0, 1))


def adam_values(weight, moment_one, moment_two, grad):
    first = beta_one * moment_one + (1.0 - beta_one) * grad
    second = beta_two * moment_two + (1.0 - beta_two) * grad * grad
    corrected = first * (1.0 / (1.0 - beta_one**STEP))
    divisor = jnp.sqrt(second * (1.0 / (1.0 - beta_two**STEP))) + adam_eps
    return weight - learn_rate * (corrected / divisor + weight_decay * weight), first, second


def owner_update_kernel(plan, small_plan, groups, steps, whole_rows, *refs):
    planes, cores, shards = groups
    qkv_state, dense_state, up_state, down_state, cat_ref, dense_grad, down_grad, small_ref = refs[:8]
    flat = refs[8:11]
    qkv_out, dense_out, up_out, down_out, cat_buf = refs[11:16]
    outs = refs[16:19]
    step_sem, rest_sem = refs[19:]
    step = pl.program_id(0)
    lane = lax.broadcasted_iota(jnp.int32, (8, 128), 1)
    sub = lax.broadcasted_iota(jnp.int32, (8, 128), 0)
    lane_row = lax.broadcasted_iota(jnp.int32, (1, 128), 1)
    wide = 1024

    @pl.when(step == 0)
    def small():
        for source, row, low, high in small_plan:
            for entry in range(3):
                old = outs[entry][pl.ds(row, 1), :]
                new = small_ref[entry, pl.ds(source, 1), :]
                outs[entry][pl.ds(row, 1), :] = jnp.where((lane_row >= low) & (lane_row < high), new, old)

    def widen(piece, carry):
        cat_buf[piece] = cat_ref[piece].astype(jnp.float32)
        return carry

    lax.fori_loop(0, cat_ref.shape[0], widen, 0)

    def place_rows(state, grad_of, rows, tiles, start, shifted, keep=None):
        chunk = min(wide, tiles * 128)

        def one_group(group, carry):
            place = pl.ds(pl.multiple_of(group * 8, 8), 8)
            base = start + (step * (rows // 8) + group) * (8 * tiles)

            def values(column, size):
                lanes = pl.ds(column, size)
                grad = grad_of(place, column, size)
                if keep is not None and size > 128:
                    keep[place, lanes] = grad
                return adam_values(
                    state[0, place, lanes], state[1, place, lanes], state[2, place, lanes], grad
                )

            if shifted:
                last = tuple(pltpu.roll(value, 64, 1) for value in values((tiles - 1) * 128, 128))
                before = tuple(
                    jnp.where(sub == 0, out[pl.ds(base, 1), :], pltpu.roll(value, 1, 0))
                    for out, value in zip(outs, last)
                )
            for column in range(0, tiles * 128, chunk):
                done = values(column, chunk)
                for entry, out in enumerate(outs):
                    for tile in range(chunk // 128):
                        value = done[entry][:, tile * 128 : (tile + 1) * 128]
                        if shifted:
                            value = pltpu.roll(value, 64, 1)
                            old = before[entry] if tile == 0 else now
                            now = value
                            value = jnp.where(lane < 64, old, value)
                        out[pl.ds(base + column // 128 + tile, 8, stride=tiles), :] = value
                    if shifted:
                        before = before[:entry] + (now,) + before[entry + 1 :]
            if shifted:
                for out, value in zip(outs, before):
                    row = pl.ds(base + 8 * tiles, 1)
                    out[row, :] = jnp.where(lane_row < 64, value[7:8], out[row, :])
            return carry

        lax.fori_loop(0, rows // 8, one_group, 0)

    def qkv_grad(place, column, size):
        tiles = []
        for start in range(column, column + size, 128):
            part, head = divmod(start // HD, planes * cores * shards)
            halves = []
            for side in range(2):
                plane, member = divmod(head + side, cores * shards)
                spot = (part * planes + plane) * HD
                half = cat_buf[member, place, pl.ds(spot // 128 * 128, 128)]
                halves.append(half if spot % 128 == side * HD else pltpu.roll(half, HD, 1))
            tiles.append(jnp.where(lane < HD, halves[0], halves[1]))
        return tiles[0] if len(tiles) == 1 else jnp.concatenate(tiles, axis=1)

    units = up_state.shape[2] // (planes * cores * shards)

    def up_grad(place, column, size):
        parts = []
        for start in range(column, column + size, min(units, size)):
            plane, member = divmod(start // units, cores * shards)
            spot = 3 * planes * HD + plane * units + start % units
            parts.append(cat_buf[member, place, pl.ds(spot, min(units, size))])
        return parts[0] if len(parts) == 1 else jnp.concatenate(parts, axis=1)

    def plain(grad):
        return lambda place, column, size: grad[place, pl.ds(column, size)]

    place_rows(qkv_state, qkv_grad, *plan[0], keep=qkv_out)
    place_rows(dense_state, plain(dense_grad), *plan[1], keep=dense_out)
    place_rows(up_state, up_grad, *plan[2], keep=up_out)
    place_rows(down_state, plain(down_grad), *plan[3], keep=down_out)

    def flush(entry, row, count, sem):
        place = pl.ds(pl.multiple_of(row * 128, 128), count * 128)
        source = outs[entry].reshape(1, 1, outs[entry].shape[0] * 128)
        return pltpu.make_async_copy(source.at[:, :, place], flat[entry].at[:, :, place], sem)

    def step_copies(at):
        copies = []
        for index, (rows, tiles, start, shifted) in enumerate(plan):
            count = rows * tiles
            skip = 1 if shifted and at == 0 else 0
            for entry in range(3):
                copies.append(
                    flush(entry, start + at * count + skip, count - skip, step_sem.at[entry, index, at])
                )
        return copies

    for at in range(steps):

        @pl.when(step == at)
        def begin(at=at):
            for copy in step_copies(at):
                copy.start()

    @pl.when(step == steps - 1)
    def end():
        covered = set()
        for rows, tiles, start, shifted in plan:
            covered |= set(range(start + (1 if shifted else 0), start + steps * rows * tiles))
        left = [row for row in range(whole_rows) if row not in covered]
        rest = [
            flush(entry, row, 1, rest_sem.at[entry, index]) for index, row in enumerate(left) for entry in range(3)
        ]
        for copy in rest:
            copy.start()
        for at in range(steps):
            for copy in step_copies(at):
                copy.wait()
        for copy in rest:
            copy.wait()


def owner_update(states, cat_sum, grads, small_states, small_grads, groups):
    steps = 4
    sizes = [state.shape[1] * state.shape[2] for state in states]
    small_sizes = [grad.size for grad in small_grads]
    order = [("m", 0), ("s", 0), ("m", 1), ("m", 2), ("s", 1), ("m", 3), ("s", 2)]
    offset = 0
    plan = [None] * 4
    small_plan = []
    pads = []
    small_row = 0
    for kind, index in order:
        if kind == "m":
            state = states[index]
            rows = state.shape[1] // steps
            plan[index] = (rows, state.shape[2] // 128, offset // 128, offset % 128 == 64)
            offset += sizes[index]
        else:
            size = small_sizes[index]
            front = offset % 128
            total = -(-(front + size) // 128)
            pads.append((front, total * 128 - front - size))
            for extra in range(total):
                low = front if extra == 0 else 0
                high = min(128, front + size - extra * 128)
                small_plan.append((small_row + extra, offset // 128 + extra, low, high))
            small_row += total
            offset += size
    entries = offset
    out_rows = -(-entries // 1024) * 8
    small_new = [
        adam_values(state[0].reshape(-1), state[1].reshape(-1), state[2].reshape(-1), grad.reshape(-1))
        for state, grad in zip(small_states, small_grads)
    ]
    small = jnp.stack(
        [
            jnp.concatenate([jnp.pad(new[entry], pad) for new, pad in zip(small_new, pads)])
            for entry in range(3)
        ]
    ).reshape(3, small_row, 128)
    in_specs = [
        pl.BlockSpec((3, rows, tiles * 128), lambda s: (0, s, 0)) for rows, tiles, start, shifted in plan
    ]
    qkv_rows = plan[0][0]
    in_specs.append(pl.BlockSpec((cat_sum.shape[0], qkv_rows, cat_sum.shape[2]), lambda s: (0, s, 0)))
    in_specs.append(pl.BlockSpec((plan[1][0], plan[1][1] * 128), lambda s: (s, 0)))
    in_specs.append(pl.BlockSpec((plan[3][0], plan[3][1] * 128), lambda s: (s, 0)))
    in_specs.append(pl.BlockSpec((3, small_row, 128), lambda s: (0, 0, 0)))
    whole_rows = entries // 128
    *outs, qkv_grad, dense_grad, up_grad, down_grad = pl.pallas_call(
        partial(owner_update_kernel, plan, small_plan, groups, steps, whole_rows),
        grid=(steps,),
        in_specs=in_specs,
        out_specs=[pl.BlockSpec(memory_space=pl.ANY)] * 3
        + [
            pl.BlockSpec((rows, tiles * 128), lambda s: (s, 0)) for rows, tiles, start, shifted in plan
        ],
        out_shape=[jax.ShapeDtypeStruct((1, 1, entries), jnp.float32)] * 3
        + [
            jax.ShapeDtypeStruct(state.shape[1:], jnp.float32) for state in states
        ],
        scratch_shapes=[pltpu.VMEM((cat_sum.shape[0], qkv_rows, cat_sum.shape[2]), jnp.float32)]
        + [pltpu.VMEM((out_rows, 128), jnp.float32)] * 3
        + [pltpu.SemaphoreType.DMA((3, 4, steps)), pltpu.SemaphoreType.DMA((3, 16))],
        compiler_params=pltpu.CompilerParams(vmem_limit_bytes=56 << 20),
        cost_estimate=pl.CostEstimate(
            flops=20 * entries, bytes_accessed=28 * entries, transcendentals=2 * entries
        ),
    )(*states, cat_sum, *grads, small)
    tail = entries - whole_rows * 128
    if tail:
        outs = [
            lax.dynamic_update_slice(out, new[entries_of][-tail:].reshape(1, 1, tail), (0, 0, whole_rows * 128))
            for out, (new, entries_of) in zip(outs, ((small_new[-1], entry) for entry in range(3)))
        ]
    return tuple(outs), qkv_grad, dense_grad, up_grad, down_grad


class Wires:
    def __init__(self, send_sems):
        self.send_sems, self.count, self.pending = send_sems, 0, []
        self.plane, self.core, self.shard = (
            lax.axis_index("plane"),
            lax.axis_index("core"),
            lax.axis_index("shard"),
        )
        self.shards = lax.axis_size("shard")
        self.group = lax.axis_size("core") * self.shards
        self.mine = self.core * self.shards + self.shard
        self.first = (self.plane ^ 1, self.core, self.shard)
        self.second = (self.plane ^ 2, self.core, self.shard)

    def member(self, index):
        return (self.plane, index // self.shards, index % self.shards)

    def barrier(self):
        barrier = pltpu.get_barrier_semaphore()
        partners = [self.member(self.mine ^ mask) for mask in range(1, self.group)]
        partners += [self.first, self.second]
        for partner in partners:
            pl.semaphore_signal(barrier, inc=1, device_id=partner, device_id_type=pl.DeviceIdType.MESH)
        pl.semaphore_wait(barrier, len(partners))

    def send(self, source, target, recv_sem, device, when=None):
        copy = pltpu.make_async_remote_copy(
            src_ref=source,
            dst_ref=target,
            send_sem=self.send_sems.at[self.count],
            recv_sem=recv_sem,
            device_id=device,
            device_id_type=pl.DeviceIdType.MESH,
        )
        self.count += 1
        self.pending.append((copy, when))
        if when is None:
            copy.start()
        else:
            pl.when(when)(copy.start)

    def arrived(self, place, recv_sem, when=None):
        copy = pltpu.make_async_remote_copy(
            src_ref=place,
            dst_ref=place,
            send_sem=self.send_sems.at[0],
            recv_sem=recv_sem,
            device_id=self.first,
            device_id_type=pl.DeviceIdType.MESH,
        )
        if when is None:
            copy.wait_recv()
        else:
            pl.when(when)(copy.wait_recv)

    def drain(self):
        for copy, when in self.pending:
            if when is None:
                copy.wait_send()
            else:
                pl.when(when)(copy.wait_send)


def pack_pieces(qkv, up, pieces, planes, cores, shards):
    rows = qkv.shape[0]
    lane = lax.broadcasted_iota(jnp.int32, (rows, 128), 1)
    units = up.shape[1] // (planes * cores * shards)
    for core in range(cores):
        for shard in range(shards):
            piece = core * shards + shard
            for tile in range(3 * planes // 2):
                halves = []
                for side in range(2):
                    part, plane = divmod(2 * tile + side, planes)
                    head = (plane * cores + core) * shards + shard
                    start = part * planes * cores * shards * HD + head * HD
                    half = qkv[:, pl.ds(start // 128 * 128, 128)]
                    halves.append(half if start % 128 == side * HD else pltpu.roll(half, HD, 1))
                pieces[piece, :, pl.ds(tile * 128, 128)] = jnp.where(lane < HD, halves[0], halves[1]).astype(
                    jnp.bfloat16
                )
            for plane in range(planes):
                block = (plane * cores + core) * shards + shard
                pieces[piece, :, pl.ds(3 * planes * HD + plane * units, units)] = up[
                    :, pl.ds(block * units, units)
                ].astype(jnp.bfloat16)


def gather_kernel(
    vector_start, qkv_state, up_state, dense_state, down_state, tokens, cotangent, vectors,
    cat_out, dense_out, down_out, x_out, dy_out, vec_out, normed_out, mean_out, inverse_out,
    qkv_buf, up_buf, dense_buf, down_buf, pieces, dense, down, x_stage, vec_stage, gain_buf,
    load_sem, send_sems, group_sem, first_sem, second_sem, far_sem, up_sem, low_sem, core_sem, local_sem,
):
    net = Wires(send_sems)
    plane, core, shard, shards, group, mine = net.plane, net.core, net.shard, net.shards, net.group, net.mine
    order = sorted(range(group), key=lambda mask: (mask % shards, mask // shards))
    partner = (plane, 1 - core, shard)

    def cat_unit(mask):
        return lambda p: cat_out.at[p, mine ^ mask]

    def vec_unit(mask):
        return lambda p: vec_out.at[p, mine ^ mask]

    units = []
    down_rows = down.shape[0] // 4
    for part in range(4):
        rows = pl.ds(part * down_rows, down_rows)
        units.append((down.at[rows], lambda p, rows=rows: down_out.at[p, rows]))
    dense_rows = dense.shape[0] // 2
    for part in range(2):
        rows = pl.ds(part * dense_rows, dense_rows)
        units.append((dense.at[rows], lambda p, rows=rows: dense_out.at[p, rows]))
    own_units = list(range(len(units)))
    cat_units, vec_units = {}, {}
    for mask in order:
        cat_units[mask] = len(units)
        units.append((pieces.at[mine] if mask == 0 else None, cat_unit(mask)))
        vec_units[mask] = len(units)
        units.append((vectors if mask == 0 else None, vec_unit(mask)))

    def spread(index):
        source, place = units[index]
        source = place(plane) if source is None else source
        net.send(source, place(plane), first_sem.at[index], net.first)
        net.send(source, place(plane), second_sem.at[index], net.second)

    def hand_on(index):
        place = units[index][1]
        if relay_first[index]:
            net.arrived(place(plane ^ 1), first_sem.at[index])
            net.send(place(plane ^ 1), place(plane ^ 1), far_sem.at[index], net.second)
        else:
            net.arrived(place(plane ^ 2), second_sem.at[index])
            net.send(place(plane ^ 2), place(plane ^ 2), far_sem.at[index], net.first)

    relay_first = {}
    for position, index in enumerate(own_units):
        relay_first[index] = position % 2 == 0
    for position, mask in enumerate(order):
        relay_first[cat_units[mask]] = position % 2 == 0
        relay_first[vec_units[mask]] = position % 2 == 1

    loads = [
        pltpu.make_async_copy(state.at[0], buffer, load_sem.at[index])
        for index, (state, buffer) in enumerate(
            ((qkv_state, qkv_buf), (up_state, up_buf), (down_state, down_buf), (dense_state, dense_buf))
        )
    ]
    for index in (2, 3, 0, 1):
        loads[index].start()
    net.barrier()
    loads[2].wait()
    down[...] = down_buf[...].astype(jnp.bfloat16)
    loads[3].wait()
    dense[...] = dense_buf[...].astype(jnp.bfloat16)
    for index in own_units:
        spread(index)
    loads[0].wait()
    loads[1].wait()
    pack_pieces(qkv_buf, up_buf, pieces, cat_out.shape[0], group // shards, shards)

    locals_ = [
        (pieces.at[mine], cat_out.at[plane, mine]),
        (dense, dense_out.at[plane]),
        (down, down_out.at[plane]),
        (tokens, x_out.at[mine]),
        (cotangent, dy_out.at[mine]),
        (vectors, vec_out.at[plane, mine]),
    ]
    copies = [
        pltpu.make_async_copy(source, target, local_sem.at[index])
        for index, (source, target) in enumerate(locals_)
    ]
    for mask in order[1:]:
        target = net.member(mine ^ mask)
        net.send(vectors, vec_out.at[plane, mine], group_sem.at[1, mask], target)
        net.send(pieces.at[mine ^ mask], cat_out.at[plane, mine], group_sem.at[0, mask], target)
    spread(cat_units[0])
    spread(vec_units[0])
    streams = ((tokens, x_out), (cotangent, dy_out))

    def block(stream, origin):
        return streams[stream][1].at[core * shards + origin]

    def to_core(stream, source, origin, slot, when=None):
        net.send(source, block(stream, origin), core_sem.at[stream, slot], partner, when)

    def hop(stream, distance):
        own = distance == 1
        for upward, sem in ((True, up_sem), (False, low_sem)):
            origin = shard - (distance - 1) if upward else shard + (distance - 1)
            there = shard + 1 if upward else shard - 1
            held = (origin >= 0) if upward else (origin < shards)
            inside = (there < shards) if upward else (there >= 0)
            near = jnp.clip(origin, 0, shards - 1)
            source = streams[stream][0] if own else block(stream, near)
            net.send(
                source,
                block(stream, near),
                sem.at[stream, distance],
                (plane, core, jnp.clip(there, 0, shards - 1)),
                inside & held,
            )

    def hop_arrived(stream, distance):
        for upward, sem in ((True, up_sem), (False, low_sem)):
            origin = shard - distance if upward else shard + distance
            held = (origin >= 0) if upward else (origin < shards)
            near = jnp.clip(origin, 0, shards - 1)
            net.arrived(block(stream, near), sem.at[stream, distance], held)
            slot = distance if upward else shards + distance
            to_core(stream, block(stream, near), near, slot, held)

    for stream in range(2):
        hop(stream, 1)
    for stream in range(2):
        to_core(stream, streams[stream][0], shard, 0)
    for copy in copies:
        copy.start()

    for position, mask in enumerate(order[1:]):
        net.arrived(vec_out.at[plane, mine ^ mask], group_sem.at[1, mask])
        spread(vec_units[mask])
        net.arrived(cat_out.at[plane, mine ^ mask], group_sem.at[0, mask])
        spread(cat_units[mask])
        if position == 2:
            for index in own_units:
                hand_on(index)
    def unit_arrived(index):
        place = units[index][1]
        if relay_first[index]:
            net.arrived(place(plane ^ 2), second_sem.at[index])
        else:
            net.arrived(place(plane ^ 1), first_sem.at[index])
        net.arrived(place(plane ^ 3), far_sem.at[index])

    def norm_vectors():
        for mask in order:
            unit_arrived(vec_units[mask])
        copies[5].wait()
        fetch = pltpu.make_async_copy(vec_out, vec_stage, load_sem.at[4])
        fetch.start()
        fetch.wait()
        lane = lax.broadcasted_iota(jnp.int32, (1, 128), 1)
        for vector in range(2):
            row, low = divmod(vector_start + vector * HD, 128)
            for pair in range(vec_stage.shape[0] * group // 2):
                halves = []
                for side in range(2):
                    owner_plane, owner = divmod(2 * pair + side, group)
                    half = vec_stage[owner_plane, owner, pl.ds(row, 1), :]
                    halves.append(half if low == side * HD else pltpu.roll(half, HD, 1))
                value = jnp.where(lane < HD, halves[0], halves[1])
                gain_buf[pl.ds(vector, 1), pl.ds(pair * 128, 128)] = value.astype(jnp.bfloat16).astype(
                    jnp.float32
                )

    def normalize(source, index):
        step = 16

        def body(turn, carry):
            rows = pl.ds(pl.multiple_of(turn * step, step), step)
            x = source[rows, :].astype(jnp.float32)
            mean = jnp.mean(x, axis=1, keepdims=True)
            center = x - mean
            inverse = lax.rsqrt(jnp.mean(center * center, axis=1, keepdims=True) + norm_eps)
            normed = center * inverse * gain_buf[0:1, :] + gain_buf[1:2, :]
            normed_out[index, rows, :] = normed.astype(jnp.bfloat16)
            mean_out[index, rows, :] = mean
            inverse_out[index, rows, :] = inverse
            return carry

        lax.fori_loop(0, source.shape[0] // step, body, 0)

    def normalize_far(which, place, when):
        index = which * shards + place

        @pl.when(when)
        def there():
            fetch = pltpu.make_async_copy(x_out.at[index], x_stage, load_sem.at[4])
            fetch.start()
            fetch.wait()
            normalize(x_stage, index)

    def normalize_at(distance):
        for upward in (True, False):
            origin = shard - distance if upward else shard + distance
            held = (origin >= 0) if upward else (origin < shards)
            near = jnp.clip(origin, 0, shards - 1)
            normalize_far(core, near, held)

    def normalize_core(distance):
        for upward in (True, False):
            if distance == 0 and not upward:
                continue
            origin = shard - distance if upward else shard + distance
            held = (origin >= 0) & (origin < shards)
            near = jnp.clip(origin, 0, shards - 1)
            slot = distance if upward else shards + distance
            net.arrived(x_out.at[(1 - core) * shards + near], core_sem.at[0, slot], held)
            normalize_far(1 - core, near, held)

    def advance(stream, distance):
        hop_arrived(stream, distance)
        if distance + 1 < shards:
            hop(stream, distance + 1)

    advance(0, 1)
    advance(1, 1)
    for mask in order:
        hand_on(vec_units[mask])
    for mask in order:
        hand_on(cat_units[mask])
    norm_vectors()
    normalize(tokens, mine)
    normalize_core(0)
    normalize_at(1)
    for distance in range(2, shards):
        advance(0, distance)
        if distance < shards - 1:
            advance(1, distance)
        normalize_core(distance - 1)
        normalize_at(distance)
    normalize_core(shards - 1)
    advance(1, shards - 1)

    for index in own_units:
        unit_arrived(index)
    for mask in order:
        unit_arrived(cat_units[mask])
    for slot in range(2 * shards):
        if slot == shards:
            continue
        origin = shard - slot if slot < shards else shard + (slot - shards)
        held = None if slot == 0 else ((origin >= 0) & (origin < shards))
        near = jnp.clip(origin, 0, shards - 1)
        net.arrived(dy_out.at[(1 - core) * shards + near], core_sem.at[1, slot], held)
    for copy in copies[:5]:
        copy.wait()
    net.drain()


def gather_wires(qkv, up, dense, down, tokens, cotangent, vectors, vector_start):
    group, shards = lax.axis_size("core") * lax.axis_size("shard"), lax.axis_size("shard")
    planes = lax.axis_size("plane")
    width = (qkv.shape[2] + up.shape[2]) // group
    units = 6 + 2 * group
    vmem = pl.BlockSpec(memory_space=pltpu.VMEM)
    hbm = pl.BlockSpec(memory_space=pl.ANY)

    def out(*shape, dtype=jnp.bfloat16):
        return jax.ShapeDtypeStruct(shape, dtype)

    dma = pltpu.SemaphoreType.DMA
    return pl.pallas_call(
        partial(gather_kernel, vector_start),
        in_specs=[hbm] * 4 + [vmem] * 3,
        out_specs=[hbm] * 6 + [vmem] * 3,
        out_shape=[
            out(planes, group, qkv.shape[1], width),
            out(planes, *dense.shape[1:]),
            out(planes, *down.shape[1:]),
            out(group, *tokens.shape),
            out(group, *cotangent.shape),
            out(planes, group, *vectors.shape, dtype=vectors.dtype),
            out(group, *tokens.shape),
            out(group, tokens.shape[0], 1, dtype=jnp.float32),
            out(group, tokens.shape[0], 1, dtype=jnp.float32),
        ],
        scratch_shapes=[
            pltpu.VMEM(qkv.shape[1:], qkv.dtype),
            pltpu.VMEM(up.shape[1:], up.dtype),
            pltpu.VMEM(dense.shape[1:], dense.dtype),
            pltpu.VMEM(down.shape[1:], down.dtype),
            pltpu.VMEM((group, qkv.shape[1], width), jnp.bfloat16),
            pltpu.VMEM(dense.shape[1:], jnp.bfloat16),
            pltpu.VMEM(down.shape[1:], jnp.bfloat16),
            pltpu.VMEM(tokens.shape, tokens.dtype),
            pltpu.VMEM((planes, group) + vectors.shape, vectors.dtype),
            pltpu.VMEM((8, tokens.shape[1]), jnp.float32),
            dma((5,)),
            dma((2 * (group - 1) + 3 * units + 2 * 2 * (shards - 1) + 2 * (2 * shards - 1),)),
            dma((2, group)),
            dma((units,)),
            dma((units,)),
            dma((units,)),
            dma((2, shards)),
            dma((2, shards)),
            dma((2, 2 * shards)),
            dma((6,)),
        ],
        compiler_params=pltpu.CompilerParams(
            collective_id=0, has_side_effects=True, vmem_limit_bytes=67043328
        ),
    )(qkv, up, dense, down, tokens, cotangent, vectors)


def add_rows(target, *sources):
    step = 16
    rows = target.shape[0]

    def body(index, carry):
        place = pl.ds(pl.multiple_of(index * step, step), step)
        total = sources[0][place, :].astype(jnp.float32)
        for source in sources[1:]:
            total = total + source[place, :].astype(jnp.float32)
        target[place, :] = total.astype(target.dtype)
        return carry

    lax.fori_loop(0, rows // step, body, 0)


def chunked(first, last, copies_of, body):
    for copy in copies_of(first, first % 2):
        copy.start()

    def step(n, carry):
        slot = lax.rem(n, 2)

        @pl.when(n + 1 < last)
        def ahead():
            for copy in copies_of(n + 1, 1 - slot):
                copy.start()

        for copy in copies_of(n, slot):
            copy.wait()
        body(n, slot)
        return carry

    lax.fori_loop(first, last, step, 0)


def reduce_kernel(
    norm, dcat, x_all, mean, inverse, attn, hidden, dy, cat_w, dense_w, down_w, sums,
    cat_out, dense_out, down_out, mixed_out, norm_out, sums_out,
    cat_part, down_part, dense_part, cat_in, down_in, dense_in,
    tokens, token_in, token_line, token_last, sum_buf,
    wide, hidden_turned, attn_turned, norm_chunk, norm_turned, cat_chunk, x_chunk, down_chunk, dense_chunk, dy_chunk,
    send_sems, near_sem, pass_sem, group_sem, core_sem, line_sem, sum_sem, local_sem, chunk_sem,
):
    PASS, KEEP, LAST = range(3)
    net = Wires(send_sems)
    plane, core, shard, shards, group, mine = net.plane, net.core, net.shard, net.shards, net.group, net.mine
    planes = cat_part.shape[0]
    partner = (plane, 1 - core, shard)
    order = sorted(range(group), key=lambda mask: (mask % shards, mask // shards), reverse=True)
    rows, width = dcat.shape
    model = norm.shape[1]
    block = cat_part.shape[2]
    token_rows = tokens.shape[2]
    units_here = hidden.shape[1]
    heads_here = attn.shape[1]
    lane = 256

    def dot(a, b, a_dim=1, b_dim=0):
        return lax.dot_general(a, b, (((a_dim,), (b_dim,)), ((), ())), preferred_element_type=jnp.float32)

    def columns(n):
        return pl.ds(pl.multiple_of(n * lane, lane), lane)

    units = [(cat_part, cat_in, mask) for mask in order]
    units += [(down_part, down_in, part) for part in range(down_part.shape[1])]
    units += [(dense_part, dense_in, part) for part in range(dense_part.shape[1])]
    down_rows, dense_rows = down_part.shape[2], dense_part.shape[2]

    def ways(index):
        return (net.first, net.second, 1, 2) if index % 2 == 0 else (net.second, net.first, 2, 1)

    def send_pass(index):
        parts, came, slot = units[index]
        net.send(parts.at[3, slot], came.at[PASS, slot], pass_sem.at[0, index], ways(index)[0])

    def send_keep(index):
        parts, came, slot = units[index]
        near, far, near_mask, far_mask = ways(index)
        net.send(parts.at[near_mask, slot], came.at[KEEP, slot], near_sem.at[index], near)

    locals_ = {}

    def local(key, source, target):
        locals_[key] = pltpu.make_async_copy(source, target, local_sem.at[len(locals_)])
        locals_[key].start()

    local("hidden", hidden, wide.at[:, pl.ds(0, units_here)])
    local("attn", attn, wide.at[:, pl.ds(units_here, heads_here)])
    net.barrier()

    places = [place for rank in range(shards // 2) for place in (shards - 1 - rank, rank)]

    def to_partner(stream):
        for place in places:
            net.send(
                tokens.at[stream, (1 - core) * shards + place],
                token_in.at[stream, place],
                core_sem.at[stream, place],
                partner,
            )

    def out_copies(n, slot):
        return [
            pltpu.make_async_copy(down_w.at[:, columns(n)], down_chunk.at[slot], chunk_sem.at[3, slot]),
            pltpu.make_async_copy(dense_w.at[:, columns(n)], dense_chunk.at[slot], chunk_sem.at[4, slot]),
        ]

    def out_step(n, slot):
        total = dot(wide[:, pl.ds(0, units_here)], down_chunk[slot]) + dot(
            wide[:, pl.ds(units_here, heads_here)], dense_chunk[slot]
        )
        for member in range(group):
            tokens[0, member, :, columns(n)] = total[member * token_rows : (member + 1) * token_rows].astype(
                jnp.bfloat16
            )

    locals_["hidden"].wait()
    locals_["attn"].wait()
    chunked(0, model // lane, out_copies, out_step)
    to_partner(0)
    hidden_turned[...] = wide[:, pl.ds(0, units_here)].T
    attn_turned[...] = wide[:, pl.ds(units_here, heads_here)].T
    local("dcat", dcat, wide.at[:, pl.ds(0, width)])

    plane_rows = group * block

    def norm_copy(turn, distance):
        place = pl.ds(pl.multiple_of((plane ^ distance) * plane_rows, plane_rows), plane_rows)
        return pltpu.make_async_copy(
            norm.at[:, place], norm_chunk.at[turn % 2], chunk_sem.at[0, turn % 2]
        )

    cats, every = range(group), range(len(units))
    chain_steps = sorted(
        ((hop, rank) for hop in range(1, shards - 1) for rank in range(shards - 1 - hop)),
        key=lambda pair: (pair[0] + 2 * pair[1], pair[0]),
    )
    turns = (3, 1, 2, 0)
    norm_copy(0, turns[0]).start()
    locals_["dcat"].wait()

    def cat_turn(turn):
        distance = turns[turn]
        if turn + 1 < planes:
            norm_copy(turn + 1, turns[turn + 1]).start()
        norm_copy(turn, distance).wait()
        norm_turned[...] = norm_chunk[turn % 2].T

        def cat_step(n, carry):
            total = dot(norm_turned[...], wide[:, columns(n)]).astype(jnp.bfloat16)
            for member in range(group):
                cat_part[distance, mine ^ member, :, columns(n)] = total[member * block : (member + 1) * block]
            return carry

        lax.fori_loop(0, width // lane, cat_step, 0)
        for index in cats:
            if distance == 3:
                send_pass(index)
            elif distance == ways(index)[2]:
                send_keep(index)

    def own(stream, place):
        return tokens.at[stream, core * shards + place]

    def chain(stream, hop, rank):
        for upward in (True, False):
            target = shards - 1 - rank if upward else rank
            here = hop if upward else shards - 1 - hop
            sems = line_sem.at[0 if upward else 1]
            came = token_line.at[stream, target]
            total = own(stream, target)
            holds = shard == here
            if hop:
                net.arrived(came, sems.at[stream, target], holds)

            @pl.when(holds)
            def add(target=target, came=came, total=total):
                add_rows(total, total, token_in.at[stream, target], *([came] if hop else []))

            there = jnp.clip(shard + (1 if upward else -1), 0, shards - 1)
            ends = (not upward) and rank == shards - 2 - hop
            landing = token_last.at[stream] if ends else came
            net.send(total, landing, sems.at[stream, target], (plane, core, there), holds)

    def final(stream):
        for place in range(shards):
            holds = shard == place
            values = [own(stream, place), token_in.at[stream, place]]
            for landing, side, present in (
                (token_line.at[stream, place], line_sem.at[0], place > 0),
                (token_last.at[stream], line_sem.at[1], place < shards - 1),
            ):
                if present:
                    values.append(landing)
                    net.arrived(landing, side.at[stream, place], holds)

            @pl.when(holds)
            def add(values=values):
                add_rows((mixed_out, norm_out)[stream], *values)

    def first_sums(stream):
        for place in places:
            net.arrived(token_in.at[stream, place], core_sem.at[stream, place])
        for rank in range(shards - 1):
            chain(stream, 0, rank)

    def pass_on(index):
        parts, came, slot = units[index]
        near, far, near_mask, far_mask = ways(index)
        total = parts.at[far_mask, slot]
        net.arrived(came.at[PASS, slot], pass_sem.at[0, index])
        add_rows(total, total, came.at[PASS, slot])
        net.send(total, came.at[LAST, slot], pass_sem.at[1, index], far)

    cat_turn(0)
    first_sums(0)

    sum_buf[4] = sums[...]
    gain_row = width // 128

    def norm_copies(n, slot):
        return [
            pltpu.make_async_copy(cat_w.at[columns(n), :], cat_chunk.at[slot], chunk_sem.at[1, slot]),
            pltpu.make_async_copy(x_all.at[:, columns(n)], x_chunk.at[slot], chunk_sem.at[2, slot]),
        ]

    def norm_step(n, slot):
        total = dot(wide[:, pl.ds(0, width)], cat_chunk[slot], 1, 1)
        x_hat = (x_chunk[slot].astype(jnp.float32) - mean[...]) * inverse[...]
        gain = jnp.sum(total * x_hat, axis=0, keepdims=True)
        shift = jnp.sum(total, axis=0, keepdims=True)
        for half in range(lane // 128):
            row = gain_row + n * (lane // 128) + half
            sum_buf[4, pl.ds(row, 1), :] = gain[:, half * 128 : (half + 1) * 128]
            sum_buf[4, pl.ds(row + model // 128, 1), :] = shift[:, half * 128 : (half + 1) * 128]
        for member in range(group):
            tokens[1, member, :, columns(n)] = total[member * token_rows : (member + 1) * token_rows].astype(
                jnp.bfloat16
            )

    chunked(0, model // lane, norm_copies, norm_step)

    net.send(sum_buf.at[4], sum_buf.at[0], sum_sem.at[0], net.first)
    to_partner(1)
    cat_turn(1)
    chain(0, 1, 0)
    first_sums(1)
    cat_turn(2)
    cat_turn(3)
    net.arrived(sum_buf.at[0], sum_sem.at[0])
    sum_buf[1] = sum_buf[4] + sum_buf[0]
    net.send(sum_buf.at[1], sum_buf.at[2], sum_sem.at[1], net.second)
    for index in cats:
        pass_on(index)

    def grad_copies(n, slot):
        return [pltpu.make_async_copy(dy.at[:, columns(n)], dy_chunk.at[slot], chunk_sem.at[5, slot])]

    def grad_step(n, slot):
        for parts, left in ((down_part, hidden_turned[...]), (dense_part, attn_turned[...])):
            grad = dot(left, dy_chunk[slot]).astype(jnp.bfloat16)
            pieces, size = parts.shape[1], parts.shape[2]
            for q in range(planes):
                for piece in range(pieces):
                    start = (q * pieces + piece) * size
                    parts[plane ^ q, piece, :, columns(n)] = grad[start : start + size]

    chunked(0, model // lane, grad_copies, grad_step)
    for index in every[group:]:
        send_pass(index)
        send_keep(index)
    for hop, rank in chain_steps[1:]:
        chain(0, hop, rank)

    def finish(index):
        parts, came, slot = units[index]
        total = parts.at[0, slot]
        net.arrived(came.at[KEEP, slot], near_sem.at[index])
        net.arrived(came.at[LAST, slot], pass_sem.at[1, index])
        values = (total, came.at[KEEP, slot], came.at[LAST, slot])
        if index < group:
            add_rows(total, *values)
            if slot:
                net.send(total, cat_out.at[mine], group_sem.at[0, slot], net.member(mine ^ slot))
            else:
                local("own", total, cat_out.at[mine])
        elif parts is down_part:
            add_rows(down_out.at[pl.ds(slot * down_rows, down_rows)], *values)
        else:
            add_rows(dense_out.at[pl.ds(slot * dense_rows, dense_rows)], *values)

    net.arrived(sum_buf.at[2], sum_sem.at[1])
    sum_buf[3] = sum_buf[1] + sum_buf[2]
    for mask in range(1, group):
        net.send(sum_buf.at[3], sums_out.at[mine], group_sem.at[1, mask], net.member(mine ^ mask))
    local("sums", sum_buf.at[3], sums_out.at[mine])
    for index in cats[: group // 2]:
        finish(index)
    chain(1, *chain_steps[0])
    for index in cats[group // 2 : group - 2]:
        finish(index)
    for hop, rank in chain_steps[1:]:
        chain(1, hop, rank)
    for index in cats[group - 2 :]:
        finish(index)
    for index in every[group:]:
        pass_on(index)
    final(0)
    for index in every[group:]:
        finish(index)
    final(1)
    for mask in range(1, group):
        net.arrived(cat_out.at[mine ^ mask], group_sem.at[0, mask])
        net.arrived(sums_out.at[mine ^ mask], group_sem.at[1, mask])
    locals_["own"].wait()
    locals_["sums"].wait()
    net.drain()


def reduce_wires(norm, dcat, x_all, mean, inverse, attn, hidden, dy, cat_w, dense_w, down_w, sums):
    planes, shards = lax.axis_size("plane"), lax.axis_size("shard")
    group = lax.axis_size("core") * shards
    units = group + 6
    rows, width = dcat.shape
    model = norm.shape[1]
    block = model // (planes * group)
    unit_rows, head_rows = down_w.shape[0] // planes, dense_w.shape[0] // planes
    token_rows = rows // group
    vmem = pl.BlockSpec(memory_space=pltpu.VMEM)
    hbm = pl.BlockSpec(memory_space=pl.ANY)
    dma = pltpu.SemaphoreType.DMA
    lane = 256

    def scratch(*shape, dtype=jnp.bfloat16):
        return pltpu.VMEM(shape, dtype)

    return pl.pallas_call(
        reduce_kernel,
        in_specs=[hbm] * 3 + [vmem] * 2 + [hbm] * 6 + [vmem],
        out_specs=[hbm] + [vmem] * 4 + [hbm],
        out_shape=[
            jax.ShapeDtypeStruct((group, block, width), jnp.bfloat16),
            jax.ShapeDtypeStruct((head_rows, model), jnp.float32),
            jax.ShapeDtypeStruct((unit_rows, model), jnp.float32),
            jax.ShapeDtypeStruct((token_rows, model), jnp.float32),
            jax.ShapeDtypeStruct((token_rows, model), jnp.float32),
            jax.ShapeDtypeStruct((group,) + sums.shape, sums.dtype),
        ],
        scratch_shapes=[
            scratch(planes, group, block, width),
            scratch(planes, 4, unit_rows // 4, model),
            scratch(planes, 2, head_rows // 2, model),
            scratch(3, group, block, width),
            scratch(3, 4, unit_rows // 4, model),
            scratch(3, 2, head_rows // 2, model),
            scratch(2, group, token_rows, model),
            scratch(2, shards, token_rows, model),
            scratch(2, shards, token_rows, model),
            scratch(2, token_rows, model),
            scratch(5, *sums.shape, dtype=jnp.float32),
            scratch(rows, max(width, hidden.shape[1] + attn.shape[1])),
            scratch(hidden.shape[1], rows),
            scratch(attn.shape[1], rows),
            scratch(2, rows, group * block),
            scratch(group * block, rows),
            scratch(2, lane, width),
            scratch(2, rows, lane),
            scratch(2, hidden.shape[1], lane),
            scratch(2, attn.shape[1], lane),
            scratch(2, rows, lane),
            dma((2 + 2 * shards + 2 * shards * (shards - 1) + 3 * units + 2 * (group - 1),)),
            dma((units,)),
            dma((2, units)),
            dma((2, group)),
            dma((2, shards)),
            dma((2, 2, shards)),
            dma((2,)),
            dma((5,)),
            dma((6, 2)),
        ],
        compiler_params=pltpu.CompilerParams(
            collective_id=1, has_side_effects=True, vmem_limit_bytes=67043328
        ),
    )(norm, dcat, x_all, mean, inverse, attn, hidden, dy, cat_w, dense_w, down_w, sums)


def fast_body(
    hidden_in,
    segment_ids,
    out_grad,
    qkv_weight_state,
    qkv_bias_state,
    dense_weight_state,
    up_weight_state,
    up_bias_state,
    down_weight_state,
    vector_state,
):
    planes, cores, shards = lax.axis_size("plane"), lax.axis_size("core"), lax.axis_size("shard")
    plane, core, shard = lax.axis_index("plane"), lax.axis_index("core"), lax.axis_index("shard")
    group = cores * shards
    owner = (plane * cores + core) * shards + shard
    owners = planes * group
    model_rows = qkv_weight_state.shape[1]
    unit_rows = down_weight_state.shape[1]
    tokens_here = hidden_in.shape[1]
    head_width = planes * HD
    unit_width = planes * unit_rows
    qkv_count, upb_count = qkv_bias_state.shape[1], up_bias_state.shape[1]

    tokens, cotangent, q_seg = hidden_in[0], out_grad[0], segment_ids[0]
    vec_list = [
        qkv_bias_state[0],
        up_bias_state[0],
        vector_state[0].T.reshape(-1),
        q_seg.astype(jnp.float32),
    ]
    vec_sizes = [value.size for value in vec_list]
    vec_rows = -(-sum(vec_sizes) // 1024) * 8
    vec_own = jnp.pad(jnp.concatenate(vec_list), (0, vec_rows * 128 - sum(vec_sizes))).reshape(vec_rows, 128)

    cat_w, dense_w, down_w, x_all, dy_all, vec_all, norm_bf, x_mean, inverse = gather_wires(
        qkv_weight_state,
        up_weight_state,
        dense_weight_state,
        down_weight_state,
        tokens,
        cotangent,
        vec_own,
        sum(vec_sizes[:2]),
    )

    cat_w = cat_w.reshape(D, 3 * head_width + unit_width)
    dense_w = dense_w.reshape(head_width, D)
    down_w = down_w.reshape(unit_width, D)
    rows = group * tokens_here
    x_all = x_all.reshape(rows, D)
    dy_all = dy_all.reshape(rows, D)
    vec_flat = vec_all.reshape(planes, cores, shards, vec_rows * 128)
    at = [0]
    for size in vec_sizes:
        at.append(at[-1] + size)

    def rounded(value):
        return value.astype(jnp.bfloat16).astype(jnp.float32)

    qkv_bias = rounded(vec_flat[..., at[0] : at[1]]).reshape(3, planes, cores, shards, HD)
    qkv_bias = lax.dynamic_index_in_dim(
        qkv_bias.transpose(2, 3, 0, 1, 4).reshape(group, 3 * head_width), core * shards + shard, 0, False
    )
    up_bias = lax.dynamic_index_in_dim(
        rounded(vec_flat[..., at[1] : at[2]]).transpose(1, 2, 0, 3).reshape(group, unit_width),
        core * shards + shard,
        0,
        False,
    )
    vec_columns = (
        rounded(vec_flat[..., at[2] : at[3]])
        .reshape(owners, 4, model_rows)
        .transpose(1, 0, 2)
        .reshape(4, D)
    )
    norm_gain, norm_shift, dense_bias, down_bias = (vec_columns[index] for index in range(4))
    segments = lax.dynamic_index_in_dim(vec_flat[..., at[3] : at[4]], plane, 0, False)
    segments = segments.astype(jnp.int32).reshape(cores, shards * tokens_here)
    cat_bias = jnp.concatenate([qkv_bias, up_bias])

    norm_bf = norm_bf.reshape(rows, D)
    x_mean = x_mean.reshape(rows, 1)
    inverse = inverse.reshape(rows, 1)

    fu = jnp.dot(norm_bf, cat_w, preferred_element_type=jnp.float32) + cat_bias
    pre_act = fu[:, 3 * head_width :]
    hidden = gelu_tanh(pre_act).astype(jnp.bfloat16)
    grad_hidden = jnp.dot(dy_all, down_w.T, preferred_element_type=jnp.float32)
    grad_pre = jax.vjp(gelu_tanh, pre_act)[1](grad_hidden)[0]
    upb_part = jnp.sum(grad_pre, axis=0)
    grad_heads = jnp.dot(dy_all, dense_w.T, preferred_element_type=jnp.float32).astype(jnp.bfloat16)
    attn, dcat, qkvb_part = attention(fu, grad_heads, grad_pre.astype(jnp.bfloat16), segments)
    bias_part = jnp.sum(cotangent.astype(jnp.float32), axis=0)
    nothing = jnp.zeros((D,), jnp.float32)
    sums = [qkvb_part, upb_part, nothing, nothing, bias_part]
    sum_sizes = [value.size for value in sums]
    sum_rows = -(-sum(sum_sizes) // 1024) * 8
    sums = jnp.pad(jnp.concatenate(sums), (0, sum_rows * 128 - sum(sum_sizes))).reshape(sum_rows, 128)

    cat_sum, dense_grad, down_grad, mixed, grad_norm, sums_all = reduce_wires(
        norm_bf,
        dcat,
        x_all,
        x_mean,
        inverse,
        attn,
        hidden,
        dy_all,
        cat_w,
        dense_w,
        down_w,
        sums,
    )

    sums_flat = sums_all.reshape(cores, shards, sum_rows * 128)
    at = [0]
    for size in sum_sizes:
        at.append(at[-1] + size)
    qkvb_grad = (
        sums_flat[..., : at[1]]
        .reshape(cores, shards, 3, planes, HD)
        .transpose(2, 3, 0, 1, 4)
        .reshape(owners, qkv_count)
    )
    qkvb_grad = lax.dynamic_index_in_dim(qkvb_grad, owner, 0, False)
    upb_grad = sums_flat[..., at[1] : at[2]].reshape(group, planes, upb_count)
    upb_grad = lax.dynamic_index_in_dim(
        lax.dynamic_index_in_dim(upb_grad, core * shards + shard, 0, False), plane, 0, False
    )
    vec_grad = jnp.sum(sums_flat[..., at[2] : at[5]], axis=(0, 1)).reshape(3, owners, model_rows)
    vec_grad = lax.dynamic_index_in_dim(vec_grad, owner, 1, False)
    vec_grad = jnp.stack([vec_grad[0], vec_grad[1], vec_grad[2], vec_grad[2]], axis=1)

    x_own = tokens.astype(jnp.float32)
    output = (x_own + (mixed.astype(jnp.float32) + dense_bias + down_bias)).astype(jnp.bfloat16)
    own_center = x_own - jnp.mean(x_own, axis=-1, keepdims=True)
    own_inverse = lax.rsqrt(jnp.mean(own_center * own_center, axis=-1, keepdims=True) + norm_eps)
    own_hat = own_center * own_inverse
    hat_grad = grad_norm.astype(jnp.float32) * norm_gain
    x_grad = own_inverse * (
        hat_grad
        - jnp.mean(hat_grad, axis=-1, keepdims=True)
        - own_hat * jnp.mean(hat_grad * own_hat, axis=-1, keepdims=True)
    )
    input_grad = cotangent.astype(jnp.float32) + x_grad

    new, qkv_grad, dense_grad, up_grad, down_grad = owner_update(
        (qkv_weight_state, dense_weight_state, up_weight_state, down_weight_state),
        cat_sum,
        (dense_grad, down_grad),
        (qkv_bias_state, up_bias_state, vector_state),
        (qkvb_grad, upb_grad, vec_grad),
        (planes, cores, shards),
    )
    return (
        output[None],
        input_grad[None],
        qkv_grad,
        qkvb_grad,
        dense_grad,
        up_grad,
        upb_grad,
        down_grad,
        vec_grad,
        *new,
    )


def fast_solution(mesh):
    rep, shard = mesh.shape["rep"], mesh.shape["shard"]
    inner = Mesh(mesh.devices.reshape(rep // 2, 2, shard), ("plane", "core", "shard"))
    both = ("plane", "core")
    every = ("plane", "core", "shard")
    in_specs = (
        P(both, "shard", None),
        P(both, "shard"),
        P(both, "shard", None),
        P(None, every, None),
        P(None, every),
        P(None, every, None),
        P(None, every, None),
        P(None, every),
        P(None, every, None),
        P(None, every, None),
    )
    out_specs = (
        P(both, "shard", None),
        P(both, "shard", None),
        P(every, None),
        P(every),
        P(every, None),
        P(every, None),
        P(every),
        P(every, None),
        P(every, None),
        P(both, "shard", None),
        P(both, "shard", None),
        P(both, "shard", None),
    )
    return jax.shard_map(fast_body, mesh=inner, in_specs=in_specs, out_specs=out_specs, check_vma=False)


def solution(mesh):
    in_specs = (
        P("rep", "shard", None),
        P("rep", "shard"),
        P("rep", "shard", None),
        P(None, ("rep", "shard"), None),
        P(None, ("rep", "shard")),
        P(None, ("rep", "shard"), None),
        P(None, ("rep", "shard"), None),
        P(None, ("rep", "shard")),
        P(None, ("rep", "shard"), None),
        P(None, ("rep", "shard"), None),
    )
    out_specs = (
        P("rep", "shard", None),
        P("rep", "shard", None),
        P(("rep", "shard"), None),
        P(("rep", "shard")),
        P(("rep", "shard"), None),
        P(("rep", "shard"), None),
        P(("rep", "shard")),
        P(("rep", "shard"), None),
        P(("rep", "shard"), None),
        P("rep", "shard", None),
        P("rep", "shard", None),
        P("rep", "shard", None),
    )
    if whole_heads(mesh):
        return fast_solution(mesh)
    return jax.shard_map(body, mesh=mesh, in_specs=in_specs, out_specs=out_specs, check_vma=False)
```

```python
from functools import partial
import math

import jax
import jax.numpy as jnp
from jax import lax
from jax.experimental import pallas as pl
from jax.experimental.pallas import tpu as pltpu
from jax.sharding import Mesh
from jax.sharding import PartitionSpec as P

D = 2048
HD = 64
ROT = 32
FF = 8192
STEP = 5


learn_rate = 0.02
beta_one = 0.9
beta_two = 0.95
adam_eps = 1e-08
weight_decay = 0.1
norm_eps = 1e-05
big_negative = -1e30


def layer_norm(x, norm_gain, norm_shift):
    center = x - jnp.mean(x, axis=-1, keepdims=True)
    variance = jnp.mean(center * center, axis=-1, keepdims=True)
    return center * lax.rsqrt(variance + norm_eps) * norm_gain + norm_shift


def gelu_tanh(v):
    return 0.5 * v * (1.0 + jnp.tanh(0.7978845608028654 * (v + 0.044715 * v * v * v)))


def rotary(x, positions):
    half_rot = ROT // 2
    frequency = jnp.exp(jnp.arange(half_rot, dtype=jnp.float32) * (-2.0 * math.log(10000.0) / ROT))
    angles = positions.astype(jnp.float32)[:, None] * frequency[None, :]
    cosine = jnp.cos(angles)[:, None, :]
    sine_val = jnp.sin(angles)[:, None, :]
    lower_part = x[..., :half_rot]
    upper_part = x[..., half_rot:ROT]
    return jnp.concatenate(
        [
            lower_part * cosine - upper_part * sine_val,
            upper_part * cosine + lower_part * sine_val,
            x[..., ROT:],
        ],
        axis=-1,
    )


def adam_update(state, grad):
    moment_one = beta_one * state[1] + (1.0 - beta_one) * grad
    moment_two = beta_two * state[2] + (1.0 - beta_two) * grad * grad
    corrected = moment_one / (1.0 - beta_one**STEP)
    divisor = jnp.sqrt(moment_two / (1.0 - beta_two**STEP)) + adam_eps
    weight = state[0] - learn_rate * (corrected / divisor + weight_decay * state[0])
    return jnp.stack([weight, moment_one, moment_two])


def owner_entries(new_states, entry):
    return jnp.concatenate(
        [state_new[entry].reshape(-1) for state_new in new_states], axis=0
    ).reshape(1, 1, -1)


def block_mask(q_pos, q_seg, k_pos, k_seg):
    return (k_pos[None, :] <= q_pos[:, None]) & (k_seg[None, :] == q_seg[:, None])


def attend_keys(kv_all, seg_all, queries, q_pos, q_seg):
    key_count = kv_all.shape[0]
    width = kv_all.shape[1] // 2
    heads_here = queries.shape[1]
    query_rows = queries.shape[0]
    block_rows = math.gcd(key_count, 512)
    block_count = key_count // block_rows
    kv_blocks = kv_all.reshape(block_count, block_rows, 2 * width)
    seg_blocks = seg_all.reshape(block_count, block_rows)
    score_scale = 1.0 / math.sqrt(HD)

    def attend_step_block(carry, block_items):
        kv_rows, seg_rows, block_index = block_items
        row_max, totals, accumulated = carry
        key_rows = kv_rows[:, :width].reshape(block_rows, heads_here, HD)
        value_rows = kv_rows[:, width:].reshape(block_rows, heads_here, HD)
        k_pos = block_index * block_rows + jnp.arange(block_rows, dtype=jnp.int32)
        allowed = block_mask(q_pos, q_seg, k_pos, seg_rows)
        scores = (
            jnp.einsum("qhd,khd->hqk", queries, key_rows, preferred_element_type=jnp.float32)
            * score_scale
        )
        scores = jnp.where(allowed[None], scores, big_negative)
        new_max = jnp.maximum(row_max, jnp.max(scores, axis=-1))
        probabilities = jnp.where(allowed[None], jnp.exp(scores - new_max[..., None]), 0.0)
        factor = jnp.exp(row_max - new_max)
        totals = totals * factor + jnp.sum(probabilities, axis=-1)
        accumulated = accumulated * factor[..., None] + jnp.einsum(
            "hqk,khd->hqd",
            probabilities.astype(jnp.bfloat16),
            value_rows,
            preferred_element_type=jnp.float32,
        )
        return ((new_max, totals, accumulated), None)

    start_state = (
        jnp.full((heads_here, query_rows), big_negative, jnp.float32),
        jnp.zeros((heads_here, query_rows), jnp.float32),
        jnp.zeros((heads_here, query_rows, HD), jnp.float32),
    )
    running, unused = lax.scan(
        attend_step_block,
        start_state,
        (kv_blocks, seg_blocks, jnp.arange(block_count, dtype=jnp.int32)),
    )
    return running


def attention_grads(queries, kv_all, seg_all, q_pos, q_seg, grad_heads, delta_all, lse_all):
    key_count = kv_all.shape[0]
    width = kv_all.shape[1] // 2
    heads_here = queries.shape[1]
    query_rows = queries.shape[0]
    block_rows = math.gcd(key_count, 512)
    block_count = key_count // block_rows
    kv_blocks = kv_all.reshape(block_count, block_rows, 2 * width)
    seg_blocks = seg_all.reshape(block_count, block_rows)
    score_scale = 1.0 / math.sqrt(HD)

    def attention_step_block(query_grad, block_items):
        kv_rows, seg_rows, block_index = block_items
        key_rows = kv_rows[:, :width].reshape(block_rows, heads_here, HD)
        value_rows = kv_rows[:, width:].reshape(block_rows, heads_here, HD)
        k_pos = block_index * block_rows + jnp.arange(block_rows, dtype=jnp.int32)
        allowed = block_mask(q_pos, q_seg, k_pos, seg_rows)
        scores = (
            jnp.einsum("qhd,khd->hqk", queries, key_rows, preferred_element_type=jnp.float32)
            * score_scale
        )
        scores = jnp.where(allowed[None], scores, big_negative)
        probabilities = jnp.where(allowed[None], jnp.exp(scores - lse_all[..., None]), 0.0)
        value_grad = jnp.einsum(
            "hqk,qhd->khd",
            probabilities.astype(jnp.bfloat16),
            grad_heads,
            preferred_element_type=jnp.float32,
        )
        prob_grad = jnp.einsum(
            "qhd,khd->hqk", grad_heads, value_rows, preferred_element_type=jnp.float32
        )
        score_grad = (probabilities * (prob_grad - delta_all[..., None]) * score_scale).astype(
            jnp.bfloat16
        )
        query_grad = query_grad + jnp.einsum(
            "hqk,khd->hqd", score_grad, key_rows, preferred_element_type=jnp.float32
        )
        key_grad = jnp.einsum(
            "hqk,qhd->khd", score_grad, queries, preferred_element_type=jnp.float32
        )
        return (
            query_grad,
            jnp.concatenate(
                [key_grad.reshape(block_rows, width), value_grad.reshape(block_rows, width)], axis=1
            ),
        )

    query_grad, kv_grad_blocks = lax.scan(
        attention_step_block,
        jnp.zeros((heads_here, query_rows, HD), jnp.float32),
        (kv_blocks, seg_blocks, jnp.arange(block_count, dtype=jnp.int32)),
    )
    return (query_grad, kv_grad_blocks.reshape(key_count, 2 * width))


def gather_vectors(own_qkvb, own_upb, own_vec):
    return (
        lax.all_gather(own_qkvb, ("rep", "shard"), axis=0, tiled=True),
        lax.all_gather(own_upb, ("rep", "shard"), axis=0, tiled=True),
        lax.all_gather(own_vec, ("rep", "shard"), axis=0, tiled=True),
    )


def sum_vectors(qkvb_grad, upb_grad, vec_grad):
    return (
        lax.psum_scatter(qkvb_grad, ("rep", "shard"), scatter_dimension=0, tiled=True),
        lax.psum_scatter(upb_grad, ("rep", "shard"), scatter_dimension=0, tiled=True),
        lax.psum_scatter(vec_grad, ("rep", "shard"), scatter_dimension=0, tiled=True),
    )


def sum_positions(partial_rows):
    return lax.psum_scatter(partial_rows, "shard", scatter_dimension=0, tiled=True)


def attention_pass(norm_rows, qkv_w, qkv_b, positions, key_width):
    row_count = norm_rows.shape[0]
    heads_here = key_width // HD
    joined = jnp.dot(norm_rows, qkv_w, preferred_element_type=jnp.float32) + qkv_b
    q_pre = joined[:, :key_width].reshape(row_count, heads_here, HD)
    k_pre = joined[:, key_width : 2 * key_width].reshape(row_count, heads_here, HD)
    queries = rotary(q_pre, positions).astype(jnp.bfloat16)
    key_local = rotary(k_pre, positions).astype(jnp.bfloat16).reshape(row_count, key_width)
    value_local = joined[:, 2 * key_width :].astype(jnp.bfloat16)
    kv_local = jnp.concatenate([key_local, value_local], axis=1)
    return (q_pre, k_pre, queries, kv_local)


def finish_qkv_grad(q_pre, k_pre, positions, query_grad, kv_grad, key_width):
    row_count = q_pre.shape[0]
    heads_here = key_width // HD
    rotate_back = partial(rotary, positions=positions)
    query_pre = jax.vjp(rotate_back, q_pre)[1](query_grad.transpose(1, 0, 2))[0]
    key_pre = jax.vjp(rotate_back, k_pre)[1](
        kv_grad[:, :key_width].reshape(row_count, heads_here, HD)
    )[0]
    return jnp.concatenate(
        [
            query_pre.reshape(row_count, key_width),
            key_pre.reshape(row_count, key_width),
            kv_grad[:, key_width:],
        ],
        axis=1,
    )


def sliced_pass(norm_bf, q_seg, cotangent, own_mats, qkv_bb, up_bb):
    own_qkv, own_dense, own_up, own_down = own_mats
    inner_count = lax.axis_size("shard")
    outer_count = lax.axis_size("rep")
    stride = outer_count // inner_count
    place = lax.axis_index("shard")
    head_width = D // inner_count
    unit_width = FF // inner_count
    qkv_rows = own_qkv.shape[0]
    dense_rows = own_dense.shape[0]
    down_rows = own_down.shape[0]
    qkv_split = own_qkv.reshape(qkv_rows, 3, inner_count, head_width)
    up_split = own_up.reshape(qkv_rows, 1, inner_count, unit_width)
    qkv_cols, up_cols = (
        lax.all_to_all(qkv_split, "shard", split_axis=2, concat_axis=0, tiled=True),
        lax.all_to_all(up_split, "shard", split_axis=2, concat_axis=0, tiled=True),
    )
    qkv_rep, up_rep, dense_rep, down_rep = (
        lax.all_gather(qkv_cols, "rep", axis=0, tiled=True),
        lax.all_gather(up_cols, "rep", axis=0, tiled=True),
        lax.all_gather(own_dense[None], "rep", axis=0, tiled=True),
        lax.all_gather(own_down[None], "rep", axis=0, tiled=True),
    )
    dense_grid = dense_rep.reshape(inner_count, stride, 1, dense_rows, D)
    down_grid = down_rep.reshape(inner_count, stride, 1, down_rows, D)
    dense_moved, down_moved = (
        lax.all_to_all(dense_grid, "shard", split_axis=0, concat_axis=2, tiled=True),
        lax.all_to_all(down_grid, "shard", split_axis=0, concat_axis=2, tiled=True),
    )
    qkv_w = qkv_rep.reshape(D, 3 * head_width)
    up_w = up_rep.reshape(D, unit_width)
    dense_w = dense_moved.reshape(head_width, D)
    down_w = down_moved.reshape(unit_width, D)
    qkv_b = lax.dynamic_index_in_dim(
        qkv_bb.astype(jnp.float32).reshape(3, inner_count, head_width), place, 1, False
    ).reshape(3 * head_width)
    up_b = lax.dynamic_slice_in_dim(up_bb.astype(jnp.float32), place * unit_width, unit_width, 0)
    norm_seq, grad_seq, seg_seq = (
        lax.all_gather(norm_bf, "shard", axis=0, tiled=True),
        lax.all_gather(cotangent, "shard", axis=0, tiled=True),
        lax.all_gather(q_seg, "shard", axis=0, tiled=True),
    )
    seq_rows = norm_seq.shape[0]
    heads_here = head_width // HD
    positions = jnp.arange(seq_rows, dtype=jnp.int32)
    q_pre, k_pre, queries, kv_seq = attention_pass(norm_seq, qkv_w, qkv_b, positions, head_width)
    row_max, totals, accumulated = attend_keys(kv_seq, seg_seq, queries, positions, seg_seq)
    lse_all = row_max + jnp.log(totals)
    out_heads = (accumulated / totals[..., None]).transpose(1, 0, 2).astype(jnp.bfloat16)
    attn_bf = out_heads.reshape(seq_rows, head_width)
    pre_act = jnp.dot(norm_seq, up_w, preferred_element_type=jnp.float32) + up_b
    hidden = gelu_tanh(pre_act).astype(jnp.bfloat16)
    partial_out = jnp.dot(attn_bf, dense_w, preferred_element_type=jnp.float32) + jnp.dot(
        hidden, down_w, preferred_element_type=jnp.float32
    )
    mixed = sum_positions(partial_out)
    grad_down = jnp.dot(hidden.T, grad_seq, preferred_element_type=jnp.float32)
    grad_dense = jnp.dot(attn_bf.T, grad_seq, preferred_element_type=jnp.float32)
    grad_hidden = jnp.dot(grad_seq, down_w.T, preferred_element_type=jnp.float32)
    grad_pre = jax.vjp(gelu_tanh, pre_act)[1](grad_hidden)[0]
    grad_pre_bf = grad_pre.astype(jnp.bfloat16)
    grad_up = jnp.dot(norm_seq.T, grad_pre_bf, preferred_element_type=jnp.float32)
    upb_part = jnp.sum(grad_pre, axis=0)
    norm_part = jnp.dot(grad_pre_bf, up_w.T, preferred_element_type=jnp.float32)
    grad_heads = (
        jnp.dot(grad_seq, dense_w.T, preferred_element_type=jnp.float32)
        .astype(jnp.bfloat16)
        .reshape(seq_rows, heads_here, HD)
    )
    delta_all = jnp.sum(grad_heads.astype(jnp.float32) * out_heads.astype(jnp.float32), axis=-1).T
    query_grad, kv_grad = attention_grads(
        queries, kv_seq, seg_seq, positions, seg_seq, grad_heads, delta_all, lse_all
    )
    grad_joined = finish_qkv_grad(q_pre, k_pre, positions, query_grad, kv_grad, head_width)
    grad_joined_bf = grad_joined.astype(jnp.bfloat16)
    grad_qkv = jnp.dot(norm_seq.T, grad_joined_bf, preferred_element_type=jnp.float32)
    qkvb_part = jnp.sum(grad_joined, axis=0)
    norm_part = norm_part + jnp.dot(grad_joined_bf, qkv_w.T, preferred_element_type=jnp.float32)
    grad_norm = sum_positions(norm_part)
    dense_grid_grad = grad_dense.reshape(1, stride, inner_count, dense_rows, D)
    down_grid_grad = grad_down.reshape(1, stride, inner_count, down_rows, D)
    dense_back, down_back = (
        lax.all_to_all(dense_grid_grad, "shard", split_axis=2, concat_axis=0, tiled=True),
        lax.all_to_all(down_grid_grad, "shard", split_axis=2, concat_axis=0, tiled=True),
    )
    qkv_sum, up_sum, dense_sum, down_sum = (
        lax.psum_scatter(
            grad_qkv.reshape(D, 3, 1, head_width), "rep", scatter_dimension=0, tiled=True
        ),
        lax.psum_scatter(
            grad_up.reshape(D, 1, 1, unit_width), "rep", scatter_dimension=0, tiled=True
        ),
        lax.psum_scatter(
            dense_back.reshape(outer_count, dense_rows, D), "rep", scatter_dimension=0, tiled=True
        ),
        lax.psum_scatter(
            down_back.reshape(outer_count, down_rows, D), "rep", scatter_dimension=0, tiled=True
        ),
    )
    qkv_home, up_home = (
        lax.all_to_all(qkv_sum, "shard", split_axis=0, concat_axis=2, tiled=True),
        lax.all_to_all(up_sum, "shard", split_axis=0, concat_axis=2, tiled=True),
    )
    qkv_own = qkv_home.reshape(qkv_rows, 3 * D)
    up_own = up_home.reshape(qkv_rows, FF)
    dense_own = dense_sum.reshape(dense_rows, D)
    down_own = down_sum.reshape(down_rows, D)
    selector = (jnp.arange(inner_count, dtype=jnp.int32) == place).astype(jnp.float32)
    qkvb_grad = (selector[None, :, None] * qkvb_part.reshape(3, 1, head_width)).reshape(3 * D)
    upb_grad = (selector[:, None] * upb_part[None, :]).reshape(FF)
    return (mixed, grad_norm, (qkv_own, dense_own, up_own, down_own), qkvb_grad, upb_grad)


def body(
    hidden_in,
    segment_ids,
    out_grad,
    qkv_weight_state,
    qkv_bias_state,
    dense_weight_state,
    up_weight_state,
    up_bias_state,
    down_weight_state,
    vector_state,
):
    own_mats = (
        qkv_weight_state[0].astype(jnp.bfloat16),
        dense_weight_state[0].astype(jnp.bfloat16),
        up_weight_state[0].astype(jnp.bfloat16),
        down_weight_state[0].astype(jnp.bfloat16),
    )
    qkv_bb, up_bb, vec_bf = gather_vectors(
        qkv_bias_state[0].astype(jnp.bfloat16),
        up_bias_state[0].astype(jnp.bfloat16),
        vector_state[0].astype(jnp.bfloat16),
    )
    vec_all = vec_bf.astype(jnp.float32)
    norm_gain = vec_all[:, 0]
    norm_shift = vec_all[:, 1]
    dense_bias = vec_all[:, 2]
    down_bias = vec_all[:, 3]
    tokens = hidden_in[0]
    q_seg = segment_ids[0]
    cotangent = out_grad[0]
    x_full = tokens.astype(jnp.float32)
    normed = layer_norm(x_full, norm_gain, norm_shift)
    norm_bf = normed.astype(jnp.bfloat16)
    mixed, grad_norm, owned, qkvb_grad, upb_grad = sliced_pass(
        norm_bf, q_seg, cotangent, own_mats, qkv_bb, up_bb
    )
    qkv_own, dense_own, up_own, down_own = owned
    output = (x_full + (mixed + dense_bias + down_bias)).astype(jnp.bfloat16)
    grad_x, grad_gain, grad_shift = jax.vjp(layer_norm, x_full, norm_gain, norm_shift)[1](grad_norm)
    out_bias_grad = jnp.sum(cotangent.astype(jnp.float32), axis=0)
    grad_vec = jnp.stack([grad_gain, grad_shift, out_bias_grad, out_bias_grad], axis=1)
    input_grad = cotangent.astype(jnp.float32) + grad_x
    qkvb_own, upb_own, vec_own = sum_vectors(qkvb_grad, upb_grad, grad_vec)
    new_states = (
        adam_update(qkv_weight_state, qkv_own),
        adam_update(qkv_bias_state, qkvb_own),
        adam_update(dense_weight_state, dense_own),
        adam_update(up_weight_state, up_own),
        adam_update(up_bias_state, upb_own),
        adam_update(down_weight_state, down_own),
        adam_update(vector_state, vec_own),
    )
    return (
        output[None],
        input_grad[None],
        qkv_own,
        qkvb_own,
        dense_own,
        up_own,
        upb_own,
        down_own,
        vec_own,
        owner_entries(new_states, 0),
        owner_entries(new_states, 1),
        owner_entries(new_states, 2),
    )


def whole_heads(mesh):
    owners = mesh.shape["rep"] * mesh.shape["shard"]
    return D % owners == 0 and D // owners == HD and mesh.shape["rep"] % 2 == 0


def rotation_tables(seq_rows):
    half_rot = ROT // 2
    lane = jnp.arange(2 * HD, dtype=jnp.int32) % HD
    frequency = jnp.exp((lane % half_rot).astype(jnp.float32) * (-2.0 * math.log(10000.0) / ROT))
    angles = jnp.arange(seq_rows, dtype=jnp.int32).astype(jnp.float32)[:, None] * frequency[None, :]
    sine = jnp.sin(angles)
    cosine = jnp.where(lane[None, :] < ROT, jnp.cos(angles), 1.0)
    low = jnp.where(lane[None, :] < half_rot, -sine, 0.0)
    high = jnp.where((lane[None, :] >= half_rot) & (lane[None, :] < ROT), sine, 0.0)
    return cosine, low, high


def attention_kernel(
    fu_ref, do_ref, du_ref, seg_col_ref, seg_row_ref, cos_ref, low_ref, high_ref, o_ref, dcat_ref, sums_ref
):
    rows, width = do_ref.shape
    scale = 1.0 / math.sqrt(HD)
    row_id = lax.broadcasted_iota(jnp.int32, (rows, rows), 0)
    col_id = lax.broadcasted_iota(jnp.int32, (rows, rows), 1)
    allowed = (col_id <= row_id) & (seg_col_ref[...] == seg_row_ref[0])
    cosine, low, high = cos_ref[...], low_ref[...], high_ref[...]
    half = ROT // 2
    lane = lax.broadcasted_iota(jnp.int32, (rows, 2 * HD), 1)

    def rotate(u):
        return (
            u * cosine
            + pltpu.roll(u, 2 * HD - half, 1) * low
            + pltpu.roll(u, half, 1) * high
        )

    def rotate_back(u):
        return (
            u * cosine
            - pltpu.roll(u, 2 * HD - half, 1) * low
            - pltpu.roll(u, half, 1) * high
        )

    def dot(a, b, a_dim, b_dim):
        return lax.dot_general(a, b, (((a_dim,), (b_dim,)), ((), ())), preferred_element_type=jnp.float32)

    zero = jnp.zeros((), jnp.bfloat16)
    for pair in range(width // (2 * HD)):
        lanes = pl.ds(pair * 2 * HD, 2 * HD)
        k_lanes = pl.ds(width + pair * 2 * HD, 2 * HD)
        v_lanes = pl.ds(2 * width + pair * 2 * HD, 2 * HD)
        q = rotate(fu_ref[:, lanes]).astype(jnp.bfloat16)
        k = rotate(fu_ref[:, k_lanes]).astype(jnp.bfloat16)
        v = fu_ref[:, v_lanes].astype(jnp.bfloat16)
        do = do_ref[:, lanes]
        o = dq = dk = dv = None
        for head in range(2):
            mine = (lane < HD) if head == 0 else (lane >= HD)
            qh = jnp.where(mine, q, zero)
            kh = jnp.where(mine, k, zero)
            vh = jnp.where(mine, v, zero)
            doh = jnp.where(mine, do, zero)
            scores = jnp.where(allowed, dot(qh, k, 1, 1) * scale, big_negative)
            row_max = jnp.max(scores, axis=1, keepdims=True)
            probs = jnp.where(allowed, jnp.exp(scores - row_max), 0.0)
            inverse = 1.0 / jnp.sum(probs, axis=1, keepdims=True)
            oh = dot(probs.astype(jnp.bfloat16), vh, 1, 0) * inverse
            delta = jnp.sum(
                doh.astype(jnp.float32) * oh.astype(jnp.bfloat16).astype(jnp.float32), axis=1, keepdims=True
            )
            probs = probs * inverse
            dvh = dot(probs.astype(jnp.bfloat16), doh, 0, 0)
            ds = (probs * (dot(doh, v, 1, 1) - delta) * scale).astype(jnp.bfloat16)
            dqh = dot(ds, kh, 1, 0)
            dkh = dot(ds, qh, 0, 0)
            if head == 0:
                o, dq, dk, dv = oh, dqh, dkh, dvh
            else:
                o, dq, dk, dv = o + oh, dq + dqh, dk + dkh, dv + dvh
        o_ref[:, lanes] = o.astype(jnp.bfloat16)
        dq = rotate_back(dq)
        dk = rotate_back(dk)
        for part, place in ((dq, lanes), (dk, k_lanes), (dv, v_lanes)):
            dcat_ref[:, place] = part.astype(jnp.bfloat16)
            sums_ref[0, :, place] = jnp.sum(part, axis=0, keepdims=True)
    dcat_ref[:, pl.ds(3 * width, du_ref.shape[1])] = du_ref[...]


def attention(fu, do, du, segments):
    count, rows = segments.shape
    width = do.shape[1]
    units = du.shape[1]
    tables = rotation_tables(rows)
    table_spec = pl.BlockSpec((rows, 2 * HD), lambda s: (0, 0))
    o, dcat, sums = pl.pallas_call(
        attention_kernel,
        grid=(count,),
        in_specs=[
            pl.BlockSpec((rows, 3 * width), lambda s: (s, 0)),
            pl.BlockSpec((rows, width), lambda s: (s, 0)),
            pl.BlockSpec((rows, units), lambda s: (s, 0)),
            pl.BlockSpec((rows, 1), lambda s: (s, 0)),
            pl.BlockSpec((1, 1, rows), lambda s: (s, 0, 0)),
            table_spec,
            table_spec,
            table_spec,
        ],
        out_specs=[
            pl.BlockSpec((rows, width), lambda s: (s, 0)),
            pl.BlockSpec((rows, 3 * width + units), lambda s: (s, 0)),
            pl.BlockSpec((1, 1, 3 * width), lambda s: (s, 0, 0)),
        ],
        out_shape=[
            jax.ShapeDtypeStruct((count * rows, width), jnp.bfloat16),
            jax.ShapeDtypeStruct((count * rows, 3 * width + units), jnp.bfloat16),
            jax.ShapeDtypeStruct((count, 1, 3 * width), jnp.float32),
        ],
        compiler_params=pltpu.CompilerParams(vmem_limit_bytes=56 << 20),
        cost_estimate=pl.CostEstimate(
            flops=count * (width // HD) * 10 * rows * rows * HD,
            bytes_accessed=count * rows * (width * 20 + units * 4),
            transcendentals=count * (width // HD) * rows * rows,
        ),
    )(fu, do, du, segments.reshape(count * rows, 1), segments.reshape(count, 1, rows), *tables)
    return o, dcat, jnp.sum(sums, axis=(0, 1))


def adam_values(weight, moment_one, moment_two, grad):
    first = beta_one * moment_one + (1.0 - beta_one) * grad
    second = beta_two * moment_two + (1.0 - beta_two) * grad * grad
    corrected = first * (1.0 / (1.0 - beta_one**STEP))
    divisor = jnp.sqrt(second * (1.0 / (1.0 - beta_two**STEP))) + adam_eps
    return weight - learn_rate * (corrected / divisor + weight_decay * weight), first, second


def owner_update_kernel(plan, small_plan, groups, steps, whole_rows, *refs):
    planes, cores, shards = groups
    qkv_state, dense_state, up_state, down_state, cat_ref, dense_grad, down_grad, small_ref = refs[:8]
    flat = refs[8:11]
    qkv_out, dense_out, up_out, down_out, cat_buf = refs[11:16]
    outs = refs[16:19]
    step_sem, rest_sem = refs[19:]
    step = pl.program_id(0)
    lane = lax.broadcasted_iota(jnp.int32, (8, 128), 1)
    sub = lax.broadcasted_iota(jnp.int32, (8, 128), 0)
    lane_row = lax.broadcasted_iota(jnp.int32, (1, 128), 1)
    wide = 1024

    @pl.when(step == 0)
    def small():
        for source, row, low, high in small_plan:
            for entry in range(3):
                old = outs[entry][pl.ds(row, 1), :]
                new = small_ref[entry, pl.ds(source, 1), :]
                outs[entry][pl.ds(row, 1), :] = jnp.where((lane_row >= low) & (lane_row < high), new, old)

    def widen(piece, carry):
        cat_buf[piece] = cat_ref[piece].astype(jnp.float32)
        return carry

    lax.fori_loop(0, cat_ref.shape[0], widen, 0)

    def place_rows(state, grad_of, rows, tiles, start, shifted, keep=None):
        chunk = min(wide, tiles * 128)

        def one_group(group, carry):
            place = pl.ds(pl.multiple_of(group * 8, 8), 8)
            base = start + (step * (rows // 8) + group) * (8 * tiles)

            def values(column, size):
                lanes = pl.ds(column, size)
                grad = grad_of(place, column, size)
                if keep is not None and size > 128:
                    keep[place, lanes] = grad
                return adam_values(
                    state[0, place, lanes], state[1, place, lanes], state[2, place, lanes], grad
                )

            if shifted:
                last = tuple(pltpu.roll(value, 64, 1) for value in values((tiles - 1) * 128, 128))
                before = tuple(
                    jnp.where(sub == 0, out[pl.ds(base, 1), :], pltpu.roll(value, 1, 0))
                    for out, value in zip(outs, last)
                )
            for column in range(0, tiles * 128, chunk):
                done = values(column, chunk)
                for entry, out in enumerate(outs):
                    for tile in range(chunk // 128):
                        value = done[entry][:, tile * 128 : (tile + 1) * 128]
                        if shifted:
                            value = pltpu.roll(value, 64, 1)
                            old = before[entry] if tile == 0 else now
                            now = value
                            value = jnp.where(lane < 64, old, value)
                        out[pl.ds(base + column // 128 + tile, 8, stride=tiles), :] = value
                    if shifted:
                        before = before[:entry] + (now,) + before[entry + 1 :]
            if shifted:
                for out, value in zip(outs, before):
                    row = pl.ds(base + 8 * tiles, 1)
                    out[row, :] = jnp.where(lane_row < 64, value[7:8], out[row, :])
            return carry

        lax.fori_loop(0, rows // 8, one_group, 0)

    def qkv_grad(place, column, size):
        tiles = []
        for start in range(column, column + size, 128):
            part, head = divmod(start // HD, planes * cores * shards)
            halves = []
            for side in range(2):
                plane, member = divmod(head + side, cores * shards)
                spot = (part * planes + plane) * HD
                half = cat_buf[member, place, pl.ds(spot // 128 * 128, 128)]
                halves.append(half if spot % 128 == side * HD else pltpu.roll(half, HD, 1))
            tiles.append(jnp.where(lane < HD, halves[0], halves[1]))
        return tiles[0] if len(tiles) == 1 else jnp.concatenate(tiles, axis=1)

    units = up_state.shape[2] // (planes * cores * shards)

    def up_grad(place, column, size):
        parts = []
        for start in range(column, column + size, min(units, size)):
            plane, member = divmod(start // units, cores * shards)
            spot = 3 * planes * HD + plane * units + start % units
            parts.append(cat_buf[member, place, pl.ds(spot, min(units, size))])
        return parts[0] if len(parts) == 1 else jnp.concatenate(parts, axis=1)

    def plain(grad):
        return lambda place, column, size: grad[place, pl.ds(column, size)]

    place_rows(qkv_state, qkv_grad, *plan[0], keep=qkv_out)
    place_rows(dense_state, plain(dense_grad), *plan[1], keep=dense_out)
    place_rows(up_state, up_grad, *plan[2], keep=up_out)
    place_rows(down_state, plain(down_grad), *plan[3], keep=down_out)

    def flush(entry, row, count, sem):
        place = pl.ds(pl.multiple_of(row * 128, 128), count * 128)
        source = outs[entry].reshape(1, 1, outs[entry].shape[0] * 128)
        return pltpu.make_async_copy(source.at[:, :, place], flat[entry].at[:, :, place], sem)

    def step_copies(at):
        copies = []
        for index, (rows, tiles, start, shifted) in enumerate(plan):
            count = rows * tiles
            skip = 1 if shifted and at == 0 else 0
            for entry in range(3):
                copies.append(
                    flush(entry, start + at * count + skip, count - skip, step_sem.at[entry, index, at])
                )
        return copies

    for at in range(steps):

        @pl.when(step == at)
        def begin(at=at):
            for copy in step_copies(at):
                copy.start()

    @pl.when(step == steps - 1)
    def end():
        covered = set()
        for rows, tiles, start, shifted in plan:
            covered |= set(range(start + (1 if shifted else 0), start + steps * rows * tiles))
        left = [row for row in range(whole_rows) if row not in covered]
        rest = [
            flush(entry, row, 1, rest_sem.at[entry, index]) for index, row in enumerate(left) for entry in range(3)
        ]
        for copy in rest:
            copy.start()
        for at in range(steps):
            for copy in step_copies(at):
                copy.wait()
        for copy in rest:
            copy.wait()


def owner_update(states, cat_sum, grads, small_states, small_grads, groups):
    steps = 4
    sizes = [state.shape[1] * state.shape[2] for state in states]
    small_sizes = [grad.size for grad in small_grads]
    order = [("m", 0), ("s", 0), ("m", 1), ("m", 2), ("s", 1), ("m", 3), ("s", 2)]
    offset = 0
    plan = [None] * 4
    small_plan = []
    pads = []
    small_row = 0
    for kind, index in order:
        if kind == "m":
            state = states[index]
            rows = state.shape[1] // steps
            plan[index] = (rows, state.shape[2] // 128, offset // 128, offset % 128 == 64)
            offset += sizes[index]
        else:
            size = small_sizes[index]
            front = offset % 128
            total = -(-(front + size) // 128)
            pads.append((front, total * 128 - front - size))
            for extra in range(total):
                low = front if extra == 0 else 0
                high = min(128, front + size - extra * 128)
                small_plan.append((small_row + extra, offset // 128 + extra, low, high))
            small_row += total
            offset += size
    entries = offset
    out_rows = -(-entries // 1024) * 8
    small_new = [
        adam_values(state[0].reshape(-1), state[1].reshape(-1), state[2].reshape(-1), grad.reshape(-1))
        for state, grad in zip(small_states, small_grads)
    ]
    small = jnp.stack(
        [
            jnp.concatenate([jnp.pad(new[entry], pad) for new, pad in zip(small_new, pads)])
            for entry in range(3)
        ]
    ).reshape(3, small_row, 128)
    in_specs = [
        pl.BlockSpec((3, rows, tiles * 128), lambda s: (0, s, 0)) for rows, tiles, start, shifted in plan
    ]
    qkv_rows = plan[0][0]
    in_specs.append(pl.BlockSpec((cat_sum.shape[0], qkv_rows, cat_sum.shape[2]), lambda s: (0, s, 0)))
    in_specs.append(pl.BlockSpec((plan[1][0], plan[1][1] * 128), lambda s: (s, 0)))
    in_specs.append(pl.BlockSpec((plan[3][0], plan[3][1] * 128), lambda s: (s, 0)))
    in_specs.append(pl.BlockSpec((3, small_row, 128), lambda s: (0, 0, 0)))
    whole_rows = entries // 128
    *outs, qkv_grad, dense_grad, up_grad, down_grad = pl.pallas_call(
        partial(owner_update_kernel, plan, small_plan, groups, steps, whole_rows),
        grid=(steps,),
        in_specs=in_specs,
        out_specs=[pl.BlockSpec(memory_space=pl.ANY)] * 3
        + [
            pl.BlockSpec((rows, tiles * 128), lambda s: (s, 0)) for rows, tiles, start, shifted in plan
        ],
        out_shape=[jax.ShapeDtypeStruct((1, 1, entries), jnp.float32)] * 3
        + [
            jax.ShapeDtypeStruct(state.shape[1:], jnp.float32) for state in states
        ],
        scratch_shapes=[pltpu.VMEM((cat_sum.shape[0], qkv_rows, cat_sum.shape[2]), jnp.float32)]
        + [pltpu.VMEM((out_rows, 128), jnp.float32)] * 3
        + [pltpu.SemaphoreType.DMA((3, 4, steps)), pltpu.SemaphoreType.DMA((3, 16))],
        compiler_params=pltpu.CompilerParams(vmem_limit_bytes=56 << 20),
        cost_estimate=pl.CostEstimate(
            flops=20 * entries, bytes_accessed=28 * entries, transcendentals=2 * entries
        ),
    )(*states, cat_sum, *grads, small)
    tail = entries - whole_rows * 128
    if tail:
        outs = [
            lax.dynamic_update_slice(out, new[entries_of][-tail:].reshape(1, 1, tail), (0, 0, whole_rows * 128))
            for out, (new, entries_of) in zip(outs, ((small_new[-1], entry) for entry in range(3)))
        ]
    return tuple(outs), qkv_grad, dense_grad, up_grad, down_grad


class Wires:
    def __init__(self, send_sems):
        self.send_sems, self.count, self.pending = send_sems, 0, []
        self.plane, self.core, self.shard = (
            lax.axis_index("plane"),
            lax.axis_index("core"),
            lax.axis_index("shard"),
        )
        self.shards = lax.axis_size("shard")
        self.group = lax.axis_size("core") * self.shards
        self.mine = self.core * self.shards + self.shard
        self.first = (self.plane ^ 1, self.core, self.shard)
        self.second = (self.plane ^ 2, self.core, self.shard)

    def member(self, index):
        return (self.plane, index // self.shards, index % self.shards)

    def barrier(self):
        barrier = pltpu.get_barrier_semaphore()
        partners = [self.member(self.mine ^ mask) for mask in range(1, self.group)]
        partners += [self.first, self.second]
        for partner in partners:
            pl.semaphore_signal(barrier, inc=1, device_id=partner, device_id_type=pl.DeviceIdType.MESH)
        pl.semaphore_wait(barrier, len(partners))

    def send(self, source, target, recv_sem, device, when=None):
        copy = pltpu.make_async_remote_copy(
            src_ref=source,
            dst_ref=target,
            send_sem=self.send_sems.at[self.count],
            recv_sem=recv_sem,
            device_id=device,
            device_id_type=pl.DeviceIdType.MESH,
        )
        self.count += 1
        self.pending.append((copy, when))
        if when is None:
            copy.start()
        else:
            pl.when(when)(copy.start)

    def arrived(self, place, recv_sem, when=None):
        copy = pltpu.make_async_remote_copy(
            src_ref=place,
            dst_ref=place,
            send_sem=self.send_sems.at[0],
            recv_sem=recv_sem,
            device_id=self.first,
            device_id_type=pl.DeviceIdType.MESH,
        )
        if when is None:
            copy.wait_recv()
        else:
            pl.when(when)(copy.wait_recv)

    def drain(self):
        for copy, when in self.pending:
            if when is None:
                copy.wait_send()
            else:
                pl.when(when)(copy.wait_send)


def pack_pieces(qkv, up, pieces, planes, cores, shards):
    rows = qkv.shape[0]
    lane = lax.broadcasted_iota(jnp.int32, (rows, 128), 1)
    units = up.shape[1] // (planes * cores * shards)
    for core in range(cores):
        for shard in range(shards):
            piece = core * shards + shard
            for tile in range(3 * planes // 2):
                halves = []
                for side in range(2):
                    part, plane = divmod(2 * tile + side, planes)
                    head = (plane * cores + core) * shards + shard
                    start = part * planes * cores * shards * HD + head * HD
                    half = qkv[:, pl.ds(start // 128 * 128, 128)]
                    halves.append(half if start % 128 == side * HD else pltpu.roll(half, HD, 1))
                pieces[piece, :, pl.ds(tile * 128, 128)] = jnp.where(lane < HD, halves[0], halves[1]).astype(
                    jnp.bfloat16
                )
            for plane in range(planes):
                block = (plane * cores + core) * shards + shard
                pieces[piece, :, pl.ds(3 * planes * HD + plane * units, units)] = up[
                    :, pl.ds(block * units, units)
                ].astype(jnp.bfloat16)


def gather_kernel(
    qkv_state, up_state, dense_state, down_state, tokens, cotangent, vectors,
    cat_out, dense_out, down_out, x_out, dy_out, vec_out,
    qkv_buf, up_buf, dense_buf, down_buf, pieces, dense, down,
    load_sem, send_sems, group_sem, first_sem, second_sem, far_sem, up_sem, low_sem, core_sem, local_sem,
):
    net = Wires(send_sems)
    plane, core, shard, shards, group, mine = net.plane, net.core, net.shard, net.shards, net.group, net.mine
    order = sorted(range(group), key=lambda mask: (mask % shards, mask // shards))
    partner = (plane, 1 - core, shard)

    def cat_unit(mask):
        return lambda p: cat_out.at[p, mine ^ mask]

    def vec_unit(mask):
        return lambda p: vec_out.at[p, mine ^ mask]

    units = []
    down_rows = down.shape[0] // 4
    for part in range(4):
        rows = pl.ds(part * down_rows, down_rows)
        units.append((down.at[rows], lambda p, rows=rows: down_out.at[p, rows]))
    dense_rows = dense.shape[0] // 2
    for part in range(2):
        rows = pl.ds(part * dense_rows, dense_rows)
        units.append((dense.at[rows], lambda p, rows=rows: dense_out.at[p, rows]))
    own_units = list(range(len(units)))
    cat_units, vec_units = {}, {}
    for mask in order:
        cat_units[mask] = len(units)
        units.append((pieces.at[mine] if mask == 0 else None, cat_unit(mask)))
        vec_units[mask] = len(units)
        units.append((vectors if mask == 0 else None, vec_unit(mask)))

    def spread(index):
        source, place = units[index]
        source = place(plane) if source is None else source
        net.send(source, place(plane), first_sem.at[index], net.first)
        net.send(source, place(plane), second_sem.at[index], net.second)

    def hand_on(index):
        place = units[index][1]
        if relay_first[index]:
            net.arrived(place(plane ^ 1), first_sem.at[index])
            net.send(place(plane ^ 1), place(plane ^ 1), far_sem.at[index], net.second)
        else:
            net.arrived(place(plane ^ 2), second_sem.at[index])
            net.send(place(plane ^ 2), place(plane ^ 2), far_sem.at[index], net.first)

    relay_first = {}
    for position, index in enumerate(own_units):
        relay_first[index] = position % 2 == 0
    for position, mask in enumerate(order):
        relay_first[cat_units[mask]] = position % 2 == 0
        relay_first[vec_units[mask]] = position % 2 == 1

    loads = [
        pltpu.make_async_copy(state.at[0], buffer, load_sem.at[index])
        for index, (state, buffer) in enumerate(
            ((qkv_state, qkv_buf), (up_state, up_buf), (down_state, down_buf), (dense_state, dense_buf))
        )
    ]
    for index in (2, 3, 0, 1):
        loads[index].start()
    net.barrier()
    loads[2].wait()
    down[...] = down_buf[...].astype(jnp.bfloat16)
    loads[3].wait()
    dense[...] = dense_buf[...].astype(jnp.bfloat16)
    for index in own_units:
        spread(index)
    loads[0].wait()
    loads[1].wait()
    pack_pieces(qkv_buf, up_buf, pieces, cat_out.shape[0], group // shards, shards)

    locals_ = [
        (pieces.at[mine], cat_out.at[plane, mine]),
        (dense, dense_out.at[plane]),
        (down, down_out.at[plane]),
        (tokens, x_out.at[mine]),
        (cotangent, dy_out.at[mine]),
        (vectors, vec_out.at[plane, mine]),
    ]
    copies = [
        pltpu.make_async_copy(source, target, local_sem.at[index])
        for index, (source, target) in enumerate(locals_)
    ]
    for mask in order[1:]:
        target = net.member(mine ^ mask)
        net.send(vectors, vec_out.at[plane, mine], group_sem.at[1, mask], target)
        net.send(pieces.at[mine ^ mask], cat_out.at[plane, mine], group_sem.at[0, mask], target)
    spread(cat_units[0])
    spread(vec_units[0])
    streams = ((tokens, x_out), (cotangent, dy_out))

    def block(stream, origin):
        return streams[stream][1].at[core * shards + origin]

    def to_core(stream, source, origin, slot, when=None):
        net.send(source, block(stream, origin), core_sem.at[stream, slot], partner, when)

    def hop(stream, distance):
        own = distance == 1
        for upward, sem in ((True, up_sem), (False, low_sem)):
            origin = shard - (distance - 1) if upward else shard + (distance - 1)
            there = shard + 1 if upward else shard - 1
            held = (origin >= 0) if upward else (origin < shards)
            inside = (there < shards) if upward else (there >= 0)
            near = jnp.clip(origin, 0, shards - 1)
            source = streams[stream][0] if own else block(stream, near)
            net.send(
                source,
                block(stream, near),
                sem.at[stream, distance],
                (plane, core, jnp.clip(there, 0, shards - 1)),
                inside & held,
            )

    def hop_arrived(stream, distance):
        for upward, sem in ((True, up_sem), (False, low_sem)):
            origin = shard - distance if upward else shard + distance
            held = (origin >= 0) if upward else (origin < shards)
            near = jnp.clip(origin, 0, shards - 1)
            net.arrived(block(stream, near), sem.at[stream, distance], held)
            slot = distance if upward else shards + distance
            to_core(stream, block(stream, near), near, slot, held)

    for stream in range(2):
        hop(stream, 1)
    for stream in range(2):
        to_core(stream, streams[stream][0], shard, 0)
    for copy in copies:
        copy.start()

    for position, mask in enumerate(order[1:]):
        net.arrived(vec_out.at[plane, mine ^ mask], group_sem.at[1, mask])
        spread(vec_units[mask])
        net.arrived(cat_out.at[plane, mine ^ mask], group_sem.at[0, mask])
        spread(cat_units[mask])
        if position == 2:
            for index in own_units:
                hand_on(index)
    hand_on(cat_units[0])
    hand_on(vec_units[0])
    for distance in range(1, shards):
        for stream in range(2):
            hop_arrived(stream, distance)
            if distance + 1 < shards:
                hop(stream, distance + 1)
        for mask in order[1 + (distance - 1) * 3 : 1 + distance * 3]:
            hand_on(vec_units[mask])
            hand_on(cat_units[mask])

    for index, (source, place) in enumerate(units):
        if relay_first[index]:
            net.arrived(place(plane ^ 2), second_sem.at[index])
        else:
            net.arrived(place(plane ^ 1), first_sem.at[index])
        net.arrived(place(plane ^ 3), far_sem.at[index])
    for stream in range(2):
        other = streams[stream][1]
        for slot in range(2 * shards):
            if slot == shards:
                continue
            origin = shard - slot if slot < shards else shard + (slot - shards)
            held = None if slot == 0 else ((origin >= 0) & (origin < shards))
            near = jnp.clip(origin, 0, shards - 1)
            net.arrived(other.at[(1 - core) * shards + near], core_sem.at[stream, slot], held)
    for copy in copies:
        copy.wait()
    net.drain()


def gather_wires(qkv, up, dense, down, tokens, cotangent, vectors):
    group, shards = lax.axis_size("core") * lax.axis_size("shard"), lax.axis_size("shard")
    planes = lax.axis_size("plane")
    width = (qkv.shape[2] + up.shape[2]) // group
    units = 6 + 2 * group
    vmem = pl.BlockSpec(memory_space=pltpu.VMEM)
    hbm = pl.BlockSpec(memory_space=pl.ANY)

    def out(*shape, dtype=jnp.bfloat16):
        return jax.ShapeDtypeStruct(shape, dtype)

    dma = pltpu.SemaphoreType.DMA
    return pl.pallas_call(
        gather_kernel,
        in_specs=[hbm] * 4 + [vmem] * 3,
        out_specs=[hbm] * 6,
        out_shape=[
            out(planes, group, qkv.shape[1], width),
            out(planes, *dense.shape[1:]),
            out(planes, *down.shape[1:]),
            out(group, *tokens.shape),
            out(group, *cotangent.shape),
            out(planes, group, *vectors.shape, dtype=vectors.dtype),
        ],
        scratch_shapes=[
            pltpu.VMEM(qkv.shape[1:], qkv.dtype),
            pltpu.VMEM(up.shape[1:], up.dtype),
            pltpu.VMEM(dense.shape[1:], dense.dtype),
            pltpu.VMEM(down.shape[1:], down.dtype),
            pltpu.VMEM((group, qkv.shape[1], width), jnp.bfloat16),
            pltpu.VMEM(dense.shape[1:], jnp.bfloat16),
            pltpu.VMEM(down.shape[1:], jnp.bfloat16),
            dma((4,)),
            dma((2 * (group - 1) + 3 * units + 2 * 2 * (shards - 1) + 2 * (2 * shards - 1),)),
            dma((2, group)),
            dma((units,)),
            dma((units,)),
            dma((units,)),
            dma((2, shards)),
            dma((2, shards)),
            dma((2, 2 * shards)),
            dma((6,)),
        ],
        compiler_params=pltpu.CompilerParams(
            collective_id=0, has_side_effects=True, vmem_limit_bytes=67043328
        ),
    )(qkv, up, dense, down, tokens, cotangent, vectors)


def add_rows(target, *sources):
    step = 16
    rows = target.shape[0]

    def body(index, carry):
        place = pl.ds(pl.multiple_of(index * step, step), step)
        total = sources[0][place, :].astype(jnp.float32)
        for source in sources[1:]:
            total = total + source[place, :].astype(jnp.float32)
        target[place, :] = total.astype(target.dtype)
        return carry

    lax.fori_loop(0, rows // step, body, 0)


def chunked(first, last, copies_of, body):
    for copy in copies_of(first, first % 2):
        copy.start()

    def step(n, carry):
        slot = lax.rem(n, 2)

        @pl.when(n + 1 < last)
        def ahead():
            for copy in copies_of(n + 1, 1 - slot):
                copy.start()

        for copy in copies_of(n, slot):
            copy.wait()
        body(n, slot)
        return carry

    lax.fori_loop(first, last, step, 0)


def reduce_kernel(
    norm, dcat, x_all, mean_rows, inverse_rows, attn, hidden, dy, cat_w, dense_w, down_w, sums,
    cat_out, dense_out, down_out, mixed_out, norm_out, sums_out,
    cat_part, down_part, dense_part, cat_in, down_in, dense_in,
    tokens, token_in, token_line, token_last, sum_buf, mean, inverse,
    wide, hidden_turned, attn_turned, norm_chunk, norm_turned, cat_chunk, x_chunk, down_chunk, dense_chunk, dy_chunk,
    send_sems, near_sem, pass_sem, group_sem, core_sem, line_sem, sum_sem, local_sem, chunk_sem,
):
    PASS, KEEP, LAST = range(3)
    net = Wires(send_sems)
    plane, core, shard, shards, group, mine = net.plane, net.core, net.shard, net.shards, net.group, net.mine
    planes = cat_part.shape[0]
    partner = (plane, 1 - core, shard)
    order = sorted(range(group), key=lambda mask: (mask % shards, mask // shards), reverse=True)
    rows, width = dcat.shape
    model = norm.shape[1]
    block = cat_part.shape[2]
    token_rows = tokens.shape[2]
    units_here = hidden.shape[1]
    heads_here = attn.shape[1]
    lane = 256

    def dot(a, b, a_dim=1, b_dim=0):
        return lax.dot_general(a, b, (((a_dim,), (b_dim,)), ((), ())), preferred_element_type=jnp.float32)

    def columns(n):
        return pl.ds(pl.multiple_of(n * lane, lane), lane)

    units = [(cat_part, cat_in, mask) for mask in order]
    units += [(down_part, down_in, part) for part in range(down_part.shape[1])]
    units += [(dense_part, dense_in, part) for part in range(dense_part.shape[1])]
    down_rows, dense_rows = down_part.shape[2], dense_part.shape[2]

    def ways(index):
        return (net.first, net.second, 1, 2) if index % 2 == 0 else (net.second, net.first, 2, 1)

    def send_pass(index):
        parts, came, slot = units[index]
        net.send(parts.at[3, slot], came.at[PASS, slot], pass_sem.at[0, index], ways(index)[0])

    def send_keep(index):
        parts, came, slot = units[index]
        near, far, near_mask, far_mask = ways(index)
        net.send(parts.at[near_mask, slot], came.at[KEEP, slot], near_sem.at[index], near)

    locals_ = {}

    def local(key, source, target):
        locals_[key] = pltpu.make_async_copy(source, target, local_sem.at[len(locals_)])
        locals_[key].start()

    local("hidden", hidden, wide.at[:, pl.ds(0, units_here)])
    local("attn", attn, wide.at[:, pl.ds(units_here, heads_here)])
    net.barrier()

    places = [place for rank in range(shards // 2) for place in (shards - 1 - rank, rank)]

    def to_partner(stream):
        for place in places:
            net.send(
                tokens.at[stream, (1 - core) * shards + place],
                token_in.at[stream, place],
                core_sem.at[stream, place],
                partner,
            )

    def out_copies(n, slot):
        return [
            pltpu.make_async_copy(down_w.at[:, columns(n)], down_chunk.at[slot], chunk_sem.at[3, slot]),
            pltpu.make_async_copy(dense_w.at[:, columns(n)], dense_chunk.at[slot], chunk_sem.at[4, slot]),
        ]

    def out_step(n, slot):
        total = dot(wide[:, pl.ds(0, units_here)], down_chunk[slot]) + dot(
            wide[:, pl.ds(units_here, heads_here)], dense_chunk[slot]
        )
        for member in range(group):
            tokens[0, member, :, columns(n)] = total[member * token_rows : (member + 1) * token_rows].astype(
                jnp.bfloat16
            )

    locals_["hidden"].wait()
    locals_["attn"].wait()
    chunked(0, model // lane, out_copies, out_step)
    to_partner(0)
    hidden_turned[...] = wide[:, pl.ds(0, units_here)].T
    attn_turned[...] = wide[:, pl.ds(units_here, heads_here)].T
    local("dcat", dcat, wide.at[:, pl.ds(0, width)])

    plane_rows = group * block

    def norm_copy(turn, distance):
        place = pl.ds(pl.multiple_of((plane ^ distance) * plane_rows, plane_rows), plane_rows)
        return pltpu.make_async_copy(
            norm.at[:, place], norm_chunk.at[turn % 2], chunk_sem.at[0, turn % 2]
        )

    cats, every = range(group), range(len(units))
    chain_steps = sorted(
        ((hop, rank) for hop in range(1, shards - 1) for rank in range(shards - 1 - hop)),
        key=lambda pair: (pair[0] + 2 * pair[1], pair[0]),
    )
    turns = (3, 1, 2, 0)
    norm_copy(0, turns[0]).start()
    locals_["dcat"].wait()

    def cat_turn(turn):
        distance = turns[turn]
        if turn + 1 < planes:
            norm_copy(turn + 1, turns[turn + 1]).start()
        norm_copy(turn, distance).wait()
        norm_turned[...] = norm_chunk[turn % 2].T

        def cat_step(n, carry):
            total = dot(norm_turned[...], wide[:, columns(n)]).astype(jnp.bfloat16)
            for member in range(group):
                cat_part[distance, mine ^ member, :, columns(n)] = total[member * block : (member + 1) * block]
            return carry

        lax.fori_loop(0, width // lane, cat_step, 0)
        for index in cats:
            if distance == 3:
                send_pass(index)
            elif distance == ways(index)[2]:
                send_keep(index)

    def own(stream, place):
        return tokens.at[stream, core * shards + place]

    def chain(stream, hop, rank):
        for upward in (True, False):
            target = shards - 1 - rank if upward else rank
            here = hop if upward else shards - 1 - hop
            sems = line_sem.at[0 if upward else 1]
            came = token_line.at[stream, target]
            total = own(stream, target)
            holds = shard == here
            if hop:
                net.arrived(came, sems.at[stream, target], holds)

            @pl.when(holds)
            def add(target=target, came=came, total=total):
                add_rows(total, total, token_in.at[stream, target], *([came] if hop else []))

            there = jnp.clip(shard + (1 if upward else -1), 0, shards - 1)
            ends = (not upward) and rank == shards - 2 - hop
            landing = token_last.at[stream] if ends else came
            net.send(total, landing, sems.at[stream, target], (plane, core, there), holds)

    def final(stream):
        for place in range(shards):
            holds = shard == place
            values = [own(stream, place), token_in.at[stream, place]]
            for landing, side, present in (
                (token_line.at[stream, place], line_sem.at[0], place > 0),
                (token_last.at[stream], line_sem.at[1], place < shards - 1),
            ):
                if present:
                    values.append(landing)
                    net.arrived(landing, side.at[stream, place], holds)

            @pl.when(holds)
            def add(values=values):
                add_rows((mixed_out, norm_out)[stream], *values)

    def first_sums(stream):
        for place in places:
            net.arrived(token_in.at[stream, place], core_sem.at[stream, place])
        for rank in range(shards - 1):
            chain(stream, 0, rank)

    def pass_on(index):
        parts, came, slot = units[index]
        near, far, near_mask, far_mask = ways(index)
        total = parts.at[far_mask, slot]
        net.arrived(came.at[PASS, slot], pass_sem.at[0, index])
        add_rows(total, total, came.at[PASS, slot])
        net.send(total, came.at[LAST, slot], pass_sem.at[1, index], far)

    cat_turn(0)
    first_sums(0)

    sum_buf[4] = sums[...]
    for flat, column in ((mean_rows, mean), (inverse_rows, inverse)):
        turned = flat[...].T
        for member in range(flat.shape[0]):
            column[pl.ds(member * flat.shape[1], flat.shape[1]), :] = turned[:, member : member + 1]
    gain_row = width // 128

    def norm_copies(n, slot):
        return [
            pltpu.make_async_copy(cat_w.at[columns(n), :], cat_chunk.at[slot], chunk_sem.at[1, slot]),
            pltpu.make_async_copy(x_all.at[:, columns(n)], x_chunk.at[slot], chunk_sem.at[2, slot]),
        ]

    def norm_step(n, slot):
        total = dot(wide[:, pl.ds(0, width)], cat_chunk[slot], 1, 1)
        x_hat = (x_chunk[slot].astype(jnp.float32) - mean[...]) * inverse[...]
        gain = jnp.sum(total * x_hat, axis=0, keepdims=True)
        shift = jnp.sum(total, axis=0, keepdims=True)
        for half in range(lane // 128):
            row = gain_row + n * (lane // 128) + half
            sum_buf[4, pl.ds(row, 1), :] = gain[:, half * 128 : (half + 1) * 128]
            sum_buf[4, pl.ds(row + model // 128, 1), :] = shift[:, half * 128 : (half + 1) * 128]
        for member in range(group):
            tokens[1, member, :, columns(n)] = total[member * token_rows : (member + 1) * token_rows].astype(
                jnp.bfloat16
            )

    chunked(0, model // lane, norm_copies, norm_step)

    net.send(sum_buf.at[4], sum_buf.at[0], sum_sem.at[0], net.first)
    to_partner(1)
    cat_turn(1)
    chain(0, 1, 0)
    first_sums(1)
    cat_turn(2)
    cat_turn(3)
    net.arrived(sum_buf.at[0], sum_sem.at[0])
    sum_buf[1] = sum_buf[4] + sum_buf[0]
    net.send(sum_buf.at[1], sum_buf.at[2], sum_sem.at[1], net.second)
    for index in cats:
        pass_on(index)

    def grad_copies(n, slot):
        return [pltpu.make_async_copy(dy.at[:, columns(n)], dy_chunk.at[slot], chunk_sem.at[5, slot])]

    def grad_step(n, slot):
        for parts, left in ((down_part, hidden_turned[...]), (dense_part, attn_turned[...])):
            grad = dot(left, dy_chunk[slot]).astype(jnp.bfloat16)
            pieces, size = parts.shape[1], parts.shape[2]
            for q in range(planes):
                for piece in range(pieces):
                    start = (q * pieces + piece) * size
                    parts[plane ^ q, piece, :, columns(n)] = grad[start : start + size]

    chunked(0, model // lane, grad_copies, grad_step)
    for index in every[group:]:
        send_pass(index)
        send_keep(index)
    for hop, rank in chain_steps[1:]:
        chain(0, hop, rank)

    def finish(index):
        parts, came, slot = units[index]
        total = parts.at[0, slot]
        net.arrived(came.at[KEEP, slot], near_sem.at[index])
        net.arrived(came.at[LAST, slot], pass_sem.at[1, index])
        values = (total, came.at[KEEP, slot], came.at[LAST, slot])
        if index < group:
            add_rows(total, *values)
            if slot:
                net.send(total, cat_out.at[mine], group_sem.at[0, slot], net.member(mine ^ slot))
            else:
                local("own", total, cat_out.at[mine])
        elif parts is down_part:
            add_rows(down_out.at[pl.ds(slot * down_rows, down_rows)], *values)
        else:
            add_rows(dense_out.at[pl.ds(slot * dense_rows, dense_rows)], *values)

    net.arrived(sum_buf.at[2], sum_sem.at[1])
    sum_buf[3] = sum_buf[1] + sum_buf[2]
    for mask in range(1, group):
        net.send(sum_buf.at[3], sums_out.at[mine], group_sem.at[1, mask], net.member(mine ^ mask))
    local("sums", sum_buf.at[3], sums_out.at[mine])
    for index in cats[: group // 2]:
        finish(index)
    chain(1, *chain_steps[0])
    for index in cats[group // 2 : group - 2]:
        finish(index)
    for hop, rank in chain_steps[1:]:
        chain(1, hop, rank)
    for index in cats[group - 2 :]:
        finish(index)
    for index in every[group:]:
        pass_on(index)
    final(0)
    for index in every[group:]:
        finish(index)
    final(1)
    for mask in range(1, group):
        net.arrived(cat_out.at[mine ^ mask], group_sem.at[0, mask])
        net.arrived(sums_out.at[mine ^ mask], group_sem.at[1, mask])
    locals_["own"].wait()
    locals_["sums"].wait()
    net.drain()


def reduce_wires(norm, dcat, x_all, mean, inverse, attn, hidden, dy, cat_w, dense_w, down_w, sums):
    planes, shards = lax.axis_size("plane"), lax.axis_size("shard")
    group = lax.axis_size("core") * shards
    units = group + 6
    rows, width = dcat.shape
    model = norm.shape[1]
    block = model // (planes * group)
    unit_rows, head_rows = down_w.shape[0] // planes, dense_w.shape[0] // planes
    token_rows = rows // group
    vmem = pl.BlockSpec(memory_space=pltpu.VMEM)
    hbm = pl.BlockSpec(memory_space=pl.ANY)
    dma = pltpu.SemaphoreType.DMA
    lane = 256

    def scratch(*shape, dtype=jnp.bfloat16):
        return pltpu.VMEM(shape, dtype)

    return pl.pallas_call(
        reduce_kernel,
        in_specs=[hbm] * 3 + [vmem] * 2 + [hbm] * 6 + [vmem],
        out_specs=[hbm] + [vmem] * 4 + [hbm],
        out_shape=[
            jax.ShapeDtypeStruct((group, block, width), jnp.bfloat16),
            jax.ShapeDtypeStruct((head_rows, model), jnp.float32),
            jax.ShapeDtypeStruct((unit_rows, model), jnp.float32),
            jax.ShapeDtypeStruct((token_rows, model), jnp.float32),
            jax.ShapeDtypeStruct((token_rows, model), jnp.float32),
            jax.ShapeDtypeStruct((group,) + sums.shape, sums.dtype),
        ],
        scratch_shapes=[
            scratch(planes, group, block, width),
            scratch(planes, 4, unit_rows // 4, model),
            scratch(planes, 2, head_rows // 2, model),
            scratch(3, group, block, width),
            scratch(3, 4, unit_rows // 4, model),
            scratch(3, 2, head_rows // 2, model),
            scratch(2, group, token_rows, model),
            scratch(2, shards, token_rows, model),
            scratch(2, shards, token_rows, model),
            scratch(2, token_rows, model),
            scratch(5, *sums.shape, dtype=jnp.float32),
            scratch(rows, 1, dtype=jnp.float32),
            scratch(rows, 1, dtype=jnp.float32),
            scratch(rows, max(width, hidden.shape[1] + attn.shape[1])),
            scratch(hidden.shape[1], rows),
            scratch(attn.shape[1], rows),
            scratch(2, rows, group * block),
            scratch(group * block, rows),
            scratch(2, lane, width),
            scratch(2, rows, lane),
            scratch(2, hidden.shape[1], lane),
            scratch(2, attn.shape[1], lane),
            scratch(2, rows, lane),
            dma((2 + 2 * shards + 2 * shards * (shards - 1) + 3 * units + 2 * (group - 1),)),
            dma((units,)),
            dma((2, units)),
            dma((2, group)),
            dma((2, shards)),
            dma((2, 2, shards)),
            dma((2,)),
            dma((5,)),
            dma((6, 2)),
        ],
        compiler_params=pltpu.CompilerParams(
            collective_id=1, has_side_effects=True, vmem_limit_bytes=67043328
        ),
    )(norm, dcat, x_all, mean, inverse, attn, hidden, dy, cat_w, dense_w, down_w, sums)


def fast_body(
    hidden_in,
    segment_ids,
    out_grad,
    qkv_weight_state,
    qkv_bias_state,
    dense_weight_state,
    up_weight_state,
    up_bias_state,
    down_weight_state,
    vector_state,
):
    planes, cores, shards = lax.axis_size("plane"), lax.axis_size("core"), lax.axis_size("shard")
    plane, core, shard = lax.axis_index("plane"), lax.axis_index("core"), lax.axis_index("shard")
    group = cores * shards
    owner = (plane * cores + core) * shards + shard
    owners = planes * group
    model_rows = qkv_weight_state.shape[1]
    unit_rows = down_weight_state.shape[1]
    tokens_here = hidden_in.shape[1]
    head_width = planes * HD
    unit_width = planes * unit_rows
    qkv_count, upb_count = qkv_bias_state.shape[1], up_bias_state.shape[1]

    tokens, cotangent, q_seg = hidden_in[0], out_grad[0], segment_ids[0]
    vec_list = [
        qkv_bias_state[0],
        up_bias_state[0],
        vector_state[0].T.reshape(-1),
        q_seg.astype(jnp.float32),
    ]
    vec_sizes = [value.size for value in vec_list]
    vec_rows = -(-sum(vec_sizes) // 1024) * 8
    vec_own = jnp.pad(jnp.concatenate(vec_list), (0, vec_rows * 128 - sum(vec_sizes))).reshape(vec_rows, 128)

    cat_w, dense_w, down_w, x_all, dy_all, vec_all = gather_wires(
        qkv_weight_state,
        up_weight_state,
        dense_weight_state,
        down_weight_state,
        tokens,
        cotangent,
        vec_own,
    )

    cat_w = cat_w.reshape(D, 3 * head_width + unit_width)
    dense_w = dense_w.reshape(head_width, D)
    down_w = down_w.reshape(unit_width, D)
    rows = group * tokens_here
    x_all = x_all.reshape(rows, D)
    dy_all = dy_all.reshape(rows, D)
    vec_flat = vec_all.reshape(planes, cores, shards, vec_rows * 128)
    at = [0]
    for size in vec_sizes:
        at.append(at[-1] + size)

    def rounded(value):
        return value.astype(jnp.bfloat16).astype(jnp.float32)

    qkv_bias = rounded(vec_flat[..., at[0] : at[1]]).reshape(3, planes, cores, shards, HD)
    qkv_bias = lax.dynamic_index_in_dim(
        qkv_bias.transpose(2, 3, 0, 1, 4).reshape(group, 3 * head_width), core * shards + shard, 0, False
    )
    up_bias = lax.dynamic_index_in_dim(
        rounded(vec_flat[..., at[1] : at[2]]).transpose(1, 2, 0, 3).reshape(group, unit_width),
        core * shards + shard,
        0,
        False,
    )
    vec_columns = (
        rounded(vec_flat[..., at[2] : at[3]])
        .reshape(owners, 4, model_rows)
        .transpose(1, 0, 2)
        .reshape(4, D)
    )
    norm_gain, norm_shift, dense_bias, down_bias = (vec_columns[index] for index in range(4))
    segments = lax.dynamic_index_in_dim(vec_flat[..., at[3] : at[4]], plane, 0, False)
    segments = segments.astype(jnp.int32).reshape(cores, shards * tokens_here)
    cat_bias = jnp.concatenate([qkv_bias, up_bias])

    x_float = x_all.astype(jnp.float32)
    x_mean = jnp.mean(x_float, axis=-1, keepdims=True)
    center = x_float - x_mean
    inverse = lax.rsqrt(jnp.mean(center * center, axis=-1, keepdims=True) + norm_eps)
    x_hat = center * inverse
    norm_bf = lax.optimization_barrier((x_hat * norm_gain + norm_shift).astype(jnp.bfloat16))

    fu = jnp.dot(norm_bf, cat_w, preferred_element_type=jnp.float32) + cat_bias
    pre_act = fu[:, 3 * head_width :]
    hidden = gelu_tanh(pre_act).astype(jnp.bfloat16)
    grad_hidden = jnp.dot(dy_all, down_w.T, preferred_element_type=jnp.float32)
    grad_pre = jax.vjp(gelu_tanh, pre_act)[1](grad_hidden)[0]
    upb_part = jnp.sum(grad_pre, axis=0)
    grad_heads = jnp.dot(dy_all, dense_w.T, preferred_element_type=jnp.float32).astype(jnp.bfloat16)
    attn, dcat, qkvb_part = attention(fu, grad_heads, grad_pre.astype(jnp.bfloat16), segments)
    bias_part = jnp.sum(cotangent.astype(jnp.float32), axis=0)
    nothing = jnp.zeros((D,), jnp.float32)
    sums = [qkvb_part, upb_part, nothing, nothing, bias_part]
    sum_sizes = [value.size for value in sums]
    sum_rows = -(-sum(sum_sizes) // 1024) * 8
    sums = jnp.pad(jnp.concatenate(sums), (0, sum_rows * 128 - sum(sum_sizes))).reshape(sum_rows, 128)

    cat_sum, dense_grad, down_grad, mixed, grad_norm, sums_all = reduce_wires(
        norm_bf,
        dcat,
        x_all,
        x_mean.reshape(group, tokens_here),
        inverse.reshape(group, tokens_here),
        attn,
        hidden,
        dy_all,
        cat_w,
        dense_w,
        down_w,
        sums,
    )

    sums_flat = sums_all.reshape(cores, shards, sum_rows * 128)
    at = [0]
    for size in sum_sizes:
        at.append(at[-1] + size)
    qkvb_grad = (
        sums_flat[..., : at[1]]
        .reshape(cores, shards, 3, planes, HD)
        .transpose(2, 3, 0, 1, 4)
        .reshape(owners, qkv_count)
    )
    qkvb_grad = lax.dynamic_index_in_dim(qkvb_grad, owner, 0, False)
    upb_grad = sums_flat[..., at[1] : at[2]].reshape(group, planes, upb_count)
    upb_grad = lax.dynamic_index_in_dim(
        lax.dynamic_index_in_dim(upb_grad, core * shards + shard, 0, False), plane, 0, False
    )
    vec_grad = jnp.sum(sums_flat[..., at[2] : at[5]], axis=(0, 1)).reshape(3, owners, model_rows)
    vec_grad = lax.dynamic_index_in_dim(vec_grad, owner, 1, False)
    vec_grad = jnp.stack([vec_grad[0], vec_grad[1], vec_grad[2], vec_grad[2]], axis=1)

    x_own = tokens.astype(jnp.float32)
    output = (x_own + (mixed.astype(jnp.float32) + dense_bias + down_bias)).astype(jnp.bfloat16)
    own_center = x_own - jnp.mean(x_own, axis=-1, keepdims=True)
    own_inverse = lax.rsqrt(jnp.mean(own_center * own_center, axis=-1, keepdims=True) + norm_eps)
    own_hat = own_center * own_inverse
    hat_grad = grad_norm.astype(jnp.float32) * norm_gain
    x_grad = own_inverse * (
        hat_grad
        - jnp.mean(hat_grad, axis=-1, keepdims=True)
        - own_hat * jnp.mean(hat_grad * own_hat, axis=-1, keepdims=True)
    )
    input_grad = cotangent.astype(jnp.float32) + x_grad

    new, qkv_grad, dense_grad, up_grad, down_grad = owner_update(
        (qkv_weight_state, dense_weight_state, up_weight_state, down_weight_state),
        cat_sum,
        (dense_grad, down_grad),
        (qkv_bias_state, up_bias_state, vector_state),
        (qkvb_grad, upb_grad, vec_grad),
        (planes, cores, shards),
    )
    return (
        output[None],
        input_grad[None],
        qkv_grad,
        qkvb_grad,
        dense_grad,
        up_grad,
        upb_grad,
        down_grad,
        vec_grad,
        *new,
    )


def fast_solution(mesh):
    rep, shard = mesh.shape["rep"], mesh.shape["shard"]
    inner = Mesh(mesh.devices.reshape(rep // 2, 2, shard), ("plane", "core", "shard"))
    both = ("plane", "core")
    every = ("plane", "core", "shard")
    in_specs = (
        P(both, "shard", None),
        P(both, "shard"),
        P(both, "shard", None),
        P(None, every, None),
        P(None, every),
        P(None, every, None),
        P(None, every, None),
        P(None, every),
        P(None, every, None),
        P(None, every, None),
    )
    out_specs = (
        P(both, "shard", None),
        P(both, "shard", None),
        P(every, None),
        P(every),
        P(every, None),
        P(every, None),
        P(every),
        P(every, None),
        P(every, None),
        P(both, "shard", None),
        P(both, "shard", None),
        P(both, "shard", None),
    )
    return jax.shard_map(fast_body, mesh=inner, in_specs=in_specs, out_specs=out_specs, check_vma=False)


def solution(mesh):
    in_specs = (
        P("rep", "shard", None),
        P("rep", "shard"),
        P("rep", "shard", None),
        P(None, ("rep", "shard"), None),
        P(None, ("rep", "shard")),
        P(None, ("rep", "shard"), None),
        P(None, ("rep", "shard"), None),
        P(None, ("rep", "shard")),
        P(None, ("rep", "shard"), None),
        P(None, ("rep", "shard"), None),
    )
    out_specs = (
        P("rep", "shard", None),
        P("rep", "shard", None),
        P(("rep", "shard"), None),
        P(("rep", "shard")),
        P(("rep", "shard"), None),
        P(("rep", "shard"), None),
        P(("rep", "shard")),
        P(("rep", "shard"), None),
        P(("rep", "shard"), None),
        P("rep", "shard", None),
        P("rep", "shard", None),
        P("rep", "shard", None),
    )
    if whole_heads(mesh):
        return fast_solution(mesh)
    return jax.shard_map(body, mesh=mesh, in_specs=in_specs, out_specs=out_specs, check_vma=False)
```
